32 devices in a mesh: dp: 4 (over z), row: 4 (over y, x), col: 2 (over core).
Axes of the slice: x: 2, y: 2, z: 4, core: 2. Of those that a mesh axis runs over, the one named last changes fastest.
Arguments:
- tokens: bfloat16 [2048, 1024], P('dp', ('row', 'col')), may hold values from -7.5 to 7.5
- out_grad: bfloat16 [2048, 1024], P('dp', ('row', 'col')), may hold values from -6 to 6
- doc_ids: int32 [2048], P('dp'), may hold values from 0 to 3, never falling along the last dimension, each value on 1 to 1024 neighbouring positions
- expert_ids: int32 [2048, 8], P('dp'), may hold values from 0 to 31, all different within a row
- gain_attn: bfloat16 [1024], P(('row', 'col')), may hold values from 0.5 to 1.5
- w_query: bfloat16 [1024, 1024], P(None, ('row', 'col')), may hold values from -1.1015625 to 1.1015625
- w_key_value: bfloat16 [1024, 8, 128], P(None, ('row', 'col')), may hold values from -0.1875 to 0.1875
- w_output: bfloat16 [1024, 1024], P(('row', 'col')), may hold values from -6 to 6
- gain_moe: bfloat16 [1024], P(('row', 'col')), may hold values from 0.5 to 1.5
- w_router: bfloat16 [1024, 32], P(('row', 'col')), may hold values from -2.75 to 2.75
- w_expert_in: bfloat16 [32, 1024, 2, 512], P('row', None, None, 'col'), may hold values from -0.1875 to 0.1875
- w_expert_out: bfloat16 [32, 512, 1024], P('row', 'col'), may hold values from -4 to 4
Outputs:
- block_out: bfloat16 [2048, 1024], P('dp', ('row', 'col'))
- in_grad: bfloat16 [2048, 1024], P('dp', ('row', 'col'))
- grad_gain_attn: float32 [1024], P(('row', 'col'))
- grad_query: float32 [1024, 1024], P(None, ('row', 'col'))
- grad_key_value: float32 [1024, 8, 128], P(None, ('row', 'col'))
- grad_output: float32 [1024, 1024], P(('row', 'col'))
- grad_gain_moe: float32 [1024], P(('row', 'col'))
- grad_router: float32 [1024, 32], P(('row', 'col'))
- grad_expert_in: float32 [32, 1024, 2, 512], P('row', None, None, 'col')
- grad_expert_out: float32 [32, 512, 1024], P('row', 'col')
The draws below stay inside these ranges and needn't reach their ends.
Inputs may be any that keep to these rules, and one draw needn't show every extreme that they name: `doc_ids`: never falling along the token stream; every document has 1 to 1024 tokens and one has exactly 1024. `expert_ids`: each row names 8 different experts; every expert is named by some row.
All inputs are finite; a program needn't handle non-finite values.
Results may differ from the reference program's by a relative error of at most 0.02555.
Values may be sent and summed in bfloat16 or wider, within the bound.
A program may use at most 192 MiB of HBM per device.

```python
import math
import jax
import jax.numpy as jnp
import numpy as np
from jax import lax

D = 1024
HEADS = 16
KV_HEADS = 8
HEAD_DIM = 64
EXPERTS = 32
TOP_K = 8
EXPERT_FF = 512
TOKENS = 2048
SEQ_LEN = 1024
DOCS = 4


def draw_tokens(key, part):
    return jax.random.truncated_normal(jax.random.fold_in(key, 11), -6.0, 6.0, (TOKENS, D), jnp.float32).astype(jnp.bfloat16)


def draw_w_query(key, part):
    spread = (D // 16) ** (-0.5)
    columns = HEADS * HEAD_DIM
    drawn_part = jax.random.truncated_normal(jax.random.fold_in(key, 21), -6.0, 6.0, (D, columns), jnp.float32) * spread
    return drawn_part.astype(jnp.bfloat16)


def draw_w_key_value(key, part):
    spread = D ** (-0.5)
    drawn_part = jax.random.truncated_normal(jax.random.fold_in(key, 31), -6.0, 6.0, (D, KV_HEADS, 2 * HEAD_DIM), jnp.float32) * spread
    return drawn_part.astype(jnp.bfloat16)


def draw_w_router(key, part):
    spread = (D // 4) ** (-0.5)
    drawn_part = jax.random.truncated_normal(jax.random.fold_in(key, 41), -6.0, 6.0, (D, EXPERTS), jnp.float32) * spread
    return drawn_part.astype(jnp.bfloat16)


def block_scale(own_key, dims, cuts, least, largest):
    level = 1.0
    for axis_at, parts in cuts:
        steps = jax.random.uniform(jax.random.fold_in(jax.random.fold_in(own_key, 6), axis_at), (parts,), jnp.float32, least / len(cuts), largest / len(cuts))
        level = level * jnp.repeat(jnp.exp(steps), dims[axis_at] // parts).reshape((-1,) + (1,) * (len(dims) - 1 - axis_at))
    return level


def distinct(rng, rows, number_of, top, lift):
    ranking = jax.random.permutation(jax.random.fold_in(rng, 1), number_of)
    pull = ranking
    for power in range(3):
        pull = pull * pull // number_of
    pull = pull * lift // number_of
    chance = jax.random.randint(jax.random.fold_in(rng, 2), (rows, number_of), 0, 4096) + pull
    holders = jax.random.permutation(jax.random.fold_in(rng, 3), rows)[jnp.arange(number_of) % rows]
    chance = jnp.where(jnp.arange(rows)[:, None] == holders[None, :], 1 << 14, chance)
    merit = chance * number_of + jnp.arange(number_of)
    return lax.top_k(merit.astype(jnp.int32), top)[1].astype(jnp.int32)


def length_profile(number_of, total, bound, slope):
    portions = [(1 << 20) // math.isqrt(rank ** slope) + 1 for rank in range(2, number_of + 1)]
    rest, counts = total - bound - (number_of - 1), [1] * (number_of - 1)
    while rest > 0:
        movable = [i for i in range(number_of - 1) if counts[i] < bound]
        pool, left = sum([portions[i] for i in movable]), rest
        for i in movable:
            more = min(bound - counts[i], max(1, left * portions[i] // pool), rest)
            counts[i] = counts[i] + more
            rest = rest - more
    return np.array([bound] + counts)


def uneven(own_key, amount, total, limit, lean):
    if amount == 2:
        one = jax.random.randint(own_key, (), max(1, total - limit), min(limit, total - 1) + 1)
        return jnp.stack([one, total - one])
    sizes = jnp.asarray(length_profile(amount, total, limit, lean), jnp.int32)
    couples = (amount - 1) // 2
    source_of, receiver = sizes[1:1 + 2 * couples:2], sizes[2:2 + 2 * couples:2]
    margin = jnp.minimum(source_of - 1, limit - receiver)
    shifted = jax.random.randint(jax.random.fold_in(own_key, 1), (couples,), 0, 1 << 20) % (margin + 1)
    sizes = sizes.at[1:1 + 2 * couples:2].set(source_of - shifted).at[2:2 + 2 * couples:2].set(receiver + shifted)
    return sizes[jax.random.permutation(jax.random.fold_in(own_key, 2), amount)]


def scatter_about(rng, dims, width, most, shards=(), held_as=jnp.bfloat16):
    gain = block_scale(rng, dims, shards, -0.22, 0.18) if shards else 1.0
    entries = jax.random.normal(rng, dims, jnp.float32) * width * gain
    return jnp.minimum(jnp.maximum(entries, -most), most).astype(held_as)


def setup_inputs(seed: int = 0) -> dict:
    streams_of = jax.random.split(jax.random.key(seed), 13)
    tokens = draw_tokens(jax.random.fold_in(streams_of[12], 71), 0)
    out_grad = scatter_about(streams_of[1], (TOKENS, D), 1.0, 6.0, ((0, 4), (1, 8)))
    doc_ids = jnp.searchsorted(jnp.cumsum(uneven(streams_of[2], DOCS, TOKENS, SEQ_LEN, 2)), jnp.arange(TOKENS), side="right").astype(jnp.int32)
    expert_ids = distinct(streams_of[3], TOKENS, EXPERTS, TOP_K, 2048)
    gain_attn = jnp.clip(1.0 + 0.1 * jax.random.normal(streams_of[4], (D,), jnp.float32), 0.5, 1.5).astype(jnp.bfloat16)
    w_query = draw_w_query(jax.random.fold_in(streams_of[12], 71), 0)
    w_key_value = draw_w_key_value(jax.random.fold_in(streams_of[12], 71), 0)
    w_output = scatter_about(streams_of[7], (HEADS * HEAD_DIM, D), 1 ** -0.5, 6.0, ((0, 8),))
    gain_moe = jnp.clip(1.0 + 0.1 * jax.random.normal(streams_of[8], (D,), jnp.float32), 0.5, 1.5).astype(jnp.bfloat16)
    w_router = draw_w_router(jax.random.fold_in(streams_of[12], 71), 0)
    w_expert_in = scatter_about(streams_of[10], (EXPERTS, D, 2, EXPERT_FF), D ** -0.5, 0.1875, ((0, 4), (3, 2)))
    w_expert_out = scatter_about(streams_of[11], (EXPERTS, EXPERT_FF, D), (max(1, EXPERT_FF // 256)) ** -0.5, 4.0, ((0, 4), (1, 2)))
    return {"tokens": tokens, "out_grad": out_grad, "doc_ids": doc_ids, "expert_ids": expert_ids, "gain_attn": gain_attn, "w_query": w_query, "w_key_value": w_key_value, "w_output": w_output, "gain_moe": gain_moe, "w_router": w_router, "w_expert_in": w_expert_in, "w_expert_out": w_expert_out}


HIGH = lax.Precision.HIGHEST
EPSILON = 1e-05
RESIDUAL_SCALE = 0.22
SCORE_SCALE = 0.015625
ROPE_BASE = 10000.0
MASKED = -1e+30

@jax.custom_vjp
def low(v):
    return lax.optimization_barrier(v.astype(jnp.bfloat16)).astype(jnp.float32)

@jax.custom_vjp
def low_back(v):
    return v

def low_keep(v):
    return (low(v), None)

def low_pass(kept, grad):
    return (grad,)

def back_keep(v):
    return (v, None)

def back_low(kept, grad):
    return (low(grad),)
low.defvjp(low_keep, low_pass)
low_back.defvjp(back_keep, back_low)

def rope_tables(positions, head_width):
    half_width = head_width // 2
    freq_table = ROPE_BASE ** (-(2.0 / head_width) * jnp.arange(half_width, dtype=jnp.float32))
    angles = positions.astype(jnp.float32)[:, None] * freq_table[None, :]
    return (jnp.cos(angles), jnp.sin(angles))

def rotate(values, cosine_table, sine_table):
    half_width = values.shape[-1] // 2
    first_half = values[..., :half_width]
    second_half = values[..., half_width:]
    cosine_cols = cosine_table[:, None, :]
    sine_cols = sine_table[:, None, :]
    return jnp.concatenate([first_half * cosine_cols - second_half * sine_cols, second_half * cosine_cols + first_half * sine_cols], axis=-1)

def rms_norm(values, gain_row):
    return values * lax.rsqrt(lax.optimization_barrier(jnp.mean(values * values, axis=-1, keepdims=True)) + EPSILON) * gain_row

def forward(doc_ids, expert_ids, tokens, gain_attn, w_query, w_key_value, w_output, gain_moe, w_router, w_expert_in, w_expert_out):
    token_count = tokens.shape[0]
    positions = jnp.arange(token_count, dtype=jnp.int32)
    cosine_table, sine_table = rope_tables(positions, HEAD_DIM)
    normed = low(rms_norm(tokens, gain_attn))
    query = low_back(jnp.dot(normed, w_query, precision=HIGH)).reshape(token_count, HEADS, HEAD_DIM)
    key_value = low_back(jnp.einsum('td,dhc->thc', normed, w_key_value, precision=HIGH))
    query = low(rotate(query, cosine_table, sine_table))
    keys = low(rotate(key_value[..., :HEAD_DIM], cosine_table, sine_table))
    values = low(key_value[..., HEAD_DIM:])
    block_rows = min(512, token_count)
    block_count = token_count // block_rows

    def attend(inputs):
        query_block, position_block, doc_block = inputs
        scores = low_back(jnp.einsum('qhgc,khc->hgqk', query_block, keys, precision=HIGH) * SCORE_SCALE)
        allowed = (doc_block[:, None] == doc_ids[None, :]) & (position_block[:, None] >= positions[None, :])
        scores = jnp.where(allowed, scores, MASKED)
        row_max = lax.optimization_barrier(jnp.max(scores, axis=-1, keepdims=True))
        exp_terms = jnp.exp(scores - row_max)
        softmax_low = low(exp_terms / lax.optimization_barrier(jnp.sum(exp_terms, axis=-1, keepdims=True)))
        mixed = jnp.einsum('hgqk,khc->qhgc', softmax_low, values, precision=HIGH)
        return low(low_back(mixed)).reshape(query_block.shape[0], HEADS * HEAD_DIM)
    outputs = lax.map(jax.checkpoint(attend), (query.reshape(block_count, block_rows, KV_HEADS, HEADS // KV_HEADS, HEAD_DIM), positions.reshape(block_count, block_rows), doc_ids.reshape(block_count, block_rows)))
    attended = outputs.reshape(token_count, HEADS * HEAD_DIM)
    attn_branch = low_back(jnp.dot(attended, w_output, precision=HIGH))
    middle = tokens + RESIDUAL_SCALE * attn_branch
    normed_moe = rms_norm(middle, gain_moe)
    logits = jnp.dot(normed_moe, w_router, precision=HIGH)
    chosen = lax.optimization_barrier(jnp.sum((expert_ids[:, :, None] == jnp.arange(EXPERTS, dtype=jnp.int32)[None, None, :]).astype(jnp.float32), axis=1))
    exp_terms = jnp.exp(logits - lax.optimization_barrier(jnp.max(logits, axis=-1, keepdims=True))) * chosen
    weights = exp_terms / lax.optimization_barrier(jnp.sum(exp_terms, axis=-1, keepdims=True))
    expert_rows = low(normed_moe)

    def run_experts(inputs):
        rows_block, weight_block = inputs
        gate_up = low_back(jnp.einsum('td,edgf->tegf', rows_block, w_expert_in, precision=HIGH))
        gate_value = gate_up[:, :, 0]
        silu_gate = gate_value * jax.nn.sigmoid(gate_value)
        active = low(silu_gate * gate_up[:, :, 1] * weight_block[:, :, None])
        return jnp.einsum('tef,efd->td', active, w_expert_out, precision=HIGH)
    moe_blocks = lax.map(jax.checkpoint(run_experts), (expert_rows.reshape(block_count, block_rows, D), weights.reshape(block_count, block_rows, EXPERTS)))
    moe_branch = low_back(moe_blocks.reshape(token_count, D))
    return middle + RESIDUAL_SCALE * moe_branch

def reference(tokens, out_grad, doc_ids, expert_ids, gain_attn, w_query, w_key_value, w_output, gain_moe, w_router, w_expert_in, w_expert_out):
    primals = tuple((item.astype(jnp.float32) for item in (tokens, gain_attn, w_query, w_key_value, w_output, gain_moe, w_router, w_expert_in, w_expert_out)))

    def apply_layer(*inputs):
        return forward(doc_ids, expert_ids, *inputs)
    result, pullback = jax.vjp(apply_layer, *primals)
    grads = pullback(out_grad.astype(jnp.float32))
    return (result.astype(jnp.bfloat16), grads[0].astype(jnp.bfloat16), grads[1], grads[2], grads[3], grads[4], grads[5], grads[6], grads[7], grads[8])
```

```python
import functools

import jax
import jax.numpy as jnp
from jax import lax
from jax.experimental import pallas as pl
from jax.experimental.pallas import tpu as pltpu
from jax.sharding import PartitionSpec as P

LONGEST = 4096
HIGH = lax.Precision.HIGHEST
EPSILON = 1e-05
RESIDUAL_SCALE = 0.22
SCORE_SCALE = 0.015625
ROPE_BASE = 10000.0
MASKED = -1e30
MESH = pl.DeviceIdType.MESH
GROUP = ("row", "col")
EVERY = ("dp", "row", "col")
LANES = 128
HBM = pl.BlockSpec(memory_space=pl.ANY)


def exchange_body(sizes, kinds, *refs):
    rows, cols, depth = sizes
    count = len(kinds)
    sources, targets = refs[:count], refs[count : 2 * count]
    send_sem, recv_sem, local_sem = refs[2 * count :]
    row, col, layer = lax.axis_index("row"), lax.axis_index("col"), lax.axis_index("dp")
    group = rows * cols
    me = row * cols + col
    barrier = pltpu.get_barrier_semaphore()
    partners = []
    if any(kind[0] == "swap" for kind in kinds):
        for k in range(1, group):
            other = lax.rem(me + k, group)
            partners.append({"row": other // cols, "col": lax.rem(other, cols)})
    elif any(kind[0] == "gather" for kind in kinds):
        for k in range(1, rows):
            partners.append({"row": lax.rem(row + k, rows)})
        for k in range(1, cols):
            partners.append({"col": lax.rem(col + k, cols)})
    shifts = set()
    for kind in kinds:
        if kind[0] == "shift":
            for d in kind[1]:
                shifts |= {d % depth, -d % depth}
    for k in sorted(shifts - {0}):
        partners.append({"dp": lax.rem(layer + k, depth)})
    for partner in partners:
        pl.semaphore_signal(barrier, inc=1, device_id=partner, device_id_type=MESH)
    pl.semaphore_wait(barrier, len(partners))

    slot = 0
    remote, local, relays = [], [], []

    def send(source, target, device):
        nonlocal slot
        copy = pltpu.make_async_remote_copy(
            src_ref=source,
            dst_ref=target,
            send_sem=send_sem.at[slot],
            recv_sem=recv_sem.at[slot],
            device_id=device,
            device_id_type=MESH,
        )
        slot += 1
        copy.start()
        return copy

    for index, (kind, source, target) in enumerate(zip(kinds, sources, targets)):
        if kind[0] == "gather":
            for k in range(1, rows):
                copy = send(source, target.at[me], {"row": lax.rem(row + k, rows)})
                origin = lax.rem(row + rows - k, rows) * cols + col
                relays.append((copy, target, origin))
            for k in range(1, cols):
                remote.append(send(source, target.at[me], {"col": lax.rem(col + k, cols)}))
            local.append(pltpu.make_async_copy(source, target.at[me], local_sem.at[index]))
        elif kind[0] == "swap":
            for k in range(1, group):
                other = lax.rem(me + k, group)
                device = {"row": other // cols, "col": lax.rem(other, cols)}
                remote.append(send(source.at[other], target.at[me], device))
            local.append(
                pltpu.make_async_copy(source.at[me], target.at[me], local_sem.at[index])
            )
        else:
            for at, d in enumerate(kind[1]):
                piece = source.at[at] if kind[2] else source
                device = {"dp": lax.rem(layer + d % depth, depth)}
                remote.append(send(piece, target.at[at], device))
    for copy in local:
        copy.start()
    for copy, target, origin in relays:
        copy.wait_recv()
        for k in range(1, cols):
            device = {"col": lax.rem(col + k, cols)}
            remote.append(send(target.at[origin], target.at[origin], device))
    for copy, _, _ in relays:
        copy.wait_send()
    for copy in remote:
        copy.wait()
    for copy in local:
        copy.wait()


def exchange(sizes, name, number, *items):
    rows, cols, depth = sizes
    group = rows * cols
    kinds, arrays, shapes, copies = [], [], [], 0
    for item in items:
        array = item[1]
        arrays.append(array)
        if item[0] == "gather":
            kinds.append(("gather",))
            shapes.append(jax.ShapeDtypeStruct((group,) + array.shape, array.dtype))
            copies += (rows - 1) * cols + cols - 1
        elif item[0] == "swap":
            kinds.append(("swap",))
            shapes.append(jax.ShapeDtypeStruct(array.shape, array.dtype))
            copies += group - 1
        else:
            distances, split = item[2], item[3]
            kinds.append(("shift", tuple(distances), split))
            block = array.shape[1:] if split else array.shape
            shapes.append(jax.ShapeDtypeStruct((len(distances),) + block, array.dtype))
            copies += len(distances)
    return pl.pallas_call(
        functools.partial(exchange_body, sizes, tuple(kinds)),
        out_shape=tuple(shapes),
        in_specs=[HBM] * len(arrays),
        out_specs=(HBM,) * len(arrays),
        scratch_shapes=[
            pltpu.SemaphoreType.DMA((copies,)),
            pltpu.SemaphoreType.DMA((copies,)),
            pltpu.SemaphoreType.DMA((len(arrays),)),
        ],
        compiler_params=pltpu.CompilerParams(collective_id=number, has_side_effects=True),
        name=name,
    )(*arrays)


def rope_tables(positions, head_width):
    half_width = head_width // 2
    freq_table = ROPE_BASE ** (-(2.0 / head_width) * jnp.arange(half_width, dtype=jnp.float32))
    angles = positions.astype(jnp.float32)[:, None] * freq_table[None, :]
    return (jnp.cos(angles), jnp.sin(angles))


def rotate(values, cosine_table, sine_table):
    half_width = values.shape[-1] // 2
    first_half = values[..., :half_width]
    second_half = values[..., half_width:]
    cosine_cols = cosine_table[:, None, :]
    sine_cols = sine_table[:, None, :]
    return jnp.concatenate(
        [
            first_half * cosine_cols - second_half * sine_cols,
            second_half * cosine_cols + first_half * sine_cols,
        ],
        axis=-1,
    )


def masked_scores(query_low, keys_low, query_position, key_position, query_docs, key_docs, present):
    scores = (
        jnp.einsum("qhgc,khc->hgqk", query_low, keys_low, preferred_element_type=jnp.float32)
        * SCORE_SCALE
    )
    allowed = (
        (query_docs[:, None] == key_docs[None, :])
        & (query_position[:, None] >= key_position[None, :])
        & present
    )
    return jnp.where(allowed, scores, MASKED)


def dot(a, b, left=1, right=0):
    return lax.dot_general(
        a, b, (((left,), (right,)), ((), ())), preferred_element_type=jnp.float32
    )


def column_of(block, column):
    lanes = lax.broadcasted_iota(jnp.int32, block.shape, 1)
    return jnp.sum(jnp.where(lanes == column, block, 0.0), axis=1, keepdims=True)


def expert_terms(rows, grads, weight, w_in, w_out):
    hidden = w_out.shape[0]
    gate_up = dot(rows, w_in)
    gate, up = gate_up[:, :hidden], gate_up[:, hidden:]
    active_grad = dot(grads, w_out, 1, 1)
    sigmoid = jax.nn.sigmoid(gate)
    silu = gate * sigmoid
    ungated = silu * up
    active = (ungated * weight).astype(jnp.bfloat16)
    scaled = active_grad * weight
    gate_grad = (scaled * up * sigmoid * (1.0 + gate * (1.0 - sigmoid))).astype(jnp.bfloat16)
    up_grad = (scaled * silu).astype(jnp.bfloat16)
    return active, jnp.concatenate([gate_grad, up_grad], axis=1), active_grad * ungated


def local_experts_body(first_of, rows_ref, grads_ref, weight_ref, in_ref, out_ref, moe_ref, back_ref, share_ref, moe_acc, back_acc, share_acc):
    expert = pl.program_id(0)

    @pl.when(expert == 0)
    def _():
        moe_acc[...] = jnp.zeros_like(moe_acc)
        back_acc[...] = jnp.zeros_like(back_acc)
        share_acc[...] = jnp.zeros_like(share_acc)

    w_in, w_out = in_ref[0], out_ref[0]
    weight = column_of(weight_ref[...], first_of(pl.num_programs(0)) + expert)
    active, gate_up_grad, shares = expert_terms(rows_ref[...], grads_ref[...], weight, w_in, w_out)
    moe_acc[...] += dot(active, w_out)
    back_acc[...] += dot(gate_up_grad, w_in, 1, 1)
    lanes = lax.broadcasted_iota(jnp.int32, share_acc.shape, 1)
    share = jnp.sum(shares, axis=1, keepdims=True)
    share_acc[...] = jnp.where(lanes == expert, share, share_acc[...])

    @pl.when(expert == pl.num_programs(0) - 1)
    def _():
        moe_ref[...] = moe_acc[...].astype(jnp.bfloat16)
        back_ref[...] = back_acc[...].astype(jnp.bfloat16)
        share_ref[...] = share_acc[...].astype(jnp.bfloat16)


def first_expert(count):
    return lax.axis_index("row") * count


def local_experts(rows, grads, weight, w_in, w_out):
    tokens, width = rows.shape
    experts, hidden = w_out.shape[0], w_out.shape[1]
    whole = lambda a: pl.BlockSpec(a.shape, lambda e: (0, 0))
    outs = [(tokens, width), (tokens, width), (tokens, LANES)]
    return pl.pallas_call(
        functools.partial(local_experts_body, first_expert),
        grid=(experts,),
        in_specs=[
            whole(rows),
            whole(grads),
            whole(weight),
            pl.BlockSpec((1, width, 2 * hidden), lambda e: (e, 0, 0)),
            pl.BlockSpec((1, hidden, width), lambda e: (e, 0, 0)),
        ],
        out_specs=tuple(pl.BlockSpec(s, lambda e: (0, 0)) for s in outs),
        out_shape=tuple(jax.ShapeDtypeStruct(s, jnp.bfloat16) for s in outs),
        scratch_shapes=[pltpu.VMEM(s, jnp.float32) for s in outs],
        name="local_experts",
    )(rows, grads, weight, w_in, w_out)


def expert_grads_body(first_of, rows_ref, grads_ref, weight_ref, in_ref, out_ref, gin_ref, gout_ref, in_acc, out_acc):
    expert, tile = pl.program_id(0), pl.program_id(1)
    hidden = out_ref.shape[1]

    @pl.when(tile == 0)
    def _():
        in_acc[...] = jnp.zeros_like(in_acc)
        out_acc[...] = jnp.zeros_like(out_acc)

    rows, grads = rows_ref[...], grads_ref[...]
    weights = weight_ref[...].astype(jnp.float32)
    column = first_of(pl.num_programs(0)) + expert
    weight = column_of(weights, column) + column_of(weights, column + LANES // 2)
    active, gate_up_grad, _ = expert_terms(rows, grads, weight, in_ref[0], out_ref[0])
    in_acc[...] += dot(rows, gate_up_grad, 0, 0)
    out_acc[...] += dot(active, grads, 0, 0)

    @pl.when(tile == pl.num_programs(1) - 1)
    def _():
        gout_ref[0] = out_acc[...]
        width = in_acc.shape[0]
        parts = hidden // LANES
        for part in range(parts):
            for half in range(2):
                at = half * hidden + part * LANES
                gin_ref[0, pl.ds(part * 2 + half, width, stride=2 * parts), :] = in_acc[
                    :, at : at + LANES
                ]


def expert_grads(rows, grads, weight, w_in, w_out):
    tokens, width = rows.shape
    experts, hidden = w_out.shape[0], w_out.shape[1]
    tile = 512
    parts = hidden // LANES
    gin, gout = pl.pallas_call(
        functools.partial(expert_grads_body, first_expert),
        grid=(experts, tokens // tile),
        in_specs=[
            pl.BlockSpec((tile, width), lambda e, t: (t, 0)),
            pl.BlockSpec((tile, width), lambda e, t: (t, 0)),
            pl.BlockSpec((tile, LANES), lambda e, t: (t, 0)),
            pl.BlockSpec((1, width, 2 * hidden), lambda e, t: (e, 0, 0)),
            pl.BlockSpec((1, hidden, width), lambda e, t: (e, 0, 0)),
        ],
        out_specs=(
            pl.BlockSpec((1, width * 2 * parts, LANES), lambda e, t: (e, 0, 0)),
            pl.BlockSpec((1, hidden, width), lambda e, t: (e, 0, 0)),
        ),
        out_shape=(
            jax.ShapeDtypeStruct((experts, width * 2 * parts, LANES), jnp.float32),
            jax.ShapeDtypeStruct((experts, hidden, width), jnp.float32),
        ),
        scratch_shapes=[
            pltpu.VMEM((width, 2 * hidden), jnp.float32),
            pltpu.VMEM((hidden, width), jnp.float32),
        ],
        name="expert_grads",
    )(rows, grads, weight, w_in, w_out)
    gin = gin.reshape(experts, width, parts, 2, LANES).transpose(0, 1, 3, 2, 4)
    return gin.reshape(experts, width, 2, hidden), gout


def local(
    sizes,
    tokens,
    out_grad,
    doc_ids,
    expert_ids,
    gain_attn,
    w_query,
    w_key_value,
    w_output,
    gain_moe,
    w_router,
    w_expert_in,
    w_expert_out,
):
    rows, cols, depth = sizes
    group = rows * cols
    tok_rows, feat_local = tokens.shape
    width = w_query.shape[0]
    head_dim = w_key_value.shape[2] // 2
    key_heads = w_key_value.shape[1]
    group_size = w_query.shape[1] // head_dim // key_heads
    experts = w_router.shape[1]
    expert_local, hidden = w_expert_out.shape[0], w_expert_out.shape[1]
    longest_doc = min(LONGEST, tok_rows * depth // 2)
    hop_count = longest_doc // tok_rows
    own = tok_rows // group
    layer = lax.axis_index("dp")
    me = lax.axis_index("row") * cols + lax.axis_index("col")
    offsets = jnp.arange(tok_rows, dtype=jnp.int32)
    positions = layer * tok_rows + offsets
    cosine_table, sine_table = rope_tables(positions, head_dim)

    def wide(blocks):
        return jnp.moveaxis(blocks, 0, 1).reshape(blocks.shape[1], -1)

    def narrow(array):
        return jnp.moveaxis(array.reshape(array.shape[0], group, -1), 1, 0)

    def gathered(array, axes, axis):
        return lax.all_gather(array, axes, axis=axis, tiled=True)

    docs_all = gathered(doc_ids, "dp", 0)
    gains = gathered(jnp.stack([gain_attn, gain_moe]), GROUP, 1).astype(jnp.float32)
    router_full = gathered(w_router, GROUP, 0).astype(jnp.float32)
    output_full = gathered(w_output, GROUP, 0)
    scaled_grad = (RESIDUAL_SCALE * out_grad.astype(jnp.float32)).astype(jnp.bfloat16)

    tokens_blocks, grad_blocks = exchange(
        sizes, "gather_tokens", 0, ("gather", tokens), ("gather", out_grad)
    )
    tokens_full = wide(tokens_blocks)
    tokens_wide = tokens_full.astype(jnp.float32)
    grad_full = wide(grad_blocks)
    moe_grad_full = (RESIDUAL_SCALE * grad_full.astype(jnp.float32)).astype(jnp.bfloat16)
    moe_grad_own = lax.dynamic_slice_in_dim(moe_grad_full, me * own, own, 0)
    moe_grad_all = gathered(moe_grad_own, EVERY, 0)
    query_full = gathered(w_query, GROUP, 1)
    key_value_full = gathered(w_key_value, GROUP, 1)

    scale_attn = lax.rsqrt(jnp.mean(tokens_wide * tokens_wide, axis=1) + EPSILON)
    normed_low = (tokens_wide * scale_attn[:, None] * gains[0]).astype(jnp.bfloat16)
    query = dot(normed_low, w_query).reshape(tok_rows, -1, head_dim)
    key_value = jnp.einsum(
        "td,dhc->thc", normed_low, w_key_value, preferred_element_type=jnp.float32
    )
    query_low = (
        rotate(query, cosine_table, sine_table)
        .astype(jnp.bfloat16)
        .reshape(tok_rows, key_heads, group_size, head_dim)
    )
    keys_low = rotate(key_value[..., :head_dim], cosine_table, sine_table).astype(jnp.bfloat16)
    values_low = key_value[..., head_dim:].astype(jnp.bfloat16)
    pair = jnp.concatenate([keys_low, values_low], axis=-1).reshape(tok_rows, -1)
    hops = list(range(1, hop_count + 1))
    (received_pairs,) = exchange(sizes, "shift_pairs", 1, ("shift", pair, hops, False))
    pairs = [pair] + [received_pairs[i] for i in range(hop_count)]
    received = [p.reshape(tok_rows, key_heads, 2 * head_dim) for p in pairs]

    def hop_scores(distance):
        origin = lax.rem(layer + depth - distance, depth)
        key_docs = lax.dynamic_slice_in_dim(docs_all, origin * tok_rows, tok_rows, 0)
        return masked_scores(
            query_low,
            received[distance][..., :head_dim],
            positions,
            (layer - distance) * tok_rows + offsets,
            doc_ids,
            key_docs,
            layer - distance >= 0,
        )

    score_list = [hop_scores(distance) for distance in range(hop_count + 1)]
    row_max = jnp.max(score_list[0], axis=-1)
    for scores in score_list[1:]:
        row_max = jnp.maximum(row_max, jnp.max(scores, axis=-1))
    row_total = jnp.zeros_like(row_max)
    for scores in score_list:
        row_total = row_total + jnp.sum(jnp.exp(scores - row_max[..., None]), axis=-1)
    mixed = jnp.zeros((tok_rows, key_heads, group_size, head_dim), jnp.float32)
    for distance, scores in enumerate(score_list):
        softmax_low = (jnp.exp(scores - row_max[..., None]) / row_total[..., None]).astype(
            jnp.bfloat16
        )
        mixed = mixed + jnp.einsum(
            "hgqk,khc->qhgc",
            softmax_low,
            received[distance][..., head_dim:],
            preferred_element_type=jnp.float32,
        )
    log_total = row_max + jnp.log(row_total)
    mixed_low = mixed.astype(jnp.bfloat16).reshape(tok_rows, -1)
    (mixed_blocks,) = exchange(
        sizes, "swap_mixed", 2, ("swap", mixed_low.reshape(group, own, -1))
    )

    mixed_own = wide(mixed_blocks)
    tokens_own = lax.dynamic_slice_in_dim(tokens_full, me * own, own, 0).astype(jnp.float32)
    middle = tokens_own + RESIDUAL_SCALE * dot(mixed_own, output_full)
    scale_moe = lax.rsqrt(jnp.mean(middle * middle, axis=1, keepdims=True) + EPSILON)
    normed_moe = middle * scale_moe * gains[1]
    logits = jnp.dot(normed_moe, router_full, precision=HIGH)
    ids_own = lax.dynamic_slice_in_dim(expert_ids, me * own, own, 0)
    chosen = jnp.sum(
        (ids_own[:, :, None] == jnp.arange(experts, dtype=jnp.int32)[None, None, :]).astype(
            jnp.float32
        ),
        axis=1,
    )
    exp_terms = jnp.exp(logits - jnp.max(logits, axis=1, keepdims=True)) * chosen
    weights = exp_terms / jnp.sum(exp_terms, axis=1, keepdims=True)
    weights_high = weights.astype(jnp.bfloat16)
    weights_low = (weights - weights_high.astype(jnp.float32)).astype(jnp.bfloat16)
    blank = jnp.zeros((own, LANES // 2 - experts), jnp.bfloat16)
    weights_pair = jnp.concatenate([weights_high, blank, weights_low, blank], axis=1)
    normed_own = normed_moe.astype(jnp.bfloat16)
    rows_blocks, weight_blocks = exchange(
        sizes, "gather_rows", 3, ("gather", normed_own), ("gather", weights_pair)
    )
    rows_all = gathered(normed_own, EVERY, 0)
    weights_all = gathered(weights_pair, EVERY, 0)
    rows_full = rows_blocks.reshape(tok_rows, width)
    weights_full = weight_blocks.reshape(tok_rows, LANES).astype(jnp.float32)
    half = LANES // 2
    weights_wide = weights_full + jnp.roll(weights_full, -half, axis=1)

    in_flat = w_expert_in.reshape(expert_local, width, 2 * hidden)
    moe_partial, back_partial, share_partial = local_experts(
        rows_full, moe_grad_full, weights_wide, in_flat, w_expert_out
    )
    moe_own = lax.psum_scatter(moe_partial, GROUP, scatter_dimension=0, tiled=True)
    back_blocks, share_blocks = exchange(
        sizes,
        "swap_back",
        4,
        ("swap", back_partial.reshape(group, own, width)),
        ("swap", share_partial.reshape(group, own, LANES)),
    )
    normed_grad = jnp.sum(back_blocks.astype(jnp.float32), axis=0)
    shares = jnp.sum(share_blocks.astype(jnp.float32).reshape(rows, cols, own, LANES), axis=1)
    weight_grad = jnp.moveaxis(shares[:, :, :expert_local], 0, 1).reshape(own, experts)
    logit_grad = weights * (weight_grad - jnp.sum(weights * weight_grad, axis=1, keepdims=True))
    normed_grad = normed_grad + jnp.dot(logit_grad, router_full.T, precision=HIGH)
    gain_moe_part = jnp.sum(normed_grad * middle * scale_moe, axis=0)
    grad_own = lax.dynamic_slice_in_dim(grad_full, me * own, own, 0).astype(jnp.float32)
    norm_dot = jnp.sum(normed_grad * gains[1] * middle, axis=1, keepdims=True)
    middle_grad = (
        grad_own + scale_moe * gains[1] * normed_grad - middle * (scale_moe**3 * norm_dot / width)
    )
    attn_grad = (RESIDUAL_SCALE * middle_grad).astype(jnp.bfloat16)
    mixed_grad_own = dot(attn_grad, output_full, 1, 1).astype(jnp.bfloat16)
    (mixed_grad_blocks,) = exchange(
        sizes, "swap_mixed_grad", 5, ("swap", narrow(mixed_grad_own))
    )
    logit_grad_all = gathered(logit_grad.astype(jnp.bfloat16), EVERY, 0)
    attn_grad_full = gathered(attn_grad, GROUP, 0)
    grad_output = dot(mixed_low, attn_grad_full, 0, 0)
    grad_output = lax.psum(grad_output.astype(jnp.bfloat16), "dp").astype(jnp.float32)

    mixed_grad_low = mixed_grad_blocks.reshape(tok_rows, key_heads, group_size, head_dim)
    row_delta = jnp.zeros((key_heads, group_size, tok_rows), jnp.float32)
    softmax_list = []
    product_list = []
    for distance in range(hop_count + 1):
        softmax_full = jnp.exp(score_list[distance] - log_total[..., None])
        softmax_grad = jnp.einsum(
            "qhgc,khc->hgqk",
            mixed_grad_low,
            received[distance][..., head_dim:],
            preferred_element_type=jnp.float32,
        )
        row_delta = row_delta + jnp.sum(softmax_full * softmax_grad, axis=-1)
        softmax_list.append(softmax_full)
        product_list.append(softmax_grad)
    query_grad = jnp.zeros((tok_rows, key_heads, group_size, head_dim), jnp.float32)
    pieces = []
    for distance in range(hop_count + 1):
        softmax_full = softmax_list[distance]
        scores_grad = (softmax_full * (product_list[distance] - row_delta[..., None])).astype(
            jnp.bfloat16
        )
        query_grad = (
            query_grad
            + jnp.einsum(
                "hgqk,khc->qhgc",
                scores_grad,
                received[distance][..., :head_dim],
                preferred_element_type=jnp.float32,
            )
            * SCORE_SCALE
        )
        keys_grad = (
            jnp.einsum("hgqk,qhgc->khc", scores_grad, query_low, preferred_element_type=jnp.float32)
            * SCORE_SCALE
        )
        values_grad = jnp.einsum(
            "hgqk,qhgc->khc",
            softmax_full.astype(jnp.bfloat16),
            mixed_grad_low,
            preferred_element_type=jnp.float32,
        )
        pieces.append(jnp.concatenate([keys_grad, values_grad], axis=-1).reshape(tok_rows, -1))
    sent = jnp.stack(pieces[1:]).astype(jnp.bfloat16)
    (returned,) = exchange(
        sizes, "shift_grads", 6, ("shift", sent, [-d for d in hops], True)
    )
    carried = pieces[0]
    for distance in hops:
        carried = carried + jnp.where(
            layer + distance < depth, returned[distance - 1].astype(jnp.float32), 0.0
        )
    carried = carried.reshape(tok_rows, key_heads, 2 * head_dim)
    keys_back = rotate(carried[..., :head_dim], cosine_table, -sine_table)
    key_value_grad = (
        jnp.concatenate([keys_back, carried[..., head_dim:]], axis=-1)
        .astype(jnp.bfloat16)
        .reshape(tok_rows, -1)
    )
    query_grad_low = (
        rotate(query_grad.reshape(tok_rows, -1, head_dim), cosine_table, -sine_table)
        .astype(jnp.bfloat16)
        .reshape(tok_rows, -1)
    )
    query_grad_blocks, key_value_grad_blocks = exchange(
        sizes,
        "swap_projection",
        7,
        ("swap", query_grad_low.reshape(group, own, -1)),
        ("swap", key_value_grad.reshape(group, own, -1)),
    )
    grad_query = dot(normed_low, query_grad_low, 0, 0)
    grad_key_value = dot(normed_low, key_value_grad, 0, 0)
    grad_query = lax.psum(grad_query.astype(jnp.bfloat16), "dp").astype(jnp.float32)
    grad_key_value = lax.psum(grad_key_value.astype(jnp.bfloat16), "dp").astype(jnp.float32)

    attn_normed_grad = dot(wide(query_grad_blocks), query_full, 1, 1) + dot(
        wide(key_value_grad_blocks), key_value_full.reshape(width, -1), 1, 1
    )
    scale_own = lax.rsqrt(jnp.mean(tokens_own * tokens_own, axis=1, keepdims=True) + EPSILON)
    attn_dot = jnp.sum(attn_normed_grad * gains[0] * tokens_own, axis=1, keepdims=True)
    gain_attn_part = jnp.sum(attn_normed_grad * tokens_own * scale_own, axis=0)
    in_grad_own = (
        middle_grad
        + scale_own * gains[0] * attn_normed_grad
        - tokens_own * (scale_own**3 * attn_dot / width)
    ).astype(jnp.bfloat16)
    block_own = (middle + RESIDUAL_SCALE * moe_own.astype(jnp.float32)).astype(jnp.bfloat16)
    block_blocks, in_grad_blocks = exchange(
        sizes,
        "swap_results",
        8,
        ("swap", narrow(block_own)),
        ("swap", narrow(in_grad_own)),
    )
    gain_parts = jnp.stack([gain_attn_part, gain_moe_part]).astype(jnp.bfloat16)
    gain_sums = lax.psum(gain_parts, EVERY).astype(jnp.float32)
    gain_mine = lax.dynamic_slice_in_dim(gain_sums, me * feat_local, feat_local, 1)

    rows_late, grads_late, weights_late, block_blocks = lax.optimization_barrier(
        (rows_all, moe_grad_all, weights_all, block_blocks)
    )
    grad_expert_in, grad_expert_out = expert_grads(
        rows_late, grads_late, weights_late, in_flat, w_expert_out
    )
    rows_mine = lax.dynamic_slice_in_dim(rows_all, me * feat_local, feat_local, 1)
    grad_router = dot(rows_mine, logit_grad_all, 0, 0)
    return (
        block_blocks.reshape(tok_rows, feat_local),
        in_grad_blocks.reshape(tok_rows, feat_local),
        gain_mine[0],
        grad_query,
        grad_key_value.reshape(width, key_heads, -1),
        grad_output,
        gain_mine[1],
        grad_router,
        grad_expert_in,
        grad_expert_out,
    )


def solution(mesh):
    in_specs = (
        P("dp", ("row", "col")),
        P("dp", ("row", "col")),
        P("dp"),
        P("dp", None),
        P(("row", "col")),
        P(None, ("row", "col")),
        P(None, ("row", "col"), None),
        P(("row", "col"), None),
        P(("row", "col")),
        P(("row", "col"), None),
        P("row", None, None, "col"),
        P("row", "col", None),
    )
    out_specs = (
        P("dp", ("row", "col")),
        P("dp", ("row", "col")),
        P(("row", "col")),
        P(None, ("row", "col")),
        P(None, ("row", "col"), None),
        P(("row", "col"), None),
        P(("row", "col")),
        P(("row", "col"), None),
        P("row", None, None, "col"),
        P("row", "col", None),
    )
    sizes = (mesh.shape["row"], mesh.shape["col"], mesh.shape["dp"])
    return jax.shard_map(
        functools.partial(local, sizes),
        mesh=mesh,
        in_specs=in_specs,
        out_specs=out_specs,
        check_vma=False,
    )
```

```python
import functools

import jax
import jax.numpy as jnp
from jax import lax
from jax.experimental import pallas as pl
from jax.experimental.pallas import tpu as pltpu
from jax.sharding import PartitionSpec as P

LONGEST = 4096
HIGH = lax.Precision.HIGHEST
EPSILON = 1e-05
RESIDUAL_SCALE = 0.22
SCORE_SCALE = 0.015625
ROPE_BASE = 10000.0
MASKED = -1e30
MESH = pl.DeviceIdType.MESH
GROUP = ("row", "col")
EVERY = ("dp", "row", "col")
LANES = 128
HBM = pl.BlockSpec(memory_space=pl.ANY)
FULL = pl.BlockSpec(memory_space=pltpu.VMEM)
TURN = LANES // 4


class Moves:
    def __init__(self, sizes, kinds, sources, targets, sems):
        self.sizes, self.kinds = sizes, kinds
        self.sources, self.targets = sources, targets
        self.send_sem, self.recv_sem, self.local_sem = sems

    def place(self):
        rows, cols, depth = self.sizes
        row, col, layer = lax.axis_index("row"), lax.axis_index("col"), lax.axis_index("dp")
        return row, col, layer, row * cols + col

    def barrier(self):
        rows, cols, depth = self.sizes
        row, col, layer, me = self.place()
        group = rows * cols
        barrier = pltpu.get_barrier_semaphore()
        partners = []
        if any(kind[0] == "spread" for kind in self.kinds):
            for k in range(1, group * depth):
                other = lax.rem(layer * group + me + k, group * depth)
                partners.append(
                    {
                        "dp": other // group,
                        "row": lax.rem(other, group) // cols,
                        "col": lax.rem(other, cols),
                    }
                )
        elif any(kind[0] == "swap" for kind in self.kinds):
            for k in range(1, group):
                other = lax.rem(me + k, group)
                partners.append({"row": other // cols, "col": lax.rem(other, cols)})
        elif any(kind[0] == "gather" for kind in self.kinds):
            for k in range(1, rows):
                partners.append({"row": lax.rem(row + k, rows)})
            for k in range(1, cols):
                partners.append({"col": lax.rem(col + k, cols)})
        shifts = set()
        for kind in self.kinds:
            if kind[0] == "shift":
                for d in kind[1]:
                    shifts |= {d % depth, -d % depth}
        if any(kind[0] == "spread" for kind in self.kinds):
            shifts = set()
        for k in sorted(shifts - {0}):
            partners.append({"dp": lax.rem(layer + k, depth)})
        for partner in partners:
            pl.semaphore_signal(barrier, inc=1, device_id=partner, device_id_type=MESH)
        pl.semaphore_wait(barrier, len(partners))

    def copies(self):
        rows, cols, depth = self.sizes
        row, col, layer, me = self.place()
        group = rows * cols
        slot = 0
        direct, relayed, local = [], [], []

        def remote(source, target, device):
            nonlocal slot
            slot += 1
            return functools.partial(
                pltpu.make_async_remote_copy,
                src_ref=source,
                dst_ref=target,
                send_sem=self.send_sem.at[slot - 1],
                recv_sem=self.recv_sem.at[slot - 1],
                device_id=device,
                device_id_type=MESH,
            )

        for index, (kind, source, target) in enumerate(
            zip(self.kinds, self.sources, self.targets)
        ):
            if kind[0] == "gather":
                at = (lambda i: target.at[:, i]) if kind[1] else (lambda i: target.at[i])
                for k in range(1, rows):
                    copy = remote(source, at(me), {"row": lax.rem(row + k, rows)})
                    origin = lax.rem(row + rows - k, rows) * cols + col
                    piece = at(origin)
                    nexts = [
                        remote(piece, piece, {"col": lax.rem(col + j, cols)})
                        for j in range(1, cols)
                    ]
                    relayed.append((copy, nexts))
                for k in range(1, cols):
                    direct.append(remote(source, at(me), {"col": lax.rem(col + k, cols)}))
                sem = self.local_sem.at[index]
                local.append(functools.partial(pltpu.make_async_copy, source, at(me), sem))
            elif kind[0] == "swap":
                for k in range(1, group):
                    other = lax.rem(me + k, group)
                    device = {"row": other // cols, "col": lax.rem(other, cols)}
                    direct.append(remote(source.at[other], target.at[me], device))
                sem = self.local_sem.at[index]
                local.append(
                    functools.partial(pltpu.make_async_copy, source.at[me], target.at[me], sem)
                )
            elif kind[0] == "spread":
                mine = layer * group + me
                for k in range(1, group * depth):
                    other = lax.rem(mine + k, group * depth)
                    block = lax.rem(other, group)
                    device = {
                        "dp": other // group,
                        "row": block // cols,
                        "col": lax.rem(other, cols),
                    }
                    direct.append(remote(source.at[block], target.at[mine], device))
                sem = self.local_sem.at[index]
                local.append(
                    functools.partial(
                        pltpu.make_async_copy, source.at[me], target.at[mine], sem
                    )
                )
            else:
                for at, d in enumerate(kind[1]):
                    piece = source.at[at] if kind[2] else source
                    device = {"dp": lax.rem(layer + d % depth, depth)}
                    direct.append(remote(piece, target.at[at], device))
        return direct, relayed, local

    def start(self):
        direct, relayed, local = self.copies()
        for copy, _ in relayed:
            copy().start()
        for copy in direct + local:
            copy().start()

    def relay(self):
        _, relayed, _ = self.copies()
        for copy, nexts in relayed:
            copy().wait_recv()
            for follower in nexts:
                follower().start()

    def finish(self):
        direct, relayed, local = self.copies()
        for copy, nexts in relayed:
            copy().wait_send()
            for follower in nexts:
                follower().wait()
        for copy in direct + local:
            copy().wait()


def exchange_body(sizes, kinds, *refs):
    count = len(kinds)
    moves = Moves(sizes, kinds, refs[:count], refs[count : 2 * count], refs[2 * count :])
    moves.barrier()
    moves.start()
    moves.relay()
    moves.finish()


def planned(sizes, items):
    rows, cols, depth = sizes
    group = rows * cols
    kinds, shapes, copies = [], [], 0
    for item in items:
        array = item[1]
        if item[0] == "gather":
            second = len(item) > 2 and item[2]
            kinds.append(("gather", second))
            shape = (array.shape[0], group) + array.shape[1:] if second else (group,) + array.shape
            shapes.append(jax.ShapeDtypeStruct(shape, array.dtype))
            copies += (rows - 1) * cols + cols - 1
        elif item[0] == "spread":
            kinds.append(("spread",))
            shapes.append(
                jax.ShapeDtypeStruct((group * depth,) + array.shape[1:], array.dtype)
            )
            copies += group * depth - 1
        elif item[0] == "swap":
            kinds.append(("swap",))
            shapes.append(jax.ShapeDtypeStruct(array.shape, array.dtype))
            copies += group - 1
        else:
            distances, split = item[2], item[3]
            kinds.append(("shift", tuple(distances), split))
            block = array.shape[1:] if split else array.shape
            shapes.append(jax.ShapeDtypeStruct((len(distances),) + block, array.dtype))
            copies += len(distances)
    sems = [
        pltpu.SemaphoreType.DMA((copies,)),
        pltpu.SemaphoreType.DMA((copies,)),
        pltpu.SemaphoreType.DMA((len(items),)),
    ]
    return tuple(kinds), shapes, sems


def exchange(sizes, name, number, *items):
    kinds, shapes, sems = planned(sizes, items)
    return pl.pallas_call(
        functools.partial(exchange_body, sizes, kinds),
        out_shape=tuple(shapes),
        in_specs=[HBM] * len(items),
        out_specs=(HBM,) * len(items),
        scratch_shapes=sems,
        compiler_params=pltpu.CompilerParams(collective_id=number, has_side_effects=True),
        name=name,
    )(*[item[1] for item in items])


def dot(a, b, left=1, right=0, precision=None):
    return lax.dot_general(
        a,
        b,
        (((left,), (right,)), ((), ())),
        preferred_element_type=jnp.float32,
        precision=precision,
    )


def call(body, name, shapes, *arrays, scratch=()):
    return pl.pallas_call(
        body,
        out_shape=tuple(jax.ShapeDtypeStruct(*shape) for shape in shapes),
        in_specs=[FULL] * len(arrays),
        out_specs=(FULL,) * len(shapes),
        scratch_shapes=list(scratch),
        name=name,
    )(*arrays)


def lanes_of(shape):
    return lax.broadcasted_iota(jnp.int32, shape, len(shape) - 1)


def flipped(values):
    lanes = lanes_of(values.shape)
    ahead = pltpu.roll(values, LANES - TURN, 1)
    behind = pltpu.roll(values, TURN, 1)
    return jnp.where(lanes % (2 * TURN) < TURN, ahead, behind)


def beside(blocks_ref):
    return jnp.concatenate([blocks_ref[i] for i in range(blocks_ref.shape[0])], axis=1)


def project_body(blocks, gains, w_query, w_pair, cosine, sine, normed, query, pair, own):
    tokens = beside(blocks).astype(jnp.float32)
    scale = lax.rsqrt(jnp.mean(tokens * tokens, axis=1, keepdims=True) + EPSILON)
    normed[...] = (tokens * scale * gains[0:1, :]).astype(jnp.bfloat16)
    raw = dot(normed[...], w_query[...])
    query[...] = (raw * cosine[...] + flipped(raw) * sine[...]).astype(jnp.bfloat16)
    raw = dot(normed[...], w_pair[...])
    keys = lanes_of(raw.shape) < LANES // 2
    turned = raw * cosine[...] + flipped(raw) * sine[...]
    pair[...] = jnp.where(keys, turned, raw).astype(jnp.bfloat16)
    rows = own.shape[0]
    cols = lax.axis_size("col")
    first = (lax.axis_index("row") * cols + lax.axis_index("col")) * rows
    for i in range(blocks.shape[0]):
        own[:, i * LANES : (i + 1) * LANES] = blocks[i, pl.ds(first, rows), :]


def doubled(pair, keys_ref, values_ref, at):
    wide = pair.astype(jnp.float32)
    other = pltpu.roll(wide, LANES // 2, 1)
    keys = lanes_of(wide.shape) < LANES // 2
    keys_ref[at] = jnp.where(keys, wide, other).astype(jnp.bfloat16)
    values_ref[at] = jnp.where(keys, other, wide).astype(jnp.bfloat16)


def per_head(values):
    first = lanes_of(values.shape) < LANES // 2
    zero = jnp.zeros_like(values)
    return jnp.concatenate(
        [jnp.where(first, values, zero), jnp.where(first, zero, values)], axis=0
    )


def tile_scores(queries, keys_ref, starts, row, block, last, tokens):
    scores = dot(queries, keys_ref[block], 1, 1) * SCORE_SCALE
    at = lanes_of(scores.shape) + block * tokens
    allowed = at >= starts
    if block == last:
        place = row + lax.broadcasted_iota(jnp.int32, scores.shape, 0)
        allowed = allowed & (at <= place + block * tokens)
    return jnp.where(allowed, scores, MASKED)


def attend_body(query, pair, far, start, mixed, log_total, keys, values, queries, out):
    tokens = query.shape[0]
    last = far.shape[0]
    doubled(pair[...], keys, values, last)
    for d in range(1, last + 1):
        doubled(far[d - 1], keys, values, last - d)
    queries[...] = per_head(query[...].astype(jnp.float32)).astype(jnp.bfloat16)
    step = 256

    def tile(i, carry):
        rows = pl.ds(pl.multiple_of(i * step, step), step)
        row = lax.rem(i * step, tokens)
        starts = start[pl.ds(pl.multiple_of(row, step), step), :]
        parts = [
            tile_scores(queries[rows, :], keys, starts, row, block, last, tokens)
            for block in range(last + 1)
        ]
        top = functools.reduce(
            jnp.maximum, [jnp.max(part, axis=1, keepdims=True) for part in parts]
        )
        parts = [jnp.exp(part - top) for part in parts]
        total = functools.reduce(jnp.add, [jnp.sum(p, axis=1, keepdims=True) for p in parts])
        sums = [
            dot(part.astype(jnp.bfloat16), values[block]) for block, part in enumerate(parts)
        ]
        out[rows, :] = functools.reduce(jnp.add, sums) / total
        log_total[rows, :] = top + jnp.log(total)
        return carry

    lax.fori_loop(0, 2 * tokens // step, tile, 0)
    first = lanes_of((tokens, LANES)) < LANES // 2
    mixed[...] = jnp.where(first, out[:tokens, :], out[tokens:, :]).astype(jnp.bfloat16)


def attend_back_body(grad, w_output, query, pair, far, start, log_total, mixed, cosine, sine, query_grad, pair_grad, far_grad, output_grad, keys, values, queries, grads, turned, key_sums, value_sums):
    tokens = query.shape[0]
    last = far.shape[0]
    doubled(pair[...], keys, values, last)
    for d in range(1, last + 1):
        doubled(far[d - 1], keys, values, last - d)
    queries[...] = per_head(query[...].astype(jnp.float32)).astype(jnp.bfloat16)
    grads[...] = per_head(dot(grad[...], w_output[...], 1, 1)).astype(jnp.bfloat16)
    output_grad[...] = dot(mixed[...], grad[...], 0, 0).astype(jnp.bfloat16)
    key_sums[...] = jnp.zeros_like(key_sums)
    value_sums[...] = jnp.zeros_like(value_sums)
    step = 256

    def tile(i, carry):
        rows = pl.ds(pl.multiple_of(i * step, step), step)
        row = lax.rem(i * step, tokens)
        starts = start[pl.ds(pl.multiple_of(row, step), step), :]
        asked, given, level = queries[rows, :], grads[rows, :], log_total[rows, :]
        chances, products = [], []
        for block in range(last + 1):
            scores = tile_scores(asked, keys, starts, row, block, last, tokens)
            chances.append(jnp.exp(scores - level))
            products.append(dot(given, values[block], 1, 1))
        delta = functools.reduce(
            jnp.add,
            [jnp.sum(p * q, axis=1, keepdims=True) for p, q in zip(chances, products)],
        )
        total = jnp.zeros((step, LANES), jnp.float32)
        for block in range(last + 1):
            back = (chances[block] * (products[block] - delta)).astype(jnp.bfloat16)
            total = total + dot(back, keys[block])
            key_sums[block] += dot(back, asked, 0, 0)
            value_sums[block] += dot(chances[block].astype(jnp.bfloat16), given, 0, 0)
        turned[rows, :] = total
        return carry

    lax.fori_loop(0, 2 * tokens // step, tile, 0)
    first = lanes_of((tokens, LANES)) < LANES // 2
    raw = jnp.where(first, turned[:tokens, :], turned[tokens:, :]) * SCORE_SCALE
    query_grad[...] = (raw * cosine[...] - flipped(raw) * sine[...]).astype(jnp.bfloat16)

    def joined(block):
        by_key, by_value = key_sums[block], value_sums[block]
        by_key = (by_key + pltpu.roll(by_key, LANES // 2, 1)) * SCORE_SCALE
        by_value = by_value + pltpu.roll(by_value, LANES // 2, 1)
        return jnp.where(first, by_key, by_value)

    pair_grad[...] = joined(last)
    for d in range(1, last + 1):
        far_grad[d - 1] = joined(last - d).astype(jnp.bfloat16)


def middle_body(experts, mixed, own, w_output, gains, router, ids_ref, rows, middle, weights):
    width = own.shape[1]
    attn = dot(beside(mixed), w_output[...])
    value = own[...].astype(jnp.float32) + RESIDUAL_SCALE * attn
    middle[...] = value
    scale = lax.rsqrt(jnp.mean(value * value, axis=1, keepdims=True) + EPSILON)
    normed = value * scale * gains[1:2, :]
    logits = dot(normed, router[...].astype(jnp.float32), precision=HIGH)
    count = own.shape[0]
    cols = lax.axis_size("col")
    first = (lax.axis_index("row") * cols + lax.axis_index("col")) * count
    ids = ids_ref[pl.ds(first, count), :]
    lanes = lanes_of((count, LANES))
    chosen = jnp.zeros((count, LANES), jnp.float32)
    for k in range(ids.shape[1]):
        chosen = chosen + (ids[:, k : k + 1] == lanes).astype(jnp.float32)
    top = jnp.max(jnp.where(lanes < experts, logits, MASKED), axis=1, keepdims=True)
    terms = jnp.exp(jnp.minimum(logits - top, 0.0)) * chosen
    share = terms / jnp.sum(terms, axis=1, keepdims=True)
    weights[...] = share
    high = share.astype(jnp.bfloat16)
    low = share - high.astype(jnp.float32)
    rows[:, :width] = normed.astype(jnp.bfloat16)
    rows[:, width:] = (high.astype(jnp.float32) + pltpu.roll(low, LANES // 2, 1)).astype(
        jnp.bfloat16
    )


def middle_back_body(back, out_grad, middle, weights, gains, router, middle_grad, attn_grad, logit_grad, gain_part):
    width = middle.shape[1]
    normed_grad = back[0, :, :width].astype(jnp.float32)
    weight_grad = back[0, :, width:].astype(jnp.float32)
    for i in range(1, back.shape[0]):
        normed_grad = normed_grad + back[i, :, :width].astype(jnp.float32)
        weight_grad = weight_grad + back[i, :, width:].astype(jnp.float32)
    share, value = weights[...], middle[...]
    mean = jnp.sum(share * weight_grad, axis=1, keepdims=True)
    logit = share * (weight_grad - mean)
    logit_grad[...] = logit.astype(jnp.bfloat16)
    normed_grad = normed_grad + dot(
        logit, router[...].astype(jnp.float32), 1, 1, precision=HIGH
    )
    scale = lax.rsqrt(jnp.mean(value * value, axis=1, keepdims=True) + EPSILON)
    gain_part[...] = jnp.sum(normed_grad * value * scale, axis=0, keepdims=True)
    scaled = normed_grad * gains[1:2, :]
    norm_dot = jnp.sum(scaled * value, axis=1, keepdims=True)
    total = (
        beside(out_grad).astype(jnp.float32)
        + scale * scaled
        - value * (scale * scale * scale * norm_dot / width)
    )
    middle_grad[...] = total
    attn_grad[...] = (RESIDUAL_SCALE * total).astype(jnp.bfloat16)


def project_back_body(query_grad, pair_grad, returned, normed, w_query, w_pair, cosine, sine, partial, query_sum, pair_sum):
    layer = lax.axis_index("dp")
    depth = lax.axis_size("dp")
    total = pair_grad[...]
    for i in range(returned.shape[0]):
        total = total + jnp.where(
            layer + i + 1 < depth, returned[i].astype(jnp.float32), 0.0
        )
    keys = lanes_of(total.shape) < LANES // 2
    turned = total * cosine[...] - flipped(total) * sine[...]
    pair_low = jnp.where(keys, turned, total).astype(jnp.bfloat16)
    query_low = query_grad[...]
    partial[...] = (
        dot(query_low, w_query[...], 1, 1) + dot(pair_low, w_pair[...], 1, 1)
    ).astype(jnp.bfloat16)
    query_sum[...] = dot(normed[...], query_low, 0, 0).astype(jnp.bfloat16)
    pair_sum[...] = dot(normed[...], pair_low, 0, 0).astype(jnp.bfloat16)


def results_body(blocks, moe, own, middle, middle_grad, gains, gain_moe, block_out, in_grad, gain_parts):
    width = own.shape[1]
    normed_grad = blocks[0].astype(jnp.float32)
    branch = moe[0].astype(jnp.float32)
    for i in range(1, blocks.shape[0]):
        normed_grad = normed_grad + blocks[i].astype(jnp.float32)
        branch = branch + moe[i].astype(jnp.float32)
    value = own[...].astype(jnp.float32)
    scale = lax.rsqrt(jnp.mean(value * value, axis=1, keepdims=True) + EPSILON)
    gain_attn = jnp.sum(normed_grad * value * scale, axis=0, keepdims=True)
    scaled = normed_grad * gains[0:1, :]
    norm_dot = jnp.sum(scaled * value, axis=1, keepdims=True)
    grad = (
        middle_grad[...] + scale * scaled - value * (scale * scale * scale * norm_dot / width)
    ).astype(jnp.bfloat16)
    out = (middle[...] + RESIDUAL_SCALE * branch).astype(jnp.bfloat16)
    gain_parts[...] = jnp.zeros_like(gain_parts)
    for i in range(block_out.shape[0]):
        at = slice(i * LANES, (i + 1) * LANES)
        block_out[i] = out[:, at]
        in_grad[i] = grad[:, at]
        gain_parts[i, 0:1, :] = gain_attn[:, at]
        gain_parts[i, 1:2, :] = gain_moe[0:1, at]


def expert_terms(gate_up, active_grad, weight):
    hidden = active_grad.shape[0]
    gate, up = gate_up[:hidden], gate_up[hidden:]
    sigmoid = jax.nn.sigmoid(gate)
    silu = gate * sigmoid
    ungated = silu * up
    active = (ungated * weight).astype(jnp.bfloat16)
    scaled = active_grad * weight
    gate_grad = (scaled * up * sigmoid * (1.0 + gate * (1.0 - sigmoid))).astype(jnp.bfloat16)
    up_grad = (scaled * silu).astype(jnp.bfloat16)
    return active, jnp.concatenate([gate_grad, up_grad], axis=0), active_grad * ungated


def weight_rows(extra):
    turned = extra.astype(jnp.float32).T
    return turned[: LANES // 2] + turned[LANES // 2 :]


def local_experts_body(sizes, kinds, rows_ref, grads_ref, in_ref, out_ref, sent_ref, moe_ref, back_ref, flat_ref, got_ref, moe_acc, back_acc, share, weights, spread, *sems):
    step, steps = pl.program_id(0), pl.num_programs(0)
    each, hidden, width = out_ref.shape
    parts = hidden // LANES
    moves = Moves(sizes, kinds, [sent_ref], [got_ref], sems)

    @pl.when(step == 0)
    def _():
        moves.barrier()
        moves.start()
        moe_acc[...] = jnp.zeros_like(moe_acc)
        back_acc[...] = jnp.zeros_like(back_acc)
        share[...] = jnp.zeros_like(share)
        weights[...] = weight_rows(rows_ref[:, width:])

    @pl.when(step == steps // 2)
    def _():
        moves.relay()

    for i in range(each):
        spread[i] = in_ref[i].astype(jnp.float32)
        for part in range(parts):
            for half in range(2):
                at = half * hidden + part * LANES
                flat_ref[i, :, at : at + LANES] = spread[
                    i, pl.ds(part * 2 + half, width, stride=2 * parts), :
                ].astype(jnp.bfloat16)
        expert = (lax.axis_index("row") * steps + step) * each + i
        active, gate_up_grad, shares = expert_terms(
            dot(flat_ref[i], rows_ref[:, :width], 0, 1),
            dot(out_ref[i], grads_ref[0]),
            weights[pl.ds(expert, 1), :],
        )
        share[pl.ds(expert, 1), :] = jnp.sum(shares, axis=0, keepdims=True)
        moe_acc[...] += dot(active, out_ref[i], 0, 0)
        back_acc[...] += dot(gate_up_grad, flat_ref[i], 0, 1)

    @pl.when(step == steps - 1)
    def _():
        moe_ref[...] = moe_acc[...].astype(jnp.bfloat16)
        back_ref[:, :width] = back_acc[...].astype(jnp.bfloat16)
        back_ref[:, width:] = share[...].T.astype(jnp.bfloat16)
        moves.finish()


def local_experts(sizes, number, rows, grads, w_in, w_out, sent):
    tokens, wide = rows.shape
    experts, hidden, width = w_out.shape
    each = 2
    kinds, shapes, sems = planned(sizes, [("gather", sent, True)])
    whole = lambda s: pl.BlockSpec(s, lambda e: (0,) * len(s))
    some = lambda s: pl.BlockSpec((each,) + s[1:], lambda e: (e,) + (0,) * (len(s) - 1))
    flat = (experts, width, 2 * hidden)
    return pl.pallas_call(
        functools.partial(local_experts_body, sizes, kinds),
        grid=(experts // each,),
        in_specs=[
            whole(rows.shape),
            pl.BlockSpec((1, width, tokens), lambda e: (lax.axis_index("dp"), 0, 0)),
            some(w_in.shape),
            some(w_out.shape),
            HBM,
        ],
        out_specs=(whole((tokens, width)), whole((tokens, wide)), some(flat), HBM),
        out_shape=(
            jax.ShapeDtypeStruct((tokens, width), jnp.bfloat16),
            jax.ShapeDtypeStruct((tokens, wide), jnp.bfloat16),
            jax.ShapeDtypeStruct(flat, jnp.bfloat16),
            shapes[0],
        ),
        scratch_shapes=[
            pltpu.VMEM((tokens, width), jnp.float32),
            pltpu.VMEM((tokens, width), jnp.float32),
            pltpu.VMEM((LANES, tokens), jnp.float32),
            pltpu.VMEM((LANES // 2, tokens), jnp.float32),
            pltpu.VMEM((each,) + w_in.shape[1:], jnp.float32),
        ]
        + sems,
        compiler_params=pltpu.CompilerParams(collective_id=number, has_side_effects=True),
        name="local_experts",
    )(rows, grads, w_in, w_out, sent)


def expert_grads_body(own_ref, far_ref, grads_ref, in_ref, out_ref, gin_ref, gout_ref, rows, weights, *sums):
    expert, experts = pl.program_id(0), pl.num_programs(0)
    hidden, width = out_ref.shape[1:]
    parts = hidden // LANES
    layers, tokens = grads_ref.shape[0], own_ref.shape[0]
    layer = lax.axis_index("dp")

    def plane(distance):
        return lax.rem(layer + layers - distance, layers)

    @pl.when(expert == 0)
    def _():
        for distance in range(layers):
            source = own_ref[...] if distance == 0 else far_ref[distance - 1]
            weights[distance] = weight_rows(source[:, width:])
            if not sums:
                rows[distance * tokens : (distance + 1) * tokens, :] = source[:, :width]

    index = lax.axis_index("row") * experts + expert

    def part_of(block, first, pieces):
        weight = jnp.concatenate(
            [weights[first + i, pl.ds(index, 1), :] for i in range(pieces)], axis=1
        )
        active_grad = jnp.concatenate(
            [dot(out_ref[0], grads_ref[plane(first + i)]) for i in range(pieces)], axis=1
        )
        active, gate_up_grad, _ = expert_terms(dot(in_ref[0], block, 0, 1), active_grad, weight)
        out_sum = functools.reduce(
            jnp.add,
            [
                dot(active[:, i * tokens : (i + 1) * tokens], grads_ref[plane(first + i)], 1, 1)
                for i in range(pieces)
            ],
        )
        return dot(gate_up_grad, block), out_sum

    if not sums:
        in_sum, out_sum = part_of(rows[...], 0, layers)
    else:
        in_acc, out_acc = sums
        in_acc[...], out_acc[...] = part_of(own_ref[:, :width], 0, 1)

        def more(distance, carry):
            in_more, out_more = part_of(far_ref[distance - 1, :, :width], distance, 1)
            in_acc[...] += in_more
            out_acc[...] += out_more
            return carry

        lax.fori_loop(1, layers, more, 0)
        in_sum, out_sum = in_acc[...], out_acc[...]
    gout_ref[0] = out_sum
    for part in range(parts):
        for half in range(2):
            at = half * hidden + part * LANES
            gin_ref[0, pl.ds(part * 2 + half, width, stride=2 * parts), :] = in_sum[
                at : at + LANES, :
            ].T


def expert_grads(own, far, grads, w_in, w_out):
    tokens, wide = own.shape
    experts, hidden, width = w_out.shape
    layers = grads.shape[0]
    parts = hidden // LANES
    once = lambda s: pl.BlockSpec(s, lambda e: (0,) * len(s), pipeline_mode=pl.Buffered(1))
    each = lambda s: pl.BlockSpec((1,) + s[1:], lambda e: (e, 0, 0))
    outs = [(experts, width * 2 * parts, LANES), (experts, hidden, width)]
    sums = [(2 * hidden, width), (hidden, width)] if layers > 4 else []
    gin, gout = pl.pallas_call(
        expert_grads_body,
        grid=(experts,),
        in_specs=[
            once(own.shape),
            once(far.shape),
            once(grads.shape),
            each(w_in.shape),
            each(w_out.shape),
        ],
        out_specs=tuple(each(s) for s in outs),
        out_shape=tuple(jax.ShapeDtypeStruct(s, jnp.float32) for s in outs),
        scratch_shapes=[
            pltpu.VMEM((8, LANES) if sums else (layers * tokens, width), jnp.bfloat16),
            pltpu.VMEM((layers, LANES // 2, tokens), jnp.float32),
        ]
        + [pltpu.VMEM(s, jnp.float32) for s in sums],
        name="expert_grads",
    )(own, far, grads, w_in, w_out)
    gin = gin.reshape(experts, width, parts, 2, LANES).transpose(0, 1, 3, 2, 4)
    return gin.reshape(experts, width, 2, hidden), gout


def local(
    sizes,
    tokens,
    out_grad,
    doc_ids,
    expert_ids,
    gain_attn,
    w_query,
    w_key_value,
    w_output,
    gain_moe,
    w_router,
    w_expert_in,
    w_expert_out,
):
    rows, cols, depth = sizes
    group = rows * cols
    tok_rows, feat_local = tokens.shape
    width = w_query.shape[0]
    experts = w_router.shape[1]
    expert_local, hidden = w_expert_out.shape[0], w_expert_out.shape[1]
    longest_doc = min(LONGEST, tok_rows * depth // 2)
    hop_count = longest_doc // tok_rows
    own = tok_rows // group
    low, full = jnp.bfloat16, jnp.float32
    layer = lax.axis_index("dp")
    me = lax.axis_index("row") * cols + lax.axis_index("col")
    everyone = list(range(1, depth))
    hops = list(range(1, hop_count + 1))

    scaled_grad = (RESIDUAL_SCALE * out_grad.astype(full)).astype(low)
    grads_all = lax.all_gather(scaled_grad.T, EVERY, axis=0, tiled=False)
    grads_all = grads_all.reshape(depth, width, tok_rows)

    gain_pad = jnp.pad(jnp.stack([gain_attn, gain_moe]), ((0, 14), (0, 0)))
    router_pad = jnp.pad(w_router, ((0, 0), (0, LANES - experts)))
    tokens_blocks, gain_blocks, router_blocks, docs_far = exchange(
        sizes,
        "gather_tokens",
        0,
        ("gather", tokens),
        ("gather", gain_pad),
        ("gather", router_pad),
        ("shift", doc_ids.reshape(-1, LANES), everyone, False),
    )
    gains = jnp.moveaxis(gain_blocks[:, :8].astype(full), 0, 1).reshape(8, width)
    router = router_blocks.reshape(width, LANES)

    half = LANES // 4
    frequencies = ROPE_BASE ** (-(1.0 / half) * jnp.arange(half, dtype=full))
    positions = (layer * tok_rows + jnp.arange(tok_rows, dtype=jnp.int32)).astype(full)
    angles = positions[:, None] * frequencies[None, :]
    cosine = jnp.tile(jnp.cos(angles), (1, 4))
    sines = jnp.sin(angles)
    sine = jnp.concatenate([-sines, sines, -sines, sines], axis=1)

    w_pair = w_key_value.reshape(width, -1)
    block = (tok_rows, LANES)
    normed, query, pair, tokens_own = call(
        project_body,
        "project",
        [((tok_rows, width), low), (block, low), (block, low), ((own, width), low)],
        tokens_blocks,
        gains,
        w_query,
        w_pair,
        cosine,
        sine,
    )
    far, output_blocks = exchange(
        sizes, "shift_pairs", 1, ("shift", pair, hops, False), ("gather", w_output)
    )
    output_full = output_blocks.reshape(-1, width)

    before = jnp.concatenate([docs_far[d - 1].reshape(-1) for d in reversed(hops)])
    absent = jnp.repeat(jnp.array(hops[::-1], jnp.int32), tok_rows) > layer
    before = jnp.concatenate([jnp.where(absent, -1, before), doc_ids])
    start = jnp.sum((before[None, :] < doc_ids[:, None]).astype(jnp.int32), axis=1, keepdims=True)

    stack = (hop_count + 1,) + block
    twice = (2 * tok_rows, LANES)
    mixed, log_total = call(
        attend_body,
        "attend",
        [(block, low), ((2 * tok_rows, 1), full)],
        query,
        pair,
        far,
        start,
        scratch=[
            pltpu.VMEM(stack, low),
            pltpu.VMEM(stack, low),
            pltpu.VMEM(twice, low),
            pltpu.VMEM(twice, full),
        ],
    )
    mixed_own, grad_own = exchange(
        sizes,
        "swap_mixed",
        2,
        ("swap", mixed.reshape(group, own, LANES)),
        ("swap", out_grad.reshape(group, own, LANES)),
    )
    rows_own, middle, weights = call(
        functools.partial(middle_body, experts),
        "middle",
        [((own, width + LANES), low), ((own, width), full), ((own, LANES), full)],
        mixed_own,
        tokens_own,
        output_full,
        gains,
        router,
        expert_ids,
    )
    rows_blocks, rows_shifted = exchange(
        sizes, "gather_rows", 3, ("gather", rows_own), ("shift", rows_own, everyone, False)
    )
    rows_near = rows_blocks.reshape(tok_rows, -1)
    parts = hidden // LANES
    in_rows = w_expert_in.reshape(expert_local, width, 2, parts, LANES)
    in_rows = in_rows.transpose(0, 1, 3, 2, 4).reshape(expert_local, -1, LANES)
    moe_partial, back_partial, in_flat, rows_far = local_experts(
        sizes, 9, rows_near, grads_all, in_rows, w_expert_out, rows_shifted
    )
    (back_blocks,) = exchange(
        sizes, "swap_back", 4, ("swap", back_partial.reshape(group, own, -1))
    )
    middle_grad, attn_grad, logit_grad, gain_moe_part = call(
        middle_back_body,
        "middle_back",
        [
            ((own, width), full),
            ((own, width), low),
            ((own, LANES), low),
            ((1, width), full),
        ],
        back_blocks,
        grad_own,
        middle,
        weights,
        gains,
        router,
    )
    attn_grad_blocks, logit_blocks = exchange(
        sizes, "gather_attn_grad", 5, ("gather", attn_grad), ("gather", logit_grad)
    )
    query_grad, pair_grad, far_grad, output_sum = call(
        attend_back_body,
        "attend_back",
        [(block, low), (block, full), ((hop_count,) + block, low), ((LANES, width), low)],
        attn_grad_blocks.reshape(tok_rows, width),
        w_output,
        query,
        pair,
        far,
        start,
        log_total,
        mixed,
        cosine,
        sine,
        scratch=[
            pltpu.VMEM(stack, low),
            pltpu.VMEM(stack, low),
            pltpu.VMEM(twice, low),
            pltpu.VMEM(twice, low),
            pltpu.VMEM(twice, full),
            pltpu.VMEM(stack, full),
            pltpu.VMEM(stack, full),
        ],
    )
    returned, moe_blocks = exchange(
        sizes,
        "shift_grads",
        6,
        ("shift", far_grad, [-d for d in hops], True),
        ("swap", moe_partial.reshape(group, own, width)),
    )
    partial, query_sum, pair_sum = call(
        project_back_body,
        "project_back",
        [((tok_rows, width), low), ((width, LANES), low), ((width, LANES), low)],
        query_grad,
        pair_grad,
        returned,
        normed,
        w_query,
        w_pair,
        cosine,
        sine,
    )
    rows_mine = lax.dynamic_slice_in_dim(rows_near, me * feat_local, feat_local, 1)
    router_sum = dot(logit_blocks.reshape(tok_rows, LANES), rows_mine, 0, 0)[:experts].astype(low)
    query_sum = jnp.concatenate([query_sum, router_sum], axis=0)
    sums = lax.psum((query_sum, pair_sum, output_sum), "dp")
    (partial_blocks,) = exchange(
        sizes, "swap_partial", 7, ("swap", partial.reshape(group, own, width))
    )
    pieces = (group, own, LANES)
    block_out, in_grad, gain_parts = call(
        results_body,
        "results",
        [(pieces, low), (pieces, low), ((group, 8, LANES), full)],
        partial_blocks,
        moe_blocks,
        tokens_own,
        middle,
        middle_grad,
        gains,
        gain_moe_part,
    )
    block_out, in_grad, gain_all = exchange(
        sizes,
        "swap_results",
        8,
        ("swap", block_out),
        ("swap", in_grad),
        ("spread", gain_parts),
    )
    gain_sums = jnp.sum(gain_all, axis=0)
    grad_query, grad_key_value, grad_output = [s.astype(full) for s in sums]
    grad_query, grad_router = grad_query[:width], grad_query[width:]
    grad_expert_in, grad_expert_out = expert_grads(
        rows_near, rows_far.reshape(depth - 1, tok_rows, -1), grads_all, in_flat, w_expert_out
    )
    return (
        block_out.reshape(tok_rows, feat_local),
        in_grad.reshape(tok_rows, feat_local),
        gain_sums[0],
        grad_query,
        grad_key_value.reshape(w_key_value.shape),
        grad_output,
        gain_sums[1],
        grad_router.T,
        grad_expert_in,
        grad_expert_out,
    )


def solution(mesh):
    in_specs = (
        P("dp", ("row", "col")),
        P("dp", ("row", "col")),
        P("dp"),
        P("dp", None),
        P(("row", "col")),
        P(None, ("row", "col")),
        P(None, ("row", "col"), None),
        P(("row", "col"), None),
        P(("row", "col")),
        P(("row", "col"), None),
        P("row", None, None, "col"),
        P("row", "col", None),
    )
    out_specs = (
        P("dp", ("row", "col")),
        P("dp", ("row", "col")),
        P(("row", "col")),
        P(None, ("row", "col")),
        P(None, ("row", "col"), None),
        P(("row", "col"), None),
        P(("row", "col")),
        P(("row", "col"), None),
        P("row", None, None, "col"),
        P("row", "col", None),
    )
    sizes = (mesh.shape["row"], mesh.shape["col"], mesh.shape["dp"])
    return jax.shard_map(
        functools.partial(local, sizes),
        mesh=mesh,
        in_specs=in_specs,
        out_specs=out_specs,
        check_vma=False,
    )
```

```python
import functools

import jax
import jax.numpy as jnp
from jax import lax
from jax.experimental import pallas as pl
from jax.experimental.pallas import tpu as pltpu
from jax.sharding import PartitionSpec as P

LONGEST = 4096
HIGH = lax.Precision.HIGHEST
EPSILON = 1e-05
RESIDUAL_SCALE = 0.22
SCORE_SCALE = 0.015625
ROPE_BASE = 10000.0
MASKED = -1e30
MESH = pl.DeviceIdType.MESH
GROUP = ("row", "col")
EVERY = ("dp", "row", "col")
LANES = 128
HBM = pl.BlockSpec(memory_space=pl.ANY)
FULL = pl.BlockSpec(memory_space=pltpu.VMEM)
TURN = LANES // 4


class Moves:
    def __init__(self, sizes, kinds, sources, targets, sems):
        self.sizes, self.kinds = sizes, kinds
        self.sources, self.targets = sources, targets
        self.send_sem, self.recv_sem, self.local_sem = sems

    def place(self):
        row, col, layer = lax.axis_index("row"), lax.axis_index("col"), lax.axis_index("dp")
        return row, col, layer, row * self.sizes[1] + col

    def member(self, index):
        rows, cols, depth = self.sizes
        return {"row": index // cols, "col": lax.rem(index, cols)}

    def barrier(self):
        rows, cols, depth = self.sizes
        row, col, layer, me = self.place()
        group = rows * cols
        names = [kind[0] for kind in self.kinds]
        barrier = pltpu.get_barrier_semaphore()
        partners = []
        if "spread" in names:
            for k in range(1, group * depth):
                other = lax.rem(layer * group + me + k, group * depth)
                partners.append({"dp": other // group, **self.member(lax.rem(other, group))})
        elif "swap" in names:
            for k in range(1, group):
                partners.append(self.member(lax.rem(me + k, group)))
        elif "gather" in names:
            for k in range(1, rows):
                partners.append({"row": lax.rem(row + k, rows)})
            for k in range(1, cols):
                partners.append({"col": lax.rem(col + k, cols)})
        shifts = set()
        for kind in self.kinds:
            if kind[0] == "shift":
                for d in kind[1]:
                    shifts |= {d % depth, -d % depth}
            elif kind[0] in ("turn", "collect"):
                shifts |= set(range(1, depth))
        if "spread" not in names:
            for k in sorted(shifts - {0}):
                partners.append({"dp": lax.rem(layer + k, depth)})
        for partner in partners:
            pl.semaphore_signal(barrier, inc=1, device_id=partner, device_id_type=MESH)
        pl.semaphore_wait(barrier, len(partners))

    def copies(self, only):
        rows, cols, depth = self.sizes
        row, col, layer, me = self.place()
        group = rows * cols
        slot = 0
        lists = []

        def remote(source, target, device):
            nonlocal slot
            slot += 1
            return functools.partial(
                pltpu.make_async_remote_copy,
                src_ref=source,
                dst_ref=target,
                send_sem=self.send_sem.at[slot - 1],
                recv_sem=self.recv_sem.at[slot - 1],
                device_id=device,
                device_id_type=MESH,
            )

        for index, (kind, source, target) in enumerate(
            zip(self.kinds, self.sources, self.targets)
        ):
            direct, relayed, local = [], [], []

            def keep(source, target):
                sem = self.local_sem.at[index]
                local.append(functools.partial(pltpu.make_async_copy, source, target, sem))

            if kind[0] == "gather":
                at = (lambda i: target.at[:, i]) if kind[1] else (lambda i: target.at[i])
                for k in range(1, rows):
                    copy = remote(source, at(me), {"row": lax.rem(row + k, rows)})
                    piece = at(lax.rem(row + rows - k, rows) * cols + col)
                    nexts = [
                        remote(piece, piece, {"col": lax.rem(col + j, cols)})
                        for j in range(1, cols)
                    ]
                    relayed.append((copy, nexts))
                for k in range(1, cols):
                    direct.append(remote(source, at(me), {"col": lax.rem(col + k, cols)}))
                keep(source, at(me))
            elif kind[0] == "swap":
                for k in range(1, group):
                    other = lax.rem(me + k, group)
                    direct.append(remote(source.at[other], target.at[me], self.member(other)))
                keep(source.at[me], target.at[me])
            elif kind[0] == "spread":
                mine = layer * group + me
                for k in range(1, group * depth):
                    other = lax.rem(mine + k, group * depth)
                    block = lax.rem(other, group)
                    device = {"dp": other // group, **self.member(block)}
                    direct.append(remote(source.at[block], target.at[mine], device))
                keep(source.at[me], target.at[mine])
            elif kind[0] in ("turn", "collect"):
                for k in range(1, depth):
                    other = lax.rem(layer + k, depth)
                    piece = source.at[other] if kind[0] == "turn" else source
                    direct.append(remote(piece, target.at[layer], {"dp": other}))
                keep(source.at[layer] if kind[0] == "turn" else source, target.at[layer])
            else:
                for at, d in enumerate(kind[1]):
                    piece = source.at[at] if kind[2] else source
                    device = {"dp": lax.rem(layer + d % depth, depth)}
                    direct.append(remote(piece, target.at[at], device))
            if only is None or index in only:
                lists.append((direct, relayed, local))
        return tuple(sum((part[i] for part in lists), []) for i in range(3))

    def start(self, only=None):
        direct, relayed, local = self.copies(only)
        for copy, _ in relayed:
            copy().start()
        for copy in direct + local:
            copy().start()

    def relay(self, only=None):
        for copy, nexts in self.copies(only)[1]:
            copy().wait_recv()
            for follower in nexts:
                follower().start()

    def finish(self, only=None):
        direct, relayed, local = self.copies(only)
        for copy, nexts in relayed:
            copy().wait_send()
            for follower in nexts:
                follower().wait()
        for copy in direct + local:
            copy().wait()


def planned(sizes, items):
    rows, cols, depth = sizes
    group = rows * cols
    kinds, shapes, copies = [], [], 0
    for item in items:
        name, array = item[0], item[1]
        shape = array.shape
        if name == "gather":
            second = len(item) > 2 and item[2]
            kinds.append((name, second))
            shape = (shape[0], group) + shape[1:] if second else (group,) + shape
            copies += (rows - 1) * cols + cols - 1
        elif name == "shift":
            distances, split = item[2], item[3]
            kinds.append((name, tuple(distances), split))
            shape = (len(distances),) + (shape[1:] if split else shape)
            copies += len(distances)
        else:
            kinds.append((name,))
            if name == "spread":
                shape = (group * depth,) + shape[1:]
            elif name == "collect":
                shape = (depth,) + shape
            copies += {"swap": group, "spread": group * depth}.get(name, depth) - 1
        shapes.append(jax.ShapeDtypeStruct(shape, array.dtype))
    sems = [
        pltpu.SemaphoreType.DMA((copies,)),
        pltpu.SemaphoreType.DMA((copies,)),
        pltpu.SemaphoreType.DMA((len(items),)),
    ]
    return tuple(kinds), shapes, sems


def exchange_body(sizes, kinds, *refs):
    count = len(kinds)
    moves = Moves(sizes, kinds, refs[:count], refs[count : 2 * count], refs[2 * count :])
    moves.barrier()
    moves.start()
    moves.relay()
    moves.finish()


def exchange(sizes, name, number, *items):
    kinds, shapes, sems = planned(sizes, items)
    return pl.pallas_call(
        functools.partial(exchange_body, sizes, kinds),
        out_shape=tuple(shapes),
        in_specs=[HBM] * len(items),
        out_specs=(HBM,) * len(items),
        scratch_shapes=sems,
        compiler_params=pltpu.CompilerParams(collective_id=number, has_side_effects=True),
        name=name,
    )(*[item[1] for item in items])


def dot(a, b, left=1, right=0, precision=None):
    return lax.dot_general(
        a,
        b,
        (((left,), (right,)), ((), ())),
        preferred_element_type=jnp.float32,
        precision=precision,
    )


def call(body, name, shapes, *arrays, scratch=()):
    return pl.pallas_call(
        body,
        out_shape=tuple(jax.ShapeDtypeStruct(*shape) for shape in shapes),
        in_specs=[FULL] * len(arrays),
        out_specs=(FULL,) * len(shapes),
        scratch_shapes=list(scratch),
        name=name,
    )(*arrays)


def hosted(body, name, shapes, *arrays, scratch=(), sizes, number, items):
    kinds, moved, sems = planned(sizes, items)
    ins, count, outs = len(arrays), len(items), len(shapes)

    def whole(*refs):
        sources = refs[ins : ins + count]
        made = refs[ins + count : ins + count + outs]
        targets = refs[ins + count + outs : ins + 2 * count + outs]
        rest = refs[ins + 2 * count + outs :]
        moves = Moves(sizes, kinds, sources, targets, rest[len(scratch) :])
        moves.barrier()
        moves.start()
        body(*refs[:ins], *made, *rest[: len(scratch)])
        moves.relay()
        moves.finish()

    return pl.pallas_call(
        whole,
        out_shape=tuple(jax.ShapeDtypeStruct(*shape) for shape in shapes) + tuple(moved),
        in_specs=[FULL] * ins + [HBM] * count,
        out_specs=(FULL,) * outs + (HBM,) * count,
        scratch_shapes=list(scratch) + sems,
        compiler_params=pltpu.CompilerParams(collective_id=number, has_side_effects=True),
        name=name,
    )(*arrays, *[item[1] for item in items])


def lanes_of(shape):
    return lax.broadcasted_iota(jnp.int32, shape, len(shape) - 1)


def flipped(values):
    lanes = lanes_of(values.shape)
    ahead = pltpu.roll(values, LANES - TURN, 1)
    behind = pltpu.roll(values, TURN, 1)
    return jnp.where(lanes % (2 * TURN) < TURN, ahead, behind)


def beside(blocks_ref):
    return jnp.concatenate([blocks_ref[i] for i in range(blocks_ref.shape[0])], axis=1)


def gain_row(gains_ref, which):
    return beside(gains_ref).astype(jnp.float32)[which : which + 1, :]


def own_rows(count):
    me = lax.axis_index("row") * lax.axis_size("col") + lax.axis_index("col")
    return pl.ds(pl.multiple_of(me * count, count), count)


def column(row):
    return jnp.broadcast_to(row, (8, row.shape[1])).T[:, 0:1]


def project_body(blocks, gains, w_query, w_pair, cosine, sine, near, far, normed, query, pair, own, near_turned, far_turned):
    tokens = beside(blocks).astype(jnp.float32)
    scale = lax.rsqrt(jnp.mean(tokens * tokens, axis=1, keepdims=True) + EPSILON)
    normed[...] = (tokens * scale * gain_row(gains, 0)).astype(jnp.bfloat16)
    raw = dot(normed[...], w_query[...])
    query[...] = (raw * cosine[...] + flipped(raw) * sine[...]).astype(jnp.bfloat16)
    raw = dot(normed[...], w_pair[...])
    keys = lanes_of(raw.shape) < LANES // 2
    turned = raw * cosine[...] + flipped(raw) * sine[...]
    pair[...] = jnp.where(keys, turned, raw).astype(jnp.bfloat16)
    for i in range(blocks.shape[0]):
        own[:, i * LANES : (i + 1) * LANES] = blocks[i, own_rows(own.shape[0]), :]
    near_turned[...] = (RESIDUAL_SCALE * near[...].astype(jnp.float32)).T.astype(jnp.bfloat16)
    for i in range(far.shape[0]):
        far_turned[i] = (RESIDUAL_SCALE * far[i].astype(jnp.float32)).T.astype(jnp.bfloat16)


def doubled(pair, keys_ref, values_ref, at):
    wide = pair.astype(jnp.float32)
    other = pltpu.roll(wide, LANES // 2, 1)
    keys = lanes_of(wide.shape) < LANES // 2
    keys_ref[at] = jnp.where(keys, wide, other).astype(jnp.bfloat16)
    values_ref[at] = jnp.where(keys, other, wide).astype(jnp.bfloat16)


def per_head(values):
    first = lanes_of(values.shape) < LANES // 2
    zero = jnp.zeros_like(values)
    return jnp.concatenate(
        [jnp.where(first, values, zero), jnp.where(first, zero, values)], axis=0
    )


def tile_scores(queries, keys_ref, starts, row, block, last, tokens):
    scores = dot(queries, keys_ref[block], 1, 1) * SCORE_SCALE
    at = lanes_of(scores.shape) + block * tokens
    allowed = at >= starts
    if block == last:
        place = row + lax.broadcasted_iota(jnp.int32, scores.shape, 0)
        allowed = allowed & (at <= place + block * tokens)
    return jnp.where(allowed, scores, MASKED)


def doc_row(docs):
    rows = [docs[i : i + 1, :] for i in range(docs.shape[0])]
    return jnp.concatenate(rows, axis=1).astype(jnp.float32)


def attend_body(query, pair, far, docs, far_docs, mixed, log_total, start, keys, values, queries, out):
    tokens = query.shape[0]
    last = far.shape[0]
    layer = lax.axis_index("dp")
    here = doc_row(docs[...])
    mine = column(here)
    before = jnp.sum((here < mine).astype(jnp.float32), axis=1, keepdims=True)
    for d in range(1, last + 1):
        fewer = (doc_row(far_docs[d - 1]) < mine) | (layer < d)
        before = before + jnp.sum(fewer.astype(jnp.float32), axis=1, keepdims=True)
    start[...] = before.astype(jnp.int32)
    doubled(pair[...], keys, values, last)
    for d in range(1, last + 1):
        doubled(far[d - 1], keys, values, last - d)
    queries[...] = per_head(query[...].astype(jnp.float32)).astype(jnp.bfloat16)
    step = 256

    def tile(i, carry):
        rows = pl.ds(pl.multiple_of(i * step, step), step)
        row = lax.rem(i * step, tokens)
        starts = start[pl.ds(pl.multiple_of(row, step), step), :]
        parts = [
            tile_scores(queries[rows, :], keys, starts, row, block, last, tokens)
            for block in range(last + 1)
        ]
        top = functools.reduce(
            jnp.maximum, [jnp.max(part, axis=1, keepdims=True) for part in parts]
        )
        parts = [jnp.exp(part - top) for part in parts]
        total = functools.reduce(jnp.add, [jnp.sum(p, axis=1, keepdims=True) for p in parts])
        sums = [
            dot(part.astype(jnp.bfloat16), values[block]) for block, part in enumerate(parts)
        ]
        out[rows, :] = functools.reduce(jnp.add, sums) / total
        log_total[rows, :] = top + jnp.log(total)
        return carry

    lax.fori_loop(0, 2 * tokens // step, tile, 0)
    first = lanes_of((tokens, LANES)) < LANES // 2
    mixed[...] = jnp.where(first, out[:tokens, :], out[tokens:, :]).astype(jnp.bfloat16)


def attend_back_body(grad, w_output, query, pair, far, start, log_total, mixed, cosine, sine, query_grad, pair_grad, far_grad, output_grad, keys, values, queries, grads, turned, key_sums, value_sums):
    tokens = query.shape[0]
    last = far.shape[0]
    doubled(pair[...], keys, values, last)
    for d in range(1, last + 1):
        doubled(far[d - 1], keys, values, last - d)
    queries[...] = per_head(query[...].astype(jnp.float32)).astype(jnp.bfloat16)
    grads[...] = per_head(dot(grad[...], w_output[...], 1, 1)).astype(jnp.bfloat16)
    output_sum = dot(mixed[...], grad[...], 0, 0).astype(jnp.bfloat16)
    for i in range(output_grad.shape[0]):
        output_grad[i] = output_sum[:, i * LANES : (i + 1) * LANES]
    key_sums[...] = jnp.zeros_like(key_sums)
    value_sums[...] = jnp.zeros_like(value_sums)
    step = 256

    def tile(i, carry):
        rows = pl.ds(pl.multiple_of(i * step, step), step)
        row = lax.rem(i * step, tokens)
        starts = start[pl.ds(pl.multiple_of(row, step), step), :]
        asked, given, level = queries[rows, :], grads[rows, :], log_total[rows, :]
        chances, products = [], []
        for block in range(last + 1):
            scores = tile_scores(asked, keys, starts, row, block, last, tokens)
            chances.append(jnp.exp(scores - level))
            products.append(dot(given, values[block], 1, 1))
        delta = functools.reduce(
            jnp.add,
            [jnp.sum(p * q, axis=1, keepdims=True) for p, q in zip(chances, products)],
        )
        total = jnp.zeros((step, LANES), jnp.float32)
        for block in range(last + 1):
            back = (chances[block] * (products[block] - delta)).astype(jnp.bfloat16)
            total = total + dot(back, keys[block])
            key_sums[block] += dot(back, asked, 0, 0)
            value_sums[block] += dot(chances[block].astype(jnp.bfloat16), given, 0, 0)
        turned[rows, :] = total
        return carry

    lax.fori_loop(0, 2 * tokens // step, tile, 0)
    first = lanes_of((tokens, LANES)) < LANES // 2
    raw = jnp.where(first, turned[:tokens, :], turned[tokens:, :]) * SCORE_SCALE
    query_grad[...] = (raw * cosine[...] - flipped(raw) * sine[...]).astype(jnp.bfloat16)

    def joined(block):
        by_key, by_value = key_sums[block], value_sums[block]
        by_key = (by_key + pltpu.roll(by_key, LANES // 2, 1)) * SCORE_SCALE
        by_value = by_value + pltpu.roll(by_value, LANES // 2, 1)
        return jnp.where(first, by_key, by_value)

    pair_grad[...] = joined(last)
    for d in range(1, last + 1):
        far_grad[d - 1] = joined(last - d).astype(jnp.bfloat16)


def router_rows(router):
    rows = beside(router).astype(jnp.float32)
    blank = jnp.zeros((LANES - rows.shape[0], rows.shape[1]), jnp.float32)
    return jnp.concatenate([rows, blank], axis=0)


def middle_body(mixed, own, w_output, gains, router, ids_turned, rows, middle, weights, ids_ref):
    experts = router.shape[1]
    width = own.shape[1]
    attn = dot(beside(mixed), w_output[...])
    value = own[...].astype(jnp.float32) + RESIDUAL_SCALE * attn
    middle[...] = value
    scale = lax.rsqrt(jnp.mean(value * value, axis=1, keepdims=True) + EPSILON)
    normed = value * scale * gain_row(gains, 1)
    logits = dot(normed, router_rows(router), 1, 1, precision=HIGH)
    count = own.shape[0]
    ids_ref[...] = ids_turned[...].astype(jnp.float32).T
    ids = ids_ref[own_rows(count), :]
    lanes = lanes_of((count, LANES))
    chosen = jnp.zeros((count, LANES), jnp.float32)
    for k in range(ids.shape[1]):
        chosen = chosen + (ids[:, k : k + 1] == lanes.astype(jnp.float32)).astype(
            jnp.float32
        )
    top = jnp.max(jnp.where(lanes < experts, logits, MASKED), axis=1, keepdims=True)
    terms = jnp.exp(jnp.minimum(logits - top, 0.0)) * chosen
    share = terms / jnp.sum(terms, axis=1, keepdims=True)
    weights[...] = share
    high = share.astype(jnp.bfloat16)
    low = share - high.astype(jnp.float32)
    rows[:, :width] = normed.astype(jnp.bfloat16)
    rows[:, width:] = (high.astype(jnp.float32) + pltpu.roll(low, LANES // 2, 1)).astype(
        jnp.bfloat16
    )


def middle_back_body(back, out_grad, middle, weights, gains, router, middle_grad, attn_grad, logit_grad, gain_part):
    width = middle.shape[1]
    normed_grad = back[0, :, :width].astype(jnp.float32)
    weight_grad = back[0, :, width:].astype(jnp.float32)
    for i in range(1, back.shape[0]):
        normed_grad = normed_grad + back[i, :, :width].astype(jnp.float32)
        weight_grad = weight_grad + back[i, :, width:].astype(jnp.float32)
    share, value = weights[...], middle[...]
    mean = jnp.sum(share * weight_grad, axis=1, keepdims=True)
    logit = share * (weight_grad - mean)
    logit_grad[...] = logit.astype(jnp.bfloat16)
    normed_grad = normed_grad + dot(logit, router_rows(router), precision=HIGH)
    scale = lax.rsqrt(jnp.mean(value * value, axis=1, keepdims=True) + EPSILON)
    gain_part[...] = jnp.sum(normed_grad * value * scale, axis=0, keepdims=True)
    scaled = normed_grad * gain_row(gains, 1)
    norm_dot = jnp.sum(scaled * value, axis=1, keepdims=True)
    total = (
        beside(out_grad).astype(jnp.float32)
        + scale * scaled
        - value * (scale * scale * scale * norm_dot / width)
    )
    middle_grad[...] = total
    attn_grad[...] = (RESIDUAL_SCALE * total).astype(jnp.bfloat16)


def project_back_body(query_grad, pair_grad, returned, normed, w_query, w_pair, cosine, sine, output_sum, logit, rows, partial, sums):
    layer = lax.axis_index("dp")
    depth = lax.axis_size("dp")
    total = pair_grad[...]
    for i in range(returned.shape[0]):
        total = total + jnp.where(
            layer + i + 1 < depth, returned[i].astype(jnp.float32), 0.0
        )
    keys = lanes_of(total.shape) < LANES // 2
    turned = total * cosine[...] - flipped(total) * sine[...]
    pair_low = jnp.where(keys, turned, total).astype(jnp.bfloat16)
    query_low = query_grad[...]
    partial[...] = (
        dot(query_low, w_query[...], 1, 1) + dot(pair_low, w_pair[...], 1, 1)
    ).astype(jnp.bfloat16)
    width = normed.shape[1]
    sums[:width, :] = dot(normed[...], query_low, 0, 0).astype(jnp.bfloat16)
    sums[width : 2 * width, :] = dot(normed[...], pair_low, 0, 0).astype(jnp.bfloat16)
    sums[2 * width : 3 * width, :] = output_sum[...].reshape(width, LANES)
    mine = rows[:, own_rows(LANES)]
    sums[3 * width : 3 * width + LANES, :] = dot(logit[...], mine, 0, 0).astype(jnp.bfloat16)


def results_body(blocks, moe, own, middle, middle_grad, gains, gain_moe, turned, block_out, in_grad, gain_parts, summed):
    summed[...] = functools.reduce(
        jnp.add, [turned[i].astype(jnp.float32) for i in range(turned.shape[0])]
    ).astype(jnp.bfloat16)
    width = own.shape[1]
    normed_grad = blocks[0].astype(jnp.float32)
    branch = moe[0].astype(jnp.float32)
    for i in range(1, blocks.shape[0]):
        normed_grad = normed_grad + blocks[i].astype(jnp.float32)
        branch = branch + moe[i].astype(jnp.float32)
    value = own[...].astype(jnp.float32)
    scale = lax.rsqrt(jnp.mean(value * value, axis=1, keepdims=True) + EPSILON)
    gain_attn = jnp.sum(normed_grad * value * scale, axis=0, keepdims=True)
    scaled = normed_grad * gain_row(gains, 0)
    norm_dot = jnp.sum(scaled * value, axis=1, keepdims=True)
    grad = (
        middle_grad[...] + scale * scaled - value * (scale * scale * scale * norm_dot / width)
    ).astype(jnp.bfloat16)
    out = (middle[...] + RESIDUAL_SCALE * branch).astype(jnp.bfloat16)
    gain_parts[...] = jnp.zeros_like(gain_parts)
    for i in range(block_out.shape[0]):
        at = slice(i * LANES, (i + 1) * LANES)
        block_out[i] = out[:, at]
        in_grad[i] = grad[:, at]
        gain_parts[i, 0:1, :] = gain_attn[:, at]
        gain_parts[i, 1:2, :] = gain_moe[0:1, at]


def expert_terms(gate_up, active_grad, weight):
    hidden = active_grad.shape[0]
    gate, up = gate_up[:hidden], gate_up[hidden:]
    sigmoid = jax.nn.sigmoid(gate)
    silu = gate * sigmoid
    ungated = silu * up
    active = (ungated * weight).astype(jnp.bfloat16)
    scaled = active_grad * weight
    gate_grad = (scaled * up * sigmoid * (1.0 + gate * (1.0 - sigmoid))).astype(jnp.bfloat16)
    up_grad = (scaled * silu).astype(jnp.bfloat16)
    return active, jnp.concatenate([gate_grad, up_grad], axis=0), active_grad * ungated


def weight_rows(extra):
    turned = extra.astype(jnp.float32).T
    return turned[: LANES // 2] + turned[LANES // 2 :]


def local_experts_body(sizes, kinds, rows_ref, grads_ref, in_ref, out_ref, sent_grads, sent_rows, moe_ref, back_ref, flat_ref, in_sum, out_sum, got_grads, got_rows, moe_acc, back_acc, share, weights, spread, *sems):
    step, steps = pl.program_id(0), pl.num_programs(0)
    each, hidden, width = out_ref.shape
    parts = hidden // LANES
    moves = Moves(sizes, kinds, [sent_grads, sent_rows], [got_grads, got_rows], sems)

    @pl.when(step == 0)
    def _():
        moves.barrier()
        moves.start([0])
        moe_acc[...] = jnp.zeros_like(moe_acc)
        back_acc[...] = jnp.zeros_like(back_acc)
        share[...] = jnp.zeros_like(share)
        weights[...] = weight_rows(rows_ref[:, width:])

    @pl.when(step == steps // 2)
    def _():
        moves.start([1])

    @pl.when(step == steps - 1)
    def _():
        moves.relay([0])

    for i in range(each):
        spread[i] = in_ref[i].astype(jnp.float32)
        for part in range(parts):
            for half in range(2):
                at = half * hidden + part * LANES
                flat_ref[i, :, at : at + LANES] = spread[
                    i, pl.ds(part * 2 + half, width, stride=2 * parts), :
                ].astype(jnp.bfloat16)
        expert = (lax.axis_index("row") * steps + step) * each + i
        active, gate_up_grad, shares = expert_terms(
            dot(flat_ref[i], rows_ref[:, :width], 0, 1),
            dot(out_ref[i], grads_ref[...]),
            weights[pl.ds(expert, 1), :],
        )
        share[pl.ds(expert, 1), :] = jnp.sum(shares, axis=0, keepdims=True)
        moe_acc[...] += dot(active, out_ref[i], 0, 0)
        back_acc[...] += dot(gate_up_grad, flat_ref[i], 0, 1)
        in_sum[i] = dot(gate_up_grad, rows_ref[:, :width]).astype(jnp.bfloat16)
        out_sum[i] = dot(active, grads_ref[...], 1, 1).astype(jnp.bfloat16)

    @pl.when(step == steps - 1)
    def _():
        moe_ref[...] = moe_acc[...].astype(jnp.bfloat16)
        back_ref[:, :width] = back_acc[...].astype(jnp.bfloat16)
        back_ref[:, width:] = share[...].T.astype(jnp.bfloat16)
        moves.relay([1])
        moves.finish()


def local_experts(sizes, number, rows, grads, w_in, w_out, sent_grads, sent_rows):
    tokens, wide = rows.shape
    experts, hidden, width = w_out.shape
    each = 2
    low = jnp.bfloat16
    kinds, shapes, sems = planned(
        sizes, [("gather", sent_grads, True), ("gather", sent_rows, True)]
    )
    whole = lambda s: pl.BlockSpec(s, lambda e: (0,) * len(s))
    some = lambda s: pl.BlockSpec((each,) + s[1:], lambda e: (e,) + (0,) * (len(s) - 1))
    outs = [
        (tokens, width),
        (tokens, wide),
        (experts, width, 2 * hidden),
        (experts, 2 * hidden, width),
        (experts, hidden, width),
    ]
    return pl.pallas_call(
        functools.partial(local_experts_body, sizes, kinds),
        grid=(experts // each,),
        in_specs=[
            whole(rows.shape),
            whole(grads.shape),
            some(w_in.shape),
            some(w_out.shape),
            HBM,
            HBM,
        ],
        out_specs=(whole(outs[0]), whole(outs[1]), *[some(s) for s in outs[2:]], HBM, HBM),
        out_shape=tuple(jax.ShapeDtypeStruct(s, low) for s in outs) + tuple(shapes),
        scratch_shapes=[
            pltpu.VMEM((tokens, width), jnp.float32),
            pltpu.VMEM((tokens, width), jnp.float32),
            pltpu.VMEM((LANES, tokens), jnp.float32),
            pltpu.VMEM((LANES // 2, tokens), jnp.float32),
            pltpu.VMEM((each,) + w_in.shape[1:], jnp.float32),
        ]
        + sems,
        compiler_params=pltpu.CompilerParams(collective_id=number, has_side_effects=True),
        name="local_experts",
    )(rows, grads, w_in, w_out, sent_grads, sent_rows)


def cover_body(sizes, kinds, experts, first, in_ref, out_ref, in_part, out_part, rows_far, grads_far, *refs):
    count = len(kinds)
    sources, in_sum, out_sum = refs[:count], refs[count], refs[count + 1]
    targets = refs[count + 2 : 2 * count + 2]
    rows, grads, weights, load_sem, *rest = refs[2 * count + 2 :]
    sums, sems = rest[:-3], rest[-3:]
    step = pl.program_id(0)
    layers, width, tokens = grads.shape
    hidden = out_ref.shape[1]
    moves = Moves(sizes, kinds, sources, targets, sems)

    @pl.when(step == 0)
    def _():
        loads = [
            pltpu.make_async_copy(rows_far, rows, load_sem.at[0]),
            pltpu.make_async_copy(grads_far, grads, load_sem.at[1]),
        ]
        for load in loads:
            load.start()
        moves.barrier()
        moves.start()
        for load in loads:
            load.wait()
        for i in range(layers):
            weights[i] = weight_rows(rows[i * tokens : (i + 1) * tokens, width:])

    index = lax.axis_index("row") * experts + first + step

    def part_of(at, pieces):
        block = rows[pl.ds(pl.multiple_of(at * tokens, tokens), pieces * tokens), :width]
        weight = jnp.concatenate(
            [weights[at + i, pl.ds(index, 1), :] for i in range(pieces)], axis=1
        )
        active_grad = jnp.concatenate(
            [dot(out_ref[0], grads[at + i]) for i in range(pieces)], axis=1
        )
        active, gate_up_grad, _ = expert_terms(dot(in_ref[0], block, 0, 1), active_grad, weight)
        out_total = functools.reduce(
            jnp.add,
            [
                dot(active[:, i * tokens : (i + 1) * tokens], grads[at + i], 1, 1)
                for i in range(pieces)
            ],
        )
        return dot(gate_up_grad, block), out_total

    if not sums:
        in_total, out_total = part_of(0, layers)
    else:
        in_acc, out_acc = sums
        in_acc[...] = jnp.zeros_like(in_acc)
        out_acc[...] = jnp.zeros_like(out_acc)

        def more(i, carry):
            in_more, out_more = part_of(i, 1)
            in_acc[...] += in_more
            out_acc[...] += out_more
            return carry

        lax.fori_loop(0, layers, more, 0)
        in_total, out_total = in_acc[...], out_acc[...]
    in_sum[0] = (in_total + in_part[0].astype(jnp.float32)).astype(jnp.bfloat16)
    out_sum[0] = (out_total + out_part[0].astype(jnp.float32)).astype(jnp.bfloat16)

    @pl.when(step == pl.num_programs(0) - 1)
    def _():
        moves.relay()
        moves.finish()


def cover(sizes, name, number, first, count, work, *items):
    w_in, w_out, in_part, out_part, rows_far, grads_far = work
    layers, width, tokens = grads_far.shape
    experts, hidden, _ = w_out.shape
    kinds, shapes, sems = planned(sizes, items)
    each = lambda s: pl.BlockSpec((1,) + s[1:], lambda e: (first + e, 0, 0))
    out = lambda s: pl.BlockSpec((1,) + s[1:], lambda e: (e, 0, 0))
    outs = [(count, 2 * hidden, width), (count, hidden, width)]
    sums = [(2 * hidden, width), (hidden, width)] if layers > 4 else []
    return pl.pallas_call(
        functools.partial(cover_body, sizes, kinds, experts, first),
        grid=(count,),
        in_specs=[each(a.shape) for a in work[:4]] + [HBM] * (2 + len(items)),
        out_specs=tuple(out(s) for s in outs) + (HBM,) * len(items),
        out_shape=tuple(jax.ShapeDtypeStruct(s, jnp.bfloat16) for s in outs) + tuple(shapes),
        scratch_shapes=[
            pltpu.VMEM(rows_far.shape, jnp.bfloat16),
            pltpu.VMEM(grads_far.shape, jnp.bfloat16),
            pltpu.VMEM((layers, LANES // 2, tokens), jnp.float32),
            pltpu.SemaphoreType.DMA((2,)),
        ]
        + [pltpu.VMEM(s, jnp.float32) for s in sums]
        + sems,
        compiler_params=pltpu.CompilerParams(collective_id=number, has_side_effects=True),
        name=name,
    )(*work, *[item[1] for item in items])


def outputs_body(counts, *refs):
    pieces = len(counts)
    in_sums, out_sums = refs[:pieces], refs[pieces : 2 * pieces]
    blocks, in_blocks, gains, sums = refs[2 * pieces : 2 * pieces + 4]
    gin, gout, block_out, in_grad, gain_sum, query, pair, output, router = refs[2 * pieces + 4 :]
    step = pl.program_id(0)
    hidden, width = gout.shape[1:]
    parts = hidden // LANES

    @pl.when(step == 0)
    def _():
        for i in range(blocks.shape[0]):
            at = pl.ds(i * blocks.shape[1], blocks.shape[1])
            block_out[at, :] = blocks[i]
            in_grad[at, :] = in_blocks[i]
        gain_sum[...] = jnp.sum(gains[...], axis=0)
        query[...] = sums[:width, :].astype(jnp.float32)
        pair[...] = sums[width : 2 * width, :].astype(jnp.float32)
        for i in range(width // LANES):
            at = 2 * width + i * LANES
            output[:, i * LANES : (i + 1) * LANES] = sums[at : at + LANES, :].astype(jnp.float32)
        router[...] = sums[3 * width : 3 * width + router.shape[0], :].astype(jnp.float32)

    first = 0
    for count, in_sum, out_sum in zip(counts, in_sums, out_sums):

        @pl.when((step >= first) & (step < first + count))
        def _(in_sum=in_sum, out_sum=out_sum):
            gout[0] = out_sum[0].astype(jnp.float32)
            for part in range(parts):
                for half in range(2):
                    at = half * hidden + part * LANES
                    gin[0, pl.ds(part * 2 + half, width, stride=2 * parts), :] = (
                        in_sum[0, at : at + LANES, :].astype(jnp.float32).T
                    )

        first += count


def outputs(in_sums, out_sums, blocks, in_blocks, gains, sums, experts):
    counts = [s.shape[0] for s in in_sums]
    hidden, width = out_sums[0].shape[1:]
    parts = hidden // LANES
    group, own, lanes = blocks.shape
    tokens = group * own
    once = lambda s: pl.BlockSpec(s, lambda e: (0,) * len(s))
    each = lambda s: pl.BlockSpec((1,) + s[1:], lambda e: (e, 0, 0))
    specs = []
    for arrays in (in_sums, out_sums):
        first = 0
        for array in arrays:
            count = array.shape[0]
            specs.append(
                pl.BlockSpec(
                    (1,) + array.shape[1:],
                    lambda e, first=first, count=count: (jnp.clip(e - first, 0, count - 1), 0, 0),
                )
            )
            first += count
    total = sum(counts)
    full = jnp.float32
    shapes = [
        ((total, width * 2 * parts, LANES), full),
        ((total, hidden, width), full),
        ((tokens, lanes), jnp.bfloat16),
        ((tokens, lanes), jnp.bfloat16),
        (gains.shape[1:], full),
        ((width, LANES), full),
        ((width, LANES), full),
        ((LANES, width), full),
        ((experts, LANES), full),
    ]
    gin, *others = pl.pallas_call(
        functools.partial(outputs_body, counts),
        grid=(total,),
        in_specs=specs + [once(a.shape) for a in (blocks, in_blocks, gains, sums)],
        out_specs=(each(shapes[0][0]), each(shapes[1][0])) + tuple(once(s) for s, _ in shapes[2:]),
        out_shape=tuple(jax.ShapeDtypeStruct(*shape) for shape in shapes),
        name="outputs",
    )(*in_sums, *out_sums, blocks, in_blocks, gains, sums)
    gin = gin.reshape(total, width, parts, 2, LANES).transpose(0, 1, 3, 2, 4)
    return gin.reshape(total, width, 2, hidden), *others


def local(
    sizes,
    tokens,
    out_grad,
    doc_ids,
    expert_ids,
    gain_attn,
    w_query,
    w_key_value,
    w_output,
    gain_moe,
    w_router,
    w_expert_in,
    w_expert_out,
):
    rows, cols, depth = sizes
    group = rows * cols
    tok_rows, feat_local = tokens.shape
    width = w_query.shape[0]
    experts = w_router.shape[1]
    expert_local, hidden = w_expert_out.shape[0], w_expert_out.shape[1]
    longest_doc = min(LONGEST, tok_rows * depth // 2)
    hop_count = longest_doc // tok_rows
    own = tok_rows // group
    low, full = jnp.bfloat16, jnp.float32
    layer = lax.axis_index("dp")
    me = lax.axis_index("row") * cols + lax.axis_index("col")
    everyone = list(range(1, depth))
    hops = list(range(1, hop_count + 1))

    tokens_blocks, gains, router, docs_far, grads_shifted = exchange(
        sizes,
        "gather_tokens",
        0,
        ("gather", tokens),
        ("gather", jnp.stack([gain_attn, gain_moe])),
        ("gather", w_router.T),
        ("shift", doc_ids.reshape(-1, LANES), everyone, False),
        ("shift", out_grad, everyone, False),
    )

    lanes = jnp.arange(LANES, dtype=jnp.int32)
    frequencies = ROPE_BASE ** ((lanes % TURN).astype(full) * (-1.0 / TURN))
    positions = (layer * tok_rows + jnp.arange(tok_rows, dtype=jnp.int32)).astype(full)
    angles = positions[:, None] * frequencies[None, :]
    cosine = jnp.cos(angles)
    sine = jnp.sin(angles) * jnp.where(lanes % (2 * TURN) < TURN, -1.0, 1.0)[None, :]

    w_pair = w_key_value.reshape(width, -1)
    block = (tok_rows, LANES)
    turned = (LANES, tok_rows)
    normed, query, pair, tokens_own, near_turned, far_turned = call(
        project_body,
        "project",
        [
            ((tok_rows, width), low),
            (block, low),
            (block, low),
            ((own, width), low),
            (turned, low),
            ((depth - 1,) + turned, low),
        ],
        tokens_blocks,
        gains,
        w_query,
        w_pair,
        cosine,
        sine,
        out_grad,
        grads_shifted,
    )
    far, output_blocks = exchange(
        sizes, "shift_pairs", 1, ("shift", pair, hops, False), ("gather", w_output)
    )
    output_full = output_blocks.reshape(-1, width)

    stack = (hop_count + 1,) + block
    twice = (2 * tok_rows, LANES)
    mixed, log_total, start, grads_near = hosted(
        attend_body,
        "attend",
        [(block, low), ((2 * tok_rows, 1), full), ((tok_rows, 1), jnp.int32)],
        query,
        pair,
        far,
        doc_ids.reshape(-1, LANES),
        docs_far,
        scratch=[
            pltpu.VMEM(stack, low),
            pltpu.VMEM(stack, low),
            pltpu.VMEM(twice, low),
            pltpu.VMEM(twice, full),
        ],
        sizes=sizes,
        number=10,
        items=[("gather", near_turned)],
    )
    mixed_own, grad_own = exchange(
        sizes,
        "swap_mixed",
        2,
        ("swap", mixed.reshape(group, own, LANES)),
        ("swap", out_grad.reshape(group, own, LANES)),
    )
    rows_own, middle, weights = call(
        middle_body,
        "middle",
        [((own, width + LANES), low), ((own, width), full), ((own, LANES), full)],
        mixed_own,
        tokens_own,
        output_full,
        gains,
        router,
        expert_ids.T,
        scratch=[pltpu.VMEM(expert_ids.shape, full)],
    )
    rows_blocks, rows_shifted = exchange(
        sizes, "gather_rows", 3, ("gather", rows_own), ("shift", rows_own, everyone, False)
    )
    rows_near = rows_blocks.reshape(tok_rows, -1)
    parts = hidden // LANES
    in_rows = w_expert_in.reshape(expert_local, width, 2, parts, LANES)
    in_rows = in_rows.transpose(0, 1, 3, 2, 4).reshape(expert_local, -1, LANES)
    moe_partial, back_partial, in_flat, in_part, out_part, grads_far, rows_far = local_experts(
        sizes,
        9,
        rows_near,
        grads_near.reshape(width, tok_rows),
        in_rows,
        w_expert_out,
        far_turned,
        rows_shifted,
    )
    rows_far = rows_far.reshape((depth - 1) * tok_rows, -1)
    grads_far = grads_far.reshape(depth - 1, width, tok_rows)
    work = (in_flat, w_expert_out, in_part, out_part, rows_far, grads_far)
    share = expert_local // 4
    in_sums, out_sums = [], []

    def beneath(name, number, *items):
        in_sum, out_sum, *moved = cover(
            sizes, name, number, len(in_sums) * share, share, work, *items
        )
        in_sums.append(in_sum)
        out_sums.append(out_sum)
        return moved

    (back_blocks,) = beneath("swap_back", 4, ("swap", back_partial.reshape(group, own, -1)))
    middle_grad, attn_grad, logit_grad, gain_moe_part = call(
        middle_back_body,
        "middle_back",
        [
            ((own, width), full),
            ((own, width), low),
            ((own, LANES), low),
            ((1, width), full),
        ],
        back_blocks,
        grad_own,
        middle,
        weights,
        gains,
        router,
    )
    attn_grad_blocks, logit_blocks = beneath(
        "gather_attn_grad", 5, ("gather", attn_grad), ("gather", logit_grad)
    )
    query_grad, pair_grad, far_grad, output_sum = call(
        attend_back_body,
        "attend_back",
        [(block, low), (block, full), ((hop_count,) + block, low), ((group, LANES, LANES), low)],
        attn_grad_blocks.reshape(tok_rows, width),
        w_output,
        query,
        pair,
        far,
        start,
        log_total,
        mixed,
        cosine,
        sine,
        scratch=[
            pltpu.VMEM(stack, low),
            pltpu.VMEM(stack, low),
            pltpu.VMEM(twice, low),
            pltpu.VMEM(twice, low),
            pltpu.VMEM(twice, full),
            pltpu.VMEM(stack, full),
            pltpu.VMEM(stack, full),
        ],
    )
    returned, moe_blocks = beneath(
        "shift_grads",
        6,
        ("shift", far_grad, [-d for d in hops], True),
        ("swap", moe_partial.reshape(group, own, width)),
    )
    unit = 16 * depth
    length = (3 * width + LANES + unit - 1) // unit * unit
    partial, sums = call(
        project_back_body,
        "project_back",
        [((tok_rows, width), low), ((length, LANES), low)],
        query_grad,
        pair_grad,
        returned,
        normed,
        w_query,
        w_pair,
        cosine,
        sine,
        output_sum,
        logit_blocks.reshape(tok_rows, LANES),
        rows_near,
    )
    partial_blocks, sums_turned = beneath(
        "swap_partial",
        7,
        ("swap", partial.reshape(group, own, width)),
        ("turn", sums.reshape(depth, length // depth, LANES)),
    )
    pieces = (group, own, LANES)
    block_out, in_grad, gain_parts, summed = call(
        results_body,
        "results",
        [
            (pieces, low),
            (pieces, low),
            ((group, 8, LANES), full),
            ((length // depth, LANES), low),
        ],
        partial_blocks,
        moe_blocks,
        tokens_own,
        middle,
        middle_grad,
        gains,
        gain_moe_part,
        sums_turned,
    )
    block_out, in_grad, gain_all, sums = exchange(
        sizes,
        "swap_results",
        8,
        ("swap", block_out),
        ("swap", in_grad),
        ("spread", gain_parts),
        ("collect", summed),
    )
    grad_in, grad_out, block_out, in_grad, gain_sums, query_sum, pair_sum, output_sum, router_sum = outputs(
        in_sums, out_sums, block_out, in_grad, gain_all, sums.reshape(length, LANES), experts
    )
    return (
        block_out,
        in_grad,
        gain_sums[0],
        query_sum,
        pair_sum.reshape(w_key_value.shape),
        output_sum,
        gain_sums[1],
        router_sum.T,
        grad_in,
        grad_out,
    )


def solution(mesh):
    in_specs = (
        P("dp", ("row", "col")),
        P("dp", ("row", "col")),
        P("dp"),
        P("dp", None),
        P(("row", "col")),
        P(None, ("row", "col")),
        P(None, ("row", "col"), None),
        P(("row", "col"), None),
        P(("row", "col")),
        P(("row", "col"), None),
        P("row", None, None, "col"),
        P("row", "col", None),
    )
    out_specs = (
        P("dp", ("row", "col")),
        P("dp", ("row", "col")),
        P(("row", "col")),
        P(None, ("row", "col")),
        P(None, ("row", "col"), None),
        P(("row", "col"), None),
        P(("row", "col")),
        P(("row", "col"), None),
        P("row", None, None, "col"),
        P("row", "col", None),
    )
    sizes = (mesh.shape["row"], mesh.shape["col"], mesh.shape["dp"])
    return jax.shard_map(
        functools.partial(local, sizes),
        mesh=mesh,
        in_specs=in_specs,
        out_specs=out_specs,
        check_vma=False,
    )
```

```python
import functools

import jax
import jax.numpy as jnp
from jax import lax
from jax.experimental import pallas as pl
from jax.experimental.pallas import tpu as pltpu
from jax.sharding import PartitionSpec as P

LONGEST = 4096
HIGH = lax.Precision.HIGHEST
EPSILON = 1e-05
RESIDUAL_SCALE = 0.22
SCORE_SCALE = 0.015625
ROPE_BASE = 10000.0
MASKED = -1e30
MESH = pl.DeviceIdType.MESH
GROUP = ("row", "col")
EVERY = ("dp", "row", "col")
LANES = 128
HBM = pl.BlockSpec(memory_space=pl.ANY)
FULL = pl.BlockSpec(memory_space=pltpu.VMEM)
TURN = LANES // 4


class Moves:
    def __init__(self, sizes, kinds, sources, targets, sems):
        self.sizes, self.kinds = sizes, kinds
        self.sources, self.targets = sources, targets
        self.send_sem, self.recv_sem, self.local_sem = sems

    def place(self):
        row, col, layer = lax.axis_index("row"), lax.axis_index("col"), lax.axis_index("dp")
        return row, col, layer, row * self.sizes[1] + col

    def member(self, index):
        rows, cols, depth = self.sizes
        return {"row": index // cols, "col": lax.rem(index, cols)}

    def barrier(self):
        rows, cols, depth = self.sizes
        row, col, layer, me = self.place()
        group = rows * cols
        names = [kind[0] for kind in self.kinds]
        barrier = pltpu.get_barrier_semaphore()
        partners = []
        if "swap" in names:
            for k in range(1, group):
                partners.append(self.member(lax.rem(me + k, group)))
        elif "gather" in names:
            for k in range(1, rows):
                partners.append({"row": lax.rem(row + k, rows)})
            for k in range(1, cols):
                partners.append({"col": lax.rem(col + k, cols)})
        shifts = set()
        for kind in self.kinds:
            if kind[0] == "shift":
                for d in kind[1]:
                    shifts |= {d % depth, -d % depth}
            elif kind[0] in ("turn", "collect"):
                shifts |= set(range(1, depth))
        for k in sorted(shifts - {0}):
            partners.append({"dp": lax.rem(layer + k, depth)})
        for partner in partners:
            pl.semaphore_signal(barrier, inc=1, device_id=partner, device_id_type=MESH)
        pl.semaphore_wait(barrier, len(partners))

    def copies(self, only):
        rows, cols, depth = self.sizes
        row, col, layer, me = self.place()
        group = rows * cols
        slot = 0
        lists = []

        def remote(source, target, device):
            nonlocal slot
            slot += 1
            return functools.partial(
                pltpu.make_async_remote_copy,
                src_ref=source,
                dst_ref=target,
                send_sem=self.send_sem.at[slot - 1],
                recv_sem=self.recv_sem.at[slot - 1],
                device_id=device,
                device_id_type=MESH,
            )

        for index, (kind, source, target) in enumerate(
            zip(self.kinds, self.sources, self.targets)
        ):
            direct, relayed, local = [], [], []

            def keep(source, target):
                sem = self.local_sem.at[index]
                local.append(functools.partial(pltpu.make_async_copy, source, target, sem))

            if kind[0] == "gather":
                second, parts = kind[1:]
                size = source.shape[0] // parts

                def at(i, part):
                    some = pl.ds(part * size, size)
                    return target.at[some, i] if second else target.at[i, some]

                for part in range(parts):
                    some = source.at[pl.ds(part * size, size)]
                    for k in range(1, rows):
                        device = {"row": lax.rem(row + k, rows)}
                        copy = remote(some, at(me, part), device)
                        piece = at(lax.rem(row + rows - k, rows) * cols + col, part)
                        nexts = [
                            remote(piece, piece, {"col": lax.rem(col + j, cols)})
                            for j in range(1, cols)
                        ]
                        relayed.append((copy, nexts))
                    for k in range(1, cols):
                        device = {"col": lax.rem(col + k, cols)}
                        direct.append(remote(some, at(me, part), device))
                keep(source, target.at[:, me] if second else target.at[me])
            elif kind[0] == "swap":
                for k in range(1, group):
                    other = lax.rem(me + k, group)
                    direct.append(remote(source.at[other], target.at[me], self.member(other)))
                keep(source.at[me], target.at[me])
            elif kind[0] in ("turn", "collect"):
                for k in range(1, depth):
                    other = lax.rem(layer + k, depth)
                    piece = source.at[other] if kind[0] == "turn" else source
                    direct.append(remote(piece, target.at[layer], {"dp": other}))
                keep(source.at[layer] if kind[0] == "turn" else source, target.at[layer])
            else:
                for at, d in enumerate(kind[1]):
                    piece = source.at[at] if kind[2] else source
                    device = {"dp": lax.rem(layer + d % depth, depth)}
                    direct.append(remote(piece, target.at[at], device))
            if only is None or index in only:
                lists.append((direct, relayed, local))
        return tuple(sum((part[i] for part in lists), []) for i in range(3))

    def start(self, only=None):
        direct, relayed, local = self.copies(only)
        for copy, _ in relayed:
            copy().start()
        for copy in direct + local:
            copy().start()

    def relay(self, only=None):
        for copy, nexts in self.copies(only)[1]:
            copy().wait_recv()
            for follower in nexts:
                follower().start()

    def finish(self, only=None):
        direct, relayed, local = self.copies(only)
        for copy, nexts in relayed:
            copy().wait_send()
            for follower in nexts:
                follower().wait()
        for copy in direct + local:
            copy().wait()


def planned(sizes, items):
    rows, cols, depth = sizes
    group = rows * cols
    kinds, shapes, copies = [], [], 0
    for item in items:
        name, array = item[0], item[1]
        shape = array.shape
        if name == "gather":
            second, parts = (item[2:] + (False, 1)[len(item) - 2 :])[:2]
            kinds.append((name, second, parts))
            shape = (shape[0], group) + shape[1:] if second else (group,) + shape
            copies += parts * ((rows - 1) * cols + cols - 1)
        elif name == "shift":
            distances, split = item[2], item[3]
            kinds.append((name, tuple(distances), split))
            shape = (len(distances),) + (shape[1:] if split else shape)
            copies += len(distances)
        else:
            kinds.append((name,))
            if name == "collect":
                shape = (depth,) + shape
            copies += (group if name == "swap" else depth) - 1
        shapes.append(jax.ShapeDtypeStruct(shape, array.dtype))
    sems = [
        pltpu.SemaphoreType.DMA((copies,)),
        pltpu.SemaphoreType.DMA((copies,)),
        pltpu.SemaphoreType.DMA((len(items),)),
    ]
    return tuple(kinds), shapes, sems


def exchange_body(sizes, kinds, *refs):
    count = len(kinds)
    moves = Moves(sizes, kinds, refs[:count], refs[count : 2 * count], refs[2 * count :])
    moves.barrier()
    moves.start()
    moves.relay()
    moves.finish()


def exchange(sizes, name, number, *items):
    kinds, shapes, sems = planned(sizes, items)
    return pl.pallas_call(
        functools.partial(exchange_body, sizes, kinds),
        out_shape=tuple(shapes),
        in_specs=[HBM] * len(items),
        out_specs=(HBM,) * len(items),
        scratch_shapes=sems,
        compiler_params=pltpu.CompilerParams(collective_id=number, has_side_effects=True),
        name=name,
    )(*[item[1] for item in items])


def dot(a, b, left=1, right=0, precision=None):
    return lax.dot_general(
        a,
        b,
        (((left,), (right,)), ((), ())),
        preferred_element_type=jnp.float32,
        precision=precision,
    )


def call(body, name, shapes, *arrays, scratch=()):
    return pl.pallas_call(
        body,
        out_shape=tuple(jax.ShapeDtypeStruct(*shape) for shape in shapes),
        in_specs=[FULL] * len(arrays),
        out_specs=(FULL,) * len(shapes),
        scratch_shapes=list(scratch),
        name=name,
    )(*arrays)


def hosted(body, name, shapes, *arrays, scratch=(), sizes, number, items):
    kinds, moved, sems = planned(sizes, items)
    ins, count, outs = len(arrays), len(items), len(shapes)

    def whole(*refs):
        sources = refs[ins : ins + count]
        made = refs[ins + count : ins + count + outs]
        targets = refs[ins + count + outs : ins + 2 * count + outs]
        rest = refs[ins + 2 * count + outs :]
        moves = Moves(sizes, kinds, sources, targets, rest[len(scratch) :])
        moves.barrier()
        moves.start()
        body(*refs[:ins], *made, *rest[: len(scratch)])
        moves.relay()
        moves.finish()

    return pl.pallas_call(
        whole,
        out_shape=tuple(jax.ShapeDtypeStruct(*shape) for shape in shapes) + tuple(moved),
        in_specs=[FULL] * ins + [HBM] * count,
        out_specs=(FULL,) * outs + (HBM,) * count,
        scratch_shapes=list(scratch) + sems,
        compiler_params=pltpu.CompilerParams(collective_id=number, has_side_effects=True),
        name=name,
    )(*arrays, *[item[1] for item in items])


def lanes_of(shape):
    return lax.broadcasted_iota(jnp.int32, shape, len(shape) - 1)


def flipped(values):
    lanes = lanes_of(values.shape)
    ahead = pltpu.roll(values, LANES - TURN, 1)
    behind = pltpu.roll(values, TURN, 1)
    return jnp.where(lanes % (2 * TURN) < TURN, ahead, behind)


def beside(blocks_ref):
    return jnp.concatenate([blocks_ref[i] for i in range(blocks_ref.shape[0])], axis=1)


def gain_row(gains_ref, which):
    return beside(gains_ref).astype(jnp.float32)[which : which + 1, :]


def added(blocks):
    return functools.reduce(
        jnp.add, [blocks[i].astype(jnp.float32) for i in range(blocks.shape[0])]
    )


def own_rows(count):
    me = lax.axis_index("row") * lax.axis_size("col") + lax.axis_index("col")
    return pl.ds(pl.multiple_of(me * count, count), count)


def column(row):
    return jnp.broadcast_to(row, (8, row.shape[1])).T[:, 0:1]


def project_body(blocks, gains, w_query, w_pair, cosine, sine, near, far, normed, query, pair, own, own_grad, near_turned, far_turned):
    tokens = beside(blocks).astype(jnp.float32)
    scale = lax.rsqrt(jnp.mean(tokens * tokens, axis=1, keepdims=True) + EPSILON)
    normed[...] = (tokens * scale * gain_row(gains, 0)).astype(jnp.bfloat16)
    raw = dot(normed[...], w_query[...])
    query[...] = (raw * cosine[...] + flipped(raw) * sine[...]).astype(jnp.bfloat16)
    raw = dot(normed[...], w_pair[...])
    keys = lanes_of(raw.shape) < LANES // 2
    turned = raw * cosine[...] + flipped(raw) * sine[...]
    pair[...] = jnp.where(keys, turned, raw).astype(jnp.bfloat16)
    for i in range(blocks.shape[0]):
        own[:, i * LANES : (i + 1) * LANES] = blocks[i, own_rows(own.shape[0]), :]
    for source, target in ((near, near_turned), (far, far_turned)):
        for i in range(source.shape[0]):
            scaled = RESIDUAL_SCALE * source[i].astype(jnp.float32)
            target[i] = scaled.T.astype(jnp.bfloat16)
    for i in range(near.shape[0]):
        own_grad[:, i * LANES : (i + 1) * LANES] = near[i, own_rows(own.shape[0]), :]


def doubled(pair, keys_ref, values_ref, at):
    wide = pair.astype(jnp.float32)
    other = pltpu.roll(wide, LANES // 2, 1)
    keys = lanes_of(wide.shape) < LANES // 2
    keys_ref[at] = jnp.where(keys, wide, other).astype(jnp.bfloat16)
    values_ref[at] = jnp.where(keys, other, wide).astype(jnp.bfloat16)


def per_head(values):
    first = lanes_of(values.shape) < LANES // 2
    zero = jnp.zeros_like(values)
    return jnp.concatenate(
        [jnp.where(first, values, zero), jnp.where(first, zero, values)], axis=0
    )


def tile_scores(queries, keys_ref, starts, row, block, last, tokens):
    scores = dot(queries, keys_ref[block], 1, 1) * SCORE_SCALE
    at = lanes_of(scores.shape) + block * tokens
    allowed = at >= starts
    if block == last:
        place = row + lax.broadcasted_iota(jnp.int32, scores.shape, 0)
        allowed = allowed & (at <= place + block * tokens)
    return jnp.where(allowed, scores, MASKED)


def doc_row(docs):
    rows = [docs[i : i + 1, :] for i in range(docs.shape[0])]
    return jnp.concatenate(rows, axis=1).astype(jnp.float32)


def attend_body(query, pair, far, docs, far_docs, mixed, log_total, start, keys, values, queries, out):
    tokens = query.shape[0]
    last = far.shape[0]
    layer = lax.axis_index("dp")
    here = doc_row(docs[...])
    mine = column(here)
    before = jnp.sum((here < mine).astype(jnp.float32), axis=1, keepdims=True)
    for d in range(1, last + 1):
        fewer = (doc_row(far_docs[d - 1]) < mine) | (layer < d)
        before = before + jnp.sum(fewer.astype(jnp.float32), axis=1, keepdims=True)
    start[...] = before.astype(jnp.int32)
    doubled(pair[...], keys, values, last)
    for d in range(1, last + 1):
        doubled(far[d - 1], keys, values, last - d)
    queries[...] = per_head(query[...].astype(jnp.float32)).astype(jnp.bfloat16)
    step = 256

    def tile(i, carry):
        rows = pl.ds(pl.multiple_of(i * step, step), step)
        row = lax.rem(i * step, tokens)
        starts = start[pl.ds(pl.multiple_of(row, step), step), :]
        parts = [
            tile_scores(queries[rows, :], keys, starts, row, block, last, tokens)
            for block in range(last + 1)
        ]
        top = functools.reduce(
            jnp.maximum, [jnp.max(part, axis=1, keepdims=True) for part in parts]
        )
        parts = [jnp.exp(part - top) for part in parts]
        total = functools.reduce(jnp.add, [jnp.sum(p, axis=1, keepdims=True) for p in parts])
        sums = [
            dot(part.astype(jnp.bfloat16), values[block]) for block, part in enumerate(parts)
        ]
        out[rows, :] = functools.reduce(jnp.add, sums) / total
        log_total[rows, :] = top + jnp.log(total)
        return carry

    lax.fori_loop(0, 2 * tokens // step, tile, 0)
    first = lanes_of((tokens, LANES)) < LANES // 2
    mixed[...] = jnp.where(first, out[:tokens, :], out[tokens:, :]).astype(jnp.bfloat16)


def attend_back_body(grad, w_output, query, pair, far, start, log_total, mixed, cosine, sine, query_grad, pair_grad, far_grad, output_grad, keys, values, queries, grads, turned, key_sums, value_sums):
    tokens = query.shape[0]
    last = far.shape[0]
    doubled(pair[...], keys, values, last)
    for d in range(1, last + 1):
        doubled(far[d - 1], keys, values, last - d)
    queries[...] = per_head(query[...].astype(jnp.float32)).astype(jnp.bfloat16)
    grads[...] = per_head(dot(grad[...], w_output[...], 1, 1)).astype(jnp.bfloat16)
    output_sum = dot(mixed[...], grad[...], 0, 0).astype(jnp.bfloat16)
    for i in range(output_grad.shape[0]):
        output_grad[i] = output_sum[:, i * LANES : (i + 1) * LANES]
    key_sums[...] = jnp.zeros_like(key_sums)
    value_sums[...] = jnp.zeros_like(value_sums)
    step = 256

    def tile(i, carry):
        rows = pl.ds(pl.multiple_of(i * step, step), step)
        row = lax.rem(i * step, tokens)
        starts = start[pl.ds(pl.multiple_of(row, step), step), :]
        asked, given, level = queries[rows, :], grads[rows, :], log_total[rows, :]
        chances, products = [], []
        for block in range(last + 1):
            scores = tile_scores(asked, keys, starts, row, block, last, tokens)
            chances.append(jnp.exp(scores - level))
            products.append(dot(given, values[block], 1, 1))
        delta = functools.reduce(
            jnp.add,
            [jnp.sum(p * q, axis=1, keepdims=True) for p, q in zip(chances, products)],
        )
        total = jnp.zeros((step, LANES), jnp.float32)
        for block in range(last + 1):
            back = (chances[block] * (products[block] - delta)).astype(jnp.bfloat16)
            total = total + dot(back, keys[block])
            key_sums[block] += dot(back, asked, 0, 0)
            value_sums[block] += dot(chances[block].astype(jnp.bfloat16), given, 0, 0)
        turned[rows, :] = total
        return carry

    lax.fori_loop(0, 2 * tokens // step, tile, 0)
    first = lanes_of((tokens, LANES)) < LANES // 2
    raw = jnp.where(first, turned[:tokens, :], turned[tokens:, :]) * SCORE_SCALE
    query_grad[...] = (raw * cosine[...] - flipped(raw) * sine[...]).astype(jnp.bfloat16)

    def joined(block):
        by_key, by_value = key_sums[block], value_sums[block]
        by_key = (by_key + pltpu.roll(by_key, LANES // 2, 1)) * SCORE_SCALE
        by_value = by_value + pltpu.roll(by_value, LANES // 2, 1)
        return jnp.where(first, by_key, by_value)

    pair_grad[...] = joined(last)
    for d in range(1, last + 1):
        far_grad[d - 1] = joined(last - d).astype(jnp.bfloat16)


def router_rows(router):
    rows = beside(router).astype(jnp.float32)
    blank = jnp.zeros((LANES - rows.shape[0], rows.shape[1]), jnp.float32)
    return jnp.concatenate([rows, blank], axis=0)


def middle_body(mixed, own, w_output, gains, router, ids_turned, rows, middle, weights, ids_ref):
    experts = router.shape[1]
    width = own.shape[1]
    attn = dot(beside(mixed), w_output[...])
    value = own[...].astype(jnp.float32) + RESIDUAL_SCALE * attn
    middle[...] = value
    scale = lax.rsqrt(jnp.mean(value * value, axis=1, keepdims=True) + EPSILON)
    normed = value * scale * gain_row(gains, 1)
    logits = dot(normed, router_rows(router), 1, 1, precision=HIGH)
    count = own.shape[0]
    ids_ref[...] = ids_turned[...].astype(jnp.float32).T
    ids = ids_ref[own_rows(count), :]
    lanes = lanes_of((count, LANES))
    chosen = jnp.zeros((count, LANES), jnp.float32)
    for k in range(ids.shape[1]):
        chosen = chosen + (ids[:, k : k + 1] == lanes.astype(jnp.float32)).astype(
            jnp.float32
        )
    top = jnp.max(jnp.where(lanes < experts, logits, MASKED), axis=1, keepdims=True)
    terms = jnp.exp(jnp.minimum(logits - top, 0.0)) * chosen
    share = terms / jnp.sum(terms, axis=1, keepdims=True)
    weights[...] = share
    high = share.astype(jnp.bfloat16)
    low = share - high.astype(jnp.float32)
    rows[:, :width] = normed.astype(jnp.bfloat16)
    rows[:, width:] = (high.astype(jnp.float32) + pltpu.roll(low, LANES // 2, 1)).astype(
        jnp.bfloat16
    )


def middle_back_body(back, out_grad, middle, weights, gains, router, middle_grad, attn_grad, logit_grad, gain_part):
    width = middle.shape[1]
    normed_grad = back[0, :, :width].astype(jnp.float32)
    weight_grad = back[0, :, width:].astype(jnp.float32)
    for i in range(1, back.shape[0]):
        normed_grad = normed_grad + back[i, :, :width].astype(jnp.float32)
        weight_grad = weight_grad + back[i, :, width:].astype(jnp.float32)
    share, value = weights[...], middle[...]
    mean = jnp.sum(share * weight_grad, axis=1, keepdims=True)
    logit = share * (weight_grad - mean)
    logit_grad[...] = logit.astype(jnp.bfloat16)
    normed_grad = normed_grad + dot(logit, router_rows(router), precision=HIGH)
    scale = lax.rsqrt(jnp.mean(value * value, axis=1, keepdims=True) + EPSILON)
    gain_part[...] = jnp.sum(normed_grad * value * scale, axis=0, keepdims=True)
    scaled = normed_grad * gain_row(gains, 1)
    norm_dot = jnp.sum(scaled * value, axis=1, keepdims=True)
    total = (
        out_grad[...].astype(jnp.float32)
        + scale * scaled
        - value * (scale * scale * scale * norm_dot / width)
    )
    middle_grad[...] = total
    attn_grad[...] = (RESIDUAL_SCALE * total).astype(jnp.bfloat16)


def project_back_body(query_grad, pair_grad, returned, normed, w_query, w_pair, cosine, sine, output_turned, logit, rows, gains, gain_moe, partial, sums, output_summed, gain_parts):
    layer = lax.axis_index("dp")
    depth = lax.axis_size("dp")
    total = pair_grad[...]
    for i in range(returned.shape[0]):
        total = total + jnp.where(
            layer + i + 1 < depth, returned[i].astype(jnp.float32), 0.0
        )
    keys = lanes_of(total.shape) < LANES // 2
    turned = total * cosine[...] - flipped(total) * sine[...]
    pair_low = jnp.where(keys, turned, total).astype(jnp.bfloat16)
    query_low = query_grad[...]
    whole = dot(query_low, w_query[...], 1, 1) + dot(pair_low, w_pair[...], 1, 1)
    partial[...] = whole.astype(jnp.bfloat16)
    gain_attn = jnp.sum(whole * normed[...].astype(jnp.float32), axis=0, keepdims=True)
    gain_attn = gain_attn / gain_row(gains, 0)
    gain_parts[...] = jnp.zeros_like(gain_parts)
    for i in range(gain_parts.shape[0]):
        at = slice(i * LANES, (i + 1) * LANES)
        gain_parts[i, 0:1, :] = gain_attn[:, at]
        gain_parts[i, 1:2, :] = gain_moe[0:1, at]
    width = normed.shape[1]
    sums[:width, :] = dot(normed[...], query_low, 0, 0).astype(jnp.bfloat16)
    sums[width : 2 * width, :] = dot(normed[...], pair_low, 0, 0).astype(jnp.bfloat16)
    output_summed[...] = added(output_turned).astype(jnp.bfloat16)
    mine = rows[:, own_rows(LANES)]
    sums[2 * width : 2 * width + LANES, :] = dot(logit[...], mine, 0, 0).astype(jnp.bfloat16)


def results_body(blocks, moe, own, middle, middle_grad, gains, gain_blocks, turned, block_out, in_grad, gain_sum, summed):
    gain_sum[...] = added(gain_blocks)
    summed[...] = added(turned).astype(jnp.bfloat16)
    width = own.shape[1]
    normed_grad = blocks[0].astype(jnp.float32)
    branch = moe[0].astype(jnp.float32)
    for i in range(1, blocks.shape[0]):
        normed_grad = normed_grad + blocks[i].astype(jnp.float32)
        branch = branch + moe[i].astype(jnp.float32)
    value = own[...].astype(jnp.float32)
    scale = lax.rsqrt(jnp.mean(value * value, axis=1, keepdims=True) + EPSILON)
    scaled = normed_grad * gain_row(gains, 0)
    norm_dot = jnp.sum(scaled * value, axis=1, keepdims=True)
    grad = (
        middle_grad[...] + scale * scaled - value * (scale * scale * scale * norm_dot / width)
    ).astype(jnp.bfloat16)
    out = (middle[...] + RESIDUAL_SCALE * branch).astype(jnp.bfloat16)
    for i in range(block_out.shape[0]):
        at = slice(i * LANES, (i + 1) * LANES)
        block_out[i] = out[:, at]
        in_grad[i] = grad[:, at]


def expert_terms(gate_up, active_grad, weight):
    hidden = active_grad.shape[0]
    gate, up = gate_up[:hidden], gate_up[hidden:]
    sigmoid = jax.nn.sigmoid(gate)
    silu = gate * sigmoid
    ungated = silu * up
    active = (ungated * weight).astype(jnp.bfloat16)
    scaled = active_grad * weight
    gate_grad = (scaled * up * sigmoid * (1.0 + gate * (1.0 - sigmoid))).astype(jnp.bfloat16)
    up_grad = (scaled * silu).astype(jnp.bfloat16)
    return active, jnp.concatenate([gate_grad, up_grad], axis=0), active_grad * ungated


def weight_rows(extra):
    turned = extra.astype(jnp.float32).T
    return turned[: LANES // 2] + turned[LANES // 2 :]


def local_experts_body(sizes, kinds, rows_ref, grads_ref, in_ref, out_ref, sent_grads, sent_rows, moe_ref, back_ref, flat_ref, in_sum, out_sum, got_grads, got_rows, moe_acc, back_acc, share, weights, spread, *sems):
    step, steps = pl.program_id(0), pl.num_programs(0)
    each, hidden, width = out_ref.shape
    parts = hidden // LANES
    moves = Moves(sizes, kinds, [sent_grads, sent_rows], [got_grads, got_rows], sems)

    @pl.when(step == 0)
    def _():
        moves.barrier()
        moves.start()
        moe_acc[...] = jnp.zeros_like(moe_acc)
        back_acc[...] = jnp.zeros_like(back_acc)
        share[...] = jnp.zeros_like(share)
        weights[...] = weight_rows(rows_ref[:, width:])

    @pl.when(step == steps // 2)
    def _():
        moves.relay([0])

    for i in range(each):
        spread[i] = in_ref[i].astype(jnp.float32)
        for part in range(parts):
            for half in range(2):
                at = half * hidden + part * LANES
                flat_ref[i, :, at : at + LANES] = spread[
                    i, pl.ds(part * 2 + half, width, stride=2 * parts), :
                ].astype(jnp.bfloat16)
        expert = (lax.axis_index("row") * steps + step) * each + i
        active, gate_up_grad, shares = expert_terms(
            dot(flat_ref[i], rows_ref[:, :width], 0, 1),
            dot(out_ref[i], grads_ref[...]),
            weights[pl.ds(expert, 1), :],
        )
        share[pl.ds(expert, 1), :] = jnp.sum(shares, axis=0, keepdims=True)
        moe_acc[...] += dot(active, out_ref[i], 0, 0)
        back_acc[...] += dot(gate_up_grad, flat_ref[i], 0, 1)
        in_sum[i] = dot(gate_up_grad, rows_ref[:, :width]).astype(jnp.bfloat16)
        out_sum[i] = dot(active, grads_ref[...], 1, 1).astype(jnp.bfloat16)

    @pl.when(step == steps - 1)
    def _():
        moe_ref[...] = moe_acc[...].astype(jnp.bfloat16)
        back_ref[:, :width] = back_acc[...].astype(jnp.bfloat16)
        back_ref[:, width:] = share[...].T.astype(jnp.bfloat16)
        moves.relay([1])
        moves.finish()


def local_experts(sizes, number, rows, grads, w_in, w_out, sent_grads, sent_rows):
    tokens, wide = rows.shape
    experts, hidden, width = w_out.shape
    each = 1
    low = jnp.bfloat16
    kinds, shapes, sems = planned(
        sizes,
        [
            ("gather", sent_grads, True, sent_grads.shape[0]),
            ("gather", sent_rows, True, sent_rows.shape[0]),
        ],
    )
    whole = lambda s: pl.BlockSpec(s, lambda e: (0,) * len(s))
    some = lambda s: pl.BlockSpec((each,) + s[1:], lambda e: (e,) + (0,) * (len(s) - 1))
    outs = [
        (tokens, width),
        (tokens, wide),
        (experts, width, 2 * hidden),
        (experts, 2 * hidden, width),
        (experts, hidden, width),
    ]
    return pl.pallas_call(
        functools.partial(local_experts_body, sizes, kinds),
        grid=(experts // each,),
        in_specs=[
            whole(rows.shape),
            whole(grads.shape),
            some(w_in.shape),
            some(w_out.shape),
            HBM,
            HBM,
        ],
        out_specs=(whole(outs[0]), whole(outs[1]), *[some(s) for s in outs[2:]], HBM, HBM),
        out_shape=tuple(jax.ShapeDtypeStruct(s, low) for s in outs) + tuple(shapes),
        scratch_shapes=[
            pltpu.VMEM((tokens, width), jnp.float32),
            pltpu.VMEM((tokens, width), jnp.float32),
            pltpu.VMEM((LANES, tokens), jnp.float32),
            pltpu.VMEM((LANES // 2, tokens), jnp.float32),
            pltpu.VMEM((each,) + w_in.shape[1:], jnp.float32),
        ]
        + sems,
        compiler_params=pltpu.CompilerParams(collective_id=number, has_side_effects=True),
        name="local_experts",
    )(rows, grads, w_in, w_out, sent_grads, sent_rows)


def cover_body(sizes, kinds, experts, first, in_ref, out_ref, in_part, out_part, rows_far, grads_first, grads_second, grads_rest, *refs):
    count = len(kinds)
    sources, in_sum, out_sum = refs[:count], refs[count], refs[count + 1]
    targets = refs[count + 2 : 2 * count + 2]
    rows, grads, weights, whole, turned, load_sem, *rest = refs[2 * count + 2 :]
    sums, sems = rest[:-3], rest[-3:]
    step = pl.program_id(0)
    layers, width, tokens = grads.shape
    hidden = out_ref.shape[1]
    moves = Moves(sizes, kinds, sources, targets, sems)

    @pl.when(step == 0)
    def _():
        loads = [
            pltpu.make_async_copy(rows_far, rows, load_sem.at[0]),
            pltpu.make_async_copy(grads_first, grads.at[pl.ds(0, 1)], load_sem.at[1]),
            pltpu.make_async_copy(grads_second, grads.at[pl.ds(1, 1)], load_sem.at[2]),
            pltpu.make_async_copy(grads_rest, grads.at[pl.ds(2, layers - 2)], load_sem.at[3]),
        ]
        for load in loads:
            load.start()
        moves.barrier()
        moves.start()
        for load in loads:
            load.wait()
        for i in range(layers):
            weights[i] = weight_rows(rows[i * tokens : (i + 1) * tokens, width:])

    index = lax.axis_index("row") * experts + first + step

    def part_of(at, pieces):
        block = rows[pl.ds(pl.multiple_of(at * tokens, tokens), pieces * tokens), :width]
        weight = jnp.concatenate(
            [weights[at + i, pl.ds(index, 1), :] for i in range(pieces)], axis=1
        )
        active_grad = jnp.concatenate(
            [dot(out_ref[0], grads[at + i]) for i in range(pieces)], axis=1
        )
        active, gate_up_grad, _ = expert_terms(dot(in_ref[0], block, 0, 1), active_grad, weight)
        out_total = functools.reduce(
            jnp.add,
            [
                dot(active[:, i * tokens : (i + 1) * tokens], grads[at + i], 1, 1)
                for i in range(pieces)
            ],
        )
        return dot(gate_up_grad, block), out_total

    if not sums:
        in_total, out_total = part_of(0, layers)
    else:
        in_acc, out_acc = sums
        in_acc[...] = jnp.zeros_like(in_acc)
        out_acc[...] = jnp.zeros_like(out_acc)

        def more(i, carry):
            in_more, out_more = part_of(i, 1)
            in_acc[...] += in_more
            out_acc[...] += out_more
            return carry

        lax.fori_loop(0, layers, more, 0)
        in_total, out_total = in_acc[...], out_acc[...]
    whole[...] = in_total
    parts = hidden // LANES

    def turn(i, carry):
        at = pl.ds(pl.multiple_of(i * LANES, LANES), LANES)
        first = lax.rem(i, parts) * 2 + i // parts
        rows_of = pl.ds(first, width, stride=2 * parts)
        turned[rows_of, :] = (whole[at, :] + in_part[0, at, :].astype(jnp.float32)).T
        return carry

    lax.fori_loop(0, 2 * parts, turn, 0)

    def narrow(i, carry):
        at = pl.ds(pl.multiple_of(i * width, width), width)
        in_sum[0, at, :] = turned[at, :].astype(jnp.bfloat16)
        return carry

    lax.fori_loop(0, 2 * parts, narrow, 0)
    out_sum[0] = (out_total + out_part[0].astype(jnp.float32)).astype(jnp.bfloat16)

    @pl.when(step == pl.num_programs(0) - 1)
    def _():
        moves.relay()
        moves.finish()


def cover(sizes, name, number, first, count, work, *items):
    w_in, w_out, in_part, out_part, rows_far, *grads_far = work
    layers = sum(g.shape[0] for g in grads_far)
    width, tokens = grads_far[0].shape[1:]
    experts, hidden, _ = w_out.shape
    kinds, shapes, sems = planned(sizes, items)
    each = lambda s: pl.BlockSpec((1,) + s[1:], lambda e: (first + e, 0, 0))
    out = lambda s: pl.BlockSpec((1,) + s[1:], lambda e: (e, 0, 0))
    turned = (width * 2 * hidden // LANES, LANES)
    outs = [(count,) + turned, (count, hidden, width)]
    sums = [(2 * hidden, width), (hidden, width)] if layers > 4 else []
    return pl.pallas_call(
        functools.partial(cover_body, sizes, kinds, experts, first),
        grid=(count,),
        in_specs=[each(a.shape) for a in work[:4]] + [HBM] * (len(work) - 4 + len(items)),
        out_specs=tuple(out(s) for s in outs) + (HBM,) * len(items),
        out_shape=tuple(jax.ShapeDtypeStruct(s, jnp.bfloat16) for s in outs) + tuple(shapes),
        scratch_shapes=[
            pltpu.VMEM(rows_far.shape, jnp.bfloat16),
            pltpu.VMEM((layers, width, tokens), jnp.bfloat16),
            pltpu.VMEM((layers, LANES // 2, tokens), jnp.float32),
            pltpu.VMEM((2 * hidden, width), jnp.float32),
            pltpu.VMEM(turned, jnp.float32),
            pltpu.SemaphoreType.DMA((1 + len(grads_far),)),
        ]
        + [pltpu.VMEM(s, jnp.float32) for s in sums]
        + sems,
        compiler_params=pltpu.CompilerParams(collective_id=number, has_side_effects=True),
        name=name,
    )(*work, *[item[1] for item in items])


def outputs_body(counts, *refs):
    pieces = len(counts)
    in_sums, out_sums = refs[:pieces], refs[pieces : 2 * pieces]
    blocks, in_blocks, gains, sums, output_all = refs[2 * pieces : 2 * pieces + 5]
    gin, gout, block_out, in_grad, gain_attn, gain_moe, query, pair, output, router = refs[
        2 * pieces + 5 :
    ]
    step = pl.program_id(0)
    width = gout.shape[2]

    @pl.when(step == 0)
    def _():
        for i in range(blocks.shape[0]):
            at = pl.ds(i * blocks.shape[1], blocks.shape[1])
            block_out[at, :] = blocks[i]
            in_grad[at, :] = in_blocks[i]
        gain_sum = jnp.sum(gains[...], axis=0)
        gain_attn[...] = gain_sum[0:1, :]
        gain_moe[...] = gain_sum[1:2, :]
        query[...] = sums[:width, :].astype(jnp.float32)
        pair[...] = sums[width : 2 * width, :].astype(jnp.float32)
        for i in range(width // LANES):
            at = slice(i * LANES, (i + 1) * LANES)
            output[:, at] = output_all[at, :].astype(jnp.float32)
        router[...] = sums[2 * width : 2 * width + router.shape[0], :].astype(jnp.float32)

    first = 0
    for count, in_sum, out_sum in zip(counts, in_sums, out_sums):

        @pl.when((step >= first) & (step < first + count))
        def _(in_sum=in_sum, out_sum=out_sum):
            gout[0] = out_sum[0].astype(jnp.float32)
            gin[0] = in_sum[0].astype(jnp.float32)

        first += count


def outputs(in_sums, out_sums, hidden, blocks, in_blocks, gains, sums, output_all, experts):
    counts = [s.shape[0] for s in in_sums]
    width = out_sums[0].shape[2]
    parts = hidden // LANES
    group, own, lanes = blocks.shape
    tokens = group * own
    once = lambda s: pl.BlockSpec(s, lambda e: (0,) * len(s))
    each = lambda s: pl.BlockSpec((1,) + s[1:], lambda e: (e, 0, 0))
    specs = []
    for arrays in (in_sums, out_sums):
        first = 0
        for array in arrays:
            count = array.shape[0]
            specs.append(
                pl.BlockSpec(
                    (1,) + array.shape[1:],
                    lambda e, first=first, count=count: (jnp.clip(e - first, 0, count - 1), 0, 0),
                )
            )
            first += count
    total = sum(counts)
    full = jnp.float32
    shapes = [
        ((total, width * 2 * parts, LANES), full),
        ((total, hidden, width), full),
        ((tokens, lanes), jnp.bfloat16),
        ((tokens, lanes), jnp.bfloat16),
        ((1, LANES), full),
        ((1, LANES), full),
        ((width, LANES), full),
        ((width, LANES), full),
        ((LANES, width), full),
        ((experts, LANES), full),
    ]
    gin, *others = pl.pallas_call(
        functools.partial(outputs_body, counts),
        grid=(total,),
        in_specs=specs + [once(a.shape) for a in (blocks, in_blocks, gains, sums, output_all)],
        out_specs=(each(shapes[0][0]), each(shapes[1][0])) + tuple(once(s) for s, _ in shapes[2:]),
        out_shape=tuple(jax.ShapeDtypeStruct(*shape) for shape in shapes),
        name="outputs",
    )(*in_sums, *out_sums, blocks, in_blocks, gains, sums, output_all)
    gin = gin.reshape(total, width, parts, 2, LANES).transpose(0, 1, 3, 2, 4)
    return gin.reshape(total, width, 2, hidden), *others


def local(
    sizes,
    tokens,
    out_grad,
    doc_ids,
    expert_ids,
    gain_attn,
    w_query,
    w_key_value,
    w_output,
    gain_moe,
    w_router,
    w_expert_in,
    w_expert_out,
):
    rows, cols, depth = sizes
    group = rows * cols
    tok_rows, feat_local = tokens.shape
    width = w_query.shape[0]
    experts = w_router.shape[1]
    expert_local, hidden = w_expert_out.shape[0], w_expert_out.shape[1]
    longest_doc = min(LONGEST, tok_rows * depth // 2)
    hop_count = longest_doc // tok_rows
    own = tok_rows // group
    low, full = jnp.bfloat16, jnp.float32
    layer = lax.axis_index("dp")
    me = lax.axis_index("row") * cols + lax.axis_index("col")
    everyone = list(range(1, depth))
    hops = list(range(1, hop_count + 1))

    tokens_blocks, gains, router, docs_far, grads_shifted, grad_blocks = exchange(
        sizes,
        "gather_tokens",
        0,
        ("gather", tokens, False, 2),
        ("gather", jnp.stack([gain_attn, gain_moe])),
        ("gather", w_router.T),
        ("shift", doc_ids.reshape(-1, LANES), everyone, False),
        ("shift", out_grad, everyone, False),
        ("gather", out_grad, False, 2),
    )

    lanes = jnp.arange(LANES, dtype=jnp.int32)
    frequencies = ROPE_BASE ** ((lanes % TURN).astype(full) * (-1.0 / TURN))
    positions = (layer * tok_rows + jnp.arange(tok_rows, dtype=jnp.int32)).astype(full)
    angles = positions[:, None] * frequencies[None, :]
    cosine = jnp.cos(angles)
    sine = jnp.sin(angles) * jnp.where(lanes % (2 * TURN) < TURN, -1.0, 1.0)[None, :]

    w_pair = w_key_value.reshape(width, -1)
    block = (tok_rows, LANES)
    turned = (LANES, tok_rows)
    normed, query, pair, tokens_own, grad_own, grads_near, far_turned = call(
        project_body,
        "project",
        [
            ((tok_rows, width), low),
            (block, low),
            (block, low),
            ((own, width), low),
            ((own, width), low),
            ((group,) + turned, low),
            ((depth - 1,) + turned, low),
        ],
        tokens_blocks,
        gains,
        w_query,
        w_pair,
        cosine,
        sine,
        grad_blocks,
        grads_shifted,
    )
    far, output_blocks = exchange(
        sizes, "shift_pairs", 1, ("shift", pair, hops, False), ("gather", w_output, False, 4)
    )
    output_full = output_blocks.reshape(-1, width)

    stack = (hop_count + 1,) + block
    twice = (2 * tok_rows, LANES)
    mixed, log_total, start, grads_first = hosted(
        attend_body,
        "attend",
        [(block, low), ((2 * tok_rows, 1), full), ((tok_rows, 1), jnp.int32)],
        query,
        pair,
        far,
        doc_ids.reshape(-1, LANES),
        docs_far,
        scratch=[
            pltpu.VMEM(stack, low),
            pltpu.VMEM(stack, low),
            pltpu.VMEM(twice, low),
            pltpu.VMEM(twice, full),
        ],
        sizes=sizes,
        number=10,
        items=[("gather", far_turned[:1], True)],
    )
    (mixed_own,) = exchange(
        sizes, "swap_mixed", 2, ("swap", mixed.reshape(group, own, LANES))
    )
    rows_own, middle, weights = call(
        middle_body,
        "middle",
        [((own, width + LANES), low), ((own, width), full), ((own, LANES), full)],
        mixed_own,
        tokens_own,
        output_full,
        gains,
        router,
        expert_ids.T,
        scratch=[pltpu.VMEM(expert_ids.shape, full)],
    )
    rows_blocks, rows_shifted, grads_second = exchange(
        sizes,
        "gather_rows",
        3,
        ("gather", rows_own, False, 2),
        ("shift", rows_own, everyone, False),
        ("gather", far_turned[1:2], True),
    )
    rows_near = rows_blocks.reshape(tok_rows, -1)
    parts = hidden // LANES
    in_rows = w_expert_in.reshape(expert_local, width, 2, parts, LANES)
    in_rows = in_rows.transpose(0, 1, 3, 2, 4).reshape(expert_local, -1, LANES)
    moe_partial, back_partial, in_flat, in_part, out_part, grads_far, rows_far = local_experts(
        sizes,
        9,
        rows_near,
        grads_near.reshape(width, tok_rows),
        in_rows,
        w_expert_out,
        far_turned[2:],
        rows_shifted,
    )
    rows_far = rows_far.reshape((depth - 1) * tok_rows, -1)
    grads_far = [
        g.reshape(-1, width, tok_rows) for g in (grads_first, grads_second, grads_far)
    ]
    work = (in_flat, w_expert_out, in_part, out_part, rows_far, *grads_far)
    share = expert_local // 4
    unit = 16 * depth
    in_sums, out_sums = [], []

    def beneath(name, number, *items):
        in_sum, out_sum, *moved = cover(
            sizes, name, number, len(in_sums) * share, share, work, *items
        )
        in_sums.append(in_sum)
        out_sums.append(out_sum)
        return moved

    (back_blocks,) = beneath("swap_back", 4, ("swap", back_partial.reshape(group, own, -1)))
    middle_grad, attn_grad, logit_grad, gain_moe_part = call(
        middle_back_body,
        "middle_back",
        [
            ((own, width), full),
            ((own, width), low),
            ((own, LANES), low),
            ((1, width), full),
        ],
        back_blocks,
        grad_own,
        middle,
        weights,
        gains,
        router,
    )
    attn_grad_blocks, logit_blocks = exchange(
        sizes,
        "gather_attn_grad",
        5,
        ("gather", attn_grad, False, 2),
        ("gather", logit_grad),
    )
    query_grad, pair_grad, far_grad, output_sum = call(
        attend_back_body,
        "attend_back",
        [(block, low), (block, full), ((hop_count,) + block, low), ((group, LANES, LANES), low)],
        attn_grad_blocks.reshape(tok_rows, width),
        w_output,
        query,
        pair,
        far,
        start,
        log_total,
        mixed,
        cosine,
        sine,
        scratch=[
            pltpu.VMEM(stack, low),
            pltpu.VMEM(stack, low),
            pltpu.VMEM(twice, low),
            pltpu.VMEM(twice, low),
            pltpu.VMEM(twice, full),
            pltpu.VMEM(stack, full),
            pltpu.VMEM(stack, full),
        ],
    )
    returned, moe_blocks, output_turned = beneath(
        "shift_grads",
        6,
        ("shift", far_grad, [-d for d in hops], True),
        ("swap", moe_partial.reshape(group, own, width)),
        ("turn", output_sum.reshape(depth, width // depth, LANES)),
    )
    length = (2 * width + LANES + unit - 1) // unit * unit
    partial, sums, output_summed, gain_parts = call(
        project_back_body,
        "project_back",
        [
            ((tok_rows, width), low),
            ((length, LANES), low),
            ((width // depth, LANES), low),
            ((group, 8, LANES), full),
        ],
        query_grad,
        pair_grad,
        returned,
        normed,
        w_query,
        w_pair,
        cosine,
        sine,
        output_turned,
        logit_blocks.reshape(tok_rows, LANES),
        rows_near,
        gains,
        gain_moe_part,
    )
    partial_blocks, sums_turned, output_all, gain_blocks = beneath(
        "swap_partial",
        7,
        ("swap", partial.reshape(group, own, width)),
        ("turn", sums.reshape(depth, length // depth, LANES)),
        ("collect", output_summed),
        ("swap", gain_parts),
    )
    pieces = (group, own, LANES)
    block_out, in_grad, gain_sum, summed = call(
        results_body,
        "results",
        [
            (pieces, low),
            (pieces, low),
            ((8, LANES), full),
            ((length // depth, LANES), low),
        ],
        partial_blocks,
        moe_blocks,
        tokens_own,
        middle,
        middle_grad,
        gains,
        gain_blocks,
        sums_turned,
    )
    block_out, in_grad, gain_all, sums = beneath(
        "swap_results",
        8,
        ("swap", block_out),
        ("swap", in_grad),
        ("collect", gain_sum),
        ("collect", summed),
    )
    grad_in, grad_out, block_out, in_grad, gain_attn_sum, gain_moe_sum, query_sum, pair_sum, output_sum, router_sum = outputs(
        in_sums,
        out_sums,
        hidden,
        block_out,
        in_grad,
        gain_all,
        sums.reshape(length, LANES),
        output_all.reshape(width, LANES),
        experts,
    )
    return (
        block_out,
        in_grad,
        gain_attn_sum.reshape(LANES),
        query_sum,
        pair_sum.reshape(w_key_value.shape),
        output_sum,
        gain_moe_sum.reshape(LANES),
        router_sum.T,
        grad_in,
        grad_out,
    )


def solution(mesh):
    in_specs = (
        P("dp", ("row", "col")),
        P("dp", ("row", "col")),
        P("dp"),
        P("dp", None),
        P(("row", "col")),
        P(None, ("row", "col")),
        P(None, ("row", "col"), None),
        P(("row", "col"), None),
        P(("row", "col")),
        P(("row", "col"), None),
        P("row", None, None, "col"),
        P("row", "col", None),
    )
    out_specs = (
        P("dp", ("row", "col")),
        P("dp", ("row", "col")),
        P(("row", "col")),
        P(None, ("row", "col")),
        P(None, ("row", "col"), None),
        P(("row", "col"), None),
        P(("row", "col")),
        P(("row", "col"), None),
        P("row", None, None, "col"),
        P("row", "col", None),
    )
    sizes = (mesh.shape["row"], mesh.shape["col"], mesh.shape["dp"])
    return jax.shard_map(
        functools.partial(local, sizes),
        mesh=mesh,
        in_specs=in_specs,
        out_specs=out_specs,
        check_vma=False,
    )
```

```python
import functools

import jax
import jax.numpy as jnp
from jax import lax
from jax.experimental import pallas as pl
from jax.experimental.pallas import tpu as pltpu
from jax.sharding import PartitionSpec as P

LONGEST = 4096
HIGH = lax.Precision.HIGHEST
EPSILON = 1e-05
RESIDUAL_SCALE = 0.22
SCORE_SCALE = 0.015625
ROPE_BASE = 10000.0
MASKED = -1e30
MESH = pl.DeviceIdType.MESH
GROUP = ("row", "col")
EVERY = ("dp", "row", "col")
LANES = 128
HBM = pl.BlockSpec(memory_space=pl.ANY)
FULL = pl.BlockSpec(memory_space=pltpu.VMEM)
TURN = LANES // 4


class Moves:
    def __init__(self, sizes, kinds, sources, targets, sems):
        self.sizes, self.kinds = sizes, kinds
        self.sources, self.targets = sources, targets
        self.send_sem, self.recv_sem, self.local_sem = sems

    def place(self):
        row, col, layer = lax.axis_index("row"), lax.axis_index("col"), lax.axis_index("dp")
        return row, col, layer, row * self.sizes[1] + col

    def member(self, index):
        rows, cols, depth = self.sizes
        return {"row": index // cols, "col": lax.rem(index, cols)}

    def across(self, row):
        low = lax.rem(row, 2)
        return row + 1 - 2 * low, lax.rem(row + 2, 4), lax.rem(row + 3 - 2 * low, 4)

    def barrier(self):
        rows, cols, depth = self.sizes
        row, col, layer, me = self.place()
        group = rows * cols
        names = [kind[0] for kind in self.kinds]
        barrier = pltpu.get_barrier_semaphore()
        partners = []
        if "swap" in names or "share" in names:
            for k in range(1, group):
                partners.append(self.member(lax.rem(me + k, group)))
        elif "gather" in names:
            for other in self.across(row)[:2]:
                partners.append({"row": other})
            for k in range(1, cols):
                partners.append({"col": lax.rem(col + k, cols)})
        shifts = set()
        for kind in self.kinds:
            if kind[0] == "shift":
                for d in kind[1]:
                    shifts |= {d % depth, -d % depth}
            elif kind[0] == "turn":
                shifts |= set(range(1, depth))
        for k in sorted(shifts - {0}):
            partners.append({"dp": lax.rem(layer + k, depth)})
        ends = [(layer > 0, layer - 1), (layer < depth - 1, layer + 1)]
        ends = ends if "line" in names and not shifts else []
        for partner in partners:
            pl.semaphore_signal(barrier, inc=1, device_id=partner, device_id_type=MESH)
        for there, other in ends:

            @pl.when(there)
            def _(device={"dp": other}):
                pl.semaphore_signal(barrier, inc=1, device_id=device, device_id_type=MESH)

        expected = len(partners)
        for there, _ in ends:
            expected = expected + there.astype(jnp.int32)
        pl.semaphore_wait(barrier, expected)

    def plan(self, only):
        rows, cols, depth = self.sizes
        row, col, layer, me = self.place()
        group = rows * cols
        slots = iter(range(self.send_sem.shape[0]))
        starts, relays, sends, arrivals, local = [], [], [], [], []

        def remote(source, target, device, slot=None):
            slot = next(slots) if slot is None else slot
            return functools.partial(
                pltpu.make_async_remote_copy,
                src_ref=source,
                dst_ref=target,
                send_sem=self.send_sem.at[slot],
                recv_sem=self.recv_sem.at[slot],
                device_id=device,
                device_id_type=MESH,
            )

        for index, (kind, source, target) in enumerate(
            zip(self.kinds, self.sources, self.targets)
        ):
            item = [], [], [], [], []
            begin, follow, sent, got, stay = item

            def keep(source, target):
                sem = self.local_sem.at[index]
                stay.append(functools.partial(pltpu.make_async_copy, source, target, sem))

            def direct(source, target, device):
                copy = None, remote(source, target, device)
                begin.append(copy)
                sent.append(copy)
                got.append(copy)

            if kind[0] == "gather":
                second, parts = kind[1:]
                size = source.shape[0] // parts
                beside, above, away = self.across(row)

                def at(other, part, piece=None):
                    member = other * cols + col
                    first, length, deep = part * size, size, ()
                    if piece is not None and size % 2 == 0:
                        length = size // 2
                        first = first + piece * length
                    elif piece is not None:
                        inner = source.shape[1] // 2
                        deep = (pl.ds(piece * inner, inner),)
                    some = pl.ds(first, length)
                    return target.at[(some, member) + deep if second else (member, some) + deep]

                def to_mates(piece):
                    made = []
                    for j in range(1, cols):
                        copy = None, remote(piece, piece, {"col": lax.rem(col + j, cols)})
                        made.append(copy)
                        sent.append(copy)
                        got.append(copy)
                    return made

                for part in range(parts):
                    some = source.at[pl.ds(part * size, size)]
                    ways = []
                    for near, other, piece in ((beside, above, 0), (above, beside, 1)):
                        first = None, remote(some, at(row, part), {"row": near})
                        passed = at(near, part, piece)
                        onward = None, remote(passed, passed, {"row": other})
                        begin.append(first)
                        sent.extend([first, onward])
                        ways.append((near, piece, first, onward))
                    for near, piece, first, onward in ways:
                        nexts = [onward] + to_mates(at(near, part))
                        follow.append((2 + 3 * part, None, first[1], nexts))
                    for near, piece, first, onward in ways:
                        nexts = to_mates(at(away, part, piece))
                        follow.append((2 + 3 * parts + part, None, onward[1], nexts))
                    for j in range(1, cols):
                        direct(some, at(row, part), {"col": lax.rem(col + j, cols)})
                keep(source, target.at[:, me] if second else target.at[me])
            elif kind[0] in ("swap", "share"):
                for k in range(1, group):
                    other = lax.rem(me + k, group)
                    piece = source.at[other] if kind[0] == "swap" else source
                    direct(piece, target.at[me], self.member(other))
                keep(source.at[me] if kind[0] == "swap" else source, target.at[me])
            elif kind[0] == "turn":
                for k in range(1, depth):
                    other = lax.rem(layer + k, depth)
                    direct(source.at[other], target.at[layer], {"dp": other})
                keep(source.at[layer], target.at[layer])
            elif kind[0] == "line":
                absolute = kind[1]
                for way in (1, -1):
                    behind = layer if way == 1 else depth - 1 - layer
                    onward = layer + way
                    more = (onward >= 0) & (onward < depth)
                    mine = [next(slots) for _ in range(1, depth)]

                    def held(step, where, way=way):
                        if step == 0:
                            return source
                        if absolute:
                            return target.at[where - way * step]
                        return target.at[step - 1 if way == 1 else depth - 1 - step]

                    def sending(step, onward=onward, mine=mine, held=held):
                        device = {"dp": onward}
                        return remote(
                            held(step - 1, layer), held(step, onward), device, mine[step - 1]
                        )

                    begin.append((more, sending(1)))
                    for step in range(1, depth):
                        sent.append((more & (behind >= step - 1), sending(step)))
                        block = held(step, layer)
                        arrival = remote(block, block, {"dp": onward}, mine[step - 1])
                        nexts = [(more, sending(step + 1))] if step + 1 < depth else []
                        follow.append((4 * step, behind >= step, arrival, nexts))
                if absolute:
                    keep(source, target.at[layer])
            else:
                for at_slot, d in enumerate(kind[1]):
                    piece = source.at[at_slot] if kind[2] else source
                    direct(piece, target.at[at_slot], {"dp": lax.rem(layer + d % depth, depth)})
            if only is None or index in only:
                starts += begin
                relays += follow
                sends += sent
                arrivals += got
                local += stay
        return starts, sorted(relays, key=lambda entry: entry[0]), sends, arrivals, local

    def given(self, condition, action):
        if condition is None:
            action()
        else:
            pl.when(condition)(action)

    def start(self, only=None):
        starts, _, _, _, local = self.plan(only)
        for condition, copy in starts:
            self.given(condition, lambda copy=copy: copy().start())
        for copy in local:
            copy().start()

    def relay(self, only=None):
        for _, condition, copy, nexts in self.plan(only)[1]:

            def action(copy=copy, nexts=nexts):
                copy().wait_recv()
                for more, follower in nexts:
                    self.given(more, lambda follower=follower: follower().start())

            self.given(condition, action)

    def finish(self, only=None):
        _, _, sends, arrivals, local = self.plan(only)
        for condition, copy in arrivals:
            self.given(condition, lambda copy=copy: copy().wait_recv())
        for condition, copy in sends:
            self.given(condition, lambda copy=copy: copy().wait_send())
        for copy in local:
            copy().wait()


def planned(sizes, items):
    rows, cols, depth = sizes
    group = rows * cols
    kinds, shapes, copies = [], [], 0
    for item in items:
        name, array = item[0], item[1]
        shape = array.shape
        if name == "gather":
            assert rows == 4
            second, parts = (item[2:] + (False, 1)[len(item) - 2 :])[:2]
            kinds.append((name, second, parts))
            shape = (shape[0], group) + shape[1:] if second else (group,) + shape
            copies += parts * (4 + 5 * (cols - 1))
        elif name == "shift":
            distances, split = item[2], item[3]
            kinds.append((name, tuple(distances), split))
            shape = (len(distances),) + (shape[1:] if split else shape)
            copies += len(distances)
        elif name == "line":
            kinds.append((name, item[2]))
            shape = (depth if item[2] else depth - 1,) + shape
            copies += 2 * (depth - 1)
        else:
            kinds.append((name,))
            if name == "share":
                shape = (group,) + shape
            copies += (depth if name == "turn" else group) - 1
        shapes.append(jax.ShapeDtypeStruct(shape, array.dtype))
    sems = [
        pltpu.SemaphoreType.DMA((copies,)),
        pltpu.SemaphoreType.DMA((copies,)),
        pltpu.SemaphoreType.DMA((len(items),)),
    ]
    return tuple(kinds), shapes, sems


def exchange_body(sizes, kinds, *refs):
    count = len(kinds)
    moves = Moves(sizes, kinds, refs[:count], refs[count : 2 * count], refs[2 * count :])
    moves.barrier()
    moves.start()
    moves.relay()
    moves.finish()


def exchange(sizes, name, number, *items):
    kinds, shapes, sems = planned(sizes, items)
    return pl.pallas_call(
        functools.partial(exchange_body, sizes, kinds),
        out_shape=tuple(shapes),
        in_specs=[HBM] * len(items),
        out_specs=(HBM,) * len(items),
        scratch_shapes=sems,
        compiler_params=pltpu.CompilerParams(collective_id=number, has_side_effects=True),
        name=name,
    )(*[item[1] for item in items])


def dot(a, b, left=1, right=0, precision=None):
    return lax.dot_general(
        a,
        b,
        (((left,), (right,)), ((), ())),
        preferred_element_type=jnp.float32,
        precision=precision,
    )


def call(body, name, shapes, *arrays, scratch=()):
    return pl.pallas_call(
        body,
        out_shape=tuple(jax.ShapeDtypeStruct(*shape) for shape in shapes),
        in_specs=[FULL] * len(arrays),
        out_specs=(FULL,) * len(shapes),
        scratch_shapes=list(scratch),
        name=name,
    )(*arrays)


def lanes_of(shape):
    return lax.broadcasted_iota(jnp.int32, shape, len(shape) - 1)


def flipped(values):
    lanes = lanes_of(values.shape)
    ahead = pltpu.roll(values, LANES - TURN, 1)
    behind = pltpu.roll(values, TURN, 1)
    return jnp.where(lanes % (2 * TURN) < TURN, ahead, behind)


def beside(blocks_ref):
    return jnp.concatenate([blocks_ref[i] for i in range(blocks_ref.shape[0])], axis=1)


def gain_row(gains_ref, which):
    return beside(gains_ref).astype(jnp.float32)[which : which + 1, :]


def added(blocks):
    return functools.reduce(
        jnp.add, [blocks[i].astype(jnp.float32) for i in range(blocks.shape[0])]
    )


def own_rows(count):
    me = lax.axis_index("row") * lax.axis_size("col") + lax.axis_index("col")
    return pl.ds(pl.multiple_of(me * count, count), count)


def column(row):
    return jnp.broadcast_to(row, (8, row.shape[1])).T[:, 0:1]


def project_body(blocks, gains, w_query, w_pair, cosine, sine, near, far, normed, query, pair, own, own_grad, near_turned, far_turned):
    tokens = beside(blocks).astype(jnp.float32)
    scale = lax.rsqrt(jnp.mean(tokens * tokens, axis=1, keepdims=True) + EPSILON)
    normed[...] = (tokens * scale * gain_row(gains, 0)).astype(jnp.bfloat16)
    raw = dot(normed[...], w_query[...])
    query[...] = (raw * cosine[...] + flipped(raw) * sine[...]).astype(jnp.bfloat16)
    raw = dot(normed[...], w_pair[...])
    keys = lanes_of(raw.shape) < LANES // 2
    turned = raw * cosine[...] + flipped(raw) * sine[...]
    pair[...] = jnp.where(keys, turned, raw).astype(jnp.bfloat16)
    for i in range(blocks.shape[0]):
        own[:, i * LANES : (i + 1) * LANES] = blocks[i, own_rows(own.shape[0]), :]
    for source, target in ((near, near_turned), (far, far_turned)):
        for i in range(source.shape[0]):
            scaled = RESIDUAL_SCALE * source[i].astype(jnp.float32)
            target[i] = scaled.T.astype(jnp.bfloat16)
    for i in range(near.shape[0]):
        own_grad[:, i * LANES : (i + 1) * LANES] = near[i, own_rows(own.shape[0]), :]


def doubled(pair, keys_ref, values_ref, at):
    wide = pair.astype(jnp.float32)
    other = pltpu.roll(wide, LANES // 2, 1)
    keys = lanes_of(wide.shape) < LANES // 2
    keys_ref[at] = jnp.where(keys, wide, other).astype(jnp.bfloat16)
    values_ref[at] = jnp.where(keys, other, wide).astype(jnp.bfloat16)


def per_head(values):
    first = lanes_of(values.shape) < LANES // 2
    zero = jnp.zeros_like(values)
    return jnp.concatenate(
        [jnp.where(first, values, zero), jnp.where(first, zero, values)], axis=0
    )


def tile_scores(queries, keys_ref, starts, row, block, last, tokens):
    scores = dot(queries, keys_ref[block], 1, 1) * SCORE_SCALE
    at = lanes_of(scores.shape) + block * tokens
    allowed = at >= starts
    if block == last:
        place = row + lax.broadcasted_iota(jnp.int32, scores.shape, 0)
        allowed = allowed & (at <= place + block * tokens)
    return jnp.where(allowed, scores, MASKED)


def doc_row(docs):
    rows = [docs[i : i + 1, :] for i in range(docs.shape[0])]
    return jnp.concatenate(rows, axis=1).astype(jnp.float32)


def attend_body(query, pair, far, docs, far_docs, mixed, log_total, start, keys, values, queries, out):
    tokens = query.shape[0]
    last = far.shape[0]
    layer = lax.axis_index("dp")
    here = doc_row(docs[...])
    mine = column(here)
    before = jnp.sum((here < mine).astype(jnp.float32), axis=1, keepdims=True)
    for d in range(1, last + 1):
        fewer = (doc_row(far_docs[d - 1]) < mine) | (layer < d)
        before = before + jnp.sum(fewer.astype(jnp.float32), axis=1, keepdims=True)
    start[...] = before.astype(jnp.int32)
    doubled(pair[...], keys, values, last)
    for d in range(1, last + 1):
        doubled(far[d - 1], keys, values, last - d)
    queries[...] = per_head(query[...].astype(jnp.float32)).astype(jnp.bfloat16)
    step = 256

    def tile(i, carry):
        rows = pl.ds(pl.multiple_of(i * step, step), step)
        row = lax.rem(i * step, tokens)
        starts = start[pl.ds(pl.multiple_of(row, step), step), :]
        parts = [
            tile_scores(queries[rows, :], keys, starts, row, block, last, tokens)
            for block in range(last + 1)
        ]
        top = functools.reduce(
            jnp.maximum, [jnp.max(part, axis=1, keepdims=True) for part in parts]
        )
        parts = [jnp.exp(part - top) for part in parts]
        total = functools.reduce(jnp.add, [jnp.sum(p, axis=1, keepdims=True) for p in parts])
        sums = [
            dot(part.astype(jnp.bfloat16), values[block]) for block, part in enumerate(parts)
        ]
        out[rows, :] = functools.reduce(jnp.add, sums) / total
        log_total[rows, :] = top + jnp.log(total)
        return carry

    lax.fori_loop(0, 2 * tokens // step, tile, 0)
    first = lanes_of((tokens, LANES)) < LANES // 2
    mixed[...] = jnp.where(first, out[:tokens, :], out[tokens:, :]).astype(jnp.bfloat16)


def attend_back_body(grad, w_output, query, pair, far, start, log_total, mixed, cosine, sine, query_grad, pair_grad, far_grad, output_grad, keys, values, queries, grads, turned, key_sums, value_sums):
    tokens = query.shape[0]
    last = far.shape[0]
    doubled(pair[...], keys, values, last)
    for d in range(1, last + 1):
        doubled(far[d - 1], keys, values, last - d)
    queries[...] = per_head(query[...].astype(jnp.float32)).astype(jnp.bfloat16)
    grads[...] = per_head(dot(grad[...], w_output[...], 1, 1)).astype(jnp.bfloat16)
    output_sum = dot(mixed[...], grad[...], 0, 0).astype(jnp.bfloat16)
    for i in range(output_grad.shape[0]):
        output_grad[i] = output_sum[:, i * LANES : (i + 1) * LANES]
    key_sums[...] = jnp.zeros_like(key_sums)
    value_sums[...] = jnp.zeros_like(value_sums)
    step = 256

    def tile(i, carry):
        rows = pl.ds(pl.multiple_of(i * step, step), step)
        row = lax.rem(i * step, tokens)
        starts = start[pl.ds(pl.multiple_of(row, step), step), :]
        asked, given, level = queries[rows, :], grads[rows, :], log_total[rows, :]
        chances, products = [], []
        for block in range(last + 1):
            scores = tile_scores(asked, keys, starts, row, block, last, tokens)
            chances.append(jnp.exp(scores - level))
            products.append(dot(given, values[block], 1, 1))
        delta = functools.reduce(
            jnp.add,
            [jnp.sum(p * q, axis=1, keepdims=True) for p, q in zip(chances, products)],
        )
        total = jnp.zeros((step, LANES), jnp.float32)
        for block in range(last + 1):
            back = (chances[block] * (products[block] - delta)).astype(jnp.bfloat16)
            total = total + dot(back, keys[block])
            key_sums[block] += dot(back, asked, 0, 0)
            value_sums[block] += dot(chances[block].astype(jnp.bfloat16), given, 0, 0)
        turned[rows, :] = total
        return carry

    lax.fori_loop(0, 2 * tokens // step, tile, 0)
    first = lanes_of((tokens, LANES)) < LANES // 2
    raw = jnp.where(first, turned[:tokens, :], turned[tokens:, :]) * SCORE_SCALE
    query_grad[...] = (raw * cosine[...] - flipped(raw) * sine[...]).astype(jnp.bfloat16)

    def joined(block):
        by_key, by_value = key_sums[block], value_sums[block]
        by_key = (by_key + pltpu.roll(by_key, LANES // 2, 1)) * SCORE_SCALE
        by_value = by_value + pltpu.roll(by_value, LANES // 2, 1)
        return jnp.where(first, by_key, by_value)

    pair_grad[...] = joined(last)
    for d in range(1, last + 1):
        far_grad[d - 1] = joined(last - d).astype(jnp.bfloat16)


def router_rows(router):
    rows = beside(router).astype(jnp.float32)
    blank = jnp.zeros((LANES - rows.shape[0], rows.shape[1]), jnp.float32)
    return jnp.concatenate([rows, blank], axis=0)


def middle_body(mixed, own, w_output, gains, router, ids_turned, rows, middle, weights, ids_ref):
    experts = router.shape[1]
    width = own.shape[1]
    attn = dot(beside(mixed), w_output[...])
    value = own[...].astype(jnp.float32) + RESIDUAL_SCALE * attn
    middle[...] = value
    scale = lax.rsqrt(jnp.mean(value * value, axis=1, keepdims=True) + EPSILON)
    normed = value * scale * gain_row(gains, 1)
    logits = dot(normed, router_rows(router), 1, 1, precision=HIGH)
    count = own.shape[0]
    ids_ref[...] = ids_turned[...].astype(jnp.float32).T
    ids = ids_ref[own_rows(count), :]
    lanes = lanes_of((count, LANES))
    chosen = jnp.zeros((count, LANES), jnp.float32)
    for k in range(ids.shape[1]):
        chosen = chosen + (ids[:, k : k + 1] == lanes.astype(jnp.float32)).astype(
            jnp.float32
        )
    top = jnp.max(jnp.where(lanes < experts, logits, MASKED), axis=1, keepdims=True)
    terms = jnp.exp(jnp.minimum(logits - top, 0.0)) * chosen
    share = terms / jnp.sum(terms, axis=1, keepdims=True)
    weights[...] = share
    high = share.astype(jnp.bfloat16)
    low = share - high.astype(jnp.float32)
    rows[:, :width] = normed.astype(jnp.bfloat16)
    rows[:, width:] = (high.astype(jnp.float32) + pltpu.roll(low, LANES // 2, 1)).astype(
        jnp.bfloat16
    )


def middle_back_body(back, out_grad, middle, weights, gains, router, middle_grad, attn_grad, logit_grad, gain_part):
    width = middle.shape[1]
    normed_grad = back[0, :, :width].astype(jnp.float32)
    weight_grad = back[0, :, width:].astype(jnp.float32)
    for i in range(1, back.shape[0]):
        normed_grad = normed_grad + back[i, :, :width].astype(jnp.float32)
        weight_grad = weight_grad + back[i, :, width:].astype(jnp.float32)
    share, value = weights[...], middle[...]
    mean = jnp.sum(share * weight_grad, axis=1, keepdims=True)
    logit = share * (weight_grad - mean)
    logit_grad[...] = logit.astype(jnp.bfloat16)
    normed_grad = normed_grad + dot(logit, router_rows(router), precision=HIGH)
    scale = lax.rsqrt(jnp.mean(value * value, axis=1, keepdims=True) + EPSILON)
    gain_part[...] = jnp.sum(normed_grad * value * scale, axis=0, keepdims=True)
    scaled = normed_grad * gain_row(gains, 1)
    norm_dot = jnp.sum(scaled * value, axis=1, keepdims=True)
    total = (
        out_grad[...].astype(jnp.float32)
        + scale * scaled
        - value * (scale * scale * scale * norm_dot / width)
    )
    middle_grad[...] = total
    attn_grad[...] = (RESIDUAL_SCALE * total).astype(jnp.bfloat16)


def project_back_body(query_grad, pair_grad, returned, normed, w_query, w_pair, cosine, sine, output_turned, logit, rows, gains, gain_moe, partial, sums, output_summed, gain_parts):
    layer = lax.axis_index("dp")
    depth = lax.axis_size("dp")
    total = pair_grad[...]
    for i in range(returned.shape[0]):
        total = total + jnp.where(
            layer + i + 1 < depth, returned[i].astype(jnp.float32), 0.0
        )
    keys = lanes_of(total.shape) < LANES // 2
    turned = total * cosine[...] - flipped(total) * sine[...]
    pair_low = jnp.where(keys, turned, total).astype(jnp.bfloat16)
    query_low = query_grad[...]
    whole = dot(query_low, w_query[...], 1, 1) + dot(pair_low, w_pair[...], 1, 1)
    partial[...] = whole.astype(jnp.bfloat16)
    gain_attn = jnp.sum(whole * normed[...].astype(jnp.float32), axis=0, keepdims=True)
    gain_attn = gain_attn / gain_row(gains, 0)
    gain_parts[...] = jnp.zeros_like(gain_parts)
    for i in range(gain_parts.shape[0]):
        at = slice(i * LANES, (i + 1) * LANES)
        gain_parts[i, 0:1, :] = gain_attn[:, at]
        gain_parts[i, 1:2, :] = gain_moe[0:1, at]
    width = normed.shape[1]
    sums[:width, :] = dot(normed[...], query_low, 0, 0).astype(jnp.bfloat16)
    sums[width : 2 * width, :] = dot(normed[...], pair_low, 0, 0).astype(jnp.bfloat16)
    output_summed[...] = added(output_turned).astype(jnp.bfloat16)
    mine = rows[:, own_rows(LANES)]
    sums[2 * width : 2 * width + LANES, :] = dot(logit[...], mine, 0, 0).astype(jnp.bfloat16)


def results_body(blocks, moe, own, middle, middle_grad, gains, gain_blocks, turned, block_out, in_grad, gain_sum, summed):
    gain_sum[...] = added(gain_blocks)
    summed[...] = added(turned).astype(jnp.bfloat16)
    width = own.shape[1]
    normed_grad = blocks[0].astype(jnp.float32)
    branch = moe[0].astype(jnp.float32)
    for i in range(1, blocks.shape[0]):
        normed_grad = normed_grad + blocks[i].astype(jnp.float32)
        branch = branch + moe[i].astype(jnp.float32)
    value = own[...].astype(jnp.float32)
    scale = lax.rsqrt(jnp.mean(value * value, axis=1, keepdims=True) + EPSILON)
    scaled = normed_grad * gain_row(gains, 0)
    norm_dot = jnp.sum(scaled * value, axis=1, keepdims=True)
    grad = (
        middle_grad[...] + scale * scaled - value * (scale * scale * scale * norm_dot / width)
    ).astype(jnp.bfloat16)
    out = (middle[...] + RESIDUAL_SCALE * branch).astype(jnp.bfloat16)
    for i in range(block_out.shape[0]):
        at = slice(i * LANES, (i + 1) * LANES)
        block_out[i] = out[:, at]
        in_grad[i] = grad[:, at]


def expert_terms(gate_up, active_grad, weight):
    hidden = active_grad.shape[0]
    gate, up = gate_up[:hidden], gate_up[hidden:]
    sigmoid = jax.nn.sigmoid(gate)
    silu = gate * sigmoid
    ungated = silu * up
    active = (ungated * weight).astype(jnp.bfloat16)
    scaled = active_grad * weight
    gate_grad = (scaled * up * sigmoid * (1.0 + gate * (1.0 - sigmoid))).astype(jnp.bfloat16)
    up_grad = (scaled * silu).astype(jnp.bfloat16)
    return active, jnp.concatenate([gate_grad, up_grad], axis=0), active_grad * ungated


def weight_rows(extra):
    turned = extra.astype(jnp.float32).T
    return turned[: LANES // 2] + turned[LANES // 2 :]


def local_experts_body(sizes, kinds, rows_ref, grads_ref, in_ref, out_ref, sent_grads, sent_rows, moe_ref, back_ref, flat_ref, in_sum, out_sum, got_grads, got_rows, moe_acc, back_acc, share, weights, spread, *sems):
    step, steps = pl.program_id(0), pl.num_programs(0)
    each, hidden, width = out_ref.shape
    parts = hidden // LANES
    moves = Moves(sizes, kinds, [sent_grads, sent_rows], [got_grads, got_rows], sems)

    @pl.when(step == 0)
    def _():
        moves.barrier()
        moves.start()
        moe_acc[...] = jnp.zeros_like(moe_acc)
        back_acc[...] = jnp.zeros_like(back_acc)
        share[...] = jnp.zeros_like(share)
        weights[...] = weight_rows(rows_ref[:, width:])

    @pl.when(step == steps // 2)
    def _():
        moves.relay([0])

    for i in range(each):
        spread[i] = in_ref[i].astype(jnp.float32)
        for part in range(parts):
            for half in range(2):
                at = half * hidden + part * LANES
                flat_ref[i, :, at : at + LANES] = spread[
                    i, pl.ds(part * 2 + half, width, stride=2 * parts), :
                ].astype(jnp.bfloat16)
        expert = (lax.axis_index("row") * steps + step) * each + i
        active, gate_up_grad, shares = expert_terms(
            dot(flat_ref[i], rows_ref[:, :width], 0, 1),
            dot(out_ref[i], grads_ref[...]),
            weights[pl.ds(expert, 1), :],
        )
        share[pl.ds(expert, 1), :] = jnp.sum(shares, axis=0, keepdims=True)
        moe_acc[...] += dot(active, out_ref[i], 0, 0)
        back_acc[...] += dot(gate_up_grad, flat_ref[i], 0, 1)
        in_sum[i] = dot(gate_up_grad, rows_ref[:, :width]).astype(jnp.bfloat16)
        out_sum[i] = dot(active, grads_ref[...], 1, 1).astype(jnp.bfloat16)

    @pl.when(step == steps - 1)
    def _():
        moe_ref[...] = moe_acc[...].astype(jnp.bfloat16)
        back_ref[:, :width] = back_acc[...].astype(jnp.bfloat16)
        back_ref[:, width:] = share[...].T.astype(jnp.bfloat16)
        moves.relay([1])
        moves.finish()


def local_experts(sizes, number, rows, grads, w_in, w_out, sent_grads, sent_rows):
    tokens, wide = rows.shape
    experts, hidden, width = w_out.shape
    each = 1
    low = jnp.bfloat16
    kinds, shapes, sems = planned(
        sizes,
        [
            ("gather", sent_grads, True, sent_grads.shape[0]),
            ("gather", sent_rows, True, sent_rows.shape[0]),
        ],
    )
    whole = lambda s: pl.BlockSpec(s, lambda e: (0,) * len(s))
    some = lambda s: pl.BlockSpec((each,) + s[1:], lambda e: (e,) + (0,) * (len(s) - 1))
    outs = [
        (tokens, width),
        (tokens, wide),
        (experts, width, 2 * hidden),
        (experts, 2 * hidden, width),
        (experts, hidden, width),
    ]
    return pl.pallas_call(
        functools.partial(local_experts_body, sizes, kinds),
        grid=(experts // each,),
        in_specs=[
            whole(rows.shape),
            whole(grads.shape),
            some(w_in.shape),
            some(w_out.shape),
            HBM,
            HBM,
        ],
        out_specs=(whole(outs[0]), whole(outs[1]), *[some(s) for s in outs[2:]], HBM, HBM),
        out_shape=tuple(jax.ShapeDtypeStruct(s, low) for s in outs) + tuple(shapes),
        scratch_shapes=[
            pltpu.VMEM((tokens, width), jnp.float32),
            pltpu.VMEM((tokens, width), jnp.float32),
            pltpu.VMEM((LANES, tokens), jnp.float32),
            pltpu.VMEM((LANES // 2, tokens), jnp.float32),
            pltpu.VMEM((each,) + w_in.shape[1:], jnp.float32),
        ]
        + sems,
        compiler_params=pltpu.CompilerParams(collective_id=number, has_side_effects=True),
        name="local_experts",
    )(rows, grads, w_in, w_out, sent_grads, sent_rows)


class Sums:
    def __init__(self, rows, grads, weights, whole, turned, load_sem, *sums):
        self.rows, self.grads, self.weights = rows, grads, weights
        self.whole, self.turned, self.load_sem, self.sums = whole, turned, load_sem, sums

    def loads(self, rows_far, grads_far):
        return [
            pltpu.make_async_copy(rows_far, self.rows, self.load_sem.at[0]),
            pltpu.make_async_copy(grads_far, self.grads, self.load_sem.at[1]),
        ]

    def ready(self):
        layers, width, tokens = self.grads.shape
        for i in range(layers):
            self.weights[i] = weight_rows(self.rows[i * tokens : (i + 1) * tokens, width:])

    def make(self, index, w_in, w_out, in_part, out_part):
        layers, width, tokens = self.grads.shape
        hidden = w_out.shape[0]

        def part_of(at, pieces):
            first = at * tokens if isinstance(at, int) else pl.multiple_of(at * tokens, tokens)
            block = self.rows[pl.ds(first, pieces * tokens), :width]
            weight = jnp.concatenate(
                [self.weights[at + i, pl.ds(index, 1), :] for i in range(pieces)], axis=1
            )
            active_grad = jnp.concatenate(
                [dot(w_out, self.grads[at + i]) for i in range(pieces)], axis=1
            )
            active, gate_up_grad, _ = expert_terms(dot(w_in, block, 0, 1), active_grad, weight)
            out_total = functools.reduce(
                jnp.add,
                [
                    dot(active[:, i * tokens : (i + 1) * tokens], self.grads[at + i], 1, 1)
                    for i in range(pieces)
                ],
            )
            return dot(gate_up_grad, block), out_total

        if not self.sums:
            self.whole[...], out_total = part_of(0, layers)
        else:
            self.whole[...] = jnp.zeros_like(self.whole)
            (out_acc,) = self.sums
            out_acc[...] = jnp.zeros_like(out_acc)

            def more(i, carry):
                in_more, out_more = part_of(i, 1)
                self.whole[...] += in_more
                out_acc[...] += out_more
                return carry

            lax.fori_loop(0, layers, more, 0)
            out_total = out_acc[...]
        parts = hidden // LANES

        def turn(i, carry):
            at = pl.ds(pl.multiple_of(i * LANES, LANES), LANES)
            rows_of = pl.ds(lax.rem(i, parts) * 2 + i // parts, width, stride=2 * parts)
            total = self.whole[at, :] + in_part[0, at, :].astype(jnp.float32)
            self.turned[rows_of, :] = total.T
            return carry

        lax.fori_loop(0, 2 * parts, turn, 0)
        return out_total + out_part[0].astype(jnp.float32)


def sums_scratch(layers, tokens, width, hidden):
    low, full = jnp.bfloat16, jnp.float32
    return [
        pltpu.VMEM((layers * tokens, width + LANES), low),
        pltpu.VMEM((layers, width, tokens), low),
        pltpu.VMEM((layers, LANES // 2, tokens), full),
        pltpu.VMEM((2 * hidden, width), full),
        pltpu.VMEM((width * 2 * hidden // LANES, LANES), full),
        pltpu.SemaphoreType.DMA((2,)),
    ] + ([pltpu.VMEM((hidden, width), full)] if layers > 4 else [])


def widened(turned, target):
    size = target.shape[1] // 4

    def piece(i, carry):
        at = pl.ds(pl.multiple_of(i * size, size), size)
        target[0, at, :] = turned[at, :].astype(target.dtype)
        return carry

    lax.fori_loop(0, 4, piece, 0)


def cover_body(sizes, kinds, experts, first, in_ref, out_ref, in_part, out_part, rows_far, grads_far, *refs):
    count = len(kinds)
    sources, in_sum, out_sum = refs[:count], refs[count], refs[count + 1]
    targets = refs[count + 2 : 2 * count + 2]
    sums = Sums(*refs[2 * count + 2 : -3])
    moves = Moves(sizes, kinds, sources, targets, refs[-3:])
    step = pl.program_id(0)

    @pl.when(step == 0)
    def _():
        loads = sums.loads(rows_far, grads_far)
        for load in loads:
            load.start()
        moves.barrier()
        moves.start()
        for load in loads:
            load.wait()
        sums.ready()

    index = lax.axis_index("row") * experts + first + step
    out_total = sums.make(index, in_ref[0], out_ref[0], in_part, out_part)
    widened(sums.turned, in_sum)
    out_sum[0] = out_total.astype(jnp.bfloat16)

    @pl.when(step == pl.num_programs(0) - 1)
    def _():
        moves.relay()
        moves.finish()


def cover(sizes, name, number, first, count, work, *items):
    w_in, w_out, in_part, out_part, rows_far, grads_far = work
    layers, width, tokens = grads_far.shape
    experts, hidden, _ = w_out.shape
    kinds, shapes, sems = planned(sizes, items)
    each = lambda s: pl.BlockSpec((1,) + s[1:], lambda e: (first + e, 0, 0))
    out = lambda s: pl.BlockSpec((1,) + s[1:], lambda e: (e, 0, 0))
    outs = [(count, width * 2 * hidden // LANES, LANES), (count, hidden, width)]
    return pl.pallas_call(
        functools.partial(cover_body, sizes, kinds, experts, first),
        grid=(count,),
        in_specs=[each(a.shape) for a in work[:4]] + [HBM] * (2 + len(items)),
        out_specs=tuple(out(s) for s in outs) + (HBM,) * len(items),
        out_shape=tuple(jax.ShapeDtypeStruct(s, jnp.bfloat16) for s in outs) + tuple(shapes),
        scratch_shapes=sums_scratch(layers, tokens, width, hidden) + sems,
        compiler_params=pltpu.CompilerParams(collective_id=number, has_side_effects=True),
        name=name,
    )(*work, *[item[1] for item in items])


def order_of(total, late):
    if not late:
        return list(range(total))
    share = (total - late) // late
    order = []
    for i in range(late):
        order += list(range(i * share, (i + 1) * share)) + [total - late + i]
    return order


def picked(values, step):
    chosen = values[0]
    for i, value in enumerate(values[1:], 1):
        if value != values[i - 1]:
            chosen = jnp.where(step >= i, value, chosen)
    return chosen


def outputs_body(counts, order, *refs):
    pieces, late = len(counts), len(order) - sum(counts)
    in_sums, out_sums = refs[:pieces], refs[pieces : 2 * pieces]
    refs = refs[2 * pieces :]
    blocks, in_blocks, gains, sums_all, output_all = refs[:5]
    work, refs = (refs[5:11], refs[11:]) if late else ((), refs[5:])
    gin, gout, block_out, in_grad, gain_attn, gain_moe, query, pair, output, router = refs[:10]
    sums = Sums(*refs[10:]) if late else None
    step = pl.program_id(0)
    width = gout.shape[2]

    @pl.when(step == 0)
    def _():
        if late:
            for load in sums.loads(*work[4:]):
                load.start()
        for i in range(blocks.shape[0]):
            at = pl.ds(i * blocks.shape[1], blocks.shape[1])
            block_out[at, :] = blocks[i]
            in_grad[at, :] = in_blocks[i]
        gain_sum = jnp.sum(gains[...], axis=0)
        gain_attn[...] = gain_sum[0:1, :]
        gain_moe[...] = gain_sum[1:2, :]
        query[...] = sums_all[:width, :].astype(jnp.float32)
        pair[...] = sums_all[width : 2 * width, :].astype(jnp.float32)
        for i in range(width // LANES):
            at = slice(i * LANES, (i + 1) * LANES)
            output[:, at] = output_all[at, :].astype(jnp.float32)
        router[...] = sums_all[2 * width : 2 * width + router.shape[0], :].astype(jnp.float32)

    expert = picked(order, step)
    first = 0
    for count, in_sum, out_sum in zip(counts, in_sums, out_sums):

        @pl.when((expert >= first) & (expert < first + count))
        def _(in_sum=in_sum, out_sum=out_sum):
            gout[0] = out_sum[0].astype(jnp.float32)
            widened(in_sum.at[0], gin)

        first += count
    if late:

        @pl.when(expert >= first)
        def _():
            @pl.when(expert == first)
            def _():
                for load in sums.loads(*work[4:]):
                    load.wait()
                sums.ready()

            index = lax.axis_index("row") * len(order) + expert
            gout[0] = sums.make(index, work[0][0], work[1][0], *work[2:4])
            widened(sums.turned, gin)


def outputs(in_sums, out_sums, work, blocks, in_blocks, gains, sums, output_all, experts):
    w_out, grads_far = work[1], work[5]
    total, hidden, width = w_out.shape
    layers, _, tokens = grads_far.shape
    counts = [s.shape[0] for s in in_sums]
    late = total - sum(counts)
    order = order_of(total, late)
    parts = hidden // LANES
    lanes = blocks.shape[2]
    once = lambda s: pl.BlockSpec(s, lambda e: (0,) * len(s))
    each = lambda s: pl.BlockSpec((1,) + s[1:], lambda e: (picked(order, e), 0, 0))
    specs = []
    for arrays in (in_sums, out_sums):
        first = 0
        for array in arrays:
            places, last = [], 0
            for expert in order:
                if first <= expert < first + array.shape[0]:
                    last = expert - first
                elif expert < total - late and expert >= first + array.shape[0]:
                    last = array.shape[0] - 1
                places.append(last)
            specs.append(
                pl.BlockSpec(
                    (1,) + array.shape[1:], lambda e, places=places: (picked(places, e), 0, 0)
                )
            )
            first += array.shape[0]
    more, scratch = (), []
    if late:
        turns, place = [], total - late
        for expert in order:
            turns.append(place)
            place = min(place + (expert >= total - late), total - 1)
        ahead = lambda s: pl.BlockSpec((1,) + s[1:], lambda e: (picked(turns, e), 0, 0))
        more = work
        scratch = sums_scratch(layers, tokens, width, hidden)
    full = jnp.float32
    shapes = [
        ((total, width * 2 * parts, LANES), full),
        ((total, hidden, width), full),
        ((tokens, lanes), jnp.bfloat16),
        ((tokens, lanes), jnp.bfloat16),
        ((1, LANES), full),
        ((1, LANES), full),
        ((width, LANES), full),
        ((width, LANES), full),
        ((LANES, width), full),
        ((experts, LANES), full),
    ]
    small = (blocks, in_blocks, gains, sums, output_all)
    gin, *others = pl.pallas_call(
        functools.partial(outputs_body, counts, order),
        grid=(total,),
        in_specs=specs
        + [once(a.shape) for a in small]
        + [ahead(a.shape) for a in more[:4]]
        + [HBM for _ in more[4:]],
        out_specs=(each(shapes[0][0]), each(shapes[1][0])) + tuple(once(s) for s, _ in shapes[2:]),
        out_shape=tuple(jax.ShapeDtypeStruct(*shape) for shape in shapes),
        scratch_shapes=scratch,
        name="outputs",
    )(*in_sums, *out_sums, *small, *more)
    gin = gin.reshape(total, width, parts, 2, LANES).transpose(0, 1, 3, 2, 4)
    return gin.reshape(total, width, 2, hidden), *others


def local(
    sizes,
    tokens,
    out_grad,
    doc_ids,
    expert_ids,
    gain_attn,
    w_query,
    w_key_value,
    w_output,
    gain_moe,
    w_router,
    w_expert_in,
    w_expert_out,
):
    rows, cols, depth = sizes
    group = rows * cols
    tok_rows, feat_local = tokens.shape
    width = w_query.shape[0]
    experts = w_router.shape[1]
    expert_local, hidden = w_expert_out.shape[0], w_expert_out.shape[1]
    longest_doc = min(LONGEST, tok_rows * depth // 2)
    hop_count = longest_doc // tok_rows
    own = tok_rows // group
    low, full = jnp.bfloat16, jnp.float32
    layer = lax.axis_index("dp")
    me = lax.axis_index("row") * cols + lax.axis_index("col")
    hops = list(range(1, hop_count + 1))

    tokens_blocks, gains, router, docs_far, grads_shifted, grad_blocks = exchange(
        sizes,
        "gather_tokens",
        0,
        ("gather", tokens, False, 2),
        ("share", jnp.stack([gain_attn, gain_moe])),
        ("share", w_router.T),
        ("line", doc_ids.reshape(-1, LANES), False),
        ("line", out_grad, False),
        ("gather", out_grad, False, 2),
    )

    lanes = jnp.arange(LANES, dtype=jnp.int32)
    frequencies = ROPE_BASE ** ((lanes % TURN).astype(full) * (-1.0 / TURN))
    positions = (layer * tok_rows + jnp.arange(tok_rows, dtype=jnp.int32)).astype(full)
    angles = positions[:, None] * frequencies[None, :]
    cosine = jnp.cos(angles)
    sine = jnp.sin(angles) * jnp.where(lanes % (2 * TURN) < TURN, -1.0, 1.0)[None, :]

    w_pair = w_key_value.reshape(width, -1)
    block = (tok_rows, LANES)
    turned = (LANES, tok_rows)
    normed, query, pair, tokens_own, grad_own, grads_near, far_turned = call(
        project_body,
        "project",
        [
            ((tok_rows, width), low),
            (block, low),
            (block, low),
            ((own, width), low),
            ((own, width), low),
            ((group,) + turned, low),
            ((depth - 1,) + turned, low),
        ],
        tokens_blocks,
        gains,
        w_query,
        w_pair,
        cosine,
        sine,
        grad_blocks,
        grads_shifted,
    )
    far, output_blocks = exchange(
        sizes, "shift_pairs", 1, ("shift", pair, hops, False), ("gather", w_output, False, 4)
    )
    output_full = output_blocks.reshape(-1, width)

    stack = (hop_count + 1,) + block
    twice = (2 * tok_rows, LANES)
    mixed, log_total, start = call(
        attend_body,
        "attend",
        [(block, low), ((2 * tok_rows, 1), full), ((tok_rows, 1), jnp.int32)],
        query,
        pair,
        far,
        doc_ids.reshape(-1, LANES),
        docs_far,
        scratch=[
            pltpu.VMEM(stack, low),
            pltpu.VMEM(stack, low),
            pltpu.VMEM(twice, low),
            pltpu.VMEM(twice, full),
        ],
    )
    (mixed_own,) = exchange(
        sizes, "swap_mixed", 2, ("swap", mixed.reshape(group, own, LANES))
    )
    rows_own, middle, weights = call(
        middle_body,
        "middle",
        [((own, width + LANES), low), ((own, width), full), ((own, LANES), full)],
        mixed_own,
        tokens_own,
        output_full,
        gains,
        router,
        expert_ids.T,
        scratch=[pltpu.VMEM(expert_ids.shape, full)],
    )
    rows_blocks, rows_shifted = exchange(
        sizes, "gather_rows", 3, ("gather", rows_own, False, 2), ("line", rows_own, False)
    )
    rows_near = rows_blocks.reshape(tok_rows, -1)
    parts = hidden // LANES
    in_rows = w_expert_in.reshape(expert_local, width, 2, parts, LANES)
    in_rows = in_rows.transpose(0, 1, 3, 2, 4).reshape(expert_local, -1, LANES)
    moe_partial, back_partial, in_flat, in_part, out_part, grads_far, rows_far = local_experts(
        sizes,
        9,
        rows_near,
        grads_near.reshape(width, tok_rows),
        in_rows,
        w_expert_out,
        far_turned,
        rows_shifted,
    )
    rows_far = rows_far.reshape((depth - 1) * tok_rows, -1)
    grads_far = grads_far.reshape(depth - 1, width, tok_rows)
    work = (in_flat, w_expert_out, in_part, out_part, rows_far, grads_far)
    share = expert_local // 4
    unit = 16 * depth
    in_sums, out_sums = [], []

    def beneath(name, number, *items):
        in_sum, out_sum, *moved = cover(
            sizes, name, number, len(in_sums) * share, share, work, *items
        )
        in_sums.append(in_sum)
        out_sums.append(out_sum)
        return moved

    (back_blocks,) = beneath("swap_back", 4, ("swap", back_partial.reshape(group, own, -1)))
    middle_grad, attn_grad, logit_grad, gain_moe_part = call(
        middle_back_body,
        "middle_back",
        [
            ((own, width), full),
            ((own, width), low),
            ((own, LANES), low),
            ((1, width), full),
        ],
        back_blocks,
        grad_own,
        middle,
        weights,
        gains,
        router,
    )
    attn_grad_blocks, logit_blocks = exchange(
        sizes,
        "gather_attn_grad",
        5,
        ("gather", attn_grad, False, 2),
        ("gather", logit_grad),
    )
    query_grad, pair_grad, far_grad, output_sum = call(
        attend_back_body,
        "attend_back",
        [(block, low), (block, full), ((hop_count,) + block, low), ((group, LANES, LANES), low)],
        attn_grad_blocks.reshape(tok_rows, width),
        w_output,
        query,
        pair,
        far,
        start,
        log_total,
        mixed,
        cosine,
        sine,
        scratch=[
            pltpu.VMEM(stack, low),
            pltpu.VMEM(stack, low),
            pltpu.VMEM(twice, low),
            pltpu.VMEM(twice, low),
            pltpu.VMEM(twice, full),
            pltpu.VMEM(stack, full),
            pltpu.VMEM(stack, full),
        ],
    )
    returned, moe_blocks, output_turned = beneath(
        "shift_grads",
        6,
        ("shift", far_grad, [-d for d in hops], True),
        ("swap", moe_partial.reshape(group, own, width)),
        ("turn", output_sum.reshape(depth, width // depth, LANES)),
    )
    length = (2 * width + LANES + unit - 1) // unit * unit
    partial, sums, output_summed, gain_parts = call(
        project_back_body,
        "project_back",
        [
            ((tok_rows, width), low),
            ((length, LANES), low),
            ((width // depth, LANES), low),
            ((group, 8, LANES), full),
        ],
        query_grad,
        pair_grad,
        returned,
        normed,
        w_query,
        w_pair,
        cosine,
        sine,
        output_turned,
        logit_blocks.reshape(tok_rows, LANES),
        rows_near,
        gains,
        gain_moe_part,
    )
    partial_blocks, sums_turned, gain_blocks = beneath(
        "swap_partial",
        7,
        ("swap", partial.reshape(group, own, width)),
        ("turn", sums.reshape(depth, length // depth, LANES)),
        ("swap", gain_parts),
    )
    pieces = (group, own, LANES)
    block_out, in_grad, gain_sum, summed = call(
        results_body,
        "results",
        [
            (pieces, low),
            (pieces, low),
            ((8, LANES), full),
            ((length // depth, LANES), low),
        ],
        partial_blocks,
        moe_blocks,
        tokens_own,
        middle,
        middle_grad,
        gains,
        gain_blocks,
        sums_turned,
    )
    results = [
        ("swap", block_out),
        ("swap", in_grad),
        ("line", gain_sum, True),
        ("line", summed, True),
        ("line", output_summed, True),
    ]
    if depth > 4:
        moved = beneath("swap_results", 8, *results)
    else:
        moved = exchange(sizes, "swap_results", 8, *results)
    block_out, in_grad, gain_all, sums, output_all = moved
    grad_in, grad_out, block_out, in_grad, gain_attn_sum, gain_moe_sum, query_sum, pair_sum, output_sum, router_sum = outputs(
        in_sums,
        out_sums,
        work,
        block_out,
        in_grad,
        gain_all,
        sums.reshape(length, LANES),
        output_all.reshape(width, LANES),
        experts,
    )
    return (
        block_out,
        in_grad,
        gain_attn_sum.reshape(LANES),
        query_sum,
        pair_sum.reshape(w_key_value.shape),
        output_sum,
        gain_moe_sum.reshape(LANES),
        router_sum.T,
        grad_in,
        grad_out,
    )


def solution(mesh):
    in_specs = (
        P("dp", ("row", "col")),
        P("dp", ("row", "col")),
        P("dp"),
        P("dp", None),
        P(("row", "col")),
        P(None, ("row", "col")),
        P(None, ("row", "col"), None),
        P(("row", "col"), None),
        P(("row", "col")),
        P(("row", "col"), None),
        P("row", None, None, "col"),
        P("row", "col", None),
    )
    out_specs = (
        P("dp", ("row", "col")),
        P("dp", ("row", "col")),
        P(("row", "col")),
        P(None, ("row", "col")),
        P(None, ("row", "col"), None),
        P(("row", "col"), None),
        P(("row", "col")),
        P(("row", "col"), None),
        P("row", None, None, "col"),
        P("row", "col", None),
    )
    sizes = (mesh.shape["row"], mesh.shape["col"], mesh.shape["dp"])
    return jax.shard_map(
        functools.partial(local, sizes),
        mesh=mesh,
        in_specs=in_specs,
        out_specs=out_specs,
        check_vma=False,
    )
```

```python
import functools

import jax
import jax.numpy as jnp
from jax import lax
from jax.experimental import pallas as pl
from jax.experimental.pallas import tpu as pltpu
from jax.sharding import PartitionSpec as P

LONGEST = 4096
HIGH = lax.Precision.HIGHEST
EPSILON = 1e-05
RESIDUAL_SCALE = 0.22
SCORE_SCALE = 0.015625
ROPE_BASE = 10000.0
MASKED = -1e30
MESH = pl.DeviceIdType.MESH
GROUP = ("row", "col")
EVERY = ("dp", "row", "col")
LANES = 128
HBM = pl.BlockSpec(memory_space=pl.ANY)
FULL = pl.BlockSpec(memory_space=pltpu.VMEM)
TURN = LANES // 4


class Moves:
    def __init__(self, sizes, kinds, sources, targets, sems):
        self.sizes, self.kinds = sizes, kinds
        self.sources, self.targets = sources, targets
        self.send_sem, self.recv_sem, self.local_sem = sems

    def place(self):
        row, col, layer = lax.axis_index("row"), lax.axis_index("col"), lax.axis_index("dp")
        return row, col, layer, row * self.sizes[1] + col

    def member(self, index):
        rows, cols, depth = self.sizes
        return {"row": index // cols, "col": lax.rem(index, cols)}

    def across(self, row):
        low = lax.rem(row, 2)
        return row + 1 - 2 * low, lax.rem(row + 2, 4), lax.rem(row + 3 - 2 * low, 4)

    def barrier(self):
        rows, cols, depth = self.sizes
        row, col, layer, me = self.place()
        group = rows * cols
        names = [kind[0] for kind in self.kinds]
        barrier = pltpu.get_barrier_semaphore()
        partners = []
        if "swap" in names or "share" in names:
            for k in range(1, group):
                partners.append(self.member(lax.rem(me + k, group)))
        elif "gather" in names:
            for other in self.across(row)[:2]:
                partners.append({"row": other})
            for k in range(1, cols):
                partners.append({"col": lax.rem(col + k, cols)})
        shifts = set()
        for kind in self.kinds:
            if kind[0] == "shift":
                for d in kind[1]:
                    shifts |= {d % depth, -d % depth}
            elif kind[0] in ("turn", "collect"):
                shifts |= set(range(1, depth))
        for k in sorted(shifts - {0}):
            partners.append({"dp": lax.rem(layer + k, depth)})
        ends = [(layer > 0, layer - 1), (layer < depth - 1, layer + 1)]
        ends = ends if "line" in names and not shifts else []
        for partner in partners:
            pl.semaphore_signal(barrier, inc=1, device_id=partner, device_id_type=MESH)
        for there, other in ends:

            @pl.when(there)
            def _(device={"dp": other}):
                pl.semaphore_signal(barrier, inc=1, device_id=device, device_id_type=MESH)

        expected = len(partners)
        for there, _ in ends:
            expected = expected + there.astype(jnp.int32)
        pl.semaphore_wait(barrier, expected)

    def plan(self, only):
        rows, cols, depth = self.sizes
        row, col, layer, me = self.place()
        group = rows * cols
        slots = iter(range(self.send_sem.shape[0]))
        starts, relays, sends, arrivals, local = [], [], [], [], []

        def remote(source, target, device, slot=None):
            slot = next(slots) if slot is None else slot
            return functools.partial(
                pltpu.make_async_remote_copy,
                src_ref=source,
                dst_ref=target,
                send_sem=self.send_sem.at[slot],
                recv_sem=self.recv_sem.at[slot],
                device_id=device,
                device_id_type=MESH,
            )

        for index, (kind, source, target) in enumerate(
            zip(self.kinds, self.sources, self.targets)
        ):
            item = [], [], [], [], []
            begin, follow, sent, got, stay = item

            def keep(source, target):
                sem = self.local_sem.at[index]
                stay.append(functools.partial(pltpu.make_async_copy, source, target, sem))

            def direct(source, target, device):
                copy = None, remote(source, target, device)
                begin.append(copy)
                sent.append(copy)
                got.append(copy)

            if kind[0] == "gather":
                second, parts = kind[1:]
                size = source.shape[0] // parts
                beside, above, away = self.across(row)

                def at(other, part, piece=None):
                    member = other * cols + col
                    first, length, deep = part * size, size, ()
                    if piece is not None and size % 2 == 0:
                        length = size // 2
                        first = first + piece * length
                    elif piece is not None:
                        inner = source.shape[1] // 2
                        deep = (pl.ds(piece * inner, inner),)
                    some = pl.ds(first, length)
                    return target.at[(some, member) + deep if second else (member, some) + deep]

                def to_mates(piece):
                    made = []
                    for j in range(1, cols):
                        copy = None, remote(piece, piece, {"col": lax.rem(col + j, cols)})
                        made.append(copy)
                        sent.append(copy)
                        got.append(copy)
                    return made

                for part in range(parts):
                    some = source.at[pl.ds(part * size, size)]
                    ways = []
                    for near, other, piece in ((beside, above, 0), (above, beside, 1)):
                        first = None, remote(some, at(row, part), {"row": near})
                        passed = at(near, part, piece)
                        onward = None, remote(passed, passed, {"row": other})
                        begin.append(first)
                        sent.extend([first, onward])
                        ways.append((near, piece, first, onward))
                    for near, piece, first, onward in ways:
                        nexts = [onward] + to_mates(at(near, part))
                        follow.append((2 + 3 * part, 0, None, first[1], nexts))
                    for near, piece, first, onward in ways:
                        nexts = to_mates(at(away, part, piece))
                        follow.append((2 + 3 * parts + part, 1, None, onward[1], nexts))
                    for j in range(1, cols):
                        direct(some, at(row, part), {"col": lax.rem(col + j, cols)})
                keep(source, target.at[:, me] if second else target.at[me])
            elif kind[0] in ("swap", "share"):
                for k in range(1, group):
                    other = lax.rem(me + k, group)
                    piece = source.at[other] if kind[0] == "swap" else source
                    direct(piece, target.at[me], self.member(other))
                keep(source.at[me] if kind[0] == "swap" else source, target.at[me])
            elif kind[0] in ("turn", "collect"):
                for k in range(1, depth):
                    other = lax.rem(layer + k, depth)
                    piece = source.at[other] if kind[0] == "turn" else source
                    direct(piece, target.at[layer], {"dp": other})
                keep(source.at[layer] if kind[0] == "turn" else source, target.at[layer])
            elif kind[0] == "line":
                absolute = kind[1]
                for way in (1, -1):
                    behind = layer if way == 1 else depth - 1 - layer
                    onward = layer + way
                    more = (onward >= 0) & (onward < depth)
                    mine = [next(slots) for _ in range(1, depth)]

                    def held(step, where, way=way):
                        if step == 0:
                            return source
                        if absolute:
                            return target.at[where - way * step]
                        return target.at[step - 1 if way == 1 else depth - 1 - step]

                    def sending(step, onward=onward, mine=mine, held=held):
                        device = {"dp": onward}
                        return remote(
                            held(step - 1, layer), held(step, onward), device, mine[step - 1]
                        )

                    begin.append((more, sending(1)))
                    for step in range(1, depth):
                        sent.append((more & (behind >= step - 1), sending(step)))
                        block = held(step, layer)
                        arrival = remote(block, block, {"dp": onward}, mine[step - 1])
                        nexts = [(more, sending(step + 1))] if step + 1 < depth else []
                        follow.append((4 * step, 0, behind >= step, arrival, nexts))
                if absolute:
                    keep(source, target.at[layer])
            else:
                for at_slot, d in enumerate(kind[1]):
                    piece = source.at[at_slot] if kind[2] else source
                    direct(piece, target.at[at_slot], {"dp": lax.rem(layer + d % depth, depth)})
            if only is None or index in only:
                starts += begin
                relays += follow
                sends += sent
                arrivals += got
                local += stay
        return starts, sorted(relays, key=lambda entry: entry[0]), sends, arrivals, local

    def given(self, condition, action):
        if condition is None:
            action()
        else:
            pl.when(condition)(action)

    def start(self, only=None):
        starts, _, _, _, local = self.plan(only)
        for condition, copy in starts:
            self.given(condition, lambda copy=copy: copy().start())
        for copy in local:
            copy().start()

    def relay(self, only=None, stage=None):
        for _, at, condition, copy, nexts in self.plan(only)[1]:
            if stage is not None and stage != at:
                continue

            def action(copy=copy, nexts=nexts):
                copy().wait_recv()
                for more, follower in nexts:
                    self.given(more, lambda follower=follower: follower().start())

            self.given(condition, action)

    def finish(self, only=None):
        _, _, sends, arrivals, local = self.plan(only)
        for condition, copy in arrivals:
            self.given(condition, lambda copy=copy: copy().wait_recv())
        for condition, copy in sends:
            self.given(condition, lambda copy=copy: copy().wait_send())
        for copy in local:
            copy().wait()


def planned(sizes, items):
    rows, cols, depth = sizes
    group = rows * cols
    kinds, shapes, copies = [], [], 0
    for item in items:
        name, array = item[0], item[1]
        shape = array.shape
        if name == "gather":
            assert rows == 4
            second, parts = (item[2:] + (False, 1)[len(item) - 2 :])[:2]
            kinds.append((name, second, parts))
            shape = (shape[0], group) + shape[1:] if second else (group,) + shape
            copies += parts * (4 + 5 * (cols - 1))
        elif name == "shift":
            distances, split = item[2], item[3]
            kinds.append((name, tuple(distances), split))
            shape = (len(distances),) + (shape[1:] if split else shape)
            copies += len(distances)
        elif name == "line":
            kinds.append((name, item[2]))
            shape = (depth if item[2] else depth - 1,) + shape
            copies += 2 * (depth - 1)
        else:
            kinds.append((name,))
            if name in ("share", "collect"):
                shape = (group if name == "share" else depth,) + shape
            copies += (depth if name in ("turn", "collect") else group) - 1
        shapes.append(jax.ShapeDtypeStruct(shape, array.dtype))
    sems = [
        pltpu.SemaphoreType.DMA((copies,)),
        pltpu.SemaphoreType.DMA((copies,)),
        pltpu.SemaphoreType.DMA((len(items),)),
    ]
    return tuple(kinds), shapes, sems


def exchange_body(sizes, kinds, *refs):
    count = len(kinds)
    moves = Moves(sizes, kinds, refs[:count], refs[count : 2 * count], refs[2 * count :])
    moves.barrier()
    moves.start()
    moves.relay()
    moves.finish()


def exchange(sizes, name, number, *items):
    kinds, shapes, sems = planned(sizes, items)
    return pl.pallas_call(
        functools.partial(exchange_body, sizes, kinds),
        out_shape=tuple(shapes),
        in_specs=[HBM] * len(items),
        out_specs=(HBM,) * len(items),
        scratch_shapes=sems,
        compiler_params=pltpu.CompilerParams(collective_id=number, has_side_effects=True),
        name=name,
    )(*[item[1] for item in items])


def dot(a, b, left=1, right=0, precision=None):
    return lax.dot_general(
        a,
        b,
        (((left,), (right,)), ((), ())),
        preferred_element_type=jnp.float32,
        precision=precision,
    )


def call(body, name, shapes, *arrays, scratch=()):
    return pl.pallas_call(
        body,
        out_shape=tuple(jax.ShapeDtypeStruct(*shape) for shape in shapes),
        in_specs=[FULL] * len(arrays),
        out_specs=(FULL,) * len(shapes),
        scratch_shapes=list(scratch),
        name=name,
    )(*arrays)


def lanes_of(shape):
    return lax.broadcasted_iota(jnp.int32, shape, len(shape) - 1)


def flipped(values):
    lanes = lanes_of(values.shape)
    ahead = pltpu.roll(values, LANES - TURN, 1)
    behind = pltpu.roll(values, TURN, 1)
    return jnp.where(lanes % (2 * TURN) < TURN, ahead, behind)


def beside(blocks_ref):
    return jnp.concatenate([blocks_ref[i] for i in range(blocks_ref.shape[0])], axis=1)


def gain_row(gains_ref, which):
    return beside(gains_ref).astype(jnp.float32)[which : which + 1, :]


def added(blocks):
    return functools.reduce(
        jnp.add, [blocks[i].astype(jnp.float32) for i in range(blocks.shape[0])]
    )


def own_rows(count):
    me = lax.axis_index("row") * lax.axis_size("col") + lax.axis_index("col")
    return pl.ds(pl.multiple_of(me * count, count), count)


def column(row):
    return jnp.broadcast_to(row, (8, row.shape[1])).T[:, 0:1]


def project_body(blocks, gains, w_query, w_pair, cosine, sine, near, far, normed, query, pair, own, own_grad, near_turned, far_turned):
    tokens = beside(blocks).astype(jnp.float32)
    scale = lax.rsqrt(jnp.mean(tokens * tokens, axis=1, keepdims=True) + EPSILON)
    normed[...] = (tokens * scale * gain_row(gains, 0)).astype(jnp.bfloat16)
    raw = dot(normed[...], w_query[...])
    query[...] = (raw * cosine[...] + flipped(raw) * sine[...]).astype(jnp.bfloat16)
    raw = dot(normed[...], w_pair[...])
    keys = lanes_of(raw.shape) < LANES // 2
    turned = raw * cosine[...] + flipped(raw) * sine[...]
    pair[...] = jnp.where(keys, turned, raw).astype(jnp.bfloat16)
    for i in range(blocks.shape[0]):
        own[:, i * LANES : (i + 1) * LANES] = blocks[i, own_rows(own.shape[0]), :]
    for source, target in ((near, near_turned), (far, far_turned)):
        for i in range(source.shape[0]):
            scaled = RESIDUAL_SCALE * source[i].astype(jnp.float32)
            target[i] = scaled.T.astype(jnp.bfloat16)
    for i in range(near.shape[0]):
        own_grad[:, i * LANES : (i + 1) * LANES] = near[i, own_rows(own.shape[0]), :]


def doubled(pair, keys_ref, values_ref, at):
    wide = pair.astype(jnp.float32)
    other = pltpu.roll(wide, LANES // 2, 1)
    keys = lanes_of(wide.shape) < LANES // 2
    keys_ref[at] = jnp.where(keys, wide, other).astype(jnp.bfloat16)
    values_ref[at] = jnp.where(keys, other, wide).astype(jnp.bfloat16)


def per_head(values):
    first = lanes_of(values.shape) < LANES // 2
    zero = jnp.zeros_like(values)
    return jnp.concatenate(
        [jnp.where(first, values, zero), jnp.where(first, zero, values)], axis=0
    )


def tile_scores(queries, keys_ref, starts, row, block, last, tokens):
    scores = dot(queries, keys_ref[block], 1, 1) * SCORE_SCALE
    at = lanes_of(scores.shape) + block * tokens
    allowed = at >= starts
    if block == last:
        place = row + lax.broadcasted_iota(jnp.int32, scores.shape, 0)
        allowed = allowed & (at <= place + block * tokens)
    return jnp.where(allowed, scores, MASKED)


def doc_row(docs):
    rows = [docs[i : i + 1, :] for i in range(docs.shape[0])]
    return jnp.concatenate(rows, axis=1).astype(jnp.float32)


def attend_body(query, pair, far, docs, far_docs, mixed, log_total, start, keys, values, queries, out):
    tokens = query.shape[0]
    last = far.shape[0]
    layer = lax.axis_index("dp")
    here = doc_row(docs[...])
    mine = column(here)
    before = jnp.sum((here < mine).astype(jnp.float32), axis=1, keepdims=True)
    for d in range(1, last + 1):
        fewer = (doc_row(far_docs[d - 1]) < mine) | (layer < d)
        before = before + jnp.sum(fewer.astype(jnp.float32), axis=1, keepdims=True)
    start[...] = before.astype(jnp.int32)
    doubled(pair[...], keys, values, last)
    for d in range(1, last + 1):
        doubled(far[d - 1], keys, values, last - d)
    queries[...] = per_head(query[...].astype(jnp.float32)).astype(jnp.bfloat16)
    step = 256

    def tile(i, carry):
        rows = pl.ds(pl.multiple_of(i * step, step), step)
        row = lax.rem(i * step, tokens)
        starts = start[pl.ds(pl.multiple_of(row, step), step), :]
        parts = [
            tile_scores(queries[rows, :], keys, starts, row, block, last, tokens)
            for block in range(last + 1)
        ]
        top = functools.reduce(
            jnp.maximum, [jnp.max(part, axis=1, keepdims=True) for part in parts]
        )
        parts = [jnp.exp(part - top) for part in parts]
        total = functools.reduce(jnp.add, [jnp.sum(p, axis=1, keepdims=True) for p in parts])
        sums = [
            dot(part.astype(jnp.bfloat16), values[block]) for block, part in enumerate(parts)
        ]
        out[rows, :] = functools.reduce(jnp.add, sums) / total
        log_total[rows, :] = top + jnp.log(total)
        return carry

    lax.fori_loop(0, 2 * tokens // step, tile, 0)
    first = lanes_of((tokens, LANES)) < LANES // 2
    mixed[...] = jnp.where(first, out[:tokens, :], out[tokens:, :]).astype(jnp.bfloat16)


def attend_back_body(grad, w_output, query, pair, far, start, log_total, mixed, cosine, sine, query_grad, pair_grad, far_grad, output_grad, keys, values, queries, grads, turned, key_sums, value_sums):
    tokens = query.shape[0]
    last = far.shape[0]
    doubled(pair[...], keys, values, last)
    for d in range(1, last + 1):
        doubled(far[d - 1], keys, values, last - d)
    queries[...] = per_head(query[...].astype(jnp.float32)).astype(jnp.bfloat16)
    grads[...] = per_head(dot(grad[...], w_output[...], 1, 1)).astype(jnp.bfloat16)
    output_sum = dot(mixed[...], grad[...], 0, 0).astype(jnp.bfloat16)
    for i in range(output_grad.shape[0]):
        output_grad[i] = output_sum[:, i * LANES : (i + 1) * LANES]
    key_sums[...] = jnp.zeros_like(key_sums)
    value_sums[...] = jnp.zeros_like(value_sums)
    step = 256

    def tile(i, carry):
        rows = pl.ds(pl.multiple_of(i * step, step), step)
        row = lax.rem(i * step, tokens)
        starts = start[pl.ds(pl.multiple_of(row, step), step), :]
        asked, given, level = queries[rows, :], grads[rows, :], log_total[rows, :]
        chances, products = [], []
        for block in range(last + 1):
            scores = tile_scores(asked, keys, starts, row, block, last, tokens)
            chances.append(jnp.exp(scores - level))
            products.append(dot(given, values[block], 1, 1))
        delta = functools.reduce(
            jnp.add,
            [jnp.sum(p * q, axis=1, keepdims=True) for p, q in zip(chances, products)],
        )
        total = jnp.zeros((step, LANES), jnp.float32)
        for block in range(last + 1):
            back = (chances[block] * (products[block] - delta)).astype(jnp.bfloat16)
            total = total + dot(back, keys[block])
            key_sums[block] += dot(back, asked, 0, 0)
            value_sums[block] += dot(chances[block].astype(jnp.bfloat16), given, 0, 0)
        turned[rows, :] = total
        return carry

    lax.fori_loop(0, 2 * tokens // step, tile, 0)
    first = lanes_of((tokens, LANES)) < LANES // 2
    raw = jnp.where(first, turned[:tokens, :], turned[tokens:, :]) * SCORE_SCALE
    query_grad[...] = (raw * cosine[...] - flipped(raw) * sine[...]).astype(jnp.bfloat16)

    def joined(block):
        by_key, by_value = key_sums[block], value_sums[block]
        by_key = (by_key + pltpu.roll(by_key, LANES // 2, 1)) * SCORE_SCALE
        by_value = by_value + pltpu.roll(by_value, LANES // 2, 1)
        return jnp.where(first, by_key, by_value)

    pair_grad[...] = joined(last)
    for d in range(1, last + 1):
        far_grad[d - 1] = joined(last - d).astype(jnp.bfloat16)


def router_rows(router):
    rows = beside(router).astype(jnp.float32)
    blank = jnp.zeros((LANES - rows.shape[0], rows.shape[1]), jnp.float32)
    return jnp.concatenate([rows, blank], axis=0)


def middle_body(mixed, own, w_output, gains, router, ids_turned, rows, middle, weights, ids_ref):
    experts = router.shape[1]
    width = own.shape[1]
    attn = dot(beside(mixed), w_output[...])
    value = own[...].astype(jnp.float32) + RESIDUAL_SCALE * attn
    middle[...] = value
    scale = lax.rsqrt(jnp.mean(value * value, axis=1, keepdims=True) + EPSILON)
    normed = value * scale * gain_row(gains, 1)
    logits = dot(normed, router_rows(router), 1, 1, precision=HIGH)
    count = own.shape[0]
    ids_ref[...] = ids_turned[...].astype(jnp.float32).T
    ids = ids_ref[own_rows(count), :]
    lanes = lanes_of((count, LANES))
    chosen = jnp.zeros((count, LANES), jnp.float32)
    for k in range(ids.shape[1]):
        chosen = chosen + (ids[:, k : k + 1] == lanes.astype(jnp.float32)).astype(
            jnp.float32
        )
    top = jnp.max(jnp.where(lanes < experts, logits, MASKED), axis=1, keepdims=True)
    terms = jnp.exp(jnp.minimum(logits - top, 0.0)) * chosen
    share = terms / jnp.sum(terms, axis=1, keepdims=True)
    weights[...] = share
    high = share.astype(jnp.bfloat16)
    low = share - high.astype(jnp.float32)
    rows[:, :width] = normed.astype(jnp.bfloat16)
    rows[:, width:] = (high.astype(jnp.float32) + pltpu.roll(low, LANES // 2, 1)).astype(
        jnp.bfloat16
    )


def middle_back_body(back, out_grad, middle, weights, gains, router, middle_grad, attn_grad, logit_grad, gain_part):
    width = middle.shape[1]
    normed_grad = back[0, :, :width].astype(jnp.float32)
    weight_grad = back[0, :, width:].astype(jnp.float32)
    for i in range(1, back.shape[0]):
        normed_grad = normed_grad + back[i, :, :width].astype(jnp.float32)
        weight_grad = weight_grad + back[i, :, width:].astype(jnp.float32)
    share, value = weights[...], middle[...]
    mean = jnp.sum(share * weight_grad, axis=1, keepdims=True)
    logit = share * (weight_grad - mean)
    logit_grad[...] = logit.astype(jnp.bfloat16)
    normed_grad = normed_grad + dot(logit, router_rows(router), precision=HIGH)
    scale = lax.rsqrt(jnp.mean(value * value, axis=1, keepdims=True) + EPSILON)
    gain_part[...] = jnp.sum(normed_grad * value * scale, axis=0, keepdims=True)
    scaled = normed_grad * gain_row(gains, 1)
    norm_dot = jnp.sum(scaled * value, axis=1, keepdims=True)
    total = (
        out_grad[...].astype(jnp.float32)
        + scale * scaled
        - value * (scale * scale * scale * norm_dot / width)
    )
    middle_grad[...] = total
    attn_grad[...] = (RESIDUAL_SCALE * total).astype(jnp.bfloat16)


def project_back_body(query_grad, pair_grad, returned, normed, w_query, w_pair, cosine, sine, output_turned, logit, rows, gains, gain_moe, partial, sums, output_summed, gain_parts):
    layer = lax.axis_index("dp")
    depth = lax.axis_size("dp")
    total = pair_grad[...]
    for i in range(returned.shape[0]):
        total = total + jnp.where(
            layer + i + 1 < depth, returned[i].astype(jnp.float32), 0.0
        )
    keys = lanes_of(total.shape) < LANES // 2
    turned = total * cosine[...] - flipped(total) * sine[...]
    pair_low = jnp.where(keys, turned, total).astype(jnp.bfloat16)
    query_low = query_grad[...]
    whole = dot(query_low, w_query[...], 1, 1) + dot(pair_low, w_pair[...], 1, 1)
    partial[...] = whole.astype(jnp.bfloat16)
    gain_attn = jnp.sum(whole * normed[...].astype(jnp.float32), axis=0, keepdims=True)
    gain_attn = gain_attn / gain_row(gains, 0)
    gain_parts[...] = jnp.zeros_like(gain_parts)
    for i in range(gain_parts.shape[0]):
        at = slice(i * LANES, (i + 1) * LANES)
        gain_parts[i, 0:1, :] = gain_attn[:, at]
        gain_parts[i, 1:2, :] = gain_moe[0:1, at]
    width = normed.shape[1]
    sums[:width, :] = dot(normed[...], query_low, 0, 0).astype(jnp.bfloat16)
    sums[width : 2 * width, :] = dot(normed[...], pair_low, 0, 0).astype(jnp.bfloat16)
    output_summed[...] = added(output_turned).astype(jnp.bfloat16)
    mine = rows[:, own_rows(LANES)]
    sums[2 * width : 2 * width + LANES, :] = dot(logit[...], mine, 0, 0).astype(jnp.bfloat16)


def results_body(blocks, moe, own, middle, middle_grad, gains, gain_blocks, turned, block_out, in_grad, gain_sum, summed):
    gain_sum[...] = added(gain_blocks)
    summed[...] = added(turned).astype(jnp.bfloat16)
    width = own.shape[1]
    normed_grad = blocks[0].astype(jnp.float32)
    branch = moe[0].astype(jnp.float32)
    for i in range(1, blocks.shape[0]):
        normed_grad = normed_grad + blocks[i].astype(jnp.float32)
        branch = branch + moe[i].astype(jnp.float32)
    value = own[...].astype(jnp.float32)
    scale = lax.rsqrt(jnp.mean(value * value, axis=1, keepdims=True) + EPSILON)
    scaled = normed_grad * gain_row(gains, 0)
    norm_dot = jnp.sum(scaled * value, axis=1, keepdims=True)
    grad = (
        middle_grad[...] + scale * scaled - value * (scale * scale * scale * norm_dot / width)
    ).astype(jnp.bfloat16)
    out = (middle[...] + RESIDUAL_SCALE * branch).astype(jnp.bfloat16)
    for i in range(block_out.shape[0]):
        at = slice(i * LANES, (i + 1) * LANES)
        block_out[i] = out[:, at]
        in_grad[i] = grad[:, at]


def expert_terms(gate_up, active_grad, weight):
    hidden = active_grad.shape[0]
    gate, up = gate_up[:hidden], gate_up[hidden:]
    sigmoid = jax.nn.sigmoid(gate)
    silu = gate * sigmoid
    ungated = silu * up
    active = (ungated * weight).astype(jnp.bfloat16)
    scaled = active_grad * weight
    gate_grad = (scaled * up * sigmoid * (1.0 + gate * (1.0 - sigmoid))).astype(jnp.bfloat16)
    up_grad = (scaled * silu).astype(jnp.bfloat16)
    return active, jnp.concatenate([gate_grad, up_grad], axis=0), active_grad * ungated


def weight_rows(extra):
    turned = extra.astype(jnp.float32).T
    return turned[: LANES // 2] + turned[LANES // 2 :]


def local_experts_body(sizes, kinds, rows_ref, grads_ref, in_ref, out_ref, sent_grads, sent_rows, moe_ref, back_ref, flat_ref, in_sum, out_sum, got_grads, got_rows, moe_acc, back_acc, share, weights, spread, *sems):
    step, steps = pl.program_id(0), pl.num_programs(0)
    each, hidden, width = out_ref.shape
    parts = hidden // LANES
    moves = Moves(sizes, kinds, [sent_grads, sent_rows], [got_grads, got_rows], sems)

    @pl.when(step == 0)
    def _():
        moves.barrier()
        moves.start()
        moe_acc[...] = jnp.zeros_like(moe_acc)
        back_acc[...] = jnp.zeros_like(back_acc)
        share[...] = jnp.zeros_like(share)
        weights[...] = weight_rows(rows_ref[:, width:])

    for when, item, stage in ((3, 0, 0), (5, 1, 0), (7, 0, 1)):

        @pl.when(step == when * steps // 8)
        def _(item=item, stage=stage):
            moves.relay([item], stage)

    for i in range(each):
        spread[i] = in_ref[i].astype(jnp.float32)
        for part in range(parts):
            for half in range(2):
                at = half * hidden + part * LANES
                flat_ref[i, :, at : at + LANES] = spread[
                    i, pl.ds(part * 2 + half, width, stride=2 * parts), :
                ].astype(jnp.bfloat16)
        expert = (lax.axis_index("row") * steps + step) * each + i
        active, gate_up_grad, shares = expert_terms(
            dot(flat_ref[i], rows_ref[:, :width], 0, 1),
            dot(out_ref[i], grads_ref[...]),
            weights[pl.ds(expert, 1), :],
        )
        share[pl.ds(expert, 1), :] = jnp.sum(shares, axis=0, keepdims=True)
        moe_acc[...] += dot(active, out_ref[i], 0, 0)
        back_acc[...] += dot(gate_up_grad, flat_ref[i], 0, 1)
        in_sum[i] = dot(gate_up_grad, rows_ref[:, :width]).astype(jnp.bfloat16)
        out_sum[i] = dot(active, grads_ref[...], 1, 1).astype(jnp.bfloat16)

    @pl.when(step == steps - 1)
    def _():
        moe_ref[...] = moe_acc[...].astype(jnp.bfloat16)
        back_ref[:, :width] = back_acc[...].astype(jnp.bfloat16)
        back_ref[:, width:] = share[...].T.astype(jnp.bfloat16)
        moves.relay([1], 1)
        moves.finish()


def local_experts(sizes, number, rows, grads, w_in, w_out, sent_grads, sent_rows):
    tokens, wide = rows.shape
    experts, hidden, width = w_out.shape
    each = 1
    low = jnp.bfloat16
    kinds, shapes, sems = planned(
        sizes,
        [
            ("gather", sent_grads, True, sent_grads.shape[0]),
            ("gather", sent_rows, True, sent_rows.shape[0]),
        ],
    )
    whole = lambda s: pl.BlockSpec(s, lambda e: (0,) * len(s))
    some = lambda s: pl.BlockSpec((each,) + s[1:], lambda e: (e,) + (0,) * (len(s) - 1))
    outs = [
        (tokens, width),
        (tokens, wide),
        (experts, width, 2 * hidden),
        (experts, 2 * hidden, width),
        (experts, hidden, width),
    ]
    return pl.pallas_call(
        functools.partial(local_experts_body, sizes, kinds),
        grid=(experts // each,),
        in_specs=[
            whole(rows.shape),
            whole(grads.shape),
            some(w_in.shape),
            some(w_out.shape),
            HBM,
            HBM,
        ],
        out_specs=(whole(outs[0]), whole(outs[1]), *[some(s) for s in outs[2:]], HBM, HBM),
        out_shape=tuple(jax.ShapeDtypeStruct(s, low) for s in outs) + tuple(shapes),
        scratch_shapes=[
            pltpu.VMEM((tokens, width), jnp.float32),
            pltpu.VMEM((tokens, width), jnp.float32),
            pltpu.VMEM((LANES, tokens), jnp.float32),
            pltpu.VMEM((LANES // 2, tokens), jnp.float32),
            pltpu.VMEM((each,) + w_in.shape[1:], jnp.float32),
        ]
        + sems,
        compiler_params=pltpu.CompilerParams(collective_id=number, has_side_effects=True),
        name="local_experts",
    )(rows, grads, w_in, w_out, sent_grads, sent_rows)


class Sums:
    def __init__(self, rows, grads, weights, whole, turned, load_sem, *sums):
        self.rows, self.grads, self.weights = rows, grads, weights
        self.whole, self.turned, self.load_sem, self.sums = whole, turned, load_sem, sums

    def loads(self, rows_far, grads_far):
        return [
            pltpu.make_async_copy(rows_far, self.rows, self.load_sem.at[0]),
            pltpu.make_async_copy(grads_far, self.grads, self.load_sem.at[1]),
        ]

    def ready(self):
        layers, width, tokens = self.grads.shape
        for i in range(layers):
            self.weights[i] = weight_rows(self.rows[i * tokens : (i + 1) * tokens, width:])

    def make(self, index, w_in, w_out, in_part, out_part):
        layers, width, tokens = self.grads.shape
        hidden = w_out.shape[0]

        def part_of(at, pieces):
            first = at * tokens if isinstance(at, int) else pl.multiple_of(at * tokens, tokens)
            block = self.rows[pl.ds(first, pieces * tokens), :width]
            weight = jnp.concatenate(
                [self.weights[at + i, pl.ds(index, 1), :] for i in range(pieces)], axis=1
            )
            active_grad = jnp.concatenate(
                [dot(w_out, self.grads[at + i]) for i in range(pieces)], axis=1
            )
            active, gate_up_grad, _ = expert_terms(dot(w_in, block, 0, 1), active_grad, weight)
            out_total = functools.reduce(
                jnp.add,
                [
                    dot(active[:, i * tokens : (i + 1) * tokens], self.grads[at + i], 1, 1)
                    for i in range(pieces)
                ],
            )
            return dot(gate_up_grad, block), out_total

        if not self.sums:
            self.whole[...], out_total = part_of(0, layers)
        else:
            self.whole[...] = jnp.zeros_like(self.whole)
            (out_acc,) = self.sums
            out_acc[...] = jnp.zeros_like(out_acc)

            def more(i, carry):
                in_more, out_more = part_of(i, 1)
                self.whole[...] += in_more
                out_acc[...] += out_more
                return carry

            lax.fori_loop(0, layers, more, 0)
            out_total = out_acc[...]
        parts = hidden // LANES

        def turn(i, carry):
            at = pl.ds(pl.multiple_of(i * LANES, LANES), LANES)
            rows_of = pl.ds(lax.rem(i, parts) * 2 + i // parts, width, stride=2 * parts)
            total = self.whole[at, :] + in_part[at, :].astype(jnp.float32)
            self.turned[rows_of, :] = total.T
            return carry

        lax.fori_loop(0, 2 * parts, turn, 0)
        return out_total + out_part[...].astype(jnp.float32)


def sums_scratch(layers, tokens, width, hidden):
    low, full = jnp.bfloat16, jnp.float32
    return [
        pltpu.VMEM((layers * tokens, width + LANES), low),
        pltpu.VMEM((layers, width, tokens), low),
        pltpu.VMEM((layers, LANES // 2, tokens), full),
        pltpu.VMEM((2 * hidden, width), full),
        pltpu.VMEM((width * 2 * hidden // LANES, LANES), full),
        pltpu.SemaphoreType.DMA((2,)),
    ] + ([pltpu.VMEM((hidden, width), full)] if layers > 4 else [])


def widened(source, target):
    size = target.shape[0] // 4

    def piece(i, carry):
        at = pl.ds(pl.multiple_of(i * size, size), size)
        target[at, :] = source[at, :].astype(target.dtype)
        return carry

    lax.fori_loop(0, 4, piece, 0)


def cover_body(sizes, kinds, experts, first, *refs):
    count = len(kinds)
    work, sources = refs[:6], refs[6 : 6 + count]
    in_sum, out_sum = refs[6 + count : 8 + count]
    targets, refs = refs[8 + count : 8 + 2 * count], refs[8 + 2 * count :]
    parts, made, part_sem, made_sem = refs[:4], refs[4:6], refs[6], refs[7]
    sums = Sums(*refs[8:-3])
    moves = Moves(sizes, kinds, sources, targets, refs[-3:])
    many = made[0].shape[0]
    loads = [
        pltpu.make_async_copy(source.at[pl.ds(first, many)], part, part_sem.at[i])
        for i, (source, part) in enumerate(zip(work[:4], parts))
    ] + sums.loads(*work[4:])
    for load in loads[4:] + loads[:4]:
        load.start()
    moves.barrier()
    moves.start()
    for load in loads:
        load.wait()
    sums.ready()

    def stores(i):
        return [
            pltpu.make_async_copy(made[0].at[i], in_sum.at[i], made_sem.at[i]),
            pltpu.make_async_copy(made[1].at[i], out_sum.at[i], made_sem.at[many + i]),
        ]

    def expert(i, carry):
        index = lax.axis_index("row") * experts + first + i
        out_total = sums.make(index, parts[0][i], parts[1][i], parts[2].at[i], parts[3].at[i])
        widened(sums.turned, made[0].at[i])
        made[1][i] = out_total.astype(jnp.bfloat16)
        for store in stores(i):
            store.start()
        return carry

    lax.fori_loop(0, many, expert, 0)
    moves.relay()
    moves.finish()
    for i in range(many):
        for store in stores(i):
            store.wait()


def cover(sizes, name, number, first, count, work, *items):
    w_in, w_out, in_part, out_part, rows_far, grads_far = work
    layers, width, tokens = grads_far.shape
    experts, hidden, _ = w_out.shape
    kinds, shapes, sems = planned(sizes, items)
    low = jnp.bfloat16
    outs = [(count, width * 2 * hidden // LANES, LANES), (count, hidden, width)]
    return pl.pallas_call(
        functools.partial(cover_body, sizes, kinds, experts, first),
        in_specs=[HBM] * (6 + len(items)),
        out_specs=(HBM,) * (2 + len(items)),
        out_shape=tuple(jax.ShapeDtypeStruct(s, low) for s in outs) + tuple(shapes),
        scratch_shapes=[pltpu.VMEM((count,) + a.shape[1:], low) for a in work[:4]]
        + [pltpu.VMEM(s, low) for s in outs]
        + [pltpu.SemaphoreType.DMA((4,)), pltpu.SemaphoreType.DMA((2 * count,))]
        + sums_scratch(layers, tokens, width, hidden)
        + sems,
        compiler_params=pltpu.CompilerParams(collective_id=number, has_side_effects=True),
        name=name,
    )(*work, *[item[1] for item in items])


def outputs_body(counts, *refs):
    pieces = len(counts)
    in_sums, out_sums = refs[:pieces], refs[pieces : 2 * pieces]
    blocks, in_blocks, gains, sums, output_all = refs[2 * pieces : 2 * pieces + 5]
    gin, gout, *others = refs[2 * pieces + 5 :]
    block_out, in_grad, gain_attn, gain_moe, query, pair, output, router = others
    step = pl.program_id(0)
    width = gout.shape[2]

    @pl.when(step == 0)
    def _():
        for i in range(blocks.shape[0]):
            at = pl.ds(i * blocks.shape[1], blocks.shape[1])
            block_out[at, :] = blocks[i]
            in_grad[at, :] = in_blocks[i]
        gain_sum = jnp.sum(gains[...], axis=0)
        gain_attn[...] = gain_sum[0:1, :]
        gain_moe[...] = gain_sum[1:2, :]
        query[...] = sums[:width, :].astype(jnp.float32)
        pair[...] = sums[width : 2 * width, :].astype(jnp.float32)
        for i in range(width // LANES):
            at = slice(i * LANES, (i + 1) * LANES)
            output[:, at] = output_all[at, :].astype(jnp.float32)
        router[...] = sums[2 * width : 2 * width + router.shape[0], :].astype(jnp.float32)

    first = 0
    for count, in_sum, out_sum in zip(counts, in_sums, out_sums):

        @pl.when((step >= first) & (step < first + count))
        def _(in_sum=in_sum, out_sum=out_sum):
            gout[0] = out_sum[0].astype(jnp.float32)
            widened(in_sum.at[0], gin.at[0])

        first += count


def outputs(in_sums, out_sums, hidden, blocks, in_blocks, gains, sums, output_all, experts):
    counts = [s.shape[0] for s in in_sums]
    total = sum(counts)
    width = out_sums[0].shape[2]
    parts = hidden // LANES
    lanes = blocks.shape[2]
    tokens = blocks.shape[0] * blocks.shape[1]
    once = lambda s: pl.BlockSpec(s, lambda e: (0,) * len(s))
    each = lambda s: pl.BlockSpec((1,) + s[1:], lambda e: (e, 0, 0))
    specs = []
    for arrays in (in_sums, out_sums):
        first = 0
        for array in arrays:
            count = array.shape[0]
            specs.append(
                pl.BlockSpec(
                    (1,) + array.shape[1:],
                    lambda e, first=first, count=count: (jnp.clip(e - first, 0, count - 1), 0, 0),
                )
            )
            first += count
    full = jnp.float32
    shapes = [
        ((total, width * 2 * parts, LANES), full),
        ((total, hidden, width), full),
        ((tokens, lanes), jnp.bfloat16),
        ((tokens, lanes), jnp.bfloat16),
        ((1, LANES), full),
        ((1, LANES), full),
        ((width, LANES), full),
        ((width, LANES), full),
        ((LANES, width), full),
        ((experts, LANES), full),
    ]
    small = (blocks, in_blocks, gains, sums, output_all)
    gin, *others = pl.pallas_call(
        functools.partial(outputs_body, counts),
        grid=(total,),
        in_specs=specs + [once(a.shape) for a in small],
        out_specs=(each(shapes[0][0]), each(shapes[1][0])) + tuple(once(s) for s, _ in shapes[2:]),
        out_shape=tuple(jax.ShapeDtypeStruct(*shape) for shape in shapes),
        name="outputs",
    )(*in_sums, *out_sums, *small)
    gin = gin.reshape(total, width, parts, 2, LANES).transpose(0, 1, 3, 2, 4)
    return gin.reshape(total, width, 2, hidden), *others


def local(
    sizes,
    tokens,
    out_grad,
    doc_ids,
    expert_ids,
    gain_attn,
    w_query,
    w_key_value,
    w_output,
    gain_moe,
    w_router,
    w_expert_in,
    w_expert_out,
):
    rows, cols, depth = sizes
    group = rows * cols
    tok_rows, feat_local = tokens.shape
    width = w_query.shape[0]
    experts = w_router.shape[1]
    expert_local, hidden = w_expert_out.shape[0], w_expert_out.shape[1]
    longest_doc = min(LONGEST, tok_rows * depth // 2)
    hop_count = longest_doc // tok_rows
    own = tok_rows // group
    low, full = jnp.bfloat16, jnp.float32
    layer = lax.axis_index("dp")
    me = lax.axis_index("row") * cols + lax.axis_index("col")
    hops = list(range(1, hop_count + 1))

    tokens_blocks, gains, router, docs_far, grads_shifted, grad_blocks = exchange(
        sizes,
        "gather_tokens",
        0,
        ("gather", tokens, False, 2),
        ("share", jnp.stack([gain_attn, gain_moe])),
        ("share", w_router.T),
        ("line", doc_ids.reshape(-1, LANES), False),
        ("line", out_grad, False),
        ("gather", out_grad, False, 2),
    )

    lanes = jnp.arange(LANES, dtype=jnp.int32)
    frequencies = ROPE_BASE ** ((lanes % TURN).astype(full) * (-1.0 / TURN))
    positions = (layer * tok_rows + jnp.arange(tok_rows, dtype=jnp.int32)).astype(full)
    angles = positions[:, None] * frequencies[None, :]
    cosine = jnp.cos(angles)
    sine = jnp.sin(angles) * jnp.where(lanes % (2 * TURN) < TURN, -1.0, 1.0)[None, :]

    w_pair = w_key_value.reshape(width, -1)
    block = (tok_rows, LANES)
    turned = (LANES, tok_rows)
    normed, query, pair, tokens_own, grad_own, grads_near, far_turned = call(
        project_body,
        "project",
        [
            ((tok_rows, width), low),
            (block, low),
            (block, low),
            ((own, width), low),
            ((own, width), low),
            ((group,) + turned, low),
            ((depth - 1,) + turned, low),
        ],
        tokens_blocks,
        gains,
        w_query,
        w_pair,
        cosine,
        sine,
        grad_blocks,
        grads_shifted,
    )
    far, output_blocks = exchange(
        sizes, "shift_pairs", 1, ("shift", pair, hops, False), ("gather", w_output, False, 4)
    )
    output_full = output_blocks.reshape(-1, width)

    stack = (hop_count + 1,) + block
    twice = (2 * tok_rows, LANES)
    mixed, log_total, start = call(
        attend_body,
        "attend",
        [(block, low), ((2 * tok_rows, 1), full), ((tok_rows, 1), jnp.int32)],
        query,
        pair,
        far,
        doc_ids.reshape(-1, LANES),
        docs_far,
        scratch=[
            pltpu.VMEM(stack, low),
            pltpu.VMEM(stack, low),
            pltpu.VMEM(twice, low),
            pltpu.VMEM(twice, full),
        ],
    )
    (mixed_own,) = exchange(
        sizes, "swap_mixed", 2, ("swap", mixed.reshape(group, own, LANES))
    )
    rows_own, middle, weights = call(
        middle_body,
        "middle",
        [((own, width + LANES), low), ((own, width), full), ((own, LANES), full)],
        mixed_own,
        tokens_own,
        output_full,
        gains,
        router,
        expert_ids.T,
        scratch=[pltpu.VMEM(expert_ids.shape, full)],
    )
    rows_blocks, rows_shifted = exchange(
        sizes, "gather_rows", 3, ("gather", rows_own, False, 2), ("line", rows_own, False)
    )
    rows_near = rows_blocks.reshape(tok_rows, -1)
    parts = hidden // LANES
    in_rows = w_expert_in.reshape(expert_local, width, 2, parts, LANES)
    in_rows = in_rows.transpose(0, 1, 3, 2, 4).reshape(expert_local, -1, LANES)
    moe_partial, back_partial, in_flat, in_part, out_part, grads_far, rows_far = local_experts(
        sizes,
        9,
        rows_near,
        grads_near.reshape(width, tok_rows),
        in_rows,
        w_expert_out,
        far_turned,
        rows_shifted,
    )
    rows_far = rows_far.reshape((depth - 1) * tok_rows, -1)
    grads_far = grads_far.reshape(depth - 1, width, tok_rows)
    work = (in_flat, w_expert_out, in_part, out_part, rows_far, grads_far)
    share = expert_local // 4
    unit = 16 * depth
    in_sums, out_sums = [], []

    def beneath(name, number, *items):
        in_sum, out_sum, *moved = cover(
            sizes, name, number, len(in_sums) * share, share, work, *items
        )
        in_sums.append(in_sum)
        out_sums.append(out_sum)
        return moved

    (back_blocks,) = beneath("swap_back", 4, ("swap", back_partial.reshape(group, own, -1)))
    middle_grad, attn_grad, logit_grad, gain_moe_part = call(
        middle_back_body,
        "middle_back",
        [
            ((own, width), full),
            ((own, width), low),
            ((own, LANES), low),
            ((1, width), full),
        ],
        back_blocks,
        grad_own,
        middle,
        weights,
        gains,
        router,
    )
    attn_grad_blocks, logit_blocks = exchange(
        sizes,
        "gather_attn_grad",
        5,
        ("gather", attn_grad, False, 2),
        ("gather", logit_grad),
    )
    query_grad, pair_grad, far_grad, output_sum = call(
        attend_back_body,
        "attend_back",
        [(block, low), (block, full), ((hop_count,) + block, low), ((group, LANES, LANES), low)],
        attn_grad_blocks.reshape(tok_rows, width),
        w_output,
        query,
        pair,
        far,
        start,
        log_total,
        mixed,
        cosine,
        sine,
        scratch=[
            pltpu.VMEM(stack, low),
            pltpu.VMEM(stack, low),
            pltpu.VMEM(twice, low),
            pltpu.VMEM(twice, low),
            pltpu.VMEM(twice, full),
            pltpu.VMEM(stack, full),
            pltpu.VMEM(stack, full),
        ],
    )
    returned, moe_blocks, output_turned = beneath(
        "shift_grads",
        6,
        ("shift", far_grad, [-d for d in hops], True),
        ("swap", moe_partial.reshape(group, own, width)),
        ("turn", output_sum.reshape(depth, width // depth, LANES)),
    )
    length = (2 * width + LANES + unit - 1) // unit * unit
    partial, sums, output_summed, gain_parts = call(
        project_back_body,
        "project_back",
        [
            ((tok_rows, width), low),
            ((length, LANES), low),
            ((width // depth, LANES), low),
            ((group, 8, LANES), full),
        ],
        query_grad,
        pair_grad,
        returned,
        normed,
        w_query,
        w_pair,
        cosine,
        sine,
        output_turned,
        logit_blocks.reshape(tok_rows, LANES),
        rows_near,
        gains,
        gain_moe_part,
    )
    partial_blocks, sums_turned, gain_blocks = beneath(
        "swap_partial",
        7,
        ("swap", partial.reshape(group, own, width)),
        ("turn", sums.reshape(depth, length // depth, LANES)),
        ("swap", gain_parts),
    )
    pieces = (group, own, LANES)
    block_out, in_grad, gain_sum, summed = call(
        results_body,
        "results",
        [
            (pieces, low),
            (pieces, low),
            ((8, LANES), full),
            ((length // depth, LANES), low),
        ],
        partial_blocks,
        moe_blocks,
        tokens_own,
        middle,
        middle_grad,
        gains,
        gain_blocks,
        sums_turned,
    )
    results = [
        ("swap", block_out),
        ("swap", in_grad),
        ("collect", summed),
        ("collect", output_summed),
        ("collect", gain_sum),
    ]
    block_out, in_grad, sums, output_all, gain_all = beneath("swap_results", 8, *results)
    grad_in, grad_out, block_out, in_grad, gain_attn_sum, gain_moe_sum, query_sum, pair_sum, output_sum, router_sum = outputs(
        in_sums,
        out_sums,
        hidden,
        block_out,
        in_grad,
        gain_all,
        sums.reshape(length, LANES),
        output_all.reshape(width, LANES),
        experts,
    )
    return (
        block_out,
        in_grad,
        gain_attn_sum.reshape(LANES),
        query_sum,
        pair_sum.reshape(w_key_value.shape),
        output_sum,
        gain_moe_sum.reshape(LANES),
        router_sum.T,
        grad_in,
        grad_out,
    )


def solution(mesh):
    in_specs = (
        P("dp", ("row", "col")),
        P("dp", ("row", "col")),
        P("dp"),
        P("dp", None),
        P(("row", "col")),
        P(None, ("row", "col")),
        P(None, ("row", "col"), None),
        P(("row", "col"), None),
        P(("row", "col")),
        P(("row", "col"), None),
        P("row", None, None, "col"),
        P("row", "col", None),
    )
    out_specs = (
        P("dp", ("row", "col")),
        P("dp", ("row", "col")),
        P(("row", "col")),
        P(None, ("row", "col")),
        P(None, ("row", "col"), None),
        P(("row", "col"), None),
        P(("row", "col")),
        P(("row", "col"), None),
        P("row", None, None, "col"),
        P("row", "col", None),
    )
    sizes = (mesh.shape["row"], mesh.shape["col"], mesh.shape["dp"])
    return jax.shard_map(
        functools.partial(local, sizes),
        mesh=mesh,
        in_specs=in_specs,
        out_specs=out_specs,
        check_vma=False,
    )
```

```python
import functools
import itertools
import math

import jax
import jax.numpy as jnp
from jax import lax
from jax.experimental import pallas as pl
from jax.experimental.pallas import tpu as pltpu
from jax.sharding import PartitionSpec as P

LONGEST = 4096
HIGH = lax.Precision.HIGHEST
EPSILON = 1e-05
RESIDUAL_SCALE = 0.22
SCORE_SCALE = 0.015625
ROPE_BASE = 10000.0
MASKED = -1e30
MESH = pl.DeviceIdType.MESH
GROUP = ("row", "col")
EVERY = ("dp", "row", "col")
LANES = 128
HBM = pl.BlockSpec(memory_space=pl.ANY)
FULL = pl.BlockSpec(memory_space=pltpu.VMEM)
TURN = LANES // 4


class Moves:
    def __init__(self, sizes, kinds, sources, targets, sems):
        self.sizes, self.kinds = sizes, kinds
        self.sources, self.targets = sources, targets
        self.send_sem, self.recv_sem, self.local_sem = sems

    def place(self):
        row, col, layer = lax.axis_index("row"), lax.axis_index("col"), lax.axis_index("dp")
        return row, col, layer, row * self.sizes[1] + col

    def member(self, index):
        rows, cols, depth = self.sizes
        return {"row": index // cols, "col": lax.rem(index, cols)}

    def across(self, row):
        low = lax.rem(row, 2)
        return row + 1 - 2 * low, lax.rem(row + 2, 4), lax.rem(row + 3 - 2 * low, 4)

    def barrier(self):
        rows, cols, depth = self.sizes
        row, col, layer, me = self.place()
        group = rows * cols
        names = [kind[0] for kind in self.kinds]
        barrier = pltpu.get_barrier_semaphore()
        partners = []
        if "swap" in names or "share" in names:
            for k in range(1, group):
                partners.append(self.member(lax.rem(me + k, group)))
        elif "gather" in names:
            for other in self.across(row)[:2]:
                partners.append({"row": other})
            for k in range(1, cols):
                partners.append({"col": lax.rem(col + k, cols)})
        shifts = set()
        for kind in self.kinds:
            if kind[0] == "shift":
                for d in kind[1]:
                    shifts |= {d % depth, -d % depth}
            elif kind[0] in ("turn", "collect"):
                shifts |= set(range(1, depth))
        for k in sorted(shifts - {0}):
            partners.append({"dp": lax.rem(layer + k, depth)})
        ends = [(layer > 0, layer - 1), (layer < depth - 1, layer + 1)]
        ends = ends if "line" in names and not shifts else []
        for partner in partners:
            pl.semaphore_signal(barrier, inc=1, device_id=partner, device_id_type=MESH)
        for there, other in ends:

            @pl.when(there)
            def _(device={"dp": other}):
                pl.semaphore_signal(barrier, inc=1, device_id=device, device_id_type=MESH)

        expected = len(partners)
        for there, _ in ends:
            expected = expected + there.astype(jnp.int32)
        pl.semaphore_wait(barrier, expected)

    def plan(self, only):
        rows, cols, depth = self.sizes
        row, col, layer, me = self.place()
        group = rows * cols
        slots = iter(range(self.send_sem.shape[0]))
        starts, relays, sends, arrivals, local = [], [], [], [], []

        def remote(source, target, device, slot=None):
            slot = next(slots) if slot is None else slot
            return functools.partial(
                pltpu.make_async_remote_copy,
                src_ref=source,
                dst_ref=target,
                send_sem=self.send_sem.at[slot],
                recv_sem=self.recv_sem.at[slot],
                device_id=device,
                device_id_type=MESH,
            )

        for index, (kind, source, target) in enumerate(
            zip(self.kinds, self.sources, self.targets)
        ):
            item = [], [], [], [], []
            begin, follow, sent, got, stay = item

            def keep(source, target):
                sem = self.local_sem.at[index]
                stay.append(functools.partial(pltpu.make_async_copy, source, target, sem))

            def direct(source, target, device):
                copy = None, remote(source, target, device)
                begin.append(copy)
                sent.append(copy)
                got.append(copy)

            if kind[0] == "gather":
                second, parts = kind[1:]
                size = source.shape[0] // parts
                beside, above, away = self.across(row)

                def at(other, part, piece=None):
                    member = other * cols + col
                    first, length, deep = part * size, size, ()
                    if piece is not None and size % 2 == 0:
                        length = size // 2
                        first = first + piece * length
                    elif piece is not None:
                        inner = source.shape[1] // 2
                        deep = (pl.ds(piece * inner, inner),)
                    some = pl.ds(first, length)
                    return target.at[(some, member) + deep if second else (member, some) + deep]

                def to_mates(piece):
                    made = []
                    for j in range(1, cols):
                        copy = None, remote(piece, piece, {"col": lax.rem(col + j, cols)})
                        made.append(copy)
                        sent.append(copy)
                        got.append(copy)
                    return made

                for part in range(parts):
                    some = source.at[pl.ds(part * size, size)]
                    ways = []
                    for near, other, piece in ((beside, above, 0), (above, beside, 1)):
                        first = None, remote(some, at(row, part), {"row": near})
                        passed = at(near, part, piece)
                        onward = None, remote(passed, passed, {"row": other})
                        begin.append(first)
                        sent.extend([first, onward])
                        ways.append((near, piece, first, onward))
                    for near, piece, first, onward in ways:
                        nexts = [onward] + to_mates(at(near, part))
                        follow.append((2 + 3 * part, 0, None, first[1], nexts))
                    for near, piece, first, onward in ways:
                        nexts = to_mates(at(away, part, piece))
                        follow.append((2 + 3 * parts + part, 1, None, onward[1], nexts))
                    for j in range(1, cols):
                        direct(some, at(row, part), {"col": lax.rem(col + j, cols)})
                keep(source, target.at[:, me] if second else target.at[me])
            elif kind[0] in ("swap", "share"):
                for k in range(1, group):
                    other = lax.rem(me + k, group)
                    piece = source.at[other] if kind[0] == "swap" else source
                    direct(piece, target.at[me], self.member(other))
                keep(source.at[me] if kind[0] == "swap" else source, target.at[me])
            elif kind[0] in ("turn", "collect"):
                for k in range(1, depth):
                    other = lax.rem(layer + k, depth)
                    piece = source.at[other] if kind[0] == "turn" else source
                    direct(piece, target.at[layer], {"dp": other})
                keep(source.at[layer] if kind[0] == "turn" else source, target.at[layer])
            elif kind[0] == "line":
                absolute, parts = kind[1:]
                size = source.shape[0] // parts
                for part, way in itertools.product(range(parts), (1, -1)):
                    behind = layer if way == 1 else depth - 1 - layer
                    onward = layer + way
                    more = (onward >= 0) & (onward < depth)
                    mine = [next(slots) for _ in range(1, depth)]
                    some = pl.ds(part * size, size)

                    def held(step, where, way=way, some=some):
                        if step == 0:
                            return source.at[some]
                        if absolute:
                            return target.at[where - way * step, some]
                        return target.at[step - 1 if way == 1 else depth - 1 - step, some]

                    def sending(step, onward=onward, mine=mine, held=held):
                        device = {"dp": onward}
                        return remote(
                            held(step - 1, layer), held(step, onward), device, mine[step - 1]
                        )

                    begin.append((more, sending(1)))
                    for step in range(1, depth):
                        sent.append((more & (behind >= step - 1), sending(step)))
                        block = held(step, layer)
                        arrival = remote(block, block, {"dp": onward}, mine[step - 1])
                        nexts = [(more, sending(step + 1))] if step + 1 < depth else []
                        when = 4 * step + part
                        follow.append((when, step - 1, behind >= step, arrival, nexts))
                if absolute:
                    keep(source, target.at[layer])
            else:
                for at_slot, d in enumerate(kind[1]):
                    piece = source.at[at_slot] if kind[2] else source
                    direct(piece, target.at[at_slot], {"dp": lax.rem(layer + d % depth, depth)})
            if only is None or index in only:
                starts += begin
                relays += follow
                sends += sent
                arrivals += got
                local += stay
        return starts, sorted(relays, key=lambda entry: entry[0]), sends, arrivals, local

    def given(self, condition, action):
        if condition is None:
            action()
        else:
            pl.when(condition)(action)

    def start(self, only=None):
        starts, _, _, _, local = self.plan(only)
        for condition, copy in starts:
            self.given(condition, lambda copy=copy: copy().start())
        for copy in local:
            copy().start()

    def relay(self, only=None, stages=None):
        for _, stage, condition, copy, nexts in self.plan(only)[1]:
            if stages is not None and stage not in stages:
                continue

            def action(copy=copy, nexts=nexts):
                copy().wait_recv()
                for more, follower in nexts:
                    self.given(more, lambda follower=follower: follower().start())

            self.given(condition, action)

    def finish(self, only=None):
        _, _, sends, arrivals, local = self.plan(only)
        for condition, copy in arrivals:
            self.given(condition, lambda copy=copy: copy().wait_recv())
        for condition, copy in sends:
            self.given(condition, lambda copy=copy: copy().wait_send())
        for copy in local:
            copy().wait()


def planned(sizes, items):
    rows, cols, depth = sizes
    group = rows * cols
    kinds, shapes, copies = [], [], 0
    for item in items:
        name, array = item[0], item[1]
        shape = array.shape
        if name == "gather":
            assert rows == 4
            second, parts = (item[2:] + (False, 1)[len(item) - 2 :])[:2]
            kinds.append((name, second, parts))
            shape = (shape[0], group) + shape[1:] if second else (group,) + shape
            copies += parts * (4 + 5 * (cols - 1))
        elif name == "shift":
            distances, split = item[2], item[3]
            kinds.append((name, tuple(distances), split))
            shape = (len(distances),) + (shape[1:] if split else shape)
            copies += len(distances)
        elif name == "line":
            parts = item[3] if len(item) > 3 else 1
            kinds.append((name, item[2], parts))
            shape = (depth if item[2] else depth - 1,) + shape
            copies += 2 * (depth - 1) * parts
        else:
            kinds.append((name,))
            if name in ("share", "collect"):
                shape = (group if name == "share" else depth,) + shape
            copies += (depth if name in ("turn", "collect") else group) - 1
        shapes.append(jax.ShapeDtypeStruct(shape, array.dtype))
    sems = [
        pltpu.SemaphoreType.DMA((copies,)),
        pltpu.SemaphoreType.DMA((copies,)),
        pltpu.SemaphoreType.DMA((len(items),)),
    ]
    return tuple(kinds), shapes, sems


class Got:
    def __init__(self, index):
        self.index = index


class Made:
    def __init__(self, index):
        self.index = index


class Stage:
    def __init__(self, body, shapes, *operands, scratch=()):
        self.body, self.shapes, self.operands = body, shapes, operands
        self.scratch = list(scratch)


def exchange(sizes, name, number, *items, before=None, after=None, cover=None, landing=(), shared=()):
    kinds, moved, sems = planned(sizes, items)
    stages = [stage for stage in (before, after) if stage]
    operands = []
    for stage in stages:
        for operand in stage.operands:
            if not isinstance(operand, (Got, Made)):
                operands.append(operand)
    work = list(cover.work) if cover else []
    outs = [s for stage in stages for s in stage.shapes]
    made_shapes = list(cover.shapes) if cover else []
    flown = [i for i in range(len(items)) if i not in landing]
    late = [o.index for o in (after.operands if after else ()) if isinstance(o, Got)]
    late = [i for i in late if i not in landing]
    scratch = []

    def take(shapes):
        first = len(scratch)
        scratch.extend(shapes)
        return slice(first, len(scratch))

    vmem = lambda s: pltpu.VMEM(tuple(s[0]), s[1])
    of = lambda a: (a.shape, a.dtype)
    operand_at = take([vmem(of(a)) for a in operands])
    result_at = take([vmem(s) for s in outs])
    landed_at = take([vmem(of(moved[i])) for i in landing])
    late_at = take([vmem(of(moved[i])) for i in late])
    stage_at = [take(stage.scratch) for stage in stages]
    shared_at = take(list(shared))
    needed = sorted({o.index for o in (after.operands if after else ()) if isinstance(o, Got)})
    others = [i for i in range(len(items)) if i not in needed]
    later = range(1, 2 * sizes[2])
    cover_at = take(cover.scratch) if cover else slice(0, 0)
    copies = len(operands) + len(outs) + len(late)
    copy_at = take([pltpu.SemaphoreType.DMA((max(1, copies),))])
    sems_at = take(sems)

    def body(*refs):
        cuts = [len(operands), len(work), len(items), len(outs), len(made_shapes), len(flown)]
        groups = []
        for cut in cuts:
            groups.append(refs[:cut])
            refs = refs[cut:]
        given, work_refs, sources, results, made_refs, flown_refs = groups
        loaded, held = refs[operand_at], refs[result_at]
        landed, lates, (copy_sem,) = refs[landed_at], refs[late_at], refs[copy_at]
        targets = [None] * len(items)
        for i, ref in zip(flown, flown_refs):
            targets[i] = ref
        for i, ref in zip(landing, landed):
            targets[i] = ref
        moves = Moves(sizes, kinds, sources, targets, refs[sems_at])
        number_of = iter(range(copies))
        copy = lambda a, b: pltpu.make_async_copy(a, b, copy_sem.at[next(number_of)])
        loads = [copy(a, b) for a, b in zip(given, loaded)]
        stores = [copy(a, b) for a, b in zip(held, results)]
        late_loads = [copy(targets[i], b) for i, b in zip(late, lates)]
        split = len([o for o in before.operands if not isinstance(o, Made)]) if before else 0
        first = len(before.shapes) if before else 0
        for load in loads:
            load.start()
        if cover:
            cover.begin(work_refs, refs[cover_at])
        moves.barrier()
        moves.start()
        if before:
            for load in loads[:split]:
                load.wait()
            before.body(*loaded[:split], *held[:first], *refs[stage_at[0]], *refs[shared_at])
            for store in stores[:first]:
                store.start()
        if cover:
            cover.run(work_refs, made_refs, refs[cover_at])
        moves.relay(None, (0,))
        if after:
            moves.relay(needed, later)
            moves.finish(needed)
            for load in late_loads:
                load.start()
            for load in loads[split:]:
                load.wait()
            for load in late_loads:
                load.wait()
            plain = iter(loaded[split:])
            values = []
            for operand in after.operands:
                if isinstance(operand, Made):
                    values.append(held[operand.index])
                elif isinstance(operand, Got) and operand.index in landing:
                    values.append(landed[landing.index(operand.index)])
                elif isinstance(operand, Got):
                    values.append(lates[late.index(operand.index)])
                else:
                    values.append(next(plain))
            after.body(*values, *held[first:], *refs[stage_at[-1]], *refs[shared_at])
            for store in stores[first:]:
                store.start()
        moves.relay(others, later)
        moves.finish(others)
        if cover:
            cover.end(made_refs, refs[cover_at])
        for store in stores:
            store.wait()

    shape = lambda s: jax.ShapeDtypeStruct(tuple(s[0]), s[1])
    return pl.pallas_call(
        body,
        out_shape=tuple(shape(s) for s in outs + made_shapes) + tuple(moved[i] for i in flown),
        in_specs=[HBM] * (len(operands) + len(work) + len(items)),
        out_specs=(HBM,) * (len(outs) + len(made_shapes) + len(flown)),
        scratch_shapes=scratch,
        compiler_params=pltpu.CompilerParams(collective_id=number, has_side_effects=True),
        name=name,
    )(*operands, *work, *[item[1] for item in items])


def dot(a, b, left=1, right=0, precision=None):
    return lax.dot_general(
        a,
        b,
        (((left,), (right,)), ((), ())),
        preferred_element_type=jnp.float32,
        precision=precision,
    )


def widened(source, target):
    size = target.shape[0] // 4

    def piece(i, carry):
        at = pl.ds(pl.multiple_of(i * size, size), size)
        target[at, :] = source[at, :].astype(target.dtype)
        return carry

    lax.fori_loop(0, 4, piece, 0)


def cleared(target):
    size = target.shape[0] // 8

    def piece(i, carry):
        at = pl.ds(pl.multiple_of(i * size, size), size)
        target[at, :] = jnp.zeros((size, target.shape[1]), target.dtype)
        return carry

    lax.fori_loop(0, 8, piece, 0)


def lanes_of(shape):
    return lax.broadcasted_iota(jnp.int32, shape, len(shape) - 1)


def flipped(values):
    lanes = lanes_of(values.shape)
    ahead = pltpu.roll(values, LANES - TURN, 1)
    behind = pltpu.roll(values, TURN, 1)
    return jnp.where(lanes % (2 * TURN) < TURN, ahead, behind)


def beside(blocks_ref):
    return jnp.concatenate([blocks_ref[i] for i in range(blocks_ref.shape[0])], axis=1)


def gain_row(gains_ref):
    return beside(gains_ref).astype(jnp.float32)


def added(blocks):
    return functools.reduce(
        jnp.add, [blocks[i].astype(jnp.float32) for i in range(blocks.shape[0])]
    )


def own_rows(count):
    me = lax.axis_index("row") * lax.axis_size("col") + lax.axis_index("col")
    return pl.ds(pl.multiple_of(me * count, count), count)


def column(row):
    return jnp.broadcast_to(row, (8, row.shape[1])).T[:, 0:1]


def tables_body(cosine, sine):
    step = 64
    lanes = lanes_of((step, LANES))
    power = (lanes % TURN).astype(jnp.float32) * (-math.log(ROPE_BASE) / TURN)
    frequencies = jnp.exp(power)
    base = lax.axis_index("dp") * cosine.shape[0]

    def piece(i, carry):
        at = pl.ds(pl.multiple_of(i * step, step), step)
        positions = base + i * step + lax.broadcasted_iota(jnp.int32, lanes.shape, 0)
        angles = positions.astype(jnp.float32) * frequencies
        cosine[at, :] = jnp.cos(angles)
        value = jnp.sin(angles)
        sine[at, :] = jnp.where(lanes % (2 * TURN) < TURN, -value, value)
        return carry

    lax.fori_loop(0, cosine.shape[0] // step, piece, 0)


def turned(source, target):
    def block(i, carry):
        scaled = RESIDUAL_SCALE * source[i].astype(jnp.float32)
        target[i] = scaled.T.astype(jnp.bfloat16)
        return carry

    lax.fori_loop(0, target.shape[0], block, 0)


def project_body(blocks, gains, w_query, w_pair, cosine, sine, normed, query, pair, own):
    gain = gain_row(gains)
    step = 128

    def piece(i, carry):
        at = pl.ds(pl.multiple_of(i * step, step), step)
        parts = [blocks[k, at, :] for k in range(blocks.shape[0])]
        tokens = jnp.concatenate(parts, axis=1).astype(jnp.float32)
        scale = lax.rsqrt(jnp.mean(tokens * tokens, axis=1, keepdims=True) + EPSILON)
        normed[at, :] = (tokens * scale * gain).astype(jnp.bfloat16)
        return carry

    lax.fori_loop(0, normed.shape[0] // step, piece, 0)
    raw = dot(normed[...], w_query[...])
    query[...] = (raw * cosine[...] + flipped(raw) * sine[...]).astype(jnp.bfloat16)
    raw = dot(normed[...], w_pair[...])
    keys = lanes_of(raw.shape) < LANES // 2
    turned = raw * cosine[...] + flipped(raw) * sine[...]
    pair[...] = jnp.where(keys, turned, raw).astype(jnp.bfloat16)
    for i in range(blocks.shape[0]):
        own[:, i * LANES : (i + 1) * LANES] = blocks[i, own_rows(own.shape[0]), :]


def doubled(pair, keys_ref, values_ref, at):
    wide = pair.astype(jnp.float32)
    other = pltpu.roll(wide, LANES // 2, 1)
    keys = lanes_of(wide.shape) < LANES // 2
    keys_ref[at] = jnp.where(keys, wide, other).astype(jnp.bfloat16)
    values_ref[at] = jnp.where(keys, other, wide).astype(jnp.bfloat16)


def per_head(values):
    first = lanes_of(values.shape) < LANES // 2
    zero = jnp.zeros_like(values)
    return jnp.concatenate(
        [jnp.where(first, values, zero), jnp.where(first, zero, values)], axis=0
    )


def tile_scores(queries, keys_ref, starts, row, block, last, tokens):
    scores = dot(queries, keys_ref[block], 1, 1) * SCORE_SCALE
    at = lanes_of(scores.shape) + block * tokens
    allowed = at >= starts
    if block == last:
        place = row + lax.broadcasted_iota(jnp.int32, scores.shape, 0)
        allowed = allowed & (at <= place + block * tokens)
    return jnp.where(allowed, scores, MASKED)


def doc_row(docs):
    rows = [docs[i : i + 1, :] for i in range(docs.shape[0])]
    return jnp.concatenate(rows, axis=1).astype(jnp.float32)


def attend_tiles(tokens, tile):
    step = 256

    def body(i, carry):
        rows = pl.ds(pl.multiple_of(i * step, step), step)
        tile(rows, lax.rem(i * step, tokens), step)
        return carry

    lax.fori_loop(0, 2 * tokens // step, body, 0)


def attend_first_body(near_grads, far_grads, query, pair, docs, far_docs, own_grad, near_turned, far_turned, start, keys, values, queries, out, tops, totals):
    turned(near_grads, near_turned)
    turned(far_grads, far_turned)
    for i in range(near_grads.shape[0]):
        own_grad[:, i * LANES : (i + 1) * LANES] = near_grads[i, own_rows(own_grad.shape[0]), :]
    tokens = query.shape[0]
    last = keys.shape[0] - 1
    layer = lax.axis_index("dp")
    here = doc_row(docs[...])
    mine = column(here)
    before = jnp.sum((here < mine).astype(jnp.float32), axis=1, keepdims=True)
    for d in range(1, last + 1):
        fewer = (doc_row(far_docs[d - 1]) < mine) | (layer < d)
        before = before + jnp.sum(fewer.astype(jnp.float32), axis=1, keepdims=True)
    start[...] = before.astype(jnp.int32)
    doubled(pair[...], keys, values, last)
    queries[...] = per_head(query[...].astype(jnp.float32)).astype(jnp.bfloat16)

    def tile(rows, row, step):
        starts = start[pl.ds(pl.multiple_of(row, step), step), :]
        scores = tile_scores(queries[rows, :], keys, starts, row, last, last, tokens)
        top = jnp.max(scores, axis=1, keepdims=True)
        terms = jnp.exp(scores - top)
        tops[rows, :] = top
        totals[rows, :] = jnp.sum(terms, axis=1, keepdims=True)
        out[rows, :] = dot(terms.astype(jnp.bfloat16), values[last])

    attend_tiles(tokens, tile)


def attend_rest_body(far, start, mixed, log_total, keys, values, queries, out, tops, totals):
    last, tokens = far.shape[0], far.shape[1]
    for d in range(1, last + 1):
        doubled(far[d - 1], keys, values, last - d)

    def tile(rows, row, step):
        starts = start[pl.ds(pl.multiple_of(row, step), step), :]
        parts = [
            tile_scores(queries[rows, :], keys, starts, row, block, last, tokens)
            for block in range(last)
        ]
        top = functools.reduce(
            jnp.maximum, [jnp.max(part, axis=1, keepdims=True) for part in parts], tops[rows, :]
        )
        parts = [jnp.exp(part - top) for part in parts]
        scale = jnp.exp(tops[rows, :] - top)
        total = functools.reduce(
            jnp.add,
            [jnp.sum(p, axis=1, keepdims=True) for p in parts],
            totals[rows, :] * scale,
        )
        sums = [
            dot(part.astype(jnp.bfloat16), values[block]) for block, part in enumerate(parts)
        ]
        out[rows, :] = functools.reduce(jnp.add, sums, out[rows, :] * scale) / total
        log_total[rows, :] = top + jnp.log(total)

    attend_tiles(tokens, tile)
    first = lanes_of((tokens, LANES)) < LANES // 2
    mixed[...] = jnp.where(first, out[:tokens, :], out[tokens:, :]).astype(jnp.bfloat16)


def attend_again_body(query, pair, far, start, log_total, keys, values, queries, chances):
    tokens = query.shape[0]
    last = far.shape[0]
    doubled(pair[...], keys, values, last)
    for d in range(1, last + 1):
        doubled(far[d - 1], keys, values, last - d)
    queries[...] = per_head(query[...].astype(jnp.float32)).astype(jnp.bfloat16)

    def tile(rows, row, step):
        starts = start[pl.ds(pl.multiple_of(row, step), step), :]
        for block in range(last + 1):
            scores = tile_scores(queries[rows, :], keys, starts, row, block, last, tokens)
            chances[block, rows, :] = jnp.exp(scores - log_total[rows, :])

    attend_tiles(tokens, tile)


def attend_back_body(grad, w_output, mixed, cosine, sine, query_grad, pair_grad, far_grad, output_grad, grads, turned, key_sums, value_sums, keys, values, queries, chances):
    tokens = mixed.shape[0]
    last = keys.shape[0] - 1
    given_grad = grad[...].reshape(tokens, -1)
    grads[...] = per_head(dot(given_grad, w_output[...], 1, 1)).astype(jnp.bfloat16)
    output_sum = dot(mixed[...], given_grad, 0, 0).astype(jnp.bfloat16)
    for i in range(output_grad.shape[0]):
        output_grad[i] = output_sum[:, i * LANES : (i + 1) * LANES]
    for block in range(last + 1):
        cleared(key_sums.at[block])
        cleared(value_sums.at[block])

    def tile(rows, row, step):
        asked, given = queries[rows, :], grads[rows, :]
        products = [dot(given, values[block], 1, 1) for block in range(last + 1)]
        delta = functools.reduce(
            jnp.add,
            [
                jnp.sum(chances[block, rows, :] * product, axis=1, keepdims=True)
                for block, product in enumerate(products)
            ],
        )
        total = jnp.zeros((step, LANES), jnp.float32)
        for block in range(last + 1):
            chance = chances[block, rows, :]
            back = (chance * (products[block] - delta)).astype(jnp.bfloat16)
            total = total + dot(back, keys[block])
            key_sums[block] += dot(back, asked, 0, 0)
            value_sums[block] += dot(chance.astype(jnp.bfloat16), given, 0, 0)
        turned[rows, :] = total

    attend_tiles(tokens, tile)
    first = lanes_of((tokens, LANES)) < LANES // 2
    raw = jnp.where(first, turned[:tokens, :], turned[tokens:, :]) * SCORE_SCALE
    query_grad[...] = (raw * cosine[...] - flipped(raw) * sine[...]).astype(jnp.bfloat16)

    def joined(block):
        by_key, by_value = key_sums[block], value_sums[block]
        by_key = (by_key + pltpu.roll(by_key, LANES // 2, 1)) * SCORE_SCALE
        by_value = by_value + pltpu.roll(by_value, LANES // 2, 1)
        return jnp.where(first, by_key, by_value)

    pair_grad[...] = joined(last)
    for d in range(1, last + 1):
        far_grad[d - 1] = joined(last - d).astype(jnp.bfloat16)


def router_rows(router):
    rows = beside(router).astype(jnp.float32)
    blank = jnp.zeros((LANES - rows.shape[0], rows.shape[1]), jnp.float32)
    return jnp.concatenate([rows, blank], axis=0)


def middle_body(mixed, own, w_output, gains, router, ids_turned, rows, middle, weights, ids_ref):
    experts = router.shape[1]
    width = own.shape[1]
    attn = dot(beside(mixed), w_output[...])
    value = own[...].astype(jnp.float32) + RESIDUAL_SCALE * attn
    middle[...] = value
    scale = lax.rsqrt(jnp.mean(value * value, axis=1, keepdims=True) + EPSILON)
    normed = value * scale * gain_row(gains)
    logits = dot(normed, router_rows(router), 1, 1, precision=HIGH)
    count = own.shape[0]
    ids_ref[...] = ids_turned[...].astype(jnp.float32).T
    ids = ids_ref[own_rows(count), :]
    lanes = lanes_of((count, LANES))
    chosen = jnp.zeros((count, LANES), jnp.float32)
    for k in range(ids.shape[1]):
        chosen = chosen + (ids[:, k : k + 1] == lanes.astype(jnp.float32)).astype(
            jnp.float32
        )
    top = jnp.max(jnp.where(lanes < experts, logits, MASKED), axis=1, keepdims=True)
    terms = jnp.exp(jnp.minimum(logits - top, 0.0)) * chosen
    share = terms / jnp.sum(terms, axis=1, keepdims=True)
    weights[...] = share
    high = share.astype(jnp.bfloat16)
    low = share - high.astype(jnp.float32)
    rows[:, :width] = normed.astype(jnp.bfloat16)
    rows[:, width:] = (high.astype(jnp.float32) + pltpu.roll(low, LANES // 2, 1)).astype(
        jnp.bfloat16
    )


def middle_back_body(back, out_grad, middle, weights, gains, router, middle_grad, attn_grad, logit_grad, gain_part):
    width = middle.shape[1]
    normed_grad = back[0, :, :width].astype(jnp.float32)
    weight_grad = back[0, :, width:].astype(jnp.float32)
    for i in range(1, back.shape[0]):
        normed_grad = normed_grad + back[i, :, :width].astype(jnp.float32)
        weight_grad = weight_grad + back[i, :, width:].astype(jnp.float32)
    share, value = weights[...], middle[...]
    mean = jnp.sum(share * weight_grad, axis=1, keepdims=True)
    logit = share * (weight_grad - mean)
    logit_grad[...] = logit.astype(jnp.bfloat16)
    normed_grad = normed_grad + dot(logit, router_rows(router), precision=HIGH)
    scale = lax.rsqrt(jnp.mean(value * value, axis=1, keepdims=True) + EPSILON)
    gain_part[...] = jnp.sum(normed_grad * value * scale, axis=0, keepdims=True)
    scaled = normed_grad * gain_row(gains)
    norm_dot = jnp.sum(scaled * value, axis=1, keepdims=True)
    total = (
        out_grad[...].astype(jnp.float32)
        + scale * scaled
        - value * (scale * scale * scale * norm_dot / width)
    )
    middle_grad[...] = total
    attn_grad[...] = (RESIDUAL_SCALE * total).astype(jnp.bfloat16)


def project_back_body(query_grad, pair_grad, returned, normed, w_query, w_pair, cosine, sine, output_turned, logit, rows, gains, gain_moe, partial, sums, output_first, output_last, gain_parts):
    layer = lax.axis_index("dp")
    depth = lax.axis_size("dp")
    total = pair_grad[...]
    for i in range(returned.shape[0]):
        total = total + jnp.where(
            layer + i + 1 < depth, returned[i].astype(jnp.float32), 0.0
        )
    keys = lanes_of(total.shape) < LANES // 2
    turned = total * cosine[...] - flipped(total) * sine[...]
    pair_low = jnp.where(keys, turned, total).astype(jnp.bfloat16)
    query_low = query_grad[...]
    whole = dot(query_low, w_query[...], 1, 1) + dot(pair_low, w_pair[...], 1, 1)
    partial[...] = whole.astype(jnp.bfloat16)
    gain_attn = jnp.sum(whole * normed[...].astype(jnp.float32), axis=0, keepdims=True)
    gain_attn = gain_attn / gain_row(gains)
    gain_parts[...] = jnp.zeros_like(gain_parts)
    for i in range(gain_parts.shape[0]):
        at = slice(i * LANES, (i + 1) * LANES)
        gain_parts[i, 0:1, :] = gain_attn[:, at]
        gain_parts[i, 1:2, :] = gain_moe[0:1, at]
    width = normed.shape[1]
    sums[:width, :] = dot(normed[...], query_low, 0, 0).astype(jnp.bfloat16)
    sums[width : 2 * width, :] = dot(normed[...], pair_low, 0, 0).astype(jnp.bfloat16)
    output_sum = added(output_turned).astype(jnp.bfloat16)
    output_first[...] = output_sum[: output_first.shape[0], :]
    output_last[...] = output_sum[output_first.shape[0] :, :]
    mine = rows[:, own_rows(LANES)]
    named = logit[...].reshape(normed.shape[0], LANES)
    sums[2 * width : 2 * width + LANES, :] = dot(named, mine, 0, 0).astype(jnp.bfloat16)


def results_body(blocks, moe, own, middle, middle_grad, gains, gain_blocks, turned, block_out, in_grad, gain_sum, summed):
    gain_sum[...] = added(gain_blocks)
    summed[...] = added(turned).astype(jnp.bfloat16)
    width = own.shape[1]
    normed_grad = blocks[0].astype(jnp.float32)
    branch = moe[0].astype(jnp.float32)
    for i in range(1, blocks.shape[0]):
        normed_grad = normed_grad + blocks[i].astype(jnp.float32)
        branch = branch + moe[i].astype(jnp.float32)
    value = own[...].astype(jnp.float32)
    scale = lax.rsqrt(jnp.mean(value * value, axis=1, keepdims=True) + EPSILON)
    scaled = normed_grad * gain_row(gains)
    norm_dot = jnp.sum(scaled * value, axis=1, keepdims=True)
    grad = (
        middle_grad[...] + scale * scaled - value * (scale * scale * scale * norm_dot / width)
    ).astype(jnp.bfloat16)
    out = (middle[...] + RESIDUAL_SCALE * branch).astype(jnp.bfloat16)
    for i in range(block_out.shape[0]):
        at = slice(i * LANES, (i + 1) * LANES)
        block_out[i] = out[:, at]
        in_grad[i] = grad[:, at]


def expert_terms(gate_up, active_grad, weight):
    hidden = active_grad.shape[0]
    gate, up = gate_up[:hidden], gate_up[hidden:]
    sigmoid = jax.nn.sigmoid(gate)
    silu = gate * sigmoid
    ungated = silu * up
    active = (ungated * weight).astype(jnp.bfloat16)
    scaled = active_grad * weight
    gate_grad = (scaled * up * sigmoid * (1.0 + gate * (1.0 - sigmoid))).astype(jnp.bfloat16)
    up_grad = (scaled * silu).astype(jnp.bfloat16)
    return active, jnp.concatenate([gate_grad, up_grad], axis=0), active_grad * ungated


def weight_rows(extra):
    turned = extra.astype(jnp.float32).T
    return turned[: LANES // 2] + turned[LANES // 2 :]


def local_experts_body(sizes, kinds, rows_ref, grads_ref, in_ref, out_ref, sent_grads, sent_rows, moe_ref, back_ref, flat_ref, in_sum, out_sum, got_grads, got_rows, moe_acc, back_acc, share, weights, spread, *sems):
    step, steps = pl.program_id(0), pl.num_programs(0)
    each, hidden, width = out_ref.shape
    parts = hidden // LANES
    moves = Moves(sizes, kinds, [sent_grads, sent_rows], [got_grads, got_rows], sems)

    @pl.when(step == 0)
    def _():
        moves.barrier()
        moves.start([0])
        cleared(moe_acc)
        cleared(back_acc)
        share[...] = jnp.zeros_like(share)
        weights[...] = weight_rows(rows_ref[:, width:])

    @pl.when(step == 2 * steps // 8)
    def _():
        moves.start([1])

    for when, item, stage in ((3, 0, 0), (6, 1, 0), (7, 0, 1)):

        @pl.when(step == when * steps // 8)
        def _(item=item, stage=stage):
            moves.relay([item], (stage,))

    for i in range(each):
        spread[i] = in_ref[i].astype(jnp.float32)
        for part in range(parts):
            for half in range(2):
                at = half * hidden + part * LANES
                flat_ref[i, :, at : at + LANES] = spread[
                    i, pl.ds(part * 2 + half, width, stride=2 * parts), :
                ].astype(jnp.bfloat16)
        expert = (lax.axis_index("row") * steps + step) * each + i
        active, gate_up_grad, shares = expert_terms(
            dot(flat_ref[i], rows_ref[:, :width], 0, 1),
            dot(out_ref[i], grads_ref[...]),
            weights[pl.ds(expert, 1), :],
        )
        share[pl.ds(expert, 1), :] = jnp.sum(shares, axis=0, keepdims=True)
        moe_acc[...] += dot(active, out_ref[i], 0, 0)
        back_acc[...] += dot(gate_up_grad, flat_ref[i], 0, 1)
        in_sum[i] = dot(gate_up_grad, rows_ref[:, :width]).astype(jnp.bfloat16)
        out_sum[i] = dot(active, grads_ref[...], 1, 1).astype(jnp.bfloat16)

    @pl.when(step == steps - 1)
    def _():
        widened(moe_acc, moe_ref)
        widened(back_acc, back_ref.at[:, :width])
        back_ref[:, width:] = share[...].T.astype(jnp.bfloat16)
        moves.relay([1], (1,))
        moves.finish()


def local_experts(sizes, number, rows, grads, w_in, w_out, sent_grads, sent_rows):
    tokens, wide = rows.shape
    experts, hidden, width = w_out.shape
    each = 1
    low = jnp.bfloat16
    kinds, shapes, sems = planned(
        sizes,
        [
            ("gather", sent_grads, True, sent_grads.shape[0]),
            ("gather", sent_rows, True, sent_rows.shape[0]),
        ],
    )
    whole = lambda s: pl.BlockSpec(s, lambda e: (0,) * len(s))
    some = lambda s: pl.BlockSpec((each,) + s[1:], lambda e: (e,) + (0,) * (len(s) - 1))
    outs = [
        (tokens, width),
        (tokens, wide),
        (experts, width, 2 * hidden),
        (experts, 2 * hidden, width),
        (experts, hidden, width),
    ]
    return pl.pallas_call(
        functools.partial(local_experts_body, sizes, kinds),
        grid=(experts // each,),
        in_specs=[
            whole(rows.shape),
            whole(grads.shape),
            some(w_in.shape),
            some(w_out.shape),
            HBM,
            HBM,
        ],
        out_specs=(whole(outs[0]), whole(outs[1]), *[some(s) for s in outs[2:]], HBM, HBM),
        out_shape=tuple(jax.ShapeDtypeStruct(s, low) for s in outs) + tuple(shapes),
        scratch_shapes=[
            pltpu.VMEM((tokens, width), jnp.float32),
            pltpu.VMEM((tokens, width), jnp.float32),
            pltpu.VMEM((LANES, tokens), jnp.float32),
            pltpu.VMEM((LANES // 2, tokens), jnp.float32),
            pltpu.VMEM((each,) + w_in.shape[1:], jnp.float32),
        ]
        + sems,
        compiler_params=pltpu.CompilerParams(collective_id=number, has_side_effects=True),
        name="local_experts",
    )(rows, grads, w_in, w_out, sent_grads, sent_rows)


class Sums:
    def __init__(self, rows, grads, weights, turned, load_sem, *sums):
        self.rows, self.grads, self.weights = rows, grads, weights
        self.turned, self.load_sem, self.sums = turned, load_sem, sums

    def load(self, which, source):
        target = (self.rows, self.grads)[which]
        return pltpu.make_async_copy(source, target, self.load_sem.at[which])

    def ready(self):
        layers, width, tokens = self.grads.shape

        def block(i, carry):
            at = pl.ds(pl.multiple_of(i * tokens, tokens), tokens)
            self.weights[i] = weight_rows(self.rows[at, width:])
            return carry

        lax.fori_loop(0, layers, block, 0)

    def make(self, index, w_in, w_out, in_part, out_part, made, arrive):
        layers, width, tokens = self.grads.shape
        hidden = w_out.shape[0]
        arrive(0)
        if self.sums:
            arrive(1)
        later = arrive

        def part_of(at, pieces, arrive=lambda i: None if self.sums else later(i)):
            first = at * tokens if isinstance(at, int) else pl.multiple_of(at * tokens, tokens)
            block = self.rows[pl.ds(first, pieces * tokens), :width]
            gate_up = dot(w_in[...], block, 0, 1)
            arrive(1)
            weight = jnp.concatenate(
                [self.weights[at + i, pl.ds(index, 1), :] for i in range(pieces)], axis=1
            )
            active_grad = jnp.concatenate(
                [dot(w_out[...], self.grads[at + i]) for i in range(pieces)], axis=1
            )
            active, gate_up_grad, _ = expert_terms(gate_up, active_grad, weight)
            out_total = functools.reduce(
                jnp.add,
                [
                    dot(active[:, i * tokens : (i + 1) * tokens], self.grads[at + i], 1, 1)
                    for i in range(pieces)
                ],
            )
            return dot(gate_up_grad, block), out_total

        if not self.sums:
            in_total, out_total = part_of(0, layers)
        else:
            whole, out_acc = self.sums
            whole[...] = jnp.zeros_like(whole)
            out_acc[...] = jnp.zeros_like(out_acc)

            def more(i, carry):
                in_more, out_more = part_of(i, 1)
                whole[...] += in_more
                out_acc[...] += out_more
                return carry

            lax.fori_loop(0, layers, more, 0)
            in_total, out_total = whole[...], out_acc[...]
        arrive(2)
        in_total = in_total + in_part[...].astype(jnp.float32)
        parts = hidden // LANES
        for part in range(parts):
            for half in range(2):
                at = half * hidden + part * LANES
                self.turned[pl.ds(part * 2 + half, width, stride=2 * parts), :] = in_total[
                    at : at + LANES, :
                ].T
        made[...] = self.turned[...].astype(jnp.bfloat16)
        return out_total + out_part[...].astype(jnp.float32)


def sums_scratch(layers, tokens, width, hidden):
    low, full = jnp.bfloat16, jnp.float32
    return [
        pltpu.VMEM((layers * tokens, width + LANES), low),
        pltpu.VMEM((layers, width, tokens), low),
        pltpu.VMEM((layers, LANES // 2, tokens), full),
        pltpu.VMEM((width * 2 * hidden // LANES, LANES), full),
        pltpu.SemaphoreType.DMA((2,)),
    ] + [pltpu.VMEM((k * hidden, width), full) for k in (2, 1) if layers > 4]


class Cover:
    def __init__(self, first, many, work):
        w_in, w_out, in_part, out_part, rows_far, grads_far = work
        layers, width, tokens = grads_far.shape
        self.experts, hidden, _ = w_out.shape
        self.first, self.many, self.work = first, many, work
        low = jnp.bfloat16
        self.shapes = [
            ((many, width * 2 * hidden // LANES, LANES), low),
            ((many, hidden, width), low),
        ]
        self.scratch = [pltpu.VMEM((many,) + a.shape[1:], low) for a in work[:4]]
        self.scratch += [pltpu.VMEM(*s) for s in self.shapes]
        self.scratch += [pltpu.SemaphoreType.DMA((4, many)), pltpu.SemaphoreType.DMA((2, many))]
        self.scratch += sums_scratch(layers, tokens, width, hidden)

    def load(self, which, i, work, refs):
        source, sem = work[which].at[self.first + i], refs[6].at[which, i]
        return pltpu.make_async_copy(source, refs[which].at[i], sem)

    def begin(self, work, refs):
        sums = Sums(*refs[8:])
        sums.load(0, work[4]).start()
        self.load(0, 0, work, refs).start()
        sums.load(1, work[5]).start()
        for which in (1, 2, 3):
            self.load(which, 0, work, refs).start()
        for i in range(1, self.many):
            for which in range(4):
                self.load(which, i, work, refs).start()

    def stores(self, i, made, refs):
        return [
            pltpu.make_async_copy(refs[4 + k].at[i], made[k].at[i], refs[7].at[k, i])
            for k in range(2)
        ]

    def run(self, work, made, refs):
        sums = Sums(*refs[8:])

        def expert(i, carry):
            def arrive(point):
                @pl.when(i == 0)
                def _():
                    if point == 0:
                        sums.load(0, work[4]).wait()
                        sums.ready()
                    if point == 1:
                        sums.load(1, work[5]).wait()

                for which in ((0,), (1,), (2, 3))[point]:
                    self.load(which, i, work, refs).wait()

            index = lax.axis_index("row") * self.experts + self.first + i
            out_total = sums.make(index, *[refs[k].at[i] for k in range(5)], arrive)
            refs[5][i] = out_total.astype(jnp.bfloat16)
            for store in self.stores(i, made, refs):
                store.start()
            return carry

        lax.fori_loop(0, self.many, expert, 0)

    def end(self, made, refs):
        for i in range(self.many):
            for store in self.stores(i, made, refs):
                store.wait()


def outputs_body(count, total, *refs):
    pieces = total // count
    sums, smalls = refs[: 2 * pieces], refs[2 * pieces : 2 * pieces + 6]
    gin, gout, *others = refs[2 * pieces + 6 : 2 * pieces + 16]
    block_out, in_grad, gain_attn, gain_moe, query, pair, output, router = others
    in_low, out_low, in_full, out_full, load_sem, store_sem = refs[2 * pieces + 16 :]
    ring = in_full.shape[0]

    def load(k, i):
        low = (in_low, out_low)[k]
        source = sums[k * pieces + i // count].at[i % count]
        return pltpu.make_async_copy(source, low.at[i], load_sem.at[k, i])

    def store(k, i):
        held, target = ((in_full, gin), (out_full, gout))[k]
        return pltpu.make_async_copy(held.at[i % ring], target.at[i], store_sem.at[k, i % ring])

    for i in range(total):
        for k in range(2):
            load(k, i).start()
    blocks, in_blocks, gains, summed, output_first, output_last = smalls
    width = gout.shape[2]
    for i in range(blocks.shape[0]):
        at = pl.ds(i * blocks.shape[1], blocks.shape[1])
        block_out[at, :] = blocks[i]
        in_grad[at, :] = in_blocks[i]
    gain_sum = jnp.sum(gains[...], axis=0)
    gain_attn[...] = gain_sum[0:1, :]
    gain_moe[...] = gain_sum[1:2, :]
    query[...] = summed[:width, :].astype(jnp.float32)
    pair[...] = summed[width : 2 * width, :].astype(jnp.float32)
    router[...] = summed[2 * width : 2 * width + router.shape[0], :].astype(jnp.float32)
    half = output_first.shape[1]
    for i in range(width // half):
        from_first = i % 2 == 0
        rows = (output_first if from_first else output_last)[i // 2].astype(jnp.float32)
        for j in range(max(1, half // LANES)):
            place = i * half + j * LANES
            at = place // LANES
            part = rows[j * LANES : (j + 1) * LANES, :]
            first = place % LANES
            output[first : first + part.shape[0], at * LANES : (at + 1) * LANES] = part
    for i in range(total):
        for k in range(2):
            load(k, i).wait()
            if i >= ring:
                store(k, i - ring).wait()
        for low, held in ((in_low, in_full), (out_low, out_full)):
            widened(low.at[i], held.at[i % ring])
        for k in range(2):
            store(k, i).start()
    for i in range(total - ring, total):
        for k in range(2):
            store(k, i).wait()


def outputs(in_sums, out_sums, hidden, experts, *smalls):
    count = in_sums[0].shape[0]
    total = count * len(in_sums)
    width = out_sums[0].shape[2]
    parts = hidden // LANES
    lanes = smalls[0].shape[2]
    tokens = smalls[0].shape[0] * smalls[0].shape[1]
    low, full = jnp.bfloat16, jnp.float32
    large = [(width * 2 * parts, LANES), (hidden, width)]
    shapes = [((total,) + s, full) for s in large] + [
        ((tokens, lanes), low),
        ((tokens, lanes), low),
        ((1, LANES), full),
        ((1, LANES), full),
        ((width, LANES), full),
        ((width, LANES), full),
        ((LANES, width), full),
        ((experts, LANES), full),
    ]
    ring = min(4, total)
    gin, *others = pl.pallas_call(
        functools.partial(outputs_body, count, total),
        in_specs=[HBM] * (2 * len(in_sums)) + [FULL] * len(smalls),
        out_specs=(HBM, HBM) + (FULL,) * (len(shapes) - 2),
        out_shape=tuple(jax.ShapeDtypeStruct(*shape) for shape in shapes),
        scratch_shapes=[pltpu.VMEM((total,) + s, low) for s in large]
        + [pltpu.VMEM((ring,) + s, full) for s in large]
        + [pltpu.SemaphoreType.DMA((2, total)), pltpu.SemaphoreType.DMA((2, ring))],
        name="outputs",
    )(*in_sums, *out_sums, *smalls)
    gin = gin.reshape(total, width, parts, 2, LANES).transpose(0, 1, 3, 2, 4)
    return gin.reshape(total, width, 2, hidden), *others


def local(
    sizes,
    tokens,
    out_grad,
    doc_ids,
    expert_ids,
    gain_attn,
    w_query,
    w_key_value,
    w_output,
    gain_moe,
    w_router,
    w_expert_in,
    w_expert_out,
):
    rows, cols, depth = sizes
    group = rows * cols
    tok_rows, feat_local = tokens.shape
    width = w_query.shape[0]
    experts = w_router.shape[1]
    expert_local, hidden = w_expert_out.shape[0], w_expert_out.shape[1]
    longest_doc = min(LONGEST, tok_rows * depth // 2)
    hop_count = longest_doc // tok_rows
    own = tok_rows // group
    low, full = jnp.bfloat16, jnp.float32
    layer = lax.axis_index("dp")
    me = lax.axis_index("row") * cols + lax.axis_index("col")
    everyone = list(range(1, depth))
    hops = list(range(1, hop_count + 1))

    w_pair = w_key_value.reshape(width, -1)
    block = (tok_rows, LANES)
    cosine, sine, normed, query, pair, tokens_own, gains, gains_moe, router, docs_far, grads_shifted, grad_blocks = exchange(
        sizes,
        "gather_tokens",
        0,
        ("gather", tokens, False, 2),
        ("share", gain_attn.reshape(1, LANES)),
        ("share", gain_moe.reshape(1, LANES)),
        ("share", w_router.T),
        ("shift", doc_ids.reshape(-1, LANES), everyone, False),
        ("shift", out_grad, everyone, False),
        ("gather", out_grad, False, 2),
        before=Stage(tables_body, [(block, full), (block, full)]),
        after=Stage(
            project_body,
            [((tok_rows, width), low), (block, low), (block, low), ((own, width), low)],
            Got(0),
            Got(1),
            w_query,
            w_pair,
            Made(0),
            Made(1),
        ),
        landing=(0,),
    )

    stack = (hop_count + 1,) + block
    twice = (2 * tok_rows, LANES)
    turned_block = (LANES, tok_rows)
    whole = (2 * tok_rows, 1)
    grad_own, grads_near, far_turned, start, mixed, log_total, far, output_blocks = exchange(
        sizes,
        "shift_pairs",
        1,
        ("shift", pair, hops, False),
        ("gather", w_output, False, 4),
        before=Stage(
            attend_first_body,
            [
                ((own, width), low),
                ((group,) + turned_block, low),
                ((depth - 1,) + turned_block, low),
                ((tok_rows, 1), jnp.int32),
            ],
            grad_blocks,
            grads_shifted,
            query,
            pair,
            doc_ids.reshape(-1, LANES),
            docs_far,
        ),
        after=Stage(
            attend_rest_body,
            [(block, low), (whole, full)],
            Got(0),
            Made(3),
        ),
        shared=[
            pltpu.VMEM(stack, low),
            pltpu.VMEM(stack, low),
            pltpu.VMEM(twice, low),
            pltpu.VMEM(twice, full),
            pltpu.VMEM(whole, full),
            pltpu.VMEM(whole, full),
        ],
    )
    output_full = output_blocks.reshape(-1, width)

    rows_own, middle, weights = exchange(
        sizes,
        "swap_mixed",
        2,
        ("swap", mixed.reshape(group, own, LANES)),
        after=Stage(
            middle_body,
            [((own, width + LANES), low), ((own, width), full), ((own, LANES), full)],
            Got(0),
            tokens_own,
            output_full,
            gains_moe,
            router,
            expert_ids.T,
            scratch=[pltpu.VMEM(expert_ids.shape, full)],
        ),
        landing=(0,),
    )
    rows_blocks, rows_shifted = exchange(
        sizes,
        "gather_rows",
        3,
        ("gather", rows_own, False, 2),
        ("line", rows_own, False, 2),
    )
    rows_near = rows_blocks.reshape(tok_rows, -1)
    parts = hidden // LANES
    in_rows = w_expert_in.reshape(expert_local, width, 2, parts, LANES)
    in_rows = in_rows.transpose(0, 1, 3, 2, 4).reshape(expert_local, -1, LANES)
    moe_partial, back_partial, in_flat, in_part, out_part, grads_far, rows_far = local_experts(
        sizes,
        9,
        rows_near,
        grads_near.reshape(width, tok_rows),
        in_rows,
        w_expert_out,
        far_turned,
        rows_shifted,
    )
    rows_far = rows_far.reshape((depth - 1) * tok_rows, -1)
    grads_far = grads_far.reshape(depth - 1, width, tok_rows)
    work = (in_flat, w_expert_out, in_part, out_part, rows_far, grads_far)
    share = expert_local // 4
    unit = 16 * depth
    in_sums, out_sums = [], []

    def beneath(name, number, *items, after=None, landing=()):
        cover = Cover(len(in_sums) * share, share, work)
        in_sum, out_sum, *moved = exchange(
            sizes, name, number, *items, after=after, cover=cover, landing=landing
        )
        if after:
            count = len(after.shapes)
            results = [in_sum, out_sum, *moved]
            in_sum, out_sum = results[count], results[count + 1]
            moved = results[:count] + results[count + 2 :]
        in_sums.append(in_sum)
        out_sums.append(out_sum)
        return moved

    middle_grad, attn_grad, logit_grad, gain_moe_part = beneath(
        "swap_back",
        4,
        ("swap", back_partial.reshape(group, own, -1)),
        after=Stage(
            middle_back_body,
            [
                ((own, width), full),
                ((own, width), low),
                ((own, LANES), low),
                ((1, width), full),
            ],
            Got(0),
            grad_own,
            middle,
            weights,
            gains_moe,
            router,
        ),
        landing=(0,),
    )
    query_grad, pair_grad, far_grad, output_sum, logit_blocks = exchange(
        sizes,
        "gather_attn_grad",
        5,
        ("gather", attn_grad, False, 2),
        ("gather", logit_grad),
        before=Stage(attend_again_body, [], query, pair, far, start, log_total),
        after=Stage(
            attend_back_body,
            [
                (block, low),
                (block, full),
                ((hop_count,) + block, low),
                ((group, LANES, LANES), low),
            ],
            Got(0),
            w_output,
            mixed,
            cosine,
            sine,
            scratch=[
                pltpu.VMEM(twice, low),
                pltpu.VMEM(twice, full),
                pltpu.VMEM(stack, full),
                pltpu.VMEM(stack, full),
            ],
        ),
        landing=(0,),
        shared=[
            pltpu.VMEM(stack, low),
            pltpu.VMEM(stack, low),
            pltpu.VMEM(twice, low),
            pltpu.VMEM((hop_count + 1, 2 * tok_rows, tok_rows), full),
        ],
    )
    length = (2 * width + LANES + unit - 1) // unit * unit
    partial, sums, output_first, output_last, gain_parts, moe_blocks = beneath(
        "shift_grads",
        6,
        ("shift", far_grad, [-d for d in hops], True),
        ("swap", moe_partial.reshape(group, own, width)),
        ("turn", output_sum.reshape(depth, width // depth, LANES)),
        after=Stage(
            project_back_body,
            [
                ((tok_rows, width), low),
                ((length, LANES), low),
                ((width // depth // 2, LANES), low),
                ((width // depth // 2, LANES), low),
                ((group, 8, LANES), full),
            ],
            query_grad,
            pair_grad,
            Got(0),
            normed,
            w_query,
            w_pair,
            cosine,
            sine,
            Got(2),
            logit_blocks,
            rows_near,
            gains,
            gain_moe_part,
        ),
        landing=(0, 2),
    )
    pieces = (group, own, LANES)
    block_out, in_grad, gain_sum, summed, output_first = beneath(
        "swap_partial",
        7,
        ("swap", partial.reshape(group, own, width)),
        ("turn", sums.reshape(depth, length // depth, LANES)),
        ("swap", gain_parts),
        ("collect", output_first),
        after=Stage(
            results_body,
            [(pieces, low), (pieces, low), ((8, LANES), full), ((length // depth, LANES), low)],
            Got(0),
            moe_blocks,
            tokens_own,
            middle,
            middle_grad,
            gains,
            Got(2),
            Got(1),
        ),
        landing=(0, 1, 2),
    )
    block_out, in_grad, sums, output_last, gain_all = beneath(
        "swap_results",
        8,
        ("swap", block_out),
        ("swap", in_grad),
        ("collect", summed),
        ("collect", output_last),
        ("collect", gain_sum),
    )
    grad_in, grad_out, block_out, in_grad, gain_attn_sum, gain_moe_sum, query_sum, pair_sum, output_sum, router_sum = outputs(
        in_sums,
        out_sums,
        hidden,
        experts,
        block_out,
        in_grad,
        gain_all,
        sums.reshape(length, LANES),
        output_first,
        output_last,
    )
    return (
        block_out,
        in_grad,
        gain_attn_sum.reshape(LANES),
        query_sum,
        pair_sum.reshape(w_key_value.shape),
        output_sum,
        gain_moe_sum.reshape(LANES),
        router_sum.T,
        grad_in,
        grad_out,
    )


def solution(mesh):
    in_specs = (
        P("dp", ("row", "col")),
        P("dp", ("row", "col")),
        P("dp"),
        P("dp", None),
        P(("row", "col")),
        P(None, ("row", "col")),
        P(None, ("row", "col"), None),
        P(("row", "col"), None),
        P(("row", "col")),
        P(("row", "col"), None),
        P("row", None, None, "col"),
        P("row", "col", None),
    )
    out_specs = (
        P("dp", ("row", "col")),
        P("dp", ("row", "col")),
        P(("row", "col")),
        P(None, ("row", "col")),
        P(None, ("row", "col"), None),
        P(("row", "col"), None),
        P(("row", "col")),
        P(("row", "col"), None),
        P("row", None, None, "col"),
        P("row", "col", None),
    )
    sizes = (mesh.shape["row"], mesh.shape["col"], mesh.shape["dp"])
    return jax.shard_map(
        functools.partial(local, sizes),
        mesh=mesh,
        in_specs=in_specs,
        out_specs=out_specs,
        check_vma=False,
    )
```

```python
import functools
import itertools
import math

import jax
import jax.numpy as jnp
from jax import lax
from jax.experimental import pallas as pl
from jax.experimental.pallas import tpu as pltpu
from jax.sharding import PartitionSpec as P

LONGEST = 4096
HIGH = lax.Precision.HIGHEST
EPSILON = 1e-05
RESIDUAL_SCALE = 0.22
SCORE_SCALE = 0.015625
ROPE_BASE = 10000.0
MASKED = -1e30
MESH = pl.DeviceIdType.MESH
GROUP = ("row", "col")
EVERY = ("dp", "row", "col")
LANES = 128
HBM = pl.BlockSpec(memory_space=pl.ANY)
FULL = pl.BlockSpec(memory_space=pltpu.VMEM)
TURN = LANES // 4


class Moves:
    def __init__(self, sizes, kinds, sources, targets, sems):
        self.sizes, self.kinds = sizes, kinds
        self.sources, self.targets = sources, targets
        self.send_sem, self.recv_sem, self.local_sem = sems

    def place(self):
        row, col, layer = lax.axis_index("row"), lax.axis_index("col"), lax.axis_index("dp")
        return row, col, layer, row * self.sizes[1] + col

    def member(self, index):
        rows, cols, depth = self.sizes
        return {"row": index // cols, "col": lax.rem(index, cols)}

    def across(self, row):
        low = lax.rem(row, 2)
        return row + 1 - 2 * low, lax.rem(row + 2, 4), lax.rem(row + 3 - 2 * low, 4)

    def barrier(self):
        rows, cols, depth = self.sizes
        row, col, layer, me = self.place()
        group = rows * cols
        names = [kind[0] for kind in self.kinds]
        barrier = pltpu.get_barrier_semaphore()
        partners = []
        if "swap" in names or "share" in names:
            for k in range(1, group):
                partners.append(self.member(lax.rem(me + k, group)))
        elif "gather" in names:
            for other in self.across(row)[:2]:
                partners.append({"row": other})
            for k in range(1, cols):
                partners.append({"col": lax.rem(col + k, cols)})
        shifts = set()
        for kind in self.kinds:
            if kind[0] == "shift":
                for d in kind[1]:
                    shifts |= {d % depth, -d % depth}
            elif kind[0] in ("turn", "collect"):
                shifts |= set(range(1, depth))
        for k in sorted(shifts - {0}):
            partners.append({"dp": lax.rem(layer + k, depth)})
        ends = [(layer > 0, layer - 1), (layer < depth - 1, layer + 1)]
        ends = ends if "line" in names and not shifts else []
        for partner in partners:
            pl.semaphore_signal(barrier, inc=1, device_id=partner, device_id_type=MESH)
        for there, other in ends:

            @pl.when(there)
            def _(device={"dp": other}):
                pl.semaphore_signal(barrier, inc=1, device_id=device, device_id_type=MESH)

        expected = len(partners)
        for there, _ in ends:
            expected = expected + there.astype(jnp.int32)
        pl.semaphore_wait(barrier, expected)

    def plan(self, only):
        rows, cols, depth = self.sizes
        row, col, layer, me = self.place()
        group = rows * cols
        slots = iter(range(self.send_sem.shape[0]))
        starts, relays, sends, arrivals, local = [], [], [], [], []

        def remote(source, target, device, slot=None):
            slot = next(slots) if slot is None else slot
            return functools.partial(
                pltpu.make_async_remote_copy,
                src_ref=source,
                dst_ref=target,
                send_sem=self.send_sem.at[slot],
                recv_sem=self.recv_sem.at[slot],
                device_id=device,
                device_id_type=MESH,
            )

        for index, (kind, source, target) in enumerate(
            zip(self.kinds, self.sources, self.targets)
        ):
            item = [], [], [], [], []
            begin, follow, sent, got, stay = item

            def keep(source, target):
                sem = self.local_sem.at[index]
                stay.append(functools.partial(pltpu.make_async_copy, source, target, sem))

            def direct(source, target, device):
                copy = None, remote(source, target, device)
                begin.append(copy)
                sent.append(copy)
                got.append(copy)

            if kind[0] == "gather":
                second, parts = kind[1:]
                size = source.shape[0] // parts
                beside, above, away = self.across(row)

                def at(other, part, piece=None):
                    member = other * cols + col
                    first, length, deep = part * size, size, ()
                    if piece is not None and size % 2 == 0:
                        length = size // 2
                        first = first + piece * length
                    elif piece is not None:
                        inner = source.shape[1] // 2
                        deep = (pl.ds(piece * inner, inner),)
                    some = pl.ds(first, length)
                    return target.at[(some, member) + deep if second else (member, some) + deep]

                def to_mates(piece):
                    made = []
                    for j in range(1, cols):
                        copy = None, remote(piece, piece, {"col": lax.rem(col + j, cols)})
                        made.append(copy)
                        sent.append(copy)
                        got.append(copy)
                    return made

                for part in range(parts):
                    some = source.at[pl.ds(part * size, size)]
                    ways = []
                    for near, other, piece in ((beside, above, 0), (above, beside, 1)):
                        first = None, remote(some, at(row, part), {"row": near})
                        passed = at(near, part, piece)
                        onward = None, remote(passed, passed, {"row": other})
                        begin.append(first)
                        sent.extend([first, onward])
                        ways.append((near, piece, first, onward))
                    for near, piece, first, onward in ways:
                        nexts = [onward] + to_mates(at(near, part))
                        follow.append((2 + 3 * part, 0, None, first[1], nexts))
                    for near, piece, first, onward in ways:
                        nexts = to_mates(at(away, part, piece))
                        follow.append((2 + 3 * parts + part, 1, None, onward[1], nexts))
                    for j in range(1, cols):
                        direct(some, at(row, part), {"col": lax.rem(col + j, cols)})
                keep(source, target.at[:, me] if second else target.at[me])
            elif kind[0] in ("swap", "share"):
                for k in range(1, group):
                    other = lax.rem(me + k, group)
                    piece = source.at[other] if kind[0] == "swap" else source
                    direct(piece, target.at[me], self.member(other))
                keep(source.at[me] if kind[0] == "swap" else source, target.at[me])
            elif kind[0] in ("turn", "collect"):
                for k in range(1, depth):
                    other = lax.rem(layer + k, depth)
                    piece = source.at[other] if kind[0] == "turn" else source
                    direct(piece, target.at[layer], {"dp": other})
                keep(source.at[layer] if kind[0] == "turn" else source, target.at[layer])
            elif kind[0] == "line":
                absolute, parts, limit = kind[1:]
                size = source.shape[0] // parts
                steps = limit or depth - 1
                ways = (1,) if limit else (1, -1)
                for part, way in itertools.product(range(parts), ways):
                    behind = layer if way == 1 else depth - 1 - layer
                    onward = layer + way
                    more = (onward >= 0) & (onward < depth)
                    mine = [next(slots) for _ in range(steps)]
                    some = pl.ds(part * size, size)

                    def held(step, where, way=way, some=some):
                        if step == 0:
                            return source.at[some]
                        if absolute:
                            return target.at[where - way * step, some]
                        return target.at[step - 1 if way == 1 else depth - 1 - step, some]

                    def sending(step, onward=onward, mine=mine, held=held):
                        device = {"dp": onward}
                        return remote(
                            held(step - 1, layer), held(step, onward), device, mine[step - 1]
                        )

                    begin.append((more, sending(1)))
                    for step in range(1, steps + 1):
                        sent.append((more & (behind >= step - 1), sending(step)))
                        block = held(step, layer)
                        arrival = remote(block, block, {"dp": onward}, mine[step - 1])
                        nexts = [(more, sending(step + 1))] if step < steps else []
                        when = 4 * step + part
                        follow.append((when, step - 1, behind >= step, arrival, nexts))
                if absolute:
                    keep(source, target.at[layer])
            else:
                for at_slot, d in enumerate(kind[1]):
                    piece = source.at[at_slot] if kind[2] else source
                    direct(piece, target.at[at_slot], {"dp": lax.rem(layer + d % depth, depth)})
            if only is None or index in only:
                starts += begin
                relays += follow
                sends += sent
                arrivals += got
                local += stay
        return starts, sorted(relays, key=lambda entry: entry[0]), sends, arrivals, local

    def given(self, condition, action):
        if condition is None:
            action()
        else:
            pl.when(condition)(action)

    def start(self, only=None):
        starts, _, _, _, local = self.plan(only)
        for condition, copy in starts:
            self.given(condition, lambda copy=copy: copy().start())
        for copy in local:
            copy().start()

    def relay(self, only=None, stages=None):
        for _, stage, condition, copy, nexts in self.plan(only)[1]:
            if stages is not None and stage not in stages:
                continue

            def action(copy=copy, nexts=nexts):
                copy().wait_recv()
                for more, follower in nexts:
                    self.given(more, lambda follower=follower: follower().start())

            self.given(condition, action)

    def finish(self, only=None):
        _, _, sends, arrivals, local = self.plan(only)
        for condition, copy in arrivals:
            self.given(condition, lambda copy=copy: copy().wait_recv())
        for condition, copy in sends:
            self.given(condition, lambda copy=copy: copy().wait_send())
        for copy in local:
            copy().wait()


def planned(sizes, items):
    rows, cols, depth = sizes
    group = rows * cols
    kinds, shapes, copies = [], [], 0
    for item in items:
        name, array = item[0], item[1]
        shape = array.shape
        if name == "gather":
            assert rows == 4
            second, parts = (item[2:] + (False, 1)[len(item) - 2 :])[:2]
            kinds.append((name, second, parts))
            shape = (shape[0], group) + shape[1:] if second else (group,) + shape
            copies += parts * (4 + 5 * (cols - 1))
        elif name == "shift":
            distances, split = item[2], item[3]
            kinds.append((name, tuple(distances), split))
            shape = (len(distances),) + (shape[1:] if split else shape)
            copies += len(distances)
        elif name == "line":
            parts, limit = (item[3:] + (1, 0)[len(item) - 3 :])[:2]
            kinds.append((name, item[2], parts, limit))
            shape = (depth if item[2] else limit or depth - 1,) + shape
            copies += (limit or 2 * (depth - 1)) * parts
        else:
            kinds.append((name,))
            if name in ("share", "collect"):
                shape = (group if name == "share" else depth,) + shape
            copies += (depth if name in ("turn", "collect") else group) - 1
        shapes.append(jax.ShapeDtypeStruct(shape, array.dtype))
    sems = [
        pltpu.SemaphoreType.DMA((copies,)),
        pltpu.SemaphoreType.DMA((copies,)),
        pltpu.SemaphoreType.DMA((len(items),)),
    ]
    return tuple(kinds), shapes, sems


class Got:
    def __init__(self, index):
        self.index = index


class Made:
    def __init__(self, index):
        self.index = index


class Stage:
    def __init__(self, body, shapes, *operands, scratch=()):
        self.body, self.shapes, self.operands = body, shapes, operands
        self.scratch = list(scratch)


def exchange(sizes, name, number, *items, before=None, after=None, cover=None, landing=(), shared=(), delayed=()):
    kinds, moved, sems = planned(sizes, items)
    stages = [stage for stage in (before, after) if stage]
    operands = []
    for stage in stages:
        for operand in stage.operands:
            if not isinstance(operand, (Got, Made)):
                operands.append(operand)
    work = list(cover.work) if cover else []
    outs = [s for stage in stages for s in stage.shapes]
    made_shapes = list(cover.shapes) if cover else []
    flown = [i for i in range(len(items)) if i not in landing]
    late = [o.index for o in (after.operands if after else ()) if isinstance(o, Got)]
    late = [i for i in late if i not in landing]
    scratch = []

    def take(shapes):
        first = len(scratch)
        scratch.extend(shapes)
        return slice(first, len(scratch))

    vmem = lambda s: pltpu.VMEM(tuple(s[0]), s[1])
    of = lambda a: (a.shape, a.dtype)
    operand_at = take([vmem(of(a)) for a in operands])
    result_at = take([vmem(s) for s in outs])
    landed_at = take([vmem(of(moved[i])) for i in landing])
    late_at = take([vmem(of(moved[i])) for i in late])
    stage_at = [take(stage.scratch) for stage in stages]
    shared_at = take(list(shared))
    needed = sorted({o.index for o in (after.operands if after else ()) if isinstance(o, Got)})
    others = [i for i in range(len(items)) if i not in needed]
    prompt = [i for i in range(len(items)) if i not in delayed]
    later = range(1, 2 * sizes[2])
    cover_at = take(cover.scratch) if cover else slice(0, 0)
    copies = len(operands) + len(outs) + len(late)
    copy_at = take([pltpu.SemaphoreType.DMA((max(1, copies),))])
    sems_at = take(sems)

    def body(*refs):
        cuts = [len(operands), len(work), len(items), len(outs), len(made_shapes), len(flown)]
        groups = []
        for cut in cuts:
            groups.append(refs[:cut])
            refs = refs[cut:]
        given, work_refs, sources, results, made_refs, flown_refs = groups
        loaded, held = refs[operand_at], refs[result_at]
        landed, lates, (copy_sem,) = refs[landed_at], refs[late_at], refs[copy_at]
        targets = [None] * len(items)
        for i, ref in zip(flown, flown_refs):
            targets[i] = ref
        for i, ref in zip(landing, landed):
            targets[i] = ref
        moves = Moves(sizes, kinds, sources, targets, refs[sems_at])
        number_of = iter(range(copies))
        copy = lambda a, b: pltpu.make_async_copy(a, b, copy_sem.at[next(number_of)])
        loads = [copy(a, b) for a, b in zip(given, loaded)]
        stores = [copy(a, b) for a, b in zip(held, results)]
        late_loads = [copy(targets[i], b) for i, b in zip(late, lates)]
        split = len([o for o in before.operands if not isinstance(o, Made)]) if before else 0
        first = len(before.shapes) if before else 0
        for load in loads:
            load.start()
        if cover:
            cover.begin(work_refs, refs[cover_at])
        moves.barrier()
        moves.start(prompt)
        if before:
            for load in loads[:split]:
                load.wait()
            before.body(*loaded[:split], *held[:first], *refs[stage_at[0]], *refs[shared_at])
            for store in stores[:first]:
                store.start()
        if cover:
            cover.run(work_refs, made_refs, refs[cover_at])
        moves.relay(prompt, (0,))
        moves.start(delayed)
        if after:
            moves.relay(needed, later)
            moves.finish(needed)
        moves.relay(delayed, (0,))
        if after:
            for load in late_loads:
                load.start()
            for load in loads[split:]:
                load.wait()
            for load in late_loads:
                load.wait()
            plain = iter(loaded[split:])
            values = []
            for operand in after.operands:
                if isinstance(operand, Made):
                    values.append(held[operand.index])
                elif isinstance(operand, Got) and operand.index in landing:
                    values.append(landed[landing.index(operand.index)])
                elif isinstance(operand, Got):
                    values.append(lates[late.index(operand.index)])
                else:
                    values.append(next(plain))
            after.body(*values, *held[first:], *refs[stage_at[-1]], *refs[shared_at])
            for store in stores[first:]:
                store.start()
        moves.relay(others, later)
        moves.finish(others)
        if cover:
            cover.end(made_refs, refs[cover_at])
        for store in stores:
            store.wait()

    shape = lambda s: jax.ShapeDtypeStruct(tuple(s[0]), s[1])
    return pl.pallas_call(
        body,
        out_shape=tuple(shape(s) for s in outs + made_shapes) + tuple(moved[i] for i in flown),
        in_specs=[HBM] * (len(operands) + len(work) + len(items)),
        out_specs=(HBM,) * (len(outs) + len(made_shapes) + len(flown)),
        scratch_shapes=scratch,
        compiler_params=pltpu.CompilerParams(collective_id=number, has_side_effects=True),
        name=name,
    )(*operands, *work, *[item[1] for item in items])


def dot(a, b, left=1, right=0, precision=None):
    return lax.dot_general(
        a,
        b,
        (((left,), (right,)), ((), ())),
        preferred_element_type=jnp.float32,
        precision=precision,
    )


def widened(source, target):
    size = target.shape[0] // 4

    def piece(i, carry):
        at = pl.ds(pl.multiple_of(i * size, size), size)
        target[at, :] = source[at, :].astype(target.dtype)
        return carry

    lax.fori_loop(0, 4, piece, 0)


def cleared(target):
    size = target.shape[0] // 8

    def piece(i, carry):
        at = pl.ds(pl.multiple_of(i * size, size), size)
        target[at, :] = jnp.zeros((size, target.shape[1]), target.dtype)
        return carry

    lax.fori_loop(0, 8, piece, 0)


def lanes_of(shape):
    return lax.broadcasted_iota(jnp.int32, shape, len(shape) - 1)


def flipped(values):
    lanes = lanes_of(values.shape)
    ahead = pltpu.roll(values, LANES - TURN, 1)
    behind = pltpu.roll(values, TURN, 1)
    return jnp.where(lanes % (2 * TURN) < TURN, ahead, behind)


def beside(blocks_ref):
    return jnp.concatenate([blocks_ref[i] for i in range(blocks_ref.shape[0])], axis=1)


def gain_row(gains_ref):
    return beside(gains_ref).astype(jnp.float32)


def added(blocks):
    return functools.reduce(
        jnp.add, [blocks[i].astype(jnp.float32) for i in range(blocks.shape[0])]
    )


def own_rows(count):
    me = lax.axis_index("row") * lax.axis_size("col") + lax.axis_index("col")
    return pl.ds(pl.multiple_of(me * count, count), count)


def column(row):
    return jnp.broadcast_to(row, (8, row.shape[1])).T[:, 0:1]


def tables_body(cosine, sine):
    step = 64
    lanes = lanes_of((step, LANES))
    power = (lanes % TURN).astype(jnp.float32) * (-math.log(ROPE_BASE) / TURN)
    frequencies = jnp.exp(power)
    base = lax.axis_index("dp") * cosine.shape[0]

    def piece(i, carry):
        at = pl.ds(pl.multiple_of(i * step, step), step)
        positions = base + i * step + lax.broadcasted_iota(jnp.int32, lanes.shape, 0)
        angles = positions.astype(jnp.float32) * frequencies
        cosine[at, :] = jnp.cos(angles)
        value = jnp.sin(angles)
        sine[at, :] = jnp.where(lanes % (2 * TURN) < TURN, -value, value)
        return carry

    lax.fori_loop(0, cosine.shape[0] // step, piece, 0)


def turned(source, target):
    def block(i, carry):
        scaled = RESIDUAL_SCALE * source[i].astype(jnp.float32)
        target[i] = scaled.T.astype(jnp.bfloat16)
        return carry

    lax.fori_loop(0, target.shape[0], block, 0)


def project_body(blocks, gains, w_query, w_pair, cosine, sine, normed, query, pair, own):
    gain = gain_row(gains)
    step = 128

    def piece(i, carry):
        at = pl.ds(pl.multiple_of(i * step, step), step)
        parts = [blocks[k, at, :] for k in range(blocks.shape[0])]
        tokens = jnp.concatenate(parts, axis=1).astype(jnp.float32)
        scale = lax.rsqrt(jnp.mean(tokens * tokens, axis=1, keepdims=True) + EPSILON)
        normed[at, :] = (tokens * scale * gain).astype(jnp.bfloat16)
        return carry

    lax.fori_loop(0, normed.shape[0] // step, piece, 0)
    raw = dot(normed[...], w_query[...])
    query[...] = (raw * cosine[...] + flipped(raw) * sine[...]).astype(jnp.bfloat16)
    raw = dot(normed[...], w_pair[...])
    keys = lanes_of(raw.shape) < LANES // 2
    turned = raw * cosine[...] + flipped(raw) * sine[...]
    pair[...] = jnp.where(keys, turned, raw).astype(jnp.bfloat16)
    for i in range(blocks.shape[0]):
        own[:, i * LANES : (i + 1) * LANES] = blocks[i, own_rows(own.shape[0]), :]


def doubled(pair, keys_ref, values_ref, at, distance=0):
    wide = pair.astype(jnp.float32)
    if distance:
        wide = jnp.where(lax.axis_index("dp") >= distance, wide, 0.0)
    other = pltpu.roll(wide, LANES // 2, 1)
    keys = lanes_of(wide.shape) < LANES // 2
    keys_ref[at] = jnp.where(keys, wide, other).astype(jnp.bfloat16)
    values_ref[at] = jnp.where(keys, other, wide).astype(jnp.bfloat16)


def per_head(values):
    first = lanes_of(values.shape) < LANES // 2
    zero = jnp.zeros_like(values)
    return jnp.concatenate(
        [jnp.where(first, values, zero), jnp.where(first, zero, values)], axis=0
    )


def tile_scores(queries, keys_ref, starts, row, block, last, tokens):
    scores = dot(queries, keys_ref[block], 1, 1) * SCORE_SCALE
    at = lanes_of(scores.shape) + block * tokens
    allowed = at >= starts
    if block == last:
        place = row + lax.broadcasted_iota(jnp.int32, scores.shape, 0)
        allowed = allowed & (at <= place + block * tokens)
    return jnp.where(allowed, scores, MASKED)


def doc_row(docs):
    rows = [docs[i : i + 1, :] for i in range(docs.shape[0])]
    return jnp.concatenate(rows, axis=1).astype(jnp.float32)


def attend_tiles(tokens, tile):
    step = 256

    def body(i, carry):
        rows = pl.ds(pl.multiple_of(i * step, step), step)
        tile(rows, lax.rem(i * step, tokens), step)
        return carry

    lax.fori_loop(0, 2 * tokens // step, body, 0)


def attend_first_body(near_grads, far_grads, query, pair, docs, far_docs, own_grad, near_turned, far_turned, start, keys, values, queries, out, tops, totals):
    turned(near_grads, near_turned)
    turned(far_grads, far_turned)
    for i in range(near_grads.shape[0]):
        own_grad[:, i * LANES : (i + 1) * LANES] = near_grads[i, own_rows(own_grad.shape[0]), :]
    tokens = query.shape[0]
    last = keys.shape[0] - 1
    layer = lax.axis_index("dp")
    here = doc_row(docs[...])
    mine = column(here)
    before = jnp.sum((here < mine).astype(jnp.float32), axis=1, keepdims=True)
    for d in range(1, last + 1):
        fewer = (doc_row(far_docs[d - 1]) < mine) | (layer < d)
        before = before + jnp.sum(fewer.astype(jnp.float32), axis=1, keepdims=True)
    start[...] = before.astype(jnp.int32)
    doubled(pair[...], keys, values, last)
    queries[...] = per_head(query[...].astype(jnp.float32)).astype(jnp.bfloat16)

    def tile(rows, row, step):
        starts = start[pl.ds(pl.multiple_of(row, step), step), :]
        scores = tile_scores(queries[rows, :], keys, starts, row, last, last, tokens)
        top = jnp.max(scores, axis=1, keepdims=True)
        terms = jnp.exp(scores - top)
        tops[rows, :] = top
        totals[rows, :] = jnp.sum(terms, axis=1, keepdims=True)
        out[rows, :] = dot(terms.astype(jnp.bfloat16), values[last])

    attend_tiles(tokens, tile)


def attend_rest_body(far, start, mixed, log_total, keys, values, queries, out, tops, totals):
    last, tokens = far.shape[0], far.shape[1]
    for d in range(1, last + 1):
        doubled(far[d - 1], keys, values, last - d, d)

    def tile(rows, row, step):
        starts = start[pl.ds(pl.multiple_of(row, step), step), :]
        parts = [
            tile_scores(queries[rows, :], keys, starts, row, block, last, tokens)
            for block in range(last)
        ]
        top = functools.reduce(
            jnp.maximum, [jnp.max(part, axis=1, keepdims=True) for part in parts], tops[rows, :]
        )
        parts = [jnp.exp(part - top) for part in parts]
        scale = jnp.exp(tops[rows, :] - top)
        total = functools.reduce(
            jnp.add,
            [jnp.sum(p, axis=1, keepdims=True) for p in parts],
            totals[rows, :] * scale,
        )
        sums = [
            dot(part.astype(jnp.bfloat16), values[block]) for block, part in enumerate(parts)
        ]
        out[rows, :] = functools.reduce(jnp.add, sums, out[rows, :] * scale) / total
        log_total[rows, :] = top + jnp.log(total)

    attend_tiles(tokens, tile)
    first = lanes_of((tokens, LANES)) < LANES // 2
    mixed[...] = jnp.where(first, out[:tokens, :], out[tokens:, :]).astype(jnp.bfloat16)


def attend_again_body(query, pair, far, start, log_total, keys, values, queries, chances):
    tokens = query.shape[0]
    last = far.shape[0]
    doubled(pair[...], keys, values, last)
    for d in range(1, last + 1):
        doubled(far[d - 1], keys, values, last - d, d)
    queries[...] = per_head(query[...].astype(jnp.float32)).astype(jnp.bfloat16)

    def tile(rows, row, step):
        starts = start[pl.ds(pl.multiple_of(row, step), step), :]
        for block in range(last + 1):
            scores = tile_scores(queries[rows, :], keys, starts, row, block, last, tokens)
            chances[block, rows, :] = jnp.exp(scores - log_total[rows, :])

    attend_tiles(tokens, tile)


def attend_back_body(grad, w_output, mixed, cosine, sine, query_grad, pair_grad, far_grad, output_grad, grads, turned, key_sums, value_sums, keys, values, queries, chances):
    tokens = mixed.shape[0]
    last = keys.shape[0] - 1
    given_grad = grad[...].reshape(tokens, -1)
    grads[...] = per_head(dot(given_grad, w_output[...], 1, 1)).astype(jnp.bfloat16)
    output_sum = dot(mixed[...], given_grad, 0, 0).astype(jnp.bfloat16)
    for i in range(output_grad.shape[0]):
        output_grad[i] = output_sum[:, i * LANES : (i + 1) * LANES]
    for block in range(last + 1):
        cleared(key_sums.at[block])
        cleared(value_sums.at[block])

    def tile(rows, row, step):
        asked, given = queries[rows, :], grads[rows, :]
        products = [dot(given, values[block], 1, 1) for block in range(last + 1)]
        delta = functools.reduce(
            jnp.add,
            [
                jnp.sum(chances[block, rows, :] * product, axis=1, keepdims=True)
                for block, product in enumerate(products)
            ],
        )
        total = jnp.zeros((step, LANES), jnp.float32)
        for block in range(last + 1):
            chance = chances[block, rows, :]
            back = (chance * (products[block] - delta)).astype(jnp.bfloat16)
            total = total + dot(back, keys[block])
            key_sums[block] += dot(back, asked, 0, 0)
            value_sums[block] += dot(chance.astype(jnp.bfloat16), given, 0, 0)
        turned[rows, :] = total

    attend_tiles(tokens, tile)
    first = lanes_of((tokens, LANES)) < LANES // 2
    raw = jnp.where(first, turned[:tokens, :], turned[tokens:, :]) * SCORE_SCALE
    query_grad[...] = (raw * cosine[...] - flipped(raw) * sine[...]).astype(jnp.bfloat16)

    def joined(block):
        by_key, by_value = key_sums[block], value_sums[block]
        by_key = (by_key + pltpu.roll(by_key, LANES // 2, 1)) * SCORE_SCALE
        by_value = by_value + pltpu.roll(by_value, LANES // 2, 1)
        return jnp.where(first, by_key, by_value)

    pair_grad[...] = joined(last)
    for d in range(1, last + 1):
        far_grad[d - 1] = joined(last - d).astype(jnp.bfloat16)


def router_rows(router):
    rows = beside(router).astype(jnp.float32)
    blank = jnp.zeros((LANES - rows.shape[0], rows.shape[1]), jnp.float32)
    return jnp.concatenate([rows, blank], axis=0)


def middle_body(mixed, own, w_output, gains, router, ids_turned, rows, middle, weights, ids_ref):
    experts = router.shape[1]
    width = own.shape[1]
    attn = dot(beside(mixed), w_output[...])
    value = own[...].astype(jnp.float32) + RESIDUAL_SCALE * attn
    middle[...] = value
    scale = lax.rsqrt(jnp.mean(value * value, axis=1, keepdims=True) + EPSILON)
    normed = value * scale * gain_row(gains)
    logits = dot(normed, router_rows(router), 1, 1, precision=HIGH)
    count = own.shape[0]
    ids_ref[...] = ids_turned[...].astype(jnp.float32).T
    ids = ids_ref[own_rows(count), :]
    lanes = lanes_of((count, LANES))
    chosen = jnp.zeros((count, LANES), jnp.float32)
    for k in range(ids.shape[1]):
        chosen = chosen + (ids[:, k : k + 1] == lanes.astype(jnp.float32)).astype(
            jnp.float32
        )
    top = jnp.max(jnp.where(lanes < experts, logits, MASKED), axis=1, keepdims=True)
    terms = jnp.exp(jnp.minimum(logits - top, 0.0)) * chosen
    share = terms / jnp.sum(terms, axis=1, keepdims=True)
    weights[...] = share
    high = share.astype(jnp.bfloat16)
    low = share - high.astype(jnp.float32)
    rows[:, :width] = normed.astype(jnp.bfloat16)
    rows[:, width:] = (high.astype(jnp.float32) + pltpu.roll(low, LANES // 2, 1)).astype(
        jnp.bfloat16
    )


def middle_back_body(back, out_grad, middle, weights, gains, router, middle_grad, attn_grad, logit_grad, gain_part):
    width = middle.shape[1]
    normed_grad = back[0, :, :width].astype(jnp.float32)
    weight_grad = back[0, :, width:].astype(jnp.float32)
    for i in range(1, back.shape[0]):
        normed_grad = normed_grad + back[i, :, :width].astype(jnp.float32)
        weight_grad = weight_grad + back[i, :, width:].astype(jnp.float32)
    share, value = weights[...], middle[...]
    mean = jnp.sum(share * weight_grad, axis=1, keepdims=True)
    logit = share * (weight_grad - mean)
    logit_grad[...] = logit.astype(jnp.bfloat16)
    normed_grad = normed_grad + dot(logit, router_rows(router), precision=HIGH)
    scale = lax.rsqrt(jnp.mean(value * value, axis=1, keepdims=True) + EPSILON)
    gain_part[...] = jnp.sum(normed_grad * value * scale, axis=0, keepdims=True)
    scaled = normed_grad * gain_row(gains)
    norm_dot = jnp.sum(scaled * value, axis=1, keepdims=True)
    total = (
        out_grad[...].astype(jnp.float32)
        + scale * scaled
        - value * (scale * scale * scale * norm_dot / width)
    )
    middle_grad[...] = total
    attn_grad[...] = (RESIDUAL_SCALE * total).astype(jnp.bfloat16)


def project_back_body(query_grad, pair_grad, returned, normed, w_query, w_pair, cosine, sine, output_turned, logit, rows, gains, gain_moe, partial, sums, output_first, output_last, gain_parts, pairs):
    layer = lax.axis_index("dp")
    depth = lax.axis_size("dp")
    total = pair_grad[...]
    for i in range(returned.shape[0]):
        total = total + jnp.where(
            layer + i + 1 < depth, returned[i].astype(jnp.float32), 0.0
        )
    keys = lanes_of(total.shape) < LANES // 2
    turned = total * cosine[...] - flipped(total) * sine[...]
    pair_low = jnp.where(keys, turned, total).astype(jnp.bfloat16)
    query_low = query_grad[...]
    pairs[...] = pair_low
    step = 256

    def piece(i, gain_sum):
        at = pl.ds(pl.multiple_of(i * step, step), step)
        whole = dot(query_grad[at, :], w_query[...], 1, 1) + dot(pairs[at, :], w_pair[...], 1, 1)
        partial[at, :] = whole.astype(jnp.bfloat16)
        named = whole * normed[at, :].astype(jnp.float32)
        return gain_sum + jnp.sum(named, axis=0, keepdims=True)

    gain_attn = jnp.zeros((1, normed.shape[1]), jnp.float32)
    gain_attn = lax.fori_loop(0, normed.shape[0] // step, piece, gain_attn)
    gain_attn = gain_attn / gain_row(gains)
    gain_parts[...] = jnp.zeros_like(gain_parts)
    for i in range(gain_parts.shape[0]):
        at = slice(i * LANES, (i + 1) * LANES)
        gain_parts[i, 0:1, :] = gain_attn[:, at]
        gain_parts[i, 1:2, :] = gain_moe[0:1, at]
    width = normed.shape[1]
    sums[:width, :] = dot(normed[...], query_low, 0, 0).astype(jnp.bfloat16)
    sums[width : 2 * width, :] = dot(normed[...], pair_low, 0, 0).astype(jnp.bfloat16)
    output_sum = added(output_turned).astype(jnp.bfloat16)
    output_first[...] = output_sum[: output_first.shape[0], :]
    output_last[...] = output_sum[output_first.shape[0] :, :]
    mine = rows[:, own_rows(LANES)]
    named = logit[...].reshape(normed.shape[0], LANES)
    sums[2 * width : 2 * width + LANES, :] = dot(named, mine, 0, 0).astype(jnp.bfloat16)


def results_body(blocks, moe, own, middle, middle_grad, gains, gain_blocks, turned, block_out, in_grad, gain_sum, summed):
    gain_sum[...] = added(gain_blocks)
    summed[...] = added(turned).astype(jnp.bfloat16)
    width = own.shape[1]
    normed_grad = blocks[0].astype(jnp.float32)
    branch = moe[0].astype(jnp.float32)
    for i in range(1, blocks.shape[0]):
        normed_grad = normed_grad + blocks[i].astype(jnp.float32)
        branch = branch + moe[i].astype(jnp.float32)
    value = own[...].astype(jnp.float32)
    scale = lax.rsqrt(jnp.mean(value * value, axis=1, keepdims=True) + EPSILON)
    scaled = normed_grad * gain_row(gains)
    norm_dot = jnp.sum(scaled * value, axis=1, keepdims=True)
    grad = (
        middle_grad[...] + scale * scaled - value * (scale * scale * scale * norm_dot / width)
    ).astype(jnp.bfloat16)
    out = (middle[...] + RESIDUAL_SCALE * branch).astype(jnp.bfloat16)
    for i in range(block_out.shape[0]):
        at = slice(i * LANES, (i + 1) * LANES)
        block_out[i] = out[:, at]
        in_grad[i] = grad[:, at]


def expert_terms(gate_up, active_grad, weight):
    hidden = active_grad.shape[0]
    gate, up = gate_up[:hidden], gate_up[hidden:]
    sigmoid = jax.nn.sigmoid(gate)
    silu = gate * sigmoid
    ungated = silu * up
    active = (ungated * weight).astype(jnp.bfloat16)
    scaled = active_grad * weight
    gate_grad = (scaled * up * sigmoid * (1.0 + gate * (1.0 - sigmoid))).astype(jnp.bfloat16)
    up_grad = (scaled * silu).astype(jnp.bfloat16)
    return active, jnp.concatenate([gate_grad, up_grad], axis=0), active_grad * ungated


def weight_rows(extra):
    turned = extra.astype(jnp.float32).T
    return turned[: LANES // 2] + turned[LANES // 2 :]


def local_experts_body(sizes, kinds, rows_ref, grads_ref, in_ref, out_ref, sent_grads, sent_rows, moe_ref, back_ref, flat_ref, in_sum, out_sum, got_grads, got_rows, moe_acc, back_acc, share, weights, spread, *sems):
    step, steps = pl.program_id(0), pl.num_programs(0)
    each, hidden, width = out_ref.shape
    parts = hidden // LANES
    moves = Moves(sizes, kinds, [sent_grads, sent_rows], [got_grads, got_rows], sems)

    @pl.when(step == 0)
    def _():
        moves.barrier()
        moves.start([0])
        cleared(moe_acc)
        cleared(back_acc)
        share[...] = jnp.zeros_like(share)
        weights[...] = weight_rows(rows_ref[:, width:])

    @pl.when(step == 2 * steps // 8)
    def _():
        moves.start([1])

    for when, item, stage in ((3, 0, 0), (6, 1, 0), (7, 0, 1)):

        @pl.when(step == when * steps // 8)
        def _(item=item, stage=stage):
            moves.relay([item], (stage,))

    for i in range(each):
        spread[i] = in_ref[i].astype(jnp.float32)
        for part in range(parts):
            for half in range(2):
                at = half * hidden + part * LANES
                flat_ref[i, :, at : at + LANES] = spread[
                    i, pl.ds(part * 2 + half, width, stride=2 * parts), :
                ].astype(jnp.bfloat16)
        expert = (lax.axis_index("row") * steps + step) * each + i
        active, gate_up_grad, shares = expert_terms(
            dot(flat_ref[i], rows_ref[:, :width], 0, 1),
            dot(out_ref[i], grads_ref[...]),
            weights[pl.ds(expert, 1), :],
        )
        share[pl.ds(expert, 1), :] = jnp.sum(shares, axis=0, keepdims=True)
        moe_acc[...] += dot(active, out_ref[i], 0, 0)
        back_acc[...] += dot(gate_up_grad, flat_ref[i], 0, 1)
        in_sum[i] = dot(gate_up_grad, rows_ref[:, :width]).astype(jnp.bfloat16)
        out_sum[i] = dot(active, grads_ref[...], 1, 1).astype(jnp.bfloat16)

    @pl.when(step == steps - 1)
    def _():
        widened(moe_acc, moe_ref)
        widened(back_acc, back_ref.at[:, :width])
        back_ref[:, width:] = share[...].T.astype(jnp.bfloat16)
        moves.relay([1], (1,))
        moves.finish()


def local_experts(sizes, number, rows, grads, w_in, w_out, sent_grads, sent_rows):
    tokens, wide = rows.shape
    experts, hidden, width = w_out.shape
    each = 1
    low = jnp.bfloat16
    kinds, shapes, sems = planned(
        sizes,
        [
            ("gather", sent_grads, True, sent_grads.shape[0]),
            ("gather", sent_rows, True, sent_rows.shape[0]),
        ],
    )
    whole = lambda s: pl.BlockSpec(s, lambda e: (0,) * len(s))
    some = lambda s: pl.BlockSpec((each,) + s[1:], lambda e: (e,) + (0,) * (len(s) - 1))
    outs = [
        (tokens, width),
        (tokens, wide),
        (experts, width, 2 * hidden),
        (experts, 2 * hidden, width),
        (experts, hidden, width),
    ]
    return pl.pallas_call(
        functools.partial(local_experts_body, sizes, kinds),
        grid=(experts // each,),
        in_specs=[
            whole(rows.shape),
            whole(grads.shape),
            some(w_in.shape),
            some(w_out.shape),
            HBM,
            HBM,
        ],
        out_specs=(whole(outs[0]), whole(outs[1]), *[some(s) for s in outs[2:]], HBM, HBM),
        out_shape=tuple(jax.ShapeDtypeStruct(s, low) for s in outs) + tuple(shapes),
        scratch_shapes=[
            pltpu.VMEM((tokens, width), jnp.float32),
            pltpu.VMEM((tokens, width), jnp.float32),
            pltpu.VMEM((LANES, tokens), jnp.float32),
            pltpu.VMEM((LANES // 2, tokens), jnp.float32),
            pltpu.VMEM((each,) + w_in.shape[1:], jnp.float32),
        ]
        + sems,
        compiler_params=pltpu.CompilerParams(collective_id=number, has_side_effects=True),
        name="local_experts",
    )(rows, grads, w_in, w_out, sent_grads, sent_rows)


class Sums:
    def __init__(self, rows, grads, weights, turned, load_sem, *sums):
        self.rows, self.grads, self.weights = rows, grads, weights
        self.turned, self.load_sem, self.sums = turned, load_sem, sums

    def load(self, which, source):
        target = (self.rows, self.grads)[which]
        return pltpu.make_async_copy(source, target, self.load_sem.at[which])

    def ready(self):
        layers, width, tokens = self.grads.shape

        def block(i, carry):
            at = pl.ds(pl.multiple_of(i * tokens, tokens), tokens)
            self.weights[i] = weight_rows(self.rows[at, width:])
            return carry

        lax.fori_loop(0, layers, block, 0)

    def make(self, index, w_in, w_out, in_part, out_part, made, arrive):
        layers, width, tokens = self.grads.shape
        hidden = w_out.shape[0]
        arrive(0)
        if self.sums:
            arrive(1)
        later = arrive

        def part_of(at, pieces, arrive=lambda i: None if self.sums else later(i)):
            first = at * tokens if isinstance(at, int) else pl.multiple_of(at * tokens, tokens)
            block = self.rows[pl.ds(first, pieces * tokens), :width]
            gate_up = dot(w_in[...], block, 0, 1)
            arrive(1)
            weight = jnp.concatenate(
                [self.weights[at + i, pl.ds(index, 1), :] for i in range(pieces)], axis=1
            )
            active_grad = jnp.concatenate(
                [dot(w_out[...], self.grads[at + i]) for i in range(pieces)], axis=1
            )
            active, gate_up_grad, _ = expert_terms(gate_up, active_grad, weight)
            out_total = functools.reduce(
                jnp.add,
                [
                    dot(active[:, i * tokens : (i + 1) * tokens], self.grads[at + i], 1, 1)
                    for i in range(pieces)
                ],
            )
            return dot(gate_up_grad, block), out_total

        if not self.sums:
            in_total, out_total = part_of(0, layers)
        else:
            whole, out_acc = self.sums
            whole[...] = jnp.zeros_like(whole)
            out_acc[...] = jnp.zeros_like(out_acc)

            def more(i, carry):
                in_more, out_more = part_of(i, 1)
                whole[...] += in_more
                out_acc[...] += out_more
                return carry

            lax.fori_loop(0, layers, more, 0)
            in_total, out_total = whole[...], out_acc[...]
        arrive(2)
        in_total = in_total + in_part[...].astype(jnp.float32)
        parts = hidden // LANES
        for part in range(parts):
            for half in range(2):
                at = half * hidden + part * LANES
                self.turned[pl.ds(part * 2 + half, width, stride=2 * parts), :] = in_total[
                    at : at + LANES, :
                ].T
        made[...] = self.turned[...].astype(jnp.bfloat16)
        return out_total + out_part[...].astype(jnp.float32)


def sums_scratch(layers, tokens, width, hidden):
    low, full = jnp.bfloat16, jnp.float32
    return [
        pltpu.VMEM((layers * tokens, width + LANES), low),
        pltpu.VMEM((layers, width, tokens), low),
        pltpu.VMEM((layers, LANES // 2, tokens), full),
        pltpu.VMEM((width * 2 * hidden // LANES, LANES), full),
        pltpu.SemaphoreType.DMA((2,)),
    ] + [pltpu.VMEM((k * hidden, width), full) for k in (2, 1) if layers > 4]


class Cover:
    def __init__(self, first, many, work):
        w_in, w_out, in_part, out_part, rows_far, grads_far = work
        layers, width, tokens = grads_far.shape
        self.experts, hidden, _ = w_out.shape
        self.first, self.many, self.work = first, many, work
        low = jnp.bfloat16
        self.shapes = [
            ((many, width * 2 * hidden // LANES, LANES), low),
            ((many, hidden, width), low),
        ]
        self.scratch = [pltpu.VMEM((many,) + a.shape[1:], low) for a in work[:4]]
        self.scratch += [pltpu.VMEM(*s) for s in self.shapes]
        self.scratch += [pltpu.SemaphoreType.DMA((4, many)), pltpu.SemaphoreType.DMA((2, many))]
        self.scratch += sums_scratch(layers, tokens, width, hidden)

    def load(self, which, i, work, refs):
        source, sem = work[which].at[self.first + i], refs[6].at[which, i]
        return pltpu.make_async_copy(source, refs[which].at[i], sem)

    def begin(self, work, refs):
        sums = Sums(*refs[8:])
        sums.load(0, work[4]).start()
        self.load(0, 0, work, refs).start()
        sums.load(1, work[5]).start()
        for which in (1, 2, 3):
            self.load(which, 0, work, refs).start()
        for i in range(1, self.many):
            for which in range(4):
                self.load(which, i, work, refs).start()

    def stores(self, i, made, refs):
        return [
            pltpu.make_async_copy(refs[4 + k].at[i], made[k].at[i], refs[7].at[k, i])
            for k in range(2)
        ]

    def run(self, work, made, refs):
        sums = Sums(*refs[8:])

        def expert(i, carry):
            def arrive(point):
                @pl.when(i == 0)
                def _():
                    if point == 0:
                        sums.load(0, work[4]).wait()
                        sums.ready()
                    if point == 1:
                        sums.load(1, work[5]).wait()

                for which in ((0,), (1,), (2, 3))[point]:
                    self.load(which, i, work, refs).wait()

            index = lax.axis_index("row") * self.experts + self.first + i
            out_total = sums.make(index, *[refs[k].at[i] for k in range(5)], arrive)
            refs[5][i] = out_total.astype(jnp.bfloat16)
            for store in self.stores(i, made, refs):
                store.start()
            return carry

        lax.fori_loop(0, self.many, expert, 0)

    def end(self, made, refs):
        for i in range(self.many):
            for store in self.stores(i, made, refs):
                store.wait()


def outputs_body(count, total, *refs):
    pieces = total // count
    sums, smalls = refs[: 2 * pieces], refs[2 * pieces : 2 * pieces + 6]
    gin, gout, *others = refs[2 * pieces + 6 : 2 * pieces + 16]
    block_out, in_grad, gain_attn, gain_moe, query, pair, output, router = others
    in_low, out_low, in_full, out_full, *refs = refs[2 * pieces + 16 :]
    held, (load_sem, store_sem, small_sem) = refs[:6], refs[6:]
    ring = in_full.shape[0]

    def load(k, i):
        low = (in_low, out_low)[k]
        source = sums[k * pieces + i // count].at[i % count]
        return pltpu.make_async_copy(source, low.at[i], load_sem.at[k, i])

    def store(k, i):
        made, target = ((in_full, gin), (out_full, gout))[k]
        return pltpu.make_async_copy(made.at[i % ring], target.at[i], store_sem.at[k, i % ring])

    for i in range(total):
        for k in range(2):
            load(k, i).start()
        if i == 0:
            fetched = [
                pltpu.make_async_copy(a, b, small_sem.at[j])
                for j, (a, b) in enumerate(zip(smalls, held))
            ]
            for copy in fetched:
                copy.start()
    for copy in fetched:
        copy.wait()
    blocks, in_blocks, gains, summed, output_first, output_last = held
    width = gout.shape[2]
    for i in range(blocks.shape[0]):
        at = pl.ds(i * blocks.shape[1], blocks.shape[1])
        block_out[at, :] = blocks[i]
        in_grad[at, :] = in_blocks[i]
    gain_sum = jnp.sum(gains[...], axis=0)
    gain_attn[...] = gain_sum[0:1, :]
    gain_moe[...] = gain_sum[1:2, :]
    query[...] = summed[:width, :].astype(jnp.float32)
    pair[...] = summed[width : 2 * width, :].astype(jnp.float32)
    router[...] = summed[2 * width : 2 * width + router.shape[0], :].astype(jnp.float32)
    half = output_first.shape[1]
    for i in range(width // half):
        from_first = i % 2 == 0
        rows = (output_first if from_first else output_last)[i // 2].astype(jnp.float32)
        for j in range(max(1, half // LANES)):
            place = i * half + j * LANES
            at = place // LANES
            part = rows[j * LANES : (j + 1) * LANES, :]
            first = place % LANES
            output[first : first + part.shape[0], at * LANES : (at + 1) * LANES] = part
    for i in range(total):
        for k in range(2):
            load(k, i).wait()
            if i >= ring:
                store(k, i - ring).wait()
        for low, made in ((in_low, in_full), (out_low, out_full)):
            widened(low.at[i], made.at[i % ring])
        for k in range(2):
            store(k, i).start()
    for i in range(total - ring, total):
        for k in range(2):
            store(k, i).wait()


def outputs(in_sums, out_sums, hidden, experts, *smalls):
    count = in_sums[0].shape[0]
    total = count * len(in_sums)
    width = out_sums[0].shape[2]
    parts = hidden // LANES
    lanes = smalls[0].shape[2]
    tokens = smalls[0].shape[0] * smalls[0].shape[1]
    low, full = jnp.bfloat16, jnp.float32
    large = [(width * 2 * parts, LANES), (hidden, width)]
    shapes = [((total,) + s, full) for s in large] + [
        ((tokens, lanes), low),
        ((tokens, lanes), low),
        ((1, LANES), full),
        ((1, LANES), full),
        ((width, LANES), full),
        ((width, LANES), full),
        ((LANES, width), full),
        ((experts, LANES), full),
    ]
    ring = min(4, total)
    gin, *others = pl.pallas_call(
        functools.partial(outputs_body, count, total),
        in_specs=[HBM] * (2 * len(in_sums) + len(smalls)),
        out_specs=(HBM, HBM) + (FULL,) * (len(shapes) - 2),
        out_shape=tuple(jax.ShapeDtypeStruct(*shape) for shape in shapes),
        scratch_shapes=[pltpu.VMEM((total,) + s, low) for s in large]
        + [pltpu.VMEM((ring,) + s, full) for s in large]
        + [pltpu.VMEM(a.shape, a.dtype) for a in smalls]
        + [pltpu.SemaphoreType.DMA(s) for s in ((2, total), (2, ring), (len(smalls),))],
        name="outputs",
    )(*in_sums, *out_sums, *smalls)
    gin = gin.reshape(total, width, parts, 2, LANES).transpose(0, 1, 3, 2, 4)
    return gin.reshape(total, width, 2, hidden), *others


def local(
    sizes,
    tokens,
    out_grad,
    doc_ids,
    expert_ids,
    gain_attn,
    w_query,
    w_key_value,
    w_output,
    gain_moe,
    w_router,
    w_expert_in,
    w_expert_out,
):
    rows, cols, depth = sizes
    group = rows * cols
    tok_rows, feat_local = tokens.shape
    width = w_query.shape[0]
    experts = w_router.shape[1]
    expert_local, hidden = w_expert_out.shape[0], w_expert_out.shape[1]
    longest_doc = min(LONGEST, tok_rows * depth // 2)
    hop_count = longest_doc // tok_rows
    own = tok_rows // group
    low, full = jnp.bfloat16, jnp.float32
    layer = lax.axis_index("dp")
    me = lax.axis_index("row") * cols + lax.axis_index("col")
    everyone = list(range(1, depth))
    hops = list(range(1, hop_count + 1))

    w_pair = w_key_value.reshape(width, -1)
    block = (tok_rows, LANES)
    cosine, sine, normed, query, pair, tokens_own, gains, gains_moe, router, docs_far, grads_shifted, grad_blocks = exchange(
        sizes,
        "gather_tokens",
        0,
        ("gather", tokens, False, 2),
        ("share", gain_attn.reshape(1, LANES)),
        ("share", gain_moe.reshape(1, LANES)),
        ("share", w_router.T),
        ("shift", doc_ids.reshape(-1, LANES), everyone, False),
        ("shift", out_grad, everyone, False),
        ("gather", out_grad, False, 2),
        before=Stage(tables_body, [(block, full), (block, full)]),
        after=Stage(
            project_body,
            [((tok_rows, width), low), (block, low), (block, low), ((own, width), low)],
            Got(0),
            Got(1),
            w_query,
            w_pair,
            Made(0),
            Made(1),
        ),
        landing=(0,),
        delayed=(6,),
    )

    stack = (hop_count + 1,) + block
    twice = (2 * tok_rows, LANES)
    turned_block = (LANES, tok_rows)
    whole = (2 * tok_rows, 1)
    grad_own, grads_near, far_turned, start, mixed, log_total, far, output_blocks = exchange(
        sizes,
        "shift_pairs",
        1,
        ("line", pair, False, 2, hop_count),
        ("gather", w_output, False, 4),
        before=Stage(
            attend_first_body,
            [
                ((own, width), low),
                ((group,) + turned_block, low),
                ((depth - 1,) + turned_block, low),
                ((tok_rows, 1), jnp.int32),
            ],
            grad_blocks,
            grads_shifted,
            query,
            pair,
            doc_ids.reshape(-1, LANES),
            docs_far,
        ),
        after=Stage(
            attend_rest_body,
            [(block, low), (whole, full)],
            Got(0),
            Made(3),
        ),
        shared=[
            pltpu.VMEM(stack, low),
            pltpu.VMEM(stack, low),
            pltpu.VMEM(twice, low),
            pltpu.VMEM(twice, full),
            pltpu.VMEM(whole, full),
            pltpu.VMEM(whole, full),
        ],
    )
    output_full = output_blocks.reshape(-1, width)

    rows_own, middle, weights = exchange(
        sizes,
        "swap_mixed",
        2,
        ("swap", mixed.reshape(group, own, LANES)),
        after=Stage(
            middle_body,
            [((own, width + LANES), low), ((own, width), full), ((own, LANES), full)],
            Got(0),
            tokens_own,
            output_full,
            gains_moe,
            router,
            expert_ids.T,
            scratch=[pltpu.VMEM(expert_ids.shape, full)],
        ),
        landing=(0,),
    )
    rows_blocks, rows_shifted = exchange(
        sizes,
        "gather_rows",
        3,
        ("gather", rows_own, False, 2),
        ("line", rows_own, False, 4),
    )
    rows_near = rows_blocks.reshape(tok_rows, -1)
    parts = hidden // LANES
    in_rows = w_expert_in.reshape(expert_local, width, 2, parts, LANES)
    in_rows = in_rows.transpose(0, 1, 3, 2, 4).reshape(expert_local, -1, LANES)
    moe_partial, back_partial, in_flat, in_part, out_part, grads_far, rows_far = local_experts(
        sizes,
        9,
        rows_near,
        grads_near.reshape(width, tok_rows),
        in_rows,
        w_expert_out,
        far_turned,
        rows_shifted,
    )
    rows_far = rows_far.reshape((depth - 1) * tok_rows, -1)
    grads_far = grads_far.reshape(depth - 1, width, tok_rows)
    work = (in_flat, w_expert_out, in_part, out_part, rows_far, grads_far)
    share = expert_local // 4
    unit = 16 * depth
    in_sums, out_sums = [], []

    def beneath(name, number, *items, after=None, landing=()):
        cover = Cover(len(in_sums) * share, share, work)
        in_sum, out_sum, *moved = exchange(
            sizes, name, number, *items, after=after, cover=cover, landing=landing
        )
        if after:
            count = len(after.shapes)
            results = [in_sum, out_sum, *moved]
            in_sum, out_sum = results[count], results[count + 1]
            moved = results[:count] + results[count + 2 :]
        in_sums.append(in_sum)
        out_sums.append(out_sum)
        return moved

    middle_grad, attn_grad, logit_grad, gain_moe_part = beneath(
        "swap_back",
        4,
        ("swap", back_partial.reshape(group, own, -1)),
        after=Stage(
            middle_back_body,
            [
                ((own, width), full),
                ((own, width), low),
                ((own, LANES), low),
                ((1, width), full),
            ],
            Got(0),
            grad_own,
            middle,
            weights,
            gains_moe,
            router,
        ),
        landing=(0,),
    )
    query_grad, pair_grad, far_grad, output_sum, logit_blocks = exchange(
        sizes,
        "gather_attn_grad",
        5,
        ("gather", attn_grad, False, 2),
        ("gather", logit_grad),
        before=Stage(attend_again_body, [], query, pair, far, start, log_total),
        after=Stage(
            attend_back_body,
            [
                (block, low),
                (block, full),
                ((hop_count,) + block, low),
                ((group, LANES, LANES), low),
            ],
            Got(0),
            w_output,
            mixed,
            cosine,
            sine,
            scratch=[
                pltpu.VMEM(twice, low),
                pltpu.VMEM(twice, full),
                pltpu.VMEM(stack, full),
                pltpu.VMEM(stack, full),
            ],
        ),
        landing=(0,),
        shared=[
            pltpu.VMEM(stack, low),
            pltpu.VMEM(stack, low),
            pltpu.VMEM(twice, low),
            pltpu.VMEM((hop_count + 1, 2 * tok_rows, tok_rows), full),
        ],
    )
    length = (2 * width + LANES + unit - 1) // unit * unit
    partial, sums, output_first, output_last, gain_parts, moe_blocks = beneath(
        "shift_grads",
        6,
        ("shift", far_grad, [-d for d in hops], True),
        ("swap", moe_partial.reshape(group, own, width)),
        ("turn", output_sum.reshape(depth, width // depth, LANES)),
        after=Stage(
            project_back_body,
            [
                ((tok_rows, width), low),
                ((length, LANES), low),
                ((width // depth // 2, LANES), low),
                ((width // depth // 2, LANES), low),
                ((group, 8, LANES), full),
            ],
            query_grad,
            pair_grad,
            Got(0),
            normed,
            w_query,
            w_pair,
            cosine,
            sine,
            Got(2),
            logit_blocks,
            rows_near,
            gains,
            gain_moe_part,
            scratch=[pltpu.VMEM(block, low)],
        ),
        landing=(0, 2),
    )
    pieces = (group, own, LANES)
    block_out, in_grad, gain_sum, summed, output_first = beneath(
        "swap_partial",
        7,
        ("swap", partial.reshape(group, own, width)),
        ("turn", sums.reshape(depth, length // depth, LANES)),
        ("swap", gain_parts),
        ("collect", output_first),
        after=Stage(
            results_body,
            [(pieces, low), (pieces, low), ((8, LANES), full), ((length // depth, LANES), low)],
            Got(0),
            moe_blocks,
            tokens_own,
            middle,
            middle_grad,
            gains,
            Got(2),
            Got(1),
        ),
        landing=(0, 1, 2),
    )
    block_out, in_grad, sums, output_last, gain_all = beneath(
        "swap_results",
        8,
        ("swap", block_out),
        ("swap", in_grad),
        ("collect", summed),
        ("collect", output_last),
        ("collect", gain_sum),
    )
    grad_in, grad_out, block_out, in_grad, gain_attn_sum, gain_moe_sum, query_sum, pair_sum, output_sum, router_sum = outputs(
        in_sums,
        out_sums,
        hidden,
        experts,
        block_out,
        in_grad,
        gain_all,
        sums.reshape(length, LANES),
        output_first,
        output_last,
    )
    return (
        block_out,
        in_grad,
        gain_attn_sum.reshape(LANES),
        query_sum,
        pair_sum.reshape(w_key_value.shape),
        output_sum,
        gain_moe_sum.reshape(LANES),
        router_sum.T,
        grad_in,
        grad_out,
    )


def solution(mesh):
    in_specs = (
        P("dp", ("row", "col")),
        P("dp", ("row", "col")),
        P("dp"),
        P("dp", None),
        P(("row", "col")),
        P(None, ("row", "col")),
        P(None, ("row", "col"), None),
        P(("row", "col"), None),
        P(("row", "col")),
        P(("row", "col"), None),
        P("row", None, None, "col"),
        P("row", "col", None),
    )
    out_specs = (
        P("dp", ("row", "col")),
        P("dp", ("row", "col")),
        P(("row", "col")),
        P(None, ("row", "col")),
        P(None, ("row", "col"), None),
        P(("row", "col"), None),
        P(("row", "col")),
        P(("row", "col"), None),
        P("row", None, None, "col"),
        P("row", "col", None),
    )
    sizes = (mesh.shape["row"], mesh.shape["col"], mesh.shape["dp"])
    return jax.shard_map(
        functools.partial(local, sizes),
        mesh=mesh,
        in_specs=in_specs,
        out_specs=out_specs,
        check_vma=False,
    )
```

```python
import functools
import itertools
import math

import jax
import jax.numpy as jnp
from jax import lax
from jax.experimental import pallas as pl
from jax.experimental.pallas import tpu as pltpu
from jax.sharding import PartitionSpec as P

LONGEST = 4096
HIGH = lax.Precision.HIGHEST
EPSILON = 1e-05
RESIDUAL_SCALE = 0.22
SCORE_SCALE = 0.015625
ROPE_BASE = 10000.0
MASKED = -1e30
MESH = pl.DeviceIdType.MESH
GROUP = ("row", "col")
EVERY = ("dp", "row", "col")
LANES = 128
HBM = pl.BlockSpec(memory_space=pl.ANY)
FULL = pl.BlockSpec(memory_space=pltpu.VMEM)
TURN = LANES // 4


class Moves:
    def __init__(self, sizes, kinds, sources, targets, sems):
        self.sizes, self.kinds = sizes, kinds
        self.sources, self.targets = sources, targets
        self.send_sem, self.recv_sem, self.local_sem = sems

    def place(self):
        row, col, layer = lax.axis_index("row"), lax.axis_index("col"), lax.axis_index("dp")
        return row, col, layer, row * self.sizes[1] + col

    def member(self, index):
        rows, cols, depth = self.sizes
        return {"row": index // cols, "col": lax.rem(index, cols)}

    def across(self, row):
        low = lax.rem(row, 2)
        return row + 1 - 2 * low, lax.rem(row + 2, 4), lax.rem(row + 3 - 2 * low, 4)

    def barrier(self):
        rows, cols, depth = self.sizes
        row, col, layer, me = self.place()
        group = rows * cols
        names = [kind[0] for kind in self.kinds]
        barrier = pltpu.get_barrier_semaphore()
        partners = []
        if "swap" in names or "share" in names:
            for k in range(1, group):
                partners.append(self.member(lax.rem(me + k, group)))
        elif "gather" in names:
            for other in self.across(row)[:2]:
                partners.append({"row": other})
            for k in range(1, cols):
                partners.append({"col": lax.rem(col + k, cols)})
        shifts = set()
        for kind in self.kinds:
            if kind[0] == "shift":
                for d in kind[1]:
                    shifts |= {d % depth, -d % depth}
            elif kind[0] in ("turn", "collect"):
                shifts |= set(range(1, depth))
        for k in sorted(shifts - {0}):
            partners.append({"dp": lax.rem(layer + k, depth)})
        ends = [(layer > 0, layer - 1), (layer < depth - 1, layer + 1)]
        ends = ends if "line" in names and not shifts else []
        for partner in partners:
            pl.semaphore_signal(barrier, inc=1, device_id=partner, device_id_type=MESH)
        for there, other in ends:

            @pl.when(there)
            def _(device={"dp": other}):
                pl.semaphore_signal(barrier, inc=1, device_id=device, device_id_type=MESH)

        expected = len(partners)
        for there, _ in ends:
            expected = expected + there.astype(jnp.int32)
        pl.semaphore_wait(barrier, expected)

    def plan(self, only):
        rows, cols, depth = self.sizes
        row, col, layer, me = self.place()
        group = rows * cols
        slots = iter(range(self.send_sem.shape[0]))
        starts, relays, sends, arrivals, local = [], [], [], [], []

        def remote(source, target, device, slot=None):
            slot = next(slots) if slot is None else slot
            return functools.partial(
                pltpu.make_async_remote_copy,
                src_ref=source,
                dst_ref=target,
                send_sem=self.send_sem.at[slot],
                recv_sem=self.recv_sem.at[slot],
                device_id=device,
                device_id_type=MESH,
            )

        for index, (kind, source, target) in enumerate(
            zip(self.kinds, self.sources, self.targets)
        ):
            item = [], [], [], [], []
            begin, follow, sent, got, stay = item

            def keep(source, target):
                sem = self.local_sem.at[index]
                stay.append(functools.partial(pltpu.make_async_copy, source, target, sem))

            def direct(source, target, device):
                copy = None, remote(source, target, device)
                begin.append(copy)
                sent.append(copy)
                got.append(copy)

            if kind[0] == "gather":
                second, parts = kind[1:]
                size = source.shape[0] // parts
                beside, above, away = self.across(row)

                def at(other, part, piece=None):
                    member = other * cols + col
                    first, length, deep = part * size, size, ()
                    if piece is not None and size % 2 == 0:
                        length = size // 2
                        first = first + piece * length
                    elif piece is not None:
                        inner = source.shape[1] // 2
                        deep = (pl.ds(piece * inner, inner),)
                    some = pl.ds(first, length)
                    return target.at[(some, member) + deep if second else (member, some) + deep]

                def to_mates(piece):
                    made = []
                    for j in range(1, cols):
                        copy = None, remote(piece, piece, {"col": lax.rem(col + j, cols)})
                        made.append(copy)
                        sent.append(copy)
                        got.append(copy)
                    return made

                for part in range(parts):
                    some = source.at[pl.ds(part * size, size)]
                    ways = []
                    for near, other, piece in ((beside, above, 0), (above, beside, 1)):
                        first = None, remote(some, at(row, part), {"row": near})
                        passed = at(near, part, piece)
                        onward = None, remote(passed, passed, {"row": other})
                        begin.append(first)
                        sent.extend([first, onward])
                        ways.append((near, piece, first, onward))
                    for near, piece, first, onward in ways:
                        nexts = [onward] + to_mates(at(near, part))
                        follow.append((2 + 3 * part, 0, None, first[1], nexts))
                    for near, piece, first, onward in ways:
                        nexts = to_mates(at(away, part, piece))
                        follow.append((2 + 3 * parts + part, 1, None, onward[1], nexts))
                    for j in range(1, cols):
                        direct(some, at(row, part), {"col": lax.rem(col + j, cols)})
                keep(source, target.at[:, me] if second else target.at[me])
            elif kind[0] in ("swap", "share"):
                for k in range(1, group):
                    other = lax.rem(me + k, group)
                    piece = source.at[other] if kind[0] == "swap" else source
                    direct(piece, target.at[me], self.member(other))
                keep(source.at[me] if kind[0] == "swap" else source, target.at[me])
            elif kind[0] in ("turn", "collect"):
                for k in range(1, depth):
                    other = lax.rem(layer + k, depth)
                    piece = source.at[other] if kind[0] == "turn" else source
                    direct(piece, target.at[layer], {"dp": other})
                keep(source.at[layer] if kind[0] == "turn" else source, target.at[layer])
            elif kind[0] == "line":
                absolute, parts, limit = kind[1:]
                size = source.shape[0] // parts
                steps = limit or depth - 1
                ways = (1,) if limit else (1, -1)
                for part, way in itertools.product(range(parts), ways):
                    behind = layer if way == 1 else depth - 1 - layer
                    onward = layer + way
                    more = (onward >= 0) & (onward < depth)
                    mine = [next(slots) for _ in range(steps)]
                    some = pl.ds(part * size, size)

                    def held(step, where, way=way, some=some):
                        if step == 0:
                            return source.at[some]
                        if absolute:
                            return target.at[where - way * step, some]
                        return target.at[step - 1 if way == 1 else depth - 1 - step, some]

                    def sending(step, onward=onward, mine=mine, held=held):
                        device = {"dp": onward}
                        return remote(
                            held(step - 1, layer), held(step, onward), device, mine[step - 1]
                        )

                    begin.append((more, sending(1)))
                    for step in range(1, steps + 1):
                        sent.append((more & (behind >= step - 1), sending(step)))
                        block = held(step, layer)
                        arrival = remote(block, block, {"dp": onward}, mine[step - 1])
                        nexts = [(more, sending(step + 1))] if step < steps else []
                        when = 4 * step + part
                        follow.append((when, step - 1, behind >= step, arrival, nexts))
                if absolute:
                    keep(source, target.at[layer])
            else:
                for at_slot, d in enumerate(kind[1]):
                    piece = source.at[at_slot] if kind[2] else source
                    direct(piece, target.at[at_slot], {"dp": lax.rem(layer + d % depth, depth)})
            if only is None or index in only:
                starts += begin
                relays += follow
                sends += sent
                arrivals += got
                local += stay
        return starts, sorted(relays, key=lambda entry: entry[0]), sends, arrivals, local

    def given(self, condition, action):
        if condition is None:
            action()
        else:
            pl.when(condition)(action)

    def start(self, only=None):
        starts, _, _, _, local = self.plan(only)
        for condition, copy in starts:
            self.given(condition, lambda copy=copy: copy().start())
        for copy in local:
            copy().start()

    def relay(self, only=None, stages=None):
        for _, stage, condition, copy, nexts in self.plan(only)[1]:
            if stages is not None and stage not in stages:
                continue

            def action(copy=copy, nexts=nexts):
                copy().wait_recv()
                for more, follower in nexts:
                    self.given(more, lambda follower=follower: follower().start())

            self.given(condition, action)

    def finish(self, only=None):
        _, _, sends, arrivals, local = self.plan(only)
        for condition, copy in arrivals:
            self.given(condition, lambda copy=copy: copy().wait_recv())
        for condition, copy in sends:
            self.given(condition, lambda copy=copy: copy().wait_send())
        for copy in local:
            copy().wait()


def planned(sizes, items):
    rows, cols, depth = sizes
    group = rows * cols
    kinds, shapes, copies = [], [], 0
    for item in items:
        name, array = item[0], item[1]
        shape = array.shape
        if name == "gather":
            assert rows == 4
            second, parts = (item[2:] + (False, 1)[len(item) - 2 :])[:2]
            kinds.append((name, second, parts))
            shape = (shape[0], group) + shape[1:] if second else (group,) + shape
            copies += parts * (4 + 5 * (cols - 1))
        elif name == "shift":
            distances, split = item[2], item[3]
            kinds.append((name, tuple(distances), split))
            shape = (len(distances),) + (shape[1:] if split else shape)
            copies += len(distances)
        elif name == "line":
            parts, limit = (item[3:] + (1, 0)[len(item) - 3 :])[:2]
            kinds.append((name, item[2], parts, limit))
            shape = (depth if item[2] else limit or depth - 1,) + shape
            copies += (limit or 2 * (depth - 1)) * parts
        else:
            kinds.append((name,))
            if name in ("share", "collect"):
                shape = (group if name == "share" else depth,) + shape
            copies += (depth if name in ("turn", "collect") else group) - 1
        shapes.append(jax.ShapeDtypeStruct(shape, array.dtype))
    sems = [
        pltpu.SemaphoreType.DMA((copies,)),
        pltpu.SemaphoreType.DMA((copies,)),
        pltpu.SemaphoreType.DMA((len(items),)),
    ]
    return tuple(kinds), shapes, sems


class Got:
    def __init__(self, index):
        self.index = index


class Made:
    def __init__(self, index):
        self.index = index


class Stage:
    def __init__(self, body, shapes, *operands, scratch=()):
        self.body, self.shapes, self.operands = body, shapes, operands
        self.scratch = list(scratch)


def exchange(sizes, name, number, *items, before=None, after=None, cover=None, landing=(), shared=(), delayed=()):
    kinds, moved, sems = planned(sizes, items)
    stages = [stage for stage in (before, after) if stage]
    operands = []
    for stage in stages:
        for operand in stage.operands:
            if not isinstance(operand, (Got, Made)):
                operands.append(operand)
    work = list(cover.work) if cover else []
    outs = [s for stage in stages for s in stage.shapes]
    made_shapes = list(cover.shapes) if cover else []
    flown = [i for i in range(len(items)) if i not in landing]
    late = [o.index for o in (after.operands if after else ()) if isinstance(o, Got)]
    late = [i for i in late if i not in landing]
    scratch = []

    def take(shapes):
        first = len(scratch)
        scratch.extend(shapes)
        return slice(first, len(scratch))

    vmem = lambda s: pltpu.VMEM(tuple(s[0]), s[1])
    of = lambda a: (a.shape, a.dtype)
    operand_at = take([vmem(of(a)) for a in operands])
    result_at = take([vmem(s) for s in outs])
    landed_at = take([vmem(of(moved[i])) for i in landing])
    late_at = take([vmem(of(moved[i])) for i in late])
    stage_at = [take(stage.scratch) for stage in stages]
    shared_at = take(list(shared))
    needed = sorted({o.index for o in (after.operands if after else ()) if isinstance(o, Got)})
    others = [i for i in range(len(items)) if i not in needed]
    prompt = [i for i in range(len(items)) if i not in delayed]
    later = range(1, 2 * sizes[2])
    cover_at = take(cover.scratch) if cover else slice(0, 0)
    copies = len(operands) + len(outs) + len(late)
    copy_at = take([pltpu.SemaphoreType.DMA((max(1, copies),))])
    sems_at = take(sems)

    def body(*refs):
        cuts = [len(operands), len(work), len(items), len(outs), len(made_shapes), len(flown)]
        groups = []
        for cut in cuts:
            groups.append(refs[:cut])
            refs = refs[cut:]
        given, work_refs, sources, results, made_refs, flown_refs = groups
        loaded, held = refs[operand_at], refs[result_at]
        landed, lates, (copy_sem,) = refs[landed_at], refs[late_at], refs[copy_at]
        targets = [None] * len(items)
        for i, ref in zip(flown, flown_refs):
            targets[i] = ref
        for i, ref in zip(landing, landed):
            targets[i] = ref
        moves = Moves(sizes, kinds, sources, targets, refs[sems_at])
        number_of = iter(range(copies))
        copy = lambda a, b: pltpu.make_async_copy(a, b, copy_sem.at[next(number_of)])
        loads = [copy(a, b) for a, b in zip(given, loaded)]
        stores = [copy(a, b) for a, b in zip(held, results)]
        late_loads = [copy(targets[i], b) for i, b in zip(late, lates)]
        split = len([o for o in before.operands if not isinstance(o, Made)]) if before else 0
        first = len(before.shapes) if before else 0
        for load in loads:
            load.start()
        if cover:
            cover.begin(work_refs, refs[cover_at])
        moves.barrier()
        moves.start(prompt)
        if before:
            for load in loads[:split]:
                load.wait()
            before.body(*loaded[:split], *held[:first], *refs[stage_at[0]], *refs[shared_at])
            for store in stores[:first]:
                store.start()
        if cover:
            cover.run(work_refs, made_refs, refs[cover_at])
        moves.relay(prompt, (0,))
        moves.start(delayed)
        if after:
            moves.relay(needed, later)
            moves.finish(needed)
        moves.relay(delayed, (0,))
        if after:
            for load in late_loads:
                load.start()
            for load in loads[split:]:
                load.wait()
            for load in late_loads:
                load.wait()
            plain = iter(loaded[split:])
            values = []
            for operand in after.operands:
                if isinstance(operand, Made):
                    values.append(held[operand.index])
                elif isinstance(operand, Got) and operand.index in landing:
                    values.append(landed[landing.index(operand.index)])
                elif isinstance(operand, Got):
                    values.append(lates[late.index(operand.index)])
                else:
                    values.append(next(plain))
            after.body(*values, *held[first:], *refs[stage_at[-1]], *refs[shared_at])
            for store in stores[first:]:
                store.start()
        moves.relay(others, later)
        moves.finish(others)
        if cover:
            cover.end(made_refs, refs[cover_at])
        for store in stores:
            store.wait()

    shape = lambda s: jax.ShapeDtypeStruct(tuple(s[0]), s[1])
    return pl.pallas_call(
        body,
        out_shape=tuple(shape(s) for s in outs + made_shapes) + tuple(moved[i] for i in flown),
        in_specs=[HBM] * (len(operands) + len(work) + len(items)),
        out_specs=(HBM,) * (len(outs) + len(made_shapes) + len(flown)),
        scratch_shapes=scratch,
        compiler_params=pltpu.CompilerParams(collective_id=number, has_side_effects=True),
        name=name,
    )(*operands, *work, *[item[1] for item in items])


def dot(a, b, left=1, right=0, precision=None):
    return lax.dot_general(
        a,
        b,
        (((left,), (right,)), ((), ())),
        preferred_element_type=jnp.float32,
        precision=precision,
    )


def widened(source, target):
    size = target.shape[0] // 4

    def piece(i, carry):
        at = pl.ds(pl.multiple_of(i * size, size), size)
        target[at, :] = source[at, :].astype(target.dtype)
        return carry

    lax.fori_loop(0, 4, piece, 0)


def cleared(target):
    size = target.shape[0] // 8

    def piece(i, carry):
        at = pl.ds(pl.multiple_of(i * size, size), size)
        target[at, :] = jnp.zeros((size, target.shape[1]), target.dtype)
        return carry

    lax.fori_loop(0, 8, piece, 0)


def lanes_of(shape):
    return lax.broadcasted_iota(jnp.int32, shape, len(shape) - 1)


def flipped(values):
    lanes = lanes_of(values.shape)
    ahead = pltpu.roll(values, LANES - TURN, 1)
    behind = pltpu.roll(values, TURN, 1)
    return jnp.where(lanes % (2 * TURN) < TURN, ahead, behind)


def beside(blocks_ref):
    return jnp.concatenate([blocks_ref[i] for i in range(blocks_ref.shape[0])], axis=1)


def gain_row(gains_ref):
    return beside(gains_ref).astype(jnp.float32)


def added(blocks):
    def more(i, total):
        return total + blocks[i].astype(jnp.float32)

    return lax.fori_loop(1, blocks.shape[0], more, blocks[0].astype(jnp.float32))


def own_rows(count):
    me = lax.axis_index("row") * lax.axis_size("col") + lax.axis_index("col")
    return pl.ds(pl.multiple_of(me * count, count), count)


def column(row):
    return jnp.broadcast_to(row, (8, row.shape[1])).T[:, 0:1]


def tables_body(cosine, sine):
    step = 64
    lanes = lanes_of((step, LANES))
    power = (lanes % TURN).astype(jnp.float32) * (-math.log(ROPE_BASE) / TURN)
    frequencies = jnp.exp(power)
    base = lax.axis_index("dp") * cosine.shape[0]

    def piece(i, carry):
        at = pl.ds(pl.multiple_of(i * step, step), step)
        positions = base + i * step + lax.broadcasted_iota(jnp.int32, lanes.shape, 0)
        angles = positions.astype(jnp.float32) * frequencies
        cosine[at, :] = jnp.cos(angles)
        value = jnp.sin(angles)
        sine[at, :] = jnp.where(lanes % (2 * TURN) < TURN, -value, value)
        return carry

    lax.fori_loop(0, cosine.shape[0] // step, piece, 0)


def turned(source, target):
    def block(i, carry):
        scaled = RESIDUAL_SCALE * source[i].astype(jnp.float32)
        target[i] = scaled.T.astype(jnp.bfloat16)
        return carry

    lax.fori_loop(0, target.shape[0], block, 0)


def project_body(blocks, gains, w_query, w_pair, cosine, sine, normed, query, pair, own):
    gain = gain_row(gains)
    step = 128

    def piece(i, carry):
        at = pl.ds(pl.multiple_of(i * step, step), step)
        parts = [blocks[k, at, :] for k in range(blocks.shape[0])]
        tokens = jnp.concatenate(parts, axis=1).astype(jnp.float32)
        scale = lax.rsqrt(jnp.mean(tokens * tokens, axis=1, keepdims=True) + EPSILON)
        normed[at, :] = (tokens * scale * gain).astype(jnp.bfloat16)
        return carry

    lax.fori_loop(0, normed.shape[0] // step, piece, 0)
    raw = dot(normed[...], w_query[...])
    query[...] = (raw * cosine[...] + flipped(raw) * sine[...]).astype(jnp.bfloat16)
    raw = dot(normed[...], w_pair[...])
    keys = lanes_of(raw.shape) < LANES // 2
    turned = raw * cosine[...] + flipped(raw) * sine[...]
    pair[...] = jnp.where(keys, turned, raw).astype(jnp.bfloat16)
    for i in range(blocks.shape[0]):
        own[:, i * LANES : (i + 1) * LANES] = blocks[i, own_rows(own.shape[0]), :]


def doubled(pair, keys_ref, values_ref, at, distance=0):
    wide = pair.astype(jnp.float32)
    if distance:
        wide = jnp.where(lax.axis_index("dp") >= distance, wide, 0.0)
    other = pltpu.roll(wide, LANES // 2, 1)
    keys = lanes_of(wide.shape) < LANES // 2
    keys_ref[at] = jnp.where(keys, wide, other).astype(jnp.bfloat16)
    values_ref[at] = jnp.where(keys, other, wide).astype(jnp.bfloat16)


def per_head(values):
    first = lanes_of(values.shape) < LANES // 2
    zero = jnp.zeros_like(values)
    return jnp.concatenate(
        [jnp.where(first, values, zero), jnp.where(first, zero, values)], axis=0
    )


def tile_scores(queries, keys_ref, starts, row, block, last, tokens):
    scores = dot(queries, keys_ref[block], 1, 1) * SCORE_SCALE
    at = lanes_of(scores.shape) + block * tokens
    allowed = at >= starts
    if block == last:
        place = row + lax.broadcasted_iota(jnp.int32, scores.shape, 0)
        allowed = allowed & (at <= place + block * tokens)
    return jnp.where(allowed, scores, MASKED)


def doc_row(docs):
    rows = [docs[i : i + 1, :] for i in range(docs.shape[0])]
    return jnp.concatenate(rows, axis=1).astype(jnp.float32)


def attend_tiles(tokens, tile):
    step = 256

    def body(i, carry):
        rows = pl.ds(pl.multiple_of(i * step, step), step)
        tile(rows, lax.rem(i * step, tokens), step)
        return carry

    lax.fori_loop(0, 2 * tokens // step, body, 0)


def attend_first_body(near_grads, far_grads, query, pair, docs, far_docs, own_grad, near_turned, far_turned, start, keys, values, queries, out, tops, totals):
    turned(near_grads, near_turned)
    turned(far_grads, far_turned)
    for i in range(near_grads.shape[0]):
        own_grad[:, i * LANES : (i + 1) * LANES] = near_grads[i, own_rows(own_grad.shape[0]), :]
    tokens = query.shape[0]
    last = keys.shape[0] - 1
    layer = lax.axis_index("dp")
    here = doc_row(docs[...])
    mine = column(here)
    before = jnp.sum((here < mine).astype(jnp.float32), axis=1, keepdims=True)
    for d in range(1, last + 1):
        fewer = (doc_row(far_docs[d - 1]) < mine) | (layer < d)
        before = before + jnp.sum(fewer.astype(jnp.float32), axis=1, keepdims=True)
    start[...] = before.astype(jnp.int32)
    doubled(pair[...], keys, values, last)
    queries[...] = per_head(query[...].astype(jnp.float32)).astype(jnp.bfloat16)

    def tile(rows, row, step):
        starts = start[pl.ds(pl.multiple_of(row, step), step), :]
        scores = tile_scores(queries[rows, :], keys, starts, row, last, last, tokens)
        top = jnp.max(scores, axis=1, keepdims=True)
        terms = jnp.exp(scores - top)
        tops[rows, :] = top
        totals[rows, :] = jnp.sum(terms, axis=1, keepdims=True)
        out[rows, :] = dot(terms.astype(jnp.bfloat16), values[last])

    attend_tiles(tokens, tile)


def attend_rest_body(far, start, mixed, log_total, keys, values, queries, out, tops, totals):
    last, tokens = far.shape[0], far.shape[1]
    for d in range(1, last + 1):
        doubled(far[d - 1], keys, values, last - d, d)

    def tile(rows, row, step):
        starts = start[pl.ds(pl.multiple_of(row, step), step), :]
        parts = [
            tile_scores(queries[rows, :], keys, starts, row, block, last, tokens)
            for block in range(last)
        ]
        top = functools.reduce(
            jnp.maximum, [jnp.max(part, axis=1, keepdims=True) for part in parts], tops[rows, :]
        )
        parts = [jnp.exp(part - top) for part in parts]
        scale = jnp.exp(tops[rows, :] - top)
        total = functools.reduce(
            jnp.add,
            [jnp.sum(p, axis=1, keepdims=True) for p in parts],
            totals[rows, :] * scale,
        )
        sums = [
            dot(part.astype(jnp.bfloat16), values[block]) for block, part in enumerate(parts)
        ]
        out[rows, :] = functools.reduce(jnp.add, sums, out[rows, :] * scale) / total
        log_total[rows, :] = top + jnp.log(total)

    attend_tiles(tokens, tile)
    first = lanes_of((tokens, LANES)) < LANES // 2
    mixed[...] = jnp.where(first, out[:tokens, :], out[tokens:, :]).astype(jnp.bfloat16)


def attend_again_body(query, pair, far, start, log_total, keys, values, queries, chances):
    tokens = query.shape[0]
    last = far.shape[0]
    doubled(pair[...], keys, values, last)
    for d in range(1, last + 1):
        doubled(far[d - 1], keys, values, last - d, d)
    queries[...] = per_head(query[...].astype(jnp.float32)).astype(jnp.bfloat16)

    def tile(rows, row, step):
        starts = start[pl.ds(pl.multiple_of(row, step), step), :]
        for block in range(last + 1):
            scores = tile_scores(queries[rows, :], keys, starts, row, block, last, tokens)
            chances[block, rows, :] = jnp.exp(scores - log_total[rows, :])

    attend_tiles(tokens, tile)


def attend_back_body(grad, w_output, mixed, cosine, sine, query_grad, pair_grad, far_grad, output_grad, grads, turned, key_sums, value_sums, keys, values, queries, chances):
    tokens = mixed.shape[0]
    last = keys.shape[0] - 1
    given_grad = grad[...].reshape(tokens, -1)
    grads[...] = per_head(dot(given_grad, w_output[...], 1, 1)).astype(jnp.bfloat16)
    output_sum = dot(mixed[...], given_grad, 0, 0).astype(jnp.bfloat16)
    for i in range(output_grad.shape[0]):
        output_grad[i] = output_sum[:, i * LANES : (i + 1) * LANES]
    for block in range(last + 1):
        cleared(key_sums.at[block])
        cleared(value_sums.at[block])

    def tile(rows, row, step):
        asked, given = queries[rows, :], grads[rows, :]
        products = [dot(given, values[block], 1, 1) for block in range(last + 1)]
        delta = functools.reduce(
            jnp.add,
            [
                jnp.sum(chances[block, rows, :] * product, axis=1, keepdims=True)
                for block, product in enumerate(products)
            ],
        )
        total = jnp.zeros((step, LANES), jnp.float32)
        for block in range(last + 1):
            chance = chances[block, rows, :]
            back = (chance * (products[block] - delta)).astype(jnp.bfloat16)
            total = total + dot(back, keys[block])
            key_sums[block] += dot(back, asked, 0, 0)
            value_sums[block] += dot(chance.astype(jnp.bfloat16), given, 0, 0)
        turned[rows, :] = total

    attend_tiles(tokens, tile)
    first = lanes_of((tokens, LANES)) < LANES // 2
    raw = jnp.where(first, turned[:tokens, :], turned[tokens:, :]) * SCORE_SCALE
    query_grad[...] = (raw * cosine[...] - flipped(raw) * sine[...]).astype(jnp.bfloat16)

    def joined(block):
        by_key, by_value = key_sums[block], value_sums[block]
        by_key = (by_key + pltpu.roll(by_key, LANES // 2, 1)) * SCORE_SCALE
        by_value = by_value + pltpu.roll(by_value, LANES // 2, 1)
        return jnp.where(first, by_key, by_value)

    pair_grad[...] = joined(last)
    for d in range(1, last + 1):
        far_grad[d - 1] = joined(last - d).astype(jnp.bfloat16)


def router_rows(router):
    rows = beside(router).astype(jnp.float32)
    blank = jnp.zeros((LANES - rows.shape[0], rows.shape[1]), jnp.float32)
    return jnp.concatenate([rows, blank], axis=0)


def middle_body(mixed, own, w_output, gains, router, ids_turned, rows, middle, weights, ids_ref):
    experts = router.shape[1]
    width = own.shape[1]
    attn = dot(beside(mixed), w_output[...])
    value = own[...].astype(jnp.float32) + RESIDUAL_SCALE * attn
    middle[...] = value
    scale = lax.rsqrt(jnp.mean(value * value, axis=1, keepdims=True) + EPSILON)
    normed = value * scale * gain_row(gains)
    logits = dot(normed, router_rows(router), 1, 1, precision=HIGH)
    count = own.shape[0]
    ids_ref[...] = ids_turned[...].astype(jnp.float32).T
    ids = ids_ref[own_rows(count), :]
    lanes = lanes_of((count, LANES))
    chosen = jnp.zeros((count, LANES), jnp.float32)
    for k in range(ids.shape[1]):
        chosen = chosen + (ids[:, k : k + 1] == lanes.astype(jnp.float32)).astype(
            jnp.float32
        )
    top = jnp.max(jnp.where(lanes < experts, logits, MASKED), axis=1, keepdims=True)
    terms = jnp.exp(jnp.minimum(logits - top, 0.0)) * chosen
    share = terms / jnp.sum(terms, axis=1, keepdims=True)
    weights[...] = share
    high = share.astype(jnp.bfloat16)
    low = share - high.astype(jnp.float32)
    rows[:, :width] = normed.astype(jnp.bfloat16)
    rows[:, width:] = (high.astype(jnp.float32) + pltpu.roll(low, LANES // 2, 1)).astype(
        jnp.bfloat16
    )


def middle_back_body(back, out_grad, middle, weights, gains, router, middle_grad, attn_grad, logit_grad, gain_part):
    width = middle.shape[1]
    normed_grad = back[0, :, :width].astype(jnp.float32)
    weight_grad = back[0, :, width:].astype(jnp.float32)
    for i in range(1, back.shape[0]):
        normed_grad = normed_grad + back[i, :, :width].astype(jnp.float32)
        weight_grad = weight_grad + back[i, :, width:].astype(jnp.float32)
    share, value = weights[...], middle[...]
    mean = jnp.sum(share * weight_grad, axis=1, keepdims=True)
    logit = share * (weight_grad - mean)
    logit_grad[...] = logit.astype(jnp.bfloat16)
    normed_grad = normed_grad + dot(logit, router_rows(router), precision=HIGH)
    scale = lax.rsqrt(jnp.mean(value * value, axis=1, keepdims=True) + EPSILON)
    gain_part[...] = jnp.sum(normed_grad * value * scale, axis=0, keepdims=True)
    scaled = normed_grad * gain_row(gains)
    norm_dot = jnp.sum(scaled * value, axis=1, keepdims=True)
    total = (
        out_grad[...].astype(jnp.float32)
        + scale * scaled
        - value * (scale * scale * scale * norm_dot / width)
    )
    middle_grad[...] = total
    attn_grad[...] = (RESIDUAL_SCALE * total).astype(jnp.bfloat16)


def project_back_body(query_grad, pair_grad, returned, normed, w_query, w_pair, cosine, sine, output_turned, logit, rows, gains, gain_moe, partial, sums, output_first, output_last, gain_parts):
    layer = lax.axis_index("dp")
    depth = lax.axis_size("dp")
    total = pair_grad[...]
    for i in range(returned.shape[0]):
        total = total + jnp.where(
            layer + i + 1 < depth, returned[i].astype(jnp.float32), 0.0
        )
    keys = lanes_of(total.shape) < LANES // 2
    turned = total * cosine[...] - flipped(total) * sine[...]
    pair_low = jnp.where(keys, turned, total).astype(jnp.bfloat16)
    query_low = query_grad[...]
    whole = dot(query_low, w_query[...], 1, 1) + dot(pair_low, w_pair[...], 1, 1)
    partial[...] = whole.astype(jnp.bfloat16)
    gain_attn = jnp.sum(whole * normed[...].astype(jnp.float32), axis=0, keepdims=True)
    gain_attn = gain_attn / gain_row(gains)
    gain_parts[...] = jnp.zeros_like(gain_parts)
    for i in range(gain_parts.shape[0]):
        at = slice(i * LANES, (i + 1) * LANES)
        gain_parts[i, 0:1, :] = gain_attn[:, at]
        gain_parts[i, 1:2, :] = gain_moe[0:1, at]
    width = normed.shape[1]
    sums[:width, :] = dot(normed[...], query_low, 0, 0).astype(jnp.bfloat16)
    sums[width : 2 * width, :] = dot(normed[...], pair_low, 0, 0).astype(jnp.bfloat16)
    output_sum = added(output_turned).astype(jnp.bfloat16)
    output_first[...] = output_sum[: output_first.shape[0], :]
    output_last[...] = output_sum[output_first.shape[0] :, :]
    mine = rows[:, own_rows(LANES)]
    named = logit[...].reshape(normed.shape[0], LANES)
    sums[2 * width : 2 * width + LANES, :] = dot(named, mine, 0, 0).astype(jnp.bfloat16)


def results_body(blocks, moe, own, middle, middle_grad, gains, gain_blocks, turned, block_out, in_grad, gain_sum, summed):
    gain_sum[...] = added(gain_blocks)
    summed[...] = added(turned).astype(jnp.bfloat16)
    width = own.shape[1]
    normed_grad = added(blocks)
    branch = added(moe)
    value = own[...].astype(jnp.float32)
    scale = lax.rsqrt(jnp.mean(value * value, axis=1, keepdims=True) + EPSILON)
    scaled = normed_grad * gain_row(gains)
    norm_dot = jnp.sum(scaled * value, axis=1, keepdims=True)
    grad = (
        middle_grad[...] + scale * scaled - value * (scale * scale * scale * norm_dot / width)
    ).astype(jnp.bfloat16)
    out = (middle[...] + RESIDUAL_SCALE * branch).astype(jnp.bfloat16)
    for i in range(block_out.shape[0]):
        at = slice(i * LANES, (i + 1) * LANES)
        block_out[i] = out[:, at]
        in_grad[i] = grad[:, at]


def expert_terms(gate_up, active_grad, weight):
    hidden = active_grad.shape[0]
    gate, up = gate_up[:hidden], gate_up[hidden:]
    sigmoid = jax.nn.sigmoid(gate)
    silu = gate * sigmoid
    ungated = silu * up
    active = (ungated * weight).astype(jnp.bfloat16)
    scaled = active_grad * weight
    gate_grad = (scaled * up * sigmoid * (1.0 + gate * (1.0 - sigmoid))).astype(jnp.bfloat16)
    up_grad = (scaled * silu).astype(jnp.bfloat16)
    return active, jnp.concatenate([gate_grad, up_grad], axis=0), active_grad * ungated


def weight_rows(extra):
    turned = extra.astype(jnp.float32).T
    return turned[: LANES // 2] + turned[LANES // 2 :]


def local_experts_body(sizes, kinds, rows_ref, grads_ref, in_ref, out_ref, sent_grads, sent_rows, moe_ref, back_ref, flat_ref, in_sum, out_sum, got_grads, got_rows, moe_acc, back_acc, share, weights, spread, *sems):
    step, steps = pl.program_id(0), pl.num_programs(0)
    each, hidden, width = out_ref.shape
    parts = hidden // LANES
    moves = Moves(sizes, kinds, [sent_grads, sent_rows], [got_grads, got_rows], sems)

    @pl.when(step == 0)
    def _():
        moves.barrier()
        moves.start([0])
        cleared(moe_acc)
        cleared(back_acc)
        share[...] = jnp.zeros_like(share)
        weights[...] = weight_rows(rows_ref[:, width:])

    @pl.when(step == 2 * steps // 8)
    def _():
        moves.start([1])

    for when, item, stage in ((3, 0, 0), (6, 1, 0), (7, 0, 1)):

        @pl.when(step == when * steps // 8)
        def _(item=item, stage=stage):
            moves.relay([item], (stage,))

    for i in range(each):
        spread[i] = in_ref[i].astype(jnp.float32)
        for part in range(parts):
            for half in range(2):
                at = half * hidden + part * LANES
                flat_ref[i, :, at : at + LANES] = spread[
                    i, pl.ds(part * 2 + half, width, stride=2 * parts), :
                ].astype(jnp.bfloat16)
        expert = (lax.axis_index("row") * steps + step) * each + i
        active, gate_up_grad, shares = expert_terms(
            dot(flat_ref[i], rows_ref[:, :width], 0, 1),
            dot(out_ref[i], grads_ref[...]),
            weights[pl.ds(expert, 1), :],
        )
        share[pl.ds(expert, 1), :] = jnp.sum(shares, axis=0, keepdims=True)
        moe_acc[...] += dot(active, out_ref[i], 0, 0)
        back_acc[...] += dot(gate_up_grad, flat_ref[i], 0, 1)
        in_sum[i] = dot(gate_up_grad, rows_ref[:, :width]).astype(jnp.bfloat16)
        out_sum[i] = dot(active, grads_ref[...], 1, 1).astype(jnp.bfloat16)

    @pl.when(step == steps - 1)
    def _():
        moves.relay([1], (1,))
        widened(moe_acc, moe_ref)
        widened(back_acc, back_ref.at[:, :width])
        back_ref[:, width:] = share[...].T.astype(jnp.bfloat16)
        moves.finish()


def local_experts(sizes, number, rows, grads, w_in, w_out, sent_grads, sent_rows):
    tokens, wide = rows.shape
    experts, hidden, width = w_out.shape
    each = 1
    low = jnp.bfloat16
    kinds, shapes, sems = planned(
        sizes,
        [
            ("gather", sent_grads, True, sent_grads.shape[0]),
            ("gather", sent_rows, True, sent_rows.shape[0]),
        ],
    )
    whole = lambda s: pl.BlockSpec(s, lambda e: (0,) * len(s))
    some = lambda s: pl.BlockSpec((each,) + s[1:], lambda e: (e,) + (0,) * (len(s) - 1))
    outs = [
        (tokens, width),
        (tokens, wide),
        (experts, width, 2 * hidden),
        (experts, 2 * hidden, width),
        (experts, hidden, width),
    ]
    return pl.pallas_call(
        functools.partial(local_experts_body, sizes, kinds),
        grid=(experts // each,),
        in_specs=[
            whole(rows.shape),
            whole(grads.shape),
            some(w_in.shape),
            some(w_out.shape),
            HBM,
            HBM,
        ],
        out_specs=(whole(outs[0]), whole(outs[1]), *[some(s) for s in outs[2:]], HBM, HBM),
        out_shape=tuple(jax.ShapeDtypeStruct(s, low) for s in outs) + tuple(shapes),
        scratch_shapes=[
            pltpu.VMEM((tokens, width), jnp.float32),
            pltpu.VMEM((tokens, width), jnp.float32),
            pltpu.VMEM((LANES, tokens), jnp.float32),
            pltpu.VMEM((LANES // 2, tokens), jnp.float32),
            pltpu.VMEM((each,) + w_in.shape[1:], jnp.float32),
        ]
        + sems,
        compiler_params=pltpu.CompilerParams(collective_id=number, has_side_effects=True),
        name="local_experts",
    )(rows, grads, w_in, w_out, sent_grads, sent_rows)


class Sums:
    def __init__(self, rows, grads, weights, turned, load_sem, *sums):
        self.rows, self.grads, self.weights = rows, grads, weights
        self.turned, self.load_sem, self.sums = turned, load_sem, sums

    def load(self, which, source):
        target = (self.rows, self.grads)[which]
        return pltpu.make_async_copy(source, target, self.load_sem.at[which])

    def ready(self):
        layers, width, tokens = self.grads.shape

        def block(i, carry):
            at = pl.ds(pl.multiple_of(i * tokens, tokens), tokens)
            self.weights[i] = weight_rows(self.rows[at, width:])
            return carry

        lax.fori_loop(0, layers, block, 0)

    def make(self, index, w_in, w_out, in_part, out_part, made, arrive):
        layers, width, tokens = self.grads.shape
        hidden = w_out.shape[0]
        arrive(0)
        if self.sums:
            arrive(1)
        later = arrive

        def part_of(at, pieces, arrive=lambda i: None if self.sums else later(i)):
            first = at * tokens if isinstance(at, int) else pl.multiple_of(at * tokens, tokens)
            block = self.rows[pl.ds(first, pieces * tokens), :width]
            gate_up = dot(w_in[...], block, 0, 1)
            arrive(1)
            weight = jnp.concatenate(
                [self.weights[at + i, pl.ds(index, 1), :] for i in range(pieces)], axis=1
            )
            active_grad = jnp.concatenate(
                [dot(w_out[...], self.grads[at + i]) for i in range(pieces)], axis=1
            )
            active, gate_up_grad, _ = expert_terms(gate_up, active_grad, weight)
            out_total = functools.reduce(
                jnp.add,
                [
                    dot(active[:, i * tokens : (i + 1) * tokens], self.grads[at + i], 1, 1)
                    for i in range(pieces)
                ],
            )
            return dot(gate_up_grad, block), out_total

        if not self.sums:
            in_total, out_total = part_of(0, layers)
        else:
            whole, out_acc = self.sums
            whole[...] = jnp.zeros_like(whole)
            out_acc[...] = jnp.zeros_like(out_acc)

            def more(i, carry):
                in_more, out_more = part_of(i, 1)
                whole[...] += in_more
                out_acc[...] += out_more
                return carry

            lax.fori_loop(0, layers, more, 0)
            in_total, out_total = whole[...], out_acc[...]
        arrive(2)
        in_total = in_total + in_part[...].astype(jnp.float32)
        parts = hidden // LANES
        for part in range(parts):
            for half in range(2):
                at = half * hidden + part * LANES
                self.turned[pl.ds(part * 2 + half, width, stride=2 * parts), :] = in_total[
                    at : at + LANES, :
                ].T
        made[...] = self.turned[...].astype(jnp.bfloat16)
        return out_total + out_part[...].astype(jnp.float32)


def sums_scratch(layers, tokens, width, hidden):
    low, full = jnp.bfloat16, jnp.float32
    return [
        pltpu.VMEM((layers * tokens, width + LANES), low),
        pltpu.VMEM((layers, width, tokens), low),
        pltpu.VMEM((layers, LANES // 2, tokens), full),
        pltpu.VMEM((width * 2 * hidden // LANES, LANES), full),
        pltpu.SemaphoreType.DMA((2,)),
    ] + [pltpu.VMEM((k * hidden, width), full) for k in (2, 1) if layers > 4]


class Cover:
    def __init__(self, first, many, work):
        w_in, w_out, in_part, out_part, rows_far, grads_far = work
        layers, width, tokens = grads_far.shape
        self.experts, hidden, _ = w_out.shape
        self.first, self.many, self.work = first, many, work
        low = jnp.bfloat16
        self.shapes = [
            ((many, width * 2 * hidden // LANES, LANES), low),
            ((many, hidden, width), low),
        ]
        self.scratch = [pltpu.VMEM((many,) + a.shape[1:], low) for a in work[:4]]
        self.scratch += [pltpu.VMEM(*s) for s in self.shapes]
        self.scratch += [pltpu.SemaphoreType.DMA((4, many)), pltpu.SemaphoreType.DMA((2, many))]
        self.scratch += sums_scratch(layers, tokens, width, hidden)

    def load(self, which, i, work, refs):
        source, sem = work[which].at[self.first + i], refs[6].at[which, i]
        return pltpu.make_async_copy(source, refs[which].at[i], sem)

    def begin(self, work, refs):
        sums = Sums(*refs[8:])
        sums.load(0, work[4]).start()
        self.load(0, 0, work, refs).start()
        sums.load(1, work[5]).start()
        for which in (1, 2, 3):
            self.load(which, 0, work, refs).start()
        for i in range(1, self.many):
            for which in range(4):
                self.load(which, i, work, refs).start()

    def stores(self, i, made, refs):
        return [
            pltpu.make_async_copy(refs[4 + k].at[i], made[k].at[i], refs[7].at[k, i])
            for k in range(2)
        ]

    def run(self, work, made, refs):
        sums = Sums(*refs[8:])

        def expert(i, carry):
            def arrive(point):
                @pl.when(i == 0)
                def _():
                    if point == 0:
                        sums.load(0, work[4]).wait()
                        sums.ready()
                    if point == 1:
                        sums.load(1, work[5]).wait()

                for which in ((0,), (1,), (2, 3))[point]:
                    self.load(which, i, work, refs).wait()

            index = lax.axis_index("row") * self.experts + self.first + i
            out_total = sums.make(index, *[refs[k].at[i] for k in range(5)], arrive)
            refs[5][i] = out_total.astype(jnp.bfloat16)
            for store in self.stores(i, made, refs):
                store.start()
            return carry

        lax.fori_loop(0, self.many, expert, 0)

    def end(self, made, refs):
        for i in range(self.many):
            for store in self.stores(i, made, refs):
                store.wait()


def outputs_body(count, total, *refs):
    pieces = total // count
    sums, smalls = refs[: 2 * pieces], refs[2 * pieces : 2 * pieces + 6]
    gin, gout, *others = refs[2 * pieces + 6 : 2 * pieces + 16]
    block_out, in_grad, gain_attn, gain_moe, query, pair, output, router = others
    in_low, out_low, in_full, out_full, *refs = refs[2 * pieces + 16 :]
    held, (load_sem, store_sem, small_sem) = refs[:6], refs[6:]
    ring = in_full.shape[0]

    def load(k, i):
        low = (in_low, out_low)[k]
        source = sums[k * pieces + i // count].at[i % count]
        return pltpu.make_async_copy(source, low.at[i], load_sem.at[k, i])

    def store(k, i):
        made, target = ((in_full, gin), (out_full, gout))[k]
        return pltpu.make_async_copy(made.at[i % ring], target.at[i], store_sem.at[k, i % ring])

    for i in range(total):
        for k in range(2):
            load(k, i).start()
        if i == 0:
            fetched = [
                pltpu.make_async_copy(a, b, small_sem.at[j])
                for j, (a, b) in enumerate(zip(smalls, held))
            ]
            for copy in fetched:
                copy.start()
    def small():
        for copy in fetched:
            copy.wait()
        blocks, in_blocks, gains, summed, output_first, output_last = held
        width = gout.shape[2]
        for i in range(blocks.shape[0]):
            at = pl.ds(i * blocks.shape[1], blocks.shape[1])
            block_out[at, :] = blocks[i]
            in_grad[at, :] = in_blocks[i]
        gain_sum = jnp.sum(gains[...], axis=0)
        gain_attn[...] = gain_sum[0:1, :]
        gain_moe[...] = gain_sum[1:2, :]
        query[...] = summed[:width, :].astype(jnp.float32)
        pair[...] = summed[width : 2 * width, :].astype(jnp.float32)
        router[...] = summed[2 * width : 2 * width + router.shape[0], :].astype(jnp.float32)
        half = output_first.shape[1]
        for i in range(width // half):
            from_first = i % 2 == 0
            rows = (output_first if from_first else output_last)[i // 2].astype(jnp.float32)
            for j in range(max(1, half // LANES)):
                place = i * half + j * LANES
                at = place // LANES
                part = rows[j * LANES : (j + 1) * LANES, :]
                first = place % LANES
                output[first : first + part.shape[0], at * LANES : (at + 1) * LANES] = part

    for i in range(total):
        for k in range(2):
            load(k, i).wait()
            if i >= ring:
                store(k, i - ring).wait()
        for low, made in ((in_low, in_full), (out_low, out_full)):
            widened(low.at[i], made.at[i % ring])
        for k in range(2):
            store(k, i).start()
        if i == 1:
            small()
    for i in range(total - ring, total):
        for k in range(2):
            store(k, i).wait()


def outputs(in_sums, out_sums, hidden, experts, *smalls):
    count = in_sums[0].shape[0]
    total = count * len(in_sums)
    width = out_sums[0].shape[2]
    parts = hidden // LANES
    lanes = smalls[0].shape[2]
    tokens = smalls[0].shape[0] * smalls[0].shape[1]
    low, full = jnp.bfloat16, jnp.float32
    large = [(width * 2 * parts, LANES), (hidden, width)]
    shapes = [((total,) + s, full) for s in large] + [
        ((tokens, lanes), low),
        ((tokens, lanes), low),
        ((1, LANES), full),
        ((1, LANES), full),
        ((width, LANES), full),
        ((width, LANES), full),
        ((LANES, width), full),
        ((experts, LANES), full),
    ]
    ring = min(4, total)
    gin, *others = pl.pallas_call(
        functools.partial(outputs_body, count, total),
        in_specs=[HBM] * (2 * len(in_sums) + len(smalls)),
        out_specs=(HBM, HBM) + (FULL,) * (len(shapes) - 2),
        out_shape=tuple(jax.ShapeDtypeStruct(*shape) for shape in shapes),
        scratch_shapes=[pltpu.VMEM((total,) + s, low) for s in large]
        + [pltpu.VMEM((ring,) + s, full) for s in large]
        + [pltpu.VMEM(a.shape, a.dtype) for a in smalls]
        + [pltpu.SemaphoreType.DMA(s) for s in ((2, total), (2, ring), (len(smalls),))],
        name="outputs",
    )(*in_sums, *out_sums, *smalls)
    gin = gin.reshape(total, width, parts, 2, LANES).transpose(0, 1, 3, 2, 4)
    return gin.reshape(total, width, 2, hidden), *others


def local(
    sizes,
    tokens,
    out_grad,
    doc_ids,
    expert_ids,
    gain_attn,
    w_query,
    w_key_value,
    w_output,
    gain_moe,
    w_router,
    w_expert_in,
    w_expert_out,
):
    rows, cols, depth = sizes
    group = rows * cols
    tok_rows, feat_local = tokens.shape
    width = w_query.shape[0]
    experts = w_router.shape[1]
    expert_local, hidden = w_expert_out.shape[0], w_expert_out.shape[1]
    longest_doc = min(LONGEST, tok_rows * depth // 2)
    hop_count = longest_doc // tok_rows
    own = tok_rows // group
    low, full = jnp.bfloat16, jnp.float32
    layer = lax.axis_index("dp")
    me = lax.axis_index("row") * cols + lax.axis_index("col")
    everyone = list(range(1, depth))
    hops = list(range(1, hop_count + 1))

    w_pair = w_key_value.reshape(width, -1)
    block = (tok_rows, LANES)
    cosine, sine, normed, query, pair, tokens_own, gains, gains_moe, router, docs_far, grads_shifted, grad_blocks = exchange(
        sizes,
        "gather_tokens",
        0,
        ("gather", tokens, False, 2),
        ("share", gain_attn.reshape(1, LANES)),
        ("share", gain_moe.reshape(1, LANES)),
        ("share", w_router.T),
        ("shift", doc_ids.reshape(-1, LANES), everyone, False),
        ("shift", out_grad, everyone, False),
        ("gather", out_grad, False, 2),
        before=Stage(tables_body, [(block, full), (block, full)]),
        after=Stage(
            project_body,
            [((tok_rows, width), low), (block, low), (block, low), ((own, width), low)],
            Got(0),
            Got(1),
            w_query,
            w_pair,
            Made(0),
            Made(1),
        ),
        landing=(0,),
        delayed=(6,),
    )

    stack = (hop_count + 1,) + block
    twice = (2 * tok_rows, LANES)
    turned_block = (LANES, tok_rows)
    whole = (2 * tok_rows, 1)
    grad_own, grads_near, far_turned, start, mixed, log_total, far, output_blocks = exchange(
        sizes,
        "shift_pairs",
        1,
        ("line", pair, False, 2, hop_count),
        ("gather", w_output, False, 4),
        before=Stage(
            attend_first_body,
            [
                ((own, width), low),
                ((group,) + turned_block, low),
                ((depth - 1,) + turned_block, low),
                ((tok_rows, 1), jnp.int32),
            ],
            grad_blocks,
            grads_shifted,
            query,
            pair,
            doc_ids.reshape(-1, LANES),
            docs_far,
        ),
        after=Stage(
            attend_rest_body,
            [(block, low), (whole, full)],
            Got(0),
            Made(3),
        ),
        shared=[
            pltpu.VMEM(stack, low),
            pltpu.VMEM(stack, low),
            pltpu.VMEM(twice, low),
            pltpu.VMEM(twice, full),
            pltpu.VMEM(whole, full),
            pltpu.VMEM(whole, full),
        ],
    )
    output_full = output_blocks.reshape(-1, width)

    rows_own, middle, weights = exchange(
        sizes,
        "swap_mixed",
        2,
        ("swap", mixed.reshape(group, own, LANES)),
        after=Stage(
            middle_body,
            [((own, width + LANES), low), ((own, width), full), ((own, LANES), full)],
            Got(0),
            tokens_own,
            output_full,
            gains_moe,
            router,
            expert_ids.T,
            scratch=[pltpu.VMEM(expert_ids.shape, full)],
        ),
        landing=(0,),
    )
    rows_blocks, rows_shifted = exchange(
        sizes,
        "gather_rows",
        3,
        ("gather", rows_own, False, 2),
        ("line", rows_own, False, 4),
    )
    rows_near = rows_blocks.reshape(tok_rows, -1)
    parts = hidden // LANES
    in_rows = w_expert_in.reshape(expert_local, width, 2, parts, LANES)
    in_rows = in_rows.transpose(0, 1, 3, 2, 4).reshape(expert_local, -1, LANES)
    moe_partial, back_partial, in_flat, in_part, out_part, grads_far, rows_far = local_experts(
        sizes,
        9,
        rows_near,
        grads_near.reshape(width, tok_rows),
        in_rows,
        w_expert_out,
        far_turned,
        rows_shifted,
    )
    rows_far = rows_far.reshape((depth - 1) * tok_rows, -1)
    grads_far = grads_far.reshape(depth - 1, width, tok_rows)
    work = (in_flat, w_expert_out, in_part, out_part, rows_far, grads_far)
    share = expert_local // 4
    unit = 16 * depth
    in_sums, out_sums = [], []

    def beneath(name, number, *items, after=None, landing=()):
        cover = Cover(len(in_sums) * share, share, work)
        in_sum, out_sum, *moved = exchange(
            sizes, name, number, *items, after=after, cover=cover, landing=landing
        )
        if after:
            count = len(after.shapes)
            results = [in_sum, out_sum, *moved]
            in_sum, out_sum = results[count], results[count + 1]
            moved = results[:count] + results[count + 2 :]
        in_sums.append(in_sum)
        out_sums.append(out_sum)
        return moved

    middle_grad, attn_grad, logit_grad, gain_moe_part = beneath(
        "swap_back",
        4,
        ("swap", back_partial.reshape(group, own, -1)),
        after=Stage(
            middle_back_body,
            [
                ((own, width), full),
                ((own, width), low),
                ((own, LANES), low),
                ((1, width), full),
            ],
            Got(0),
            grad_own,
            middle,
            weights,
            gains_moe,
            router,
        ),
        landing=(0,),
    )
    query_grad, pair_grad, far_grad, output_sum, logit_blocks = exchange(
        sizes,
        "gather_attn_grad",
        5,
        ("gather", attn_grad, False, 2),
        ("gather", logit_grad),
        before=Stage(attend_again_body, [], query, pair, far, start, log_total),
        after=Stage(
            attend_back_body,
            [
                (block, low),
                (block, full),
                ((hop_count,) + block, low),
                ((group, LANES, LANES), low),
            ],
            Got(0),
            w_output,
            mixed,
            cosine,
            sine,
            scratch=[
                pltpu.VMEM(twice, low),
                pltpu.VMEM(twice, full),
                pltpu.VMEM(stack, full),
                pltpu.VMEM(stack, full),
            ],
        ),
        landing=(0,),
        shared=[
            pltpu.VMEM(stack, low),
            pltpu.VMEM(stack, low),
            pltpu.VMEM(twice, low),
            pltpu.VMEM((hop_count + 1, 2 * tok_rows, tok_rows), full),
        ],
    )
    length = (2 * width + LANES + unit - 1) // unit * unit
    partial, sums, output_first, output_last, gain_parts, moe_blocks = beneath(
        "shift_grads",
        6,
        ("shift", far_grad, [-d for d in hops], True),
        ("swap", moe_partial.reshape(group, own, width)),
        ("turn", output_sum.reshape(depth, width // depth, LANES)),
        after=Stage(
            project_back_body,
            [
                ((tok_rows, width), low),
                ((length, LANES), low),
                ((width // depth // 2, LANES), low),
                ((width // depth // 2, LANES), low),
                ((group, 8, LANES), full),
            ],
            query_grad,
            pair_grad,
            Got(0),
            normed,
            w_query,
            w_pair,
            cosine,
            sine,
            Got(2),
            logit_blocks,
            rows_near,
            gains,
            gain_moe_part,
        ),
        landing=(0, 2),
    )
    pieces = (group, own, LANES)
    block_out, in_grad, gain_sum, summed, output_first = beneath(
        "swap_partial",
        7,
        ("swap", partial.reshape(group, own, width)),
        ("turn", sums.reshape(depth, length // depth, LANES)),
        ("swap", gain_parts),
        ("collect", output_first),
        after=Stage(
            results_body,
            [(pieces, low), (pieces, low), ((8, LANES), full), ((length // depth, LANES), low)],
            Got(0),
            moe_blocks,
            tokens_own,
            middle,
            middle_grad,
            gains,
            Got(2),
            Got(1),
        ),
        landing=(0, 1, 2),
    )
    block_out, in_grad, sums, output_last, gain_all = beneath(
        "swap_results",
        8,
        ("swap", block_out),
        ("swap", in_grad),
        ("collect", summed),
        ("collect", output_last),
        ("collect", gain_sum),
    )
    grad_in, grad_out, block_out, in_grad, gain_attn_sum, gain_moe_sum, query_sum, pair_sum, output_sum, router_sum = outputs(
        in_sums,
        out_sums,
        hidden,
        experts,
        block_out,
        in_grad,
        gain_all,
        sums.reshape(length, LANES),
        output_first,
        output_last,
    )
    return (
        block_out,
        in_grad,
        gain_attn_sum.reshape(LANES),
        query_sum,
        pair_sum.reshape(w_key_value.shape),
        output_sum,
        gain_moe_sum.reshape(LANES),
        router_sum.T,
        grad_in,
        grad_out,
    )


def solution(mesh):
    in_specs = (
        P("dp", ("row", "col")),
        P("dp", ("row", "col")),
        P("dp"),
        P("dp", None),
        P(("row", "col")),
        P(None, ("row", "col")),
        P(None, ("row", "col"), None),
        P(("row", "col"), None),
        P(("row", "col")),
        P(("row", "col"), None),
        P("row", None, None, "col"),
        P("row", "col", None),
    )
    out_specs = (
        P("dp", ("row", "col")),
        P("dp", ("row", "col")),
        P(("row", "col")),
        P(None, ("row", "col")),
        P(None, ("row", "col"), None),
        P(("row", "col"), None),
        P(("row", "col")),
        P(("row", "col"), None),
        P("row", None, None, "col"),
        P("row", "col", None),
    )
    sizes = (mesh.shape["row"], mesh.shape["col"], mesh.shape["dp"])
    return jax.shard_map(
        functools.partial(local, sizes),
        mesh=mesh,
        in_specs=in_specs,
        out_specs=out_specs,
        check_vma=False,
    )
```

```python
import functools
import itertools
import math

import jax
import jax.numpy as jnp
from jax import lax
from jax.experimental import pallas as pl
from jax.experimental.pallas import tpu as pltpu
from jax.sharding import PartitionSpec as P

LONGEST = 4096
HIGH = lax.Precision.HIGHEST
EPSILON = 1e-05
RESIDUAL_SCALE = 0.22
SCORE_SCALE = 0.015625
ROPE_BASE = 10000.0
MASKED = -1e30
MESH = pl.DeviceIdType.MESH
GROUP = ("row", "col")
EVERY = ("dp", "row", "col")
LANES = 128
HBM = pl.BlockSpec(memory_space=pl.ANY)
FULL = pl.BlockSpec(memory_space=pltpu.VMEM)
TURN = LANES // 4


class Moves:
    def __init__(self, sizes, kinds, sources, targets, sems):
        self.sizes, self.kinds = sizes, kinds
        self.sources, self.targets = sources, targets
        self.send_sem, self.recv_sem, self.local_sem = sems

    def place(self):
        row, col, layer = lax.axis_index("row"), lax.axis_index("col"), lax.axis_index("dp")
        return row, col, layer, row * self.sizes[1] + col

    def member(self, index):
        rows, cols, depth = self.sizes
        return {"row": index // cols, "col": lax.rem(index, cols)}

    def across(self, row):
        low = lax.rem(row, 2)
        return row + 1 - 2 * low, lax.rem(row + 2, 4), lax.rem(row + 3 - 2 * low, 4)

    def barrier(self):
        rows, cols, depth = self.sizes
        row, col, layer, me = self.place()
        group = rows * cols
        names = [kind[0] for kind in self.kinds]
        barrier = pltpu.get_barrier_semaphore()
        partners = []
        if "swap" in names or "share" in names:
            for k in range(1, group):
                partners.append(self.member(lax.rem(me + k, group)))
        elif "gather" in names:
            for other in self.across(row)[:2]:
                partners.append({"row": other})
            for k in range(1, cols):
                partners.append({"col": lax.rem(col + k, cols)})
        shifts = set()
        for kind in self.kinds:
            if kind[0] == "shift":
                for d in kind[1]:
                    shifts |= {d % depth, -d % depth}
            elif kind[0] in ("turn", "collect"):
                shifts |= set(range(1, depth))
        for k in sorted(shifts - {0}):
            partners.append({"dp": lax.rem(layer + k, depth)})
        ends = [(layer > 0, layer - 1), (layer < depth - 1, layer + 1)]
        ends = ends if "line" in names and not shifts else []
        for partner in partners:
            pl.semaphore_signal(barrier, inc=1, device_id=partner, device_id_type=MESH)
        for there, other in ends:

            @pl.when(there)
            def _(device={"dp": other}):
                pl.semaphore_signal(barrier, inc=1, device_id=device, device_id_type=MESH)

        expected = len(partners)
        for there, _ in ends:
            expected = expected + there.astype(jnp.int32)
        pl.semaphore_wait(barrier, expected)

    def plan(self, only):
        rows, cols, depth = self.sizes
        row, col, layer, me = self.place()
        group = rows * cols
        slots = iter(range(self.send_sem.shape[0]))
        starts, relays, sends, arrivals, local = [], [], [], [], []

        def remote(source, target, device, slot=None):
            slot = next(slots) if slot is None else slot
            return functools.partial(
                pltpu.make_async_remote_copy,
                src_ref=source,
                dst_ref=target,
                send_sem=self.send_sem.at[slot],
                recv_sem=self.recv_sem.at[slot],
                device_id=device,
                device_id_type=MESH,
            )

        for index, (kind, source, target) in enumerate(
            zip(self.kinds, self.sources, self.targets)
        ):
            item = [], [], [], [], []
            begin, follow, sent, got, stay = item

            def keep(source, target):
                sem = self.local_sem.at[index]
                stay.append(functools.partial(pltpu.make_async_copy, source, target, sem))

            def direct(source, target, device):
                copy = None, remote(source, target, device)
                begin.append(copy)
                sent.append(copy)
                got.append(copy)

            if kind[0] == "gather":
                second, parts = kind[1:]
                size = source.shape[0] // parts
                beside, above, away = self.across(row)

                def at(other, part, piece=None):
                    member = other * cols + col
                    first, length, deep = part * size, size, ()
                    if piece is not None and size % 2 == 0:
                        length = size // 2
                        first = first + piece * length
                    elif piece is not None:
                        inner = source.shape[1] // 2
                        deep = (pl.ds(piece * inner, inner),)
                    some = pl.ds(first, length)
                    return target.at[(some, member) + deep if second else (member, some) + deep]

                def to_mates(piece):
                    made = []
                    for j in range(1, cols):
                        copy = None, remote(piece, piece, {"col": lax.rem(col + j, cols)})
                        made.append(copy)
                        sent.append(copy)
                        got.append(copy)
                    return made

                for part in range(parts):
                    some = source.at[pl.ds(part * size, size)]
                    ways = []
                    for near, other, piece in ((beside, above, 0), (above, beside, 1)):
                        first = None, remote(some, at(row, part), {"row": near})
                        passed = at(near, part, piece)
                        onward = None, remote(passed, passed, {"row": other})
                        begin.append(first)
                        sent.extend([first, onward])
                        ways.append((near, piece, first, onward))
                    for near, piece, first, onward in ways:
                        nexts = [onward] + to_mates(at(near, part))
                        follow.append((2 + 3 * part, 0, None, first[1], nexts))
                    for near, piece, first, onward in ways:
                        nexts = to_mates(at(away, part, piece))
                        follow.append((2 + 3 * parts + part, 1, None, onward[1], nexts))
                    for j in range(1, cols):
                        direct(some, at(row, part), {"col": lax.rem(col + j, cols)})
                keep(source, target.at[:, me] if second else target.at[me])
            elif kind[0] in ("swap", "share"):
                for k in range(1, group):
                    other = lax.rem(me + k, group)
                    piece = source.at[other] if kind[0] == "swap" else source
                    direct(piece, target.at[me], self.member(other))
                keep(source.at[me] if kind[0] == "swap" else source, target.at[me])
            elif kind[0] in ("turn", "collect"):
                for k in range(1, depth):
                    other = lax.rem(layer + k, depth)
                    piece = source.at[other] if kind[0] == "turn" else source
                    direct(piece, target.at[layer], {"dp": other})
                keep(source.at[layer] if kind[0] == "turn" else source, target.at[layer])
            elif kind[0] == "line":
                absolute, parts, limit = kind[1:]
                size = source.shape[0] // parts
                steps = limit or depth - 1
                ways = (1,) if limit else (1, -1)
                for part, way in itertools.product(range(parts), ways):
                    behind = layer if way == 1 else depth - 1 - layer
                    onward = layer + way
                    more = (onward >= 0) & (onward < depth)
                    mine = [next(slots) for _ in range(steps)]
                    some = pl.ds(part * size, size)

                    def held(step, where, way=way, some=some):
                        if step == 0:
                            return source.at[some]
                        if absolute:
                            return target.at[where - way * step, some]
                        return target.at[step - 1 if way == 1 else depth - 1 - step, some]

                    def sending(step, onward=onward, mine=mine, held=held):
                        device = {"dp": onward}
                        return remote(
                            held(step - 1, layer), held(step, onward), device, mine[step - 1]
                        )

                    begin.append((more, sending(1)))
                    for step in range(1, steps + 1):
                        sent.append((more & (behind >= step - 1), sending(step)))
                        block = held(step, layer)
                        arrival = remote(block, block, {"dp": onward}, mine[step - 1])
                        nexts = [(more, sending(step + 1))] if step < steps else []
                        when = 4 * step + part
                        follow.append((when, step - 1, behind >= step, arrival, nexts))
                if absolute:
                    keep(source, target.at[layer])
            else:
                for at_slot, d in enumerate(kind[1]):
                    piece = source.at[at_slot] if kind[2] else source
                    direct(piece, target.at[at_slot], {"dp": lax.rem(layer + d % depth, depth)})
            if only is None or index in only:
                starts += begin
                relays += follow
                sends += sent
                arrivals += got
                local += stay
        return starts, sorted(relays, key=lambda entry: entry[0]), sends, arrivals, local

    def given(self, condition, action):
        if condition is None:
            action()
        else:
            pl.when(condition)(action)

    def start(self, only=None):
        starts, _, _, _, local = self.plan(only)
        for condition, copy in starts:
            self.given(condition, lambda copy=copy: copy().start())
        for copy in local:
            copy().start()

    def relay(self, only=None, stages=None):
        for _, stage, condition, copy, nexts in self.plan(only)[1]:
            if stages is not None and stage not in stages:
                continue

            def action(copy=copy, nexts=nexts):
                copy().wait_recv()
                for more, follower in nexts:
                    self.given(more, lambda follower=follower: follower().start())

            self.given(condition, action)

    def finish(self, only=None):
        _, _, sends, arrivals, local = self.plan(only)
        for condition, copy in arrivals:
            self.given(condition, lambda copy=copy: copy().wait_recv())
        for condition, copy in sends:
            self.given(condition, lambda copy=copy: copy().wait_send())
        for copy in local:
            copy().wait()


def planned(sizes, items):
    rows, cols, depth = sizes
    group = rows * cols
    kinds, shapes, copies = [], [], 0
    for item in items:
        name, array = item[0], item[1]
        shape = array.shape
        if name == "gather":
            assert rows == 4
            second, parts = (item[2:] + (False, 1)[len(item) - 2 :])[:2]
            kinds.append((name, second, parts))
            shape = (shape[0], group) + shape[1:] if second else (group,) + shape
            copies += parts * (4 + 5 * (cols - 1))
        elif name == "shift":
            distances, split = item[2], item[3]
            kinds.append((name, tuple(distances), split))
            shape = (len(distances),) + (shape[1:] if split else shape)
            copies += len(distances)
        elif name == "line":
            parts, limit = (item[3:] + (1, 0)[len(item) - 3 :])[:2]
            kinds.append((name, item[2], parts, limit))
            shape = (depth if item[2] else limit or depth - 1,) + shape
            copies += (limit or 2 * (depth - 1)) * parts
        else:
            kinds.append((name,))
            if name in ("share", "collect"):
                shape = (group if name == "share" else depth,) + shape
            copies += (depth if name in ("turn", "collect") else group) - 1
        shapes.append(jax.ShapeDtypeStruct(shape, array.dtype))
    sems = [
        pltpu.SemaphoreType.DMA((copies,)),
        pltpu.SemaphoreType.DMA((copies,)),
        pltpu.SemaphoreType.DMA((len(items),)),
    ]
    return tuple(kinds), shapes, sems


class Got:
    def __init__(self, index):
        self.index = index


class Made:
    def __init__(self, index):
        self.index = index


class Stage:
    def __init__(self, body, shapes, *operands, scratch=()):
        self.body, self.shapes, self.operands = body, shapes, operands
        self.scratch = list(scratch)


def exchange(sizes, name, number, *items, before=None, after=None, cover=None, landing=(), shared=(), delayed=()):
    kinds, moved, sems = planned(sizes, items)
    stages = [stage for stage in (before, after) if stage]
    operands = []
    for stage in stages:
        for operand in stage.operands:
            if not isinstance(operand, (Got, Made)):
                operands.append(operand)
    work = list(cover.work) if cover else []
    outs = [s for stage in stages for s in stage.shapes]
    made_shapes = list(cover.shapes) if cover else []
    flown = [i for i in range(len(items)) if i not in landing]
    late = [o.index for o in (after.operands if after else ()) if isinstance(o, Got)]
    late = [i for i in late if i not in landing]
    scratch = []

    def take(shapes):
        first = len(scratch)
        scratch.extend(shapes)
        return slice(first, len(scratch))

    vmem = lambda s: pltpu.VMEM(tuple(s[0]), s[1])
    of = lambda a: (a.shape, a.dtype)
    operand_at = take([vmem(of(a)) for a in operands])
    result_at = take([vmem(s) for s in outs])
    landed_at = take([vmem(of(moved[i])) for i in landing])
    late_at = take([vmem(of(moved[i])) for i in late])
    stage_at = [take(stage.scratch) for stage in stages]
    shared_at = take(list(shared))
    needed = sorted({o.index for o in (after.operands if after else ()) if isinstance(o, Got)})
    others = [i for i in range(len(items)) if i not in needed]
    prompt = [i for i in range(len(items)) if i not in delayed]
    later = range(1, 2 * sizes[2])
    cover_at = take(cover.scratch) if cover else slice(0, 0)
    copies = len(operands) + len(outs) + len(late)
    copy_at = take([pltpu.SemaphoreType.DMA((max(1, copies),))])
    sems_at = take(sems)

    def body(*refs):
        cuts = [len(operands), len(work), len(items), len(outs), len(made_shapes), len(flown)]
        groups = []
        for cut in cuts:
            groups.append(refs[:cut])
            refs = refs[cut:]
        given, work_refs, sources, results, made_refs, flown_refs = groups
        loaded, held = refs[operand_at], refs[result_at]
        landed, lates, (copy_sem,) = refs[landed_at], refs[late_at], refs[copy_at]
        targets = [None] * len(items)
        for i, ref in zip(flown, flown_refs):
            targets[i] = ref
        for i, ref in zip(landing, landed):
            targets[i] = ref
        moves = Moves(sizes, kinds, sources, targets, refs[sems_at])
        number_of = iter(range(copies))
        copy = lambda a, b: pltpu.make_async_copy(a, b, copy_sem.at[next(number_of)])
        loads = [copy(a, b) for a, b in zip(given, loaded)]
        stores = [copy(a, b) for a, b in zip(held, results)]
        late_loads = [copy(targets[i], b) for i, b in zip(late, lates)]
        split = len([o for o in before.operands if not isinstance(o, Made)]) if before else 0
        first = len(before.shapes) if before else 0
        for load in loads:
            load.start()
        if cover:
            cover.begin(work_refs, refs[cover_at])
        moves.barrier()
        moves.start(prompt)
        if before:
            for load in loads[:split]:
                load.wait()
            before.body(*loaded[:split], *held[:first], *refs[stage_at[0]], *refs[shared_at])
            for store in stores[:first]:
                store.start()
        if cover:
            cover.run(work_refs, made_refs, refs[cover_at])
        moves.relay(prompt, (0,))
        moves.start(delayed)
        if after:
            moves.relay(needed, later)
            moves.finish(needed)
        moves.relay(delayed, (0,))
        if after:
            for load in late_loads:
                load.start()
            for load in loads[split:]:
                load.wait()
            for load in late_loads:
                load.wait()
            plain = iter(loaded[split:])
            values = []
            for operand in after.operands:
                if isinstance(operand, Made):
                    values.append(held[operand.index])
                elif isinstance(operand, Got) and operand.index in landing:
                    values.append(landed[landing.index(operand.index)])
                elif isinstance(operand, Got):
                    values.append(lates[late.index(operand.index)])
                else:
                    values.append(next(plain))
            after.body(*values, *held[first:], *refs[stage_at[-1]], *refs[shared_at])
            for store in stores[first:]:
                store.start()
        moves.relay(others, later)
        moves.finish(others)
        if cover:
            cover.end(made_refs, refs[cover_at])
        for store in stores:
            store.wait()

    shape = lambda s: jax.ShapeDtypeStruct(tuple(s[0]), s[1])
    return pl.pallas_call(
        body,
        out_shape=tuple(shape(s) for s in outs + made_shapes) + tuple(moved[i] for i in flown),
        in_specs=[HBM] * (len(operands) + len(work) + len(items)),
        out_specs=(HBM,) * (len(outs) + len(made_shapes) + len(flown)),
        scratch_shapes=scratch,
        compiler_params=pltpu.CompilerParams(collective_id=number, has_side_effects=True),
        name=name,
    )(*operands, *work, *[item[1] for item in items])


def dot(a, b, left=1, right=0, precision=None):
    return lax.dot_general(
        a,
        b,
        (((left,), (right,)), ((), ())),
        preferred_element_type=jnp.float32,
        precision=precision,
    )


def widened(source, target):
    size = target.shape[0] // 4

    def piece(i, carry):
        at = pl.ds(pl.multiple_of(i * size, size), size)
        target[at, :] = source[at, :].astype(target.dtype)
        return carry

    lax.fori_loop(0, 4, piece, 0)


def cleared(target):
    size = target.shape[0] // 8

    def piece(i, carry):
        at = pl.ds(pl.multiple_of(i * size, size), size)
        target[at, :] = jnp.zeros((size, target.shape[1]), target.dtype)
        return carry

    lax.fori_loop(0, 8, piece, 0)


def lanes_of(shape):
    return lax.broadcasted_iota(jnp.int32, shape, len(shape) - 1)


def flipped(values):
    lanes = lanes_of(values.shape)
    ahead = pltpu.roll(values, LANES - TURN, 1)
    behind = pltpu.roll(values, TURN, 1)
    return jnp.where(lanes % (2 * TURN) < TURN, ahead, behind)


def beside(blocks_ref):
    return jnp.concatenate([blocks_ref[i] for i in range(blocks_ref.shape[0])], axis=1)


def gain_row(gains_ref):
    return beside(gains_ref).astype(jnp.float32)


def added(blocks):
    def more(i, total):
        return total + blocks[i].astype(jnp.float32)

    return lax.fori_loop(1, blocks.shape[0], more, blocks[0].astype(jnp.float32))


def own_rows(count):
    me = lax.axis_index("row") * lax.axis_size("col") + lax.axis_index("col")
    return pl.ds(pl.multiple_of(me * count, count), count)


def column(row):
    return jnp.broadcast_to(row, (8, row.shape[1])).T[:, 0:1]


def tables_body(cosine, sine):
    step = 64
    lanes = lanes_of((step, LANES))
    power = (lanes % TURN).astype(jnp.float32) * (-math.log(ROPE_BASE) / TURN)
    frequencies = jnp.exp(power)
    base = lax.axis_index("dp") * cosine.shape[0]

    def piece(i, carry):
        at = pl.ds(pl.multiple_of(i * step, step), step)
        positions = base + i * step + lax.broadcasted_iota(jnp.int32, lanes.shape, 0)
        angles = positions.astype(jnp.float32) * frequencies
        cosine[at, :] = jnp.cos(angles)
        value = jnp.sin(angles)
        sine[at, :] = jnp.where(lanes % (2 * TURN) < TURN, -value, value)
        return carry

    lax.fori_loop(0, cosine.shape[0] // step, piece, 0)


def turned(source, target):
    def block(i, carry):
        scaled = RESIDUAL_SCALE * source[i].astype(jnp.float32)
        target[i] = scaled.T.astype(jnp.bfloat16)
        return carry

    lax.fori_loop(0, target.shape[0], block, 0)


def project_body(blocks, gains, w_query, w_pair, cosine, sine, normed, query, pair, own):
    gain = gain_row(gains)
    step = 128

    def piece(i, carry):
        at = pl.ds(pl.multiple_of(i * step, step), step)
        parts = [blocks[k, at, :] for k in range(blocks.shape[0])]
        tokens = jnp.concatenate(parts, axis=1).astype(jnp.float32)
        scale = lax.rsqrt(jnp.mean(tokens * tokens, axis=1, keepdims=True) + EPSILON)
        normed[at, :] = (tokens * scale * gain).astype(jnp.bfloat16)
        return carry

    lax.fori_loop(0, normed.shape[0] // step, piece, 0)
    raw = dot(normed[...], w_query[...])
    query[...] = (raw * cosine[...] + flipped(raw) * sine[...]).astype(jnp.bfloat16)
    raw = dot(normed[...], w_pair[...])
    keys = lanes_of(raw.shape) < LANES // 2
    turned = raw * cosine[...] + flipped(raw) * sine[...]
    pair[...] = jnp.where(keys, turned, raw).astype(jnp.bfloat16)
    for i in range(blocks.shape[0]):
        own[:, i * LANES : (i + 1) * LANES] = blocks[i, own_rows(own.shape[0]), :]


def doubled(pair, keys_ref, values_ref, at, distance=0):
    wide = pair.astype(jnp.float32)
    if distance:
        wide = jnp.where(lax.axis_index("dp") >= distance, wide, 0.0)
    other = pltpu.roll(wide, LANES // 2, 1)
    keys = lanes_of(wide.shape) < LANES // 2
    keys_ref[at] = jnp.where(keys, wide, other).astype(jnp.bfloat16)
    values_ref[at] = jnp.where(keys, other, wide).astype(jnp.bfloat16)


def per_head(values):
    first = lanes_of(values.shape) < LANES // 2
    zero = jnp.zeros_like(values)
    return jnp.concatenate(
        [jnp.where(first, values, zero), jnp.where(first, zero, values)], axis=0
    )


def tile_scores(queries, keys_ref, starts, row, block, last, tokens):
    scores = dot(queries, keys_ref[block], 1, 1) * SCORE_SCALE
    at = lanes_of(scores.shape) + block * tokens
    allowed = at >= starts
    if block == last:
        place = row + lax.broadcasted_iota(jnp.int32, scores.shape, 0)
        allowed = allowed & (at <= place + block * tokens)
    return jnp.where(allowed, scores, MASKED)


def doc_row(docs):
    rows = [docs[i : i + 1, :] for i in range(docs.shape[0])]
    return jnp.concatenate(rows, axis=1).astype(jnp.float32)


def attend_tiles(tokens, tile):
    step = 256

    def body(i, carry):
        rows = pl.ds(pl.multiple_of(i * step, step), step)
        tile(rows, lax.rem(i * step, tokens), step)
        return carry

    lax.fori_loop(0, 2 * tokens // step, body, 0)


def attend_first_body(near_grads, far_grads, query, pair, docs, far_docs, own_grad, near_turned, far_turned, start, keys, values, queries, out, tops, totals):
    turned(near_grads, near_turned)
    turned(far_grads, far_turned)
    for i in range(near_grads.shape[0]):
        own_grad[:, i * LANES : (i + 1) * LANES] = near_grads[i, own_rows(own_grad.shape[0]), :]
    tokens = query.shape[0]
    last = keys.shape[0] - 1
    layer = lax.axis_index("dp")
    here = doc_row(docs[...])
    mine = column(here)
    before = jnp.sum((here < mine).astype(jnp.float32), axis=1, keepdims=True)
    for d in range(1, last + 1):
        fewer = (doc_row(far_docs[d - 1]) < mine) | (layer < d)
        before = before + jnp.sum(fewer.astype(jnp.float32), axis=1, keepdims=True)
    start[...] = before.astype(jnp.int32)
    doubled(pair[...], keys, values, last)
    queries[...] = per_head(query[...].astype(jnp.float32)).astype(jnp.bfloat16)

    def tile(rows, row, step):
        starts = start[pl.ds(pl.multiple_of(row, step), step), :]
        scores = tile_scores(queries[rows, :], keys, starts, row, last, last, tokens)
        top = jnp.max(scores, axis=1, keepdims=True)
        terms = jnp.exp(scores - top)
        tops[rows, :] = top
        totals[rows, :] = jnp.sum(terms, axis=1, keepdims=True)
        out[rows, :] = dot(terms.astype(jnp.bfloat16), values[last])

    attend_tiles(tokens, tile)


def attend_rest_body(far, start, mixed, log_total, keys, values, queries, out, tops, totals):
    last, tokens = far.shape[0], far.shape[1]
    for d in range(1, last + 1):
        doubled(far[d - 1], keys, values, last - d, d)

    def tile(rows, row, step):
        starts = start[pl.ds(pl.multiple_of(row, step), step), :]
        parts = [
            tile_scores(queries[rows, :], keys, starts, row, block, last, tokens)
            for block in range(last)
        ]
        top = functools.reduce(
            jnp.maximum, [jnp.max(part, axis=1, keepdims=True) for part in parts], tops[rows, :]
        )
        parts = [jnp.exp(part - top) for part in parts]
        scale = jnp.exp(tops[rows, :] - top)
        total = functools.reduce(
            jnp.add,
            [jnp.sum(p, axis=1, keepdims=True) for p in parts],
            totals[rows, :] * scale,
        )
        sums = [
            dot(part.astype(jnp.bfloat16), values[block]) for block, part in enumerate(parts)
        ]
        out[rows, :] = functools.reduce(jnp.add, sums, out[rows, :] * scale) / total
        log_total[rows, :] = top + jnp.log(total)

    attend_tiles(tokens, tile)
    first = lanes_of((tokens, LANES)) < LANES // 2
    mixed[...] = jnp.where(first, out[:tokens, :], out[tokens:, :]).astype(jnp.bfloat16)


def attend_again_body(query, pair, far, start, log_total, keys, values, queries, chances):
    tokens = query.shape[0]
    last = far.shape[0]
    doubled(pair[...], keys, values, last)
    for d in range(1, last + 1):
        doubled(far[d - 1], keys, values, last - d, d)
    queries[...] = per_head(query[...].astype(jnp.float32)).astype(jnp.bfloat16)

    def tile(rows, row, step):
        starts = start[pl.ds(pl.multiple_of(row, step), step), :]
        for block in range(last + 1):
            scores = tile_scores(queries[rows, :], keys, starts, row, block, last, tokens)
            chances[block, rows, :] = jnp.exp(scores - log_total[rows, :])

    attend_tiles(tokens, tile)


def attend_back_body(grad, w_output, mixed, cosine, sine, query_grad, pair_grad, far_grad, output_grad, grads, turned, key_sums, value_sums, keys, values, queries, chances):
    tokens = mixed.shape[0]
    last = keys.shape[0] - 1
    given_grad = grad[...].reshape(tokens, -1)
    grads[...] = per_head(dot(given_grad, w_output[...], 1, 1)).astype(jnp.bfloat16)
    output_sum = dot(mixed[...], given_grad, 0, 0).astype(jnp.bfloat16)
    for i in range(output_grad.shape[0]):
        output_grad[i] = output_sum[:, i * LANES : (i + 1) * LANES]
    for block in range(last + 1):
        cleared(key_sums.at[block])
        cleared(value_sums.at[block])

    def tile(rows, row, step):
        asked, given = queries[rows, :], grads[rows, :]
        products = [dot(given, values[block], 1, 1) for block in range(last + 1)]
        delta = functools.reduce(
            jnp.add,
            [
                jnp.sum(chances[block, rows, :] * product, axis=1, keepdims=True)
                for block, product in enumerate(products)
            ],
        )
        total = jnp.zeros((step, LANES), jnp.float32)
        for block in range(last + 1):
            chance = chances[block, rows, :]
            back = (chance * (products[block] - delta)).astype(jnp.bfloat16)
            total = total + dot(back, keys[block])
            key_sums[block] += dot(back, asked, 0, 0)
            value_sums[block] += dot(chance.astype(jnp.bfloat16), given, 0, 0)
        turned[rows, :] = total

    attend_tiles(tokens, tile)
    first = lanes_of((tokens, LANES)) < LANES // 2
    raw = jnp.where(first, turned[:tokens, :], turned[tokens:, :]) * SCORE_SCALE
    query_grad[...] = (raw * cosine[...] - flipped(raw) * sine[...]).astype(jnp.bfloat16)

    def joined(block):
        by_key, by_value = key_sums[block], value_sums[block]
        by_key = (by_key + pltpu.roll(by_key, LANES // 2, 1)) * SCORE_SCALE
        by_value = by_value + pltpu.roll(by_value, LANES // 2, 1)
        return jnp.where(first, by_key, by_value)

    pair_grad[...] = joined(last)
    for d in range(1, last + 1):
        far_grad[d - 1] = joined(last - d).astype(jnp.bfloat16)


def router_rows(router):
    rows = beside(router)
    blank = jnp.zeros((LANES - rows.shape[0], rows.shape[1]), rows.dtype)
    return jnp.concatenate([rows, blank], axis=0)


def full_dot(wide, low, left=1, right=0):
    parts, rest = [], wide
    for _ in range(3):
        parts.append(rest.astype(jnp.bfloat16))
        rest = rest - parts[-1].astype(jnp.float32)
    count = wide.shape[0]
    sums = dot(jnp.concatenate(parts, axis=0), low, left, right)
    return sums[:count] + (sums[count : 2 * count] + sums[2 * count :])


def middle_body(mixed, own, w_output, gains, router, ids_turned, rows, middle, weights, ids_ref):
    experts = router.shape[1]
    width = own.shape[1]
    attn = dot(beside(mixed), w_output[...])
    value = own[...].astype(jnp.float32) + RESIDUAL_SCALE * attn
    middle[...] = value
    scale = lax.rsqrt(jnp.mean(value * value, axis=1, keepdims=True) + EPSILON)
    normed = value * scale * gain_row(gains)
    logits = full_dot(normed, router_rows(router), 1, 1)
    count = own.shape[0]
    ids_ref[...] = ids_turned[...].astype(jnp.float32).T
    ids = ids_ref[own_rows(count), :]
    lanes = lanes_of((count, LANES))
    chosen = jnp.zeros((count, LANES), jnp.float32)
    for k in range(ids.shape[1]):
        chosen = chosen + (ids[:, k : k + 1] == lanes.astype(jnp.float32)).astype(
            jnp.float32
        )
    top = jnp.max(jnp.where(lanes < experts, logits, MASKED), axis=1, keepdims=True)
    terms = jnp.exp(jnp.minimum(logits - top, 0.0)) * chosen
    share = terms / jnp.sum(terms, axis=1, keepdims=True)
    weights[...] = share
    high = share.astype(jnp.bfloat16)
    low = share - high.astype(jnp.float32)
    rows[:, :width] = normed.astype(jnp.bfloat16)
    rows[:, width:] = (high.astype(jnp.float32) + pltpu.roll(low, LANES // 2, 1)).astype(
        jnp.bfloat16
    )


def middle_back_body(back, out_grad, middle, weights, gains, router, middle_grad, attn_grad, logit_grad, gain_part):
    width = middle.shape[1]
    normed_grad = back[0, :, :width].astype(jnp.float32)
    weight_grad = back[0, :, width:].astype(jnp.float32)
    for i in range(1, back.shape[0]):
        normed_grad = normed_grad + back[i, :, :width].astype(jnp.float32)
        weight_grad = weight_grad + back[i, :, width:].astype(jnp.float32)
    share, value = weights[...], middle[...]
    mean = jnp.sum(share * weight_grad, axis=1, keepdims=True)
    logit = share * (weight_grad - mean)
    logit_grad[...] = logit.astype(jnp.bfloat16)
    normed_grad = normed_grad + full_dot(logit, router_rows(router))
    scale = lax.rsqrt(jnp.mean(value * value, axis=1, keepdims=True) + EPSILON)
    gain_part[...] = jnp.sum(normed_grad * value * scale, axis=0, keepdims=True)
    scaled = normed_grad * gain_row(gains)
    norm_dot = jnp.sum(scaled * value, axis=1, keepdims=True)
    total = (
        out_grad[...].astype(jnp.float32)
        + scale * scaled
        - value * (scale * scale * scale * norm_dot / width)
    )
    middle_grad[...] = total
    attn_grad[...] = (RESIDUAL_SCALE * total).astype(jnp.bfloat16)


def project_back_body(query_grad, pair_grad, returned, normed, w_query, w_pair, cosine, sine, output_turned, logit, rows, gains, gain_moe, partial, sums, output_first, output_last, gain_parts):
    layer = lax.axis_index("dp")
    depth = lax.axis_size("dp")
    total = pair_grad[...]
    for i in range(returned.shape[0]):
        total = total + jnp.where(
            layer + i + 1 < depth, returned[i].astype(jnp.float32), 0.0
        )
    keys = lanes_of(total.shape) < LANES // 2
    turned = total * cosine[...] - flipped(total) * sine[...]
    pair_low = jnp.where(keys, turned, total).astype(jnp.bfloat16)
    query_low = query_grad[...]
    whole = dot(query_low, w_query[...], 1, 1) + dot(pair_low, w_pair[...], 1, 1)
    partial[...] = whole.astype(jnp.bfloat16)
    gain_attn = jnp.sum(whole * normed[...].astype(jnp.float32), axis=0, keepdims=True)
    gain_attn = gain_attn / gain_row(gains)
    gain_parts[...] = jnp.zeros_like(gain_parts)
    for i in range(gain_parts.shape[0]):
        at = slice(i * LANES, (i + 1) * LANES)
        gain_parts[i, 0:1, :] = gain_attn[:, at]
        gain_parts[i, 1:2, :] = gain_moe[0:1, at]
    width = normed.shape[1]
    sums[:width, :] = dot(normed[...], query_low, 0, 0).astype(jnp.bfloat16)
    sums[width : 2 * width, :] = dot(normed[...], pair_low, 0, 0).astype(jnp.bfloat16)
    output_sum = added(output_turned).astype(jnp.bfloat16)
    output_first[...] = output_sum[: output_first.shape[0], :]
    output_last[...] = output_sum[output_first.shape[0] :, :]
    mine = rows[:, own_rows(LANES)]
    named = logit[...].reshape(normed.shape[0], LANES)
    sums[2 * width : 2 * width + LANES, :] = dot(named, mine, 0, 0).astype(jnp.bfloat16)


def results_body(blocks, moe, own, middle, middle_grad, gains, gain_blocks, turned, block_out, in_grad, gain_sum, summed):
    gain_sum[...] = added(gain_blocks)
    summed[...] = added(turned).astype(jnp.bfloat16)
    width = own.shape[1]
    normed_grad = added(blocks)
    branch = added(moe)
    value = own[...].astype(jnp.float32)
    scale = lax.rsqrt(jnp.mean(value * value, axis=1, keepdims=True) + EPSILON)
    scaled = normed_grad * gain_row(gains)
    norm_dot = jnp.sum(scaled * value, axis=1, keepdims=True)
    grad = (
        middle_grad[...] + scale * scaled - value * (scale * scale * scale * norm_dot / width)
    ).astype(jnp.bfloat16)
    out = (middle[...] + RESIDUAL_SCALE * branch).astype(jnp.bfloat16)
    for i in range(block_out.shape[0]):
        at = slice(i * LANES, (i + 1) * LANES)
        block_out[i] = out[:, at]
        in_grad[i] = grad[:, at]


def expert_terms(gate_up, active_grad, weight):
    hidden = active_grad.shape[0]
    gate, up = gate_up[:hidden], gate_up[hidden:]
    sigmoid = jax.nn.sigmoid(gate)
    silu = gate * sigmoid
    ungated = silu * up
    active = (ungated * weight).astype(jnp.bfloat16)
    scaled = active_grad * weight
    gate_grad = (scaled * up * sigmoid * (1.0 + gate * (1.0 - sigmoid))).astype(jnp.bfloat16)
    up_grad = (scaled * silu).astype(jnp.bfloat16)
    return active, jnp.concatenate([gate_grad, up_grad], axis=0), active_grad * ungated


def weight_rows(extra):
    turned = extra.astype(jnp.float32).T
    return turned[: LANES // 2] + turned[LANES // 2 :]


def local_experts_body(sizes, kinds, rows_ref, grads_ref, in_ref, out_ref, sent_grads, sent_rows, moe_ref, back_ref, flat_ref, in_sum, out_sum, got_grads, got_rows, moe_acc, back_acc, share, weights, spread, *sems):
    step, steps = pl.program_id(0), pl.num_programs(0)
    each, hidden, width = out_ref.shape
    parts = hidden // LANES
    moves = Moves(sizes, kinds, [sent_grads, sent_rows], [got_grads, got_rows], sems)

    @pl.when(step == 0)
    def _():
        moves.barrier()
        moves.start([0])
        cleared(moe_acc)
        cleared(back_acc)
        share[...] = jnp.zeros_like(share)
        weights[...] = weight_rows(rows_ref[:, width:])

    @pl.when(step == 2 * steps // 8)
    def _():
        moves.start([1])

    for when, item, stage in ((3, 0, 0), (6, 1, 0), (7, 0, 1)):

        @pl.when(step == when * steps // 8)
        def _(item=item, stage=stage):
            moves.relay([item], (stage,))

    for i in range(each):
        spread[i] = in_ref[i].astype(jnp.float32)
        for part in range(parts):
            for half in range(2):
                at = half * hidden + part * LANES
                flat_ref[i, :, at : at + LANES] = spread[
                    i, pl.ds(part * 2 + half, width, stride=2 * parts), :
                ].astype(jnp.bfloat16)
        expert = (lax.axis_index("row") * steps + step) * each + i
        active, gate_up_grad, shares = expert_terms(
            dot(flat_ref[i], rows_ref[:, :width], 0, 1),
            dot(out_ref[i], grads_ref[...]),
            weights[pl.ds(expert, 1), :],
        )
        share[pl.ds(expert, 1), :] = jnp.sum(shares, axis=0, keepdims=True)
        moe_acc[...] += dot(active, out_ref[i], 0, 0)
        back_acc[...] += dot(gate_up_grad, flat_ref[i], 0, 1)
        in_sum[i] = dot(gate_up_grad, rows_ref[:, :width]).astype(jnp.bfloat16)
        out_sum[i] = dot(active, grads_ref[...], 1, 1).astype(jnp.bfloat16)

    @pl.when(step == steps - 1)
    def _():
        moves.relay([1], (1,))
        widened(moe_acc, moe_ref)
        widened(back_acc, back_ref.at[:, :width])
        back_ref[:, width:] = share[...].T.astype(jnp.bfloat16)
        moves.finish()


def local_experts(sizes, number, rows, grads, w_in, w_out, sent_grads, sent_rows):
    tokens, wide = rows.shape
    experts, hidden, width = w_out.shape
    each = 1
    low = jnp.bfloat16
    kinds, shapes, sems = planned(
        sizes,
        [
            ("gather", sent_grads, True, sent_grads.shape[0]),
            ("gather", sent_rows, True, sent_rows.shape[0]),
        ],
    )
    whole = lambda s: pl.BlockSpec(s, lambda e: (0,) * len(s))
    some = lambda s: pl.BlockSpec((each,) + s[1:], lambda e: (e,) + (0,) * (len(s) - 1))
    outs = [
        (tokens, width),
        (tokens, wide),
        (experts, width, 2 * hidden),
        (experts, 2 * hidden, width),
        (experts, hidden, width),
    ]
    return pl.pallas_call(
        functools.partial(local_experts_body, sizes, kinds),
        grid=(experts // each,),
        in_specs=[
            whole(rows.shape),
            whole(grads.shape),
            some(w_in.shape),
            some(w_out.shape),
            HBM,
            HBM,
        ],
        out_specs=(whole(outs[0]), whole(outs[1]), *[some(s) for s in outs[2:]], HBM, HBM),
        out_shape=tuple(jax.ShapeDtypeStruct(s, low) for s in outs) + tuple(shapes),
        scratch_shapes=[
            pltpu.VMEM((tokens, width), jnp.float32),
            pltpu.VMEM((tokens, width), jnp.float32),
            pltpu.VMEM((LANES, tokens), jnp.float32),
            pltpu.VMEM((LANES // 2, tokens), jnp.float32),
            pltpu.VMEM((each,) + w_in.shape[1:], jnp.float32),
        ]
        + sems,
        compiler_params=pltpu.CompilerParams(collective_id=number, has_side_effects=True),
        name="local_experts",
    )(rows, grads, w_in, w_out, sent_grads, sent_rows)


class Sums:
    def __init__(self, rows, grads, weights, turned, load_sem, *sums):
        self.rows, self.grads, self.weights = rows, grads, weights
        self.turned, self.load_sem, self.sums = turned, load_sem, sums

    def load(self, which, source):
        target = (self.rows, self.grads)[which]
        return pltpu.make_async_copy(source, target, self.load_sem.at[which])

    def ready(self):
        layers, width, tokens = self.grads.shape

        def block(i, carry):
            at = pl.ds(pl.multiple_of(i * tokens, tokens), tokens)
            self.weights[i] = weight_rows(self.rows[at, width:])
            return carry

        lax.fori_loop(0, layers, block, 0)

    def make(self, index, w_in, w_out, in_part, out_part, made, arrive):
        layers, width, tokens = self.grads.shape
        hidden = w_out.shape[0]
        arrive(0)
        if self.sums:
            arrive(1)
        later = arrive

        def part_of(at, pieces, arrive=lambda i: None if self.sums else later(i)):
            first = at * tokens if isinstance(at, int) else pl.multiple_of(at * tokens, tokens)
            block = self.rows[pl.ds(first, pieces * tokens), :width]
            gate_up = dot(w_in[...], block, 0, 1)
            arrive(1)
            weight = jnp.concatenate(
                [self.weights[at + i, pl.ds(index, 1), :] for i in range(pieces)], axis=1
            )
            active_grad = jnp.concatenate(
                [dot(w_out[...], self.grads[at + i]) for i in range(pieces)], axis=1
            )
            active, gate_up_grad, _ = expert_terms(gate_up, active_grad, weight)
            out_total = functools.reduce(
                jnp.add,
                [
                    dot(active[:, i * tokens : (i + 1) * tokens], self.grads[at + i], 1, 1)
                    for i in range(pieces)
                ],
            )
            return dot(gate_up_grad, block), out_total

        if not self.sums:
            in_total, out_total = part_of(0, layers)
        else:
            whole, out_acc = self.sums
            whole[...] = jnp.zeros_like(whole)
            out_acc[...] = jnp.zeros_like(out_acc)

            def more(i, carry):
                in_more, out_more = part_of(i, 1)
                whole[...] += in_more
                out_acc[...] += out_more
                return carry

            lax.fori_loop(0, layers, more, 0)
            in_total, out_total = whole[...], out_acc[...]
        arrive(2)
        in_total = in_total + in_part[...].astype(jnp.float32)
        parts = hidden // LANES
        for part in range(parts):
            for half in range(2):
                at = half * hidden + part * LANES
                self.turned[pl.ds(part * 2 + half, width, stride=2 * parts), :] = in_total[
                    at : at + LANES, :
                ].T
        made[...] = self.turned[...].astype(jnp.bfloat16)
        return out_total + out_part[...].astype(jnp.float32)


def sums_scratch(layers, tokens, width, hidden):
    low, full = jnp.bfloat16, jnp.float32
    return [
        pltpu.VMEM((layers * tokens, width + LANES), low),
        pltpu.VMEM((layers, width, tokens), low),
        pltpu.VMEM((layers, LANES // 2, tokens), full),
        pltpu.VMEM((width * 2 * hidden // LANES, LANES), full),
        pltpu.SemaphoreType.DMA((2,)),
    ] + [pltpu.VMEM((k * hidden, width), full) for k in (2, 1) if layers > 4]


class Cover:
    def __init__(self, first, many, work):
        w_in, w_out, in_part, out_part, rows_far, grads_far = work
        layers, width, tokens = grads_far.shape
        self.experts, hidden, _ = w_out.shape
        self.first, self.many, self.work = first, many, work
        low = jnp.bfloat16
        self.shapes = [
            ((many, width * 2 * hidden // LANES, LANES), low),
            ((many, hidden, width), low),
        ]
        self.scratch = [pltpu.VMEM((many,) + a.shape[1:], low) for a in work[:4]]
        self.scratch += [pltpu.VMEM(*s) for s in self.shapes]
        self.scratch += [pltpu.SemaphoreType.DMA((4, many)), pltpu.SemaphoreType.DMA((2, many))]
        self.scratch += sums_scratch(layers, tokens, width, hidden)

    def load(self, which, i, work, refs):
        source, sem = work[which].at[self.first + i], refs[6].at[which, i]
        return pltpu.make_async_copy(source, refs[which].at[i], sem)

    def begin(self, work, refs):
        sums = Sums(*refs[8:])
        sums.load(0, work[4]).start()
        self.load(0, 0, work, refs).start()
        sums.load(1, work[5]).start()
        for which in (1, 2, 3):
            self.load(which, 0, work, refs).start()
        for i in range(1, self.many):
            for which in range(4):
                self.load(which, i, work, refs).start()

    def stores(self, i, made, refs):
        return [
            pltpu.make_async_copy(refs[4 + k].at[i], made[k].at[i], refs[7].at[k, i])
            for k in range(2)
        ]

    def run(self, work, made, refs):
        sums = Sums(*refs[8:])

        def expert(i, carry):
            def arrive(point):
                @pl.when(i == 0)
                def _():
                    if point == 0:
                        sums.load(0, work[4]).wait()
                        sums.ready()
                    if point == 1:
                        sums.load(1, work[5]).wait()

                for which in ((0,), (1,), (2, 3))[point]:
                    self.load(which, i, work, refs).wait()

            index = lax.axis_index("row") * self.experts + self.first + i
            out_total = sums.make(index, *[refs[k].at[i] for k in range(5)], arrive)
            refs[5][i] = out_total.astype(jnp.bfloat16)
            for store in self.stores(i, made, refs):
                store.start()
            return carry

        lax.fori_loop(0, self.many, expert, 0)

    def end(self, made, refs):
        for i in range(self.many):
            for store in self.stores(i, made, refs):
                store.wait()


def outputs_body(count, total, *refs):
    pieces = total // count
    sums, smalls = refs[: 2 * pieces], refs[2 * pieces : 2 * pieces + 6]
    gin, gout, *others = refs[2 * pieces + 6 : 2 * pieces + 16]
    block_out, in_grad, gain_attn, gain_moe, query, pair, output, router = others
    in_low, out_low, in_full, out_full, *refs = refs[2 * pieces + 16 :]
    held, (load_sem, store_sem, small_sem) = refs[:6], refs[6:]
    ring = in_full.shape[0]

    def load(k, i):
        low = (in_low, out_low)[k]
        source = sums[k * pieces + i // count].at[i % count]
        return pltpu.make_async_copy(source, low.at[i], load_sem.at[k, i])

    def store(k, i):
        made, target = ((in_full, gin), (out_full, gout))[k]
        return pltpu.make_async_copy(made.at[i % ring], target.at[i], store_sem.at[k, i % ring])

    for i in range(total):
        for k in range(2):
            load(k, i).start()
        if i == 0:
            fetched = [
                pltpu.make_async_copy(a, b, small_sem.at[j])
                for j, (a, b) in enumerate(zip(smalls, held))
            ]
            for copy in fetched:
                copy.start()
    def small():
        for copy in fetched:
            copy.wait()
        blocks, in_blocks, gains, summed, output_first, output_last = held
        width = gout.shape[2]
        for i in range(blocks.shape[0]):
            at = pl.ds(i * blocks.shape[1], blocks.shape[1])
            block_out[at, :] = blocks[i]
            in_grad[at, :] = in_blocks[i]
        gain_sum = jnp.sum(gains[...], axis=0)
        gain_attn[...] = gain_sum[0:1, :]
        gain_moe[...] = gain_sum[1:2, :]
        query[...] = summed[:width, :].astype(jnp.float32)
        pair[...] = summed[width : 2 * width, :].astype(jnp.float32)
        router[...] = summed[2 * width : 2 * width + router.shape[0], :].astype(jnp.float32)
        half = output_first.shape[1]
        for i in range(width // half):
            from_first = i % 2 == 0
            rows = (output_first if from_first else output_last)[i // 2].astype(jnp.float32)
            for j in range(max(1, half // LANES)):
                place = i * half + j * LANES
                at = place // LANES
                part = rows[j * LANES : (j + 1) * LANES, :]
                first = place % LANES
                output[first : first + part.shape[0], at * LANES : (at + 1) * LANES] = part

    for i in range(total):
        for k in range(2):
            load(k, i).wait()
            if i >= ring:
                store(k, i - ring).wait()
        for low, made in ((in_low, in_full), (out_low, out_full)):
            widened(low.at[i], made.at[i % ring])
        for k in range(2):
            store(k, i).start()
        if i == total - 3:
            small()
    for i in range(total - ring, total):
        for k in range(2):
            store(k, i).wait()


def outputs(in_sums, out_sums, hidden, experts, *smalls):
    count = in_sums[0].shape[0]
    total = count * len(in_sums)
    width = out_sums[0].shape[2]
    parts = hidden // LANES
    lanes = smalls[0].shape[2]
    tokens = smalls[0].shape[0] * smalls[0].shape[1]
    low, full = jnp.bfloat16, jnp.float32
    large = [(width * 2 * parts, LANES), (hidden, width)]
    shapes = [((total,) + s, full) for s in large] + [
        ((tokens, lanes), low),
        ((tokens, lanes), low),
        ((1, LANES), full),
        ((1, LANES), full),
        ((width, LANES), full),
        ((width, LANES), full),
        ((LANES, width), full),
        ((experts, LANES), full),
    ]
    ring = min(4, total)
    gin, *others = pl.pallas_call(
        functools.partial(outputs_body, count, total),
        in_specs=[HBM] * (2 * len(in_sums) + len(smalls)),
        out_specs=(HBM, HBM) + (FULL,) * (len(shapes) - 2),
        out_shape=tuple(jax.ShapeDtypeStruct(*shape) for shape in shapes),
        scratch_shapes=[pltpu.VMEM((total,) + s, low) for s in large]
        + [pltpu.VMEM((ring,) + s, full) for s in large]
        + [pltpu.VMEM(a.shape, a.dtype) for a in smalls]
        + [pltpu.SemaphoreType.DMA(s) for s in ((2, total), (2, ring), (len(smalls),))],
        name="outputs",
    )(*in_sums, *out_sums, *smalls)
    gin = gin.reshape(total, width, parts, 2, LANES).transpose(0, 1, 3, 2, 4)
    return gin.reshape(total, width, 2, hidden), *others


def local(
    sizes,
    tokens,
    out_grad,
    doc_ids,
    expert_ids,
    gain_attn,
    w_query,
    w_key_value,
    w_output,
    gain_moe,
    w_router,
    w_expert_in,
    w_expert_out,
):
    rows, cols, depth = sizes
    group = rows * cols
    tok_rows, feat_local = tokens.shape
    width = w_query.shape[0]
    experts = w_router.shape[1]
    expert_local, hidden = w_expert_out.shape[0], w_expert_out.shape[1]
    longest_doc = min(LONGEST, tok_rows * depth // 2)
    hop_count = longest_doc // tok_rows
    own = tok_rows // group
    low, full = jnp.bfloat16, jnp.float32
    layer = lax.axis_index("dp")
    me = lax.axis_index("row") * cols + lax.axis_index("col")
    everyone = list(range(1, depth))
    hops = list(range(1, hop_count + 1))

    w_pair = w_key_value.reshape(width, -1)
    block = (tok_rows, LANES)
    cosine, sine, normed, query, pair, tokens_own, gains, gains_moe, router, docs_far, grads_shifted, grad_blocks = exchange(
        sizes,
        "gather_tokens",
        0,
        ("gather", tokens, False, 2),
        ("share", gain_attn.reshape(1, LANES)),
        ("share", gain_moe.reshape(1, LANES)),
        ("share", w_router.T),
        ("shift", doc_ids.reshape(-1, LANES), everyone, False),
        ("shift", out_grad, everyone, False),
        ("gather", out_grad, False, 2),
        before=Stage(tables_body, [(block, full), (block, full)]),
        after=Stage(
            project_body,
            [((tok_rows, width), low), (block, low), (block, low), ((own, width), low)],
            Got(0),
            Got(1),
            w_query,
            w_pair,
            Made(0),
            Made(1),
        ),
        landing=(0,),
        delayed=(6,),
    )

    stack = (hop_count + 1,) + block
    twice = (2 * tok_rows, LANES)
    turned_block = (LANES, tok_rows)
    whole = (2 * tok_rows, 1)
    grad_own, grads_near, far_turned, start, mixed, log_total, far, output_blocks = exchange(
        sizes,
        "shift_pairs",
        1,
        ("line", pair, False, 2, hop_count),
        ("gather", w_output, False, 4),
        before=Stage(
            attend_first_body,
            [
                ((own, width), low),
                ((group,) + turned_block, low),
                ((depth - 1,) + turned_block, low),
                ((tok_rows, 1), jnp.int32),
            ],
            grad_blocks,
            grads_shifted,
            query,
            pair,
            doc_ids.reshape(-1, LANES),
            docs_far,
        ),
        after=Stage(
            attend_rest_body,
            [(block, low), (whole, full)],
            Got(0),
            Made(3),
        ),
        shared=[
            pltpu.VMEM(stack, low),
            pltpu.VMEM(stack, low),
            pltpu.VMEM(twice, low),
            pltpu.VMEM(twice, full),
            pltpu.VMEM(whole, full),
            pltpu.VMEM(whole, full),
        ],
    )
    output_full = output_blocks.reshape(-1, width)

    rows_own, middle, weights = exchange(
        sizes,
        "swap_mixed",
        2,
        ("swap", mixed.reshape(group, own, LANES)),
        after=Stage(
            middle_body,
            [((own, width + LANES), low), ((own, width), full), ((own, LANES), full)],
            Got(0),
            tokens_own,
            output_full,
            gains_moe,
            router,
            expert_ids.T,
            scratch=[pltpu.VMEM(expert_ids.shape, full)],
        ),
        landing=(0,),
    )
    rows_blocks, rows_shifted = exchange(
        sizes,
        "gather_rows",
        3,
        ("gather", rows_own, False, 2),
        ("line", rows_own, False, 4),
    )
    rows_near = rows_blocks.reshape(tok_rows, -1)
    parts = hidden // LANES
    in_rows = w_expert_in.reshape(expert_local, width, 2, parts, LANES)
    in_rows = in_rows.transpose(0, 1, 3, 2, 4).reshape(expert_local, -1, LANES)
    moe_partial, back_partial, in_flat, in_part, out_part, grads_far, rows_far = local_experts(
        sizes,
        9,
        rows_near,
        grads_near.reshape(width, tok_rows),
        in_rows,
        w_expert_out,
        far_turned,
        rows_shifted,
    )
    rows_far = rows_far.reshape((depth - 1) * tok_rows, -1)
    grads_far = grads_far.reshape(depth - 1, width, tok_rows)
    work = (in_flat, w_expert_out, in_part, out_part, rows_far, grads_far)
    share = expert_local // 4
    unit = 16 * depth
    in_sums, out_sums = [], []

    def beneath(name, number, *items, after=None, landing=()):
        cover = Cover(len(in_sums) * share, share, work)
        in_sum, out_sum, *moved = exchange(
            sizes, name, number, *items, after=after, cover=cover, landing=landing
        )
        if after:
            count = len(after.shapes)
            results = [in_sum, out_sum, *moved]
            in_sum, out_sum = results[count], results[count + 1]
            moved = results[:count] + results[count + 2 :]
        in_sums.append(in_sum)
        out_sums.append(out_sum)
        return moved

    middle_grad, attn_grad, logit_grad, gain_moe_part = beneath(
        "swap_back",
        4,
        ("swap", back_partial.reshape(group, own, -1)),
        after=Stage(
            middle_back_body,
            [
                ((own, width), full),
                ((own, width), low),
                ((own, LANES), low),
                ((1, width), full),
            ],
            Got(0),
            grad_own,
            middle,
            weights,
            gains_moe,
            router,
        ),
        landing=(0,),
    )
    query_grad, pair_grad, far_grad, output_sum, logit_blocks = exchange(
        sizes,
        "gather_attn_grad",
        5,
        ("gather", attn_grad, False, 2),
        ("gather", logit_grad),
        delayed=(1,),
        before=Stage(attend_again_body, [], query, pair, far, start, log_total),
        after=Stage(
            attend_back_body,
            [
                (block, low),
                (block, full),
                ((hop_count,) + block, low),
                ((group, LANES, LANES), low),
            ],
            Got(0),
            w_output,
            mixed,
            cosine,
            sine,
            scratch=[
                pltpu.VMEM(twice, low),
                pltpu.VMEM(twice, full),
                pltpu.VMEM(stack, full),
                pltpu.VMEM(stack, full),
            ],
        ),
        landing=(0,),
        shared=[
            pltpu.VMEM(stack, low),
            pltpu.VMEM(stack, low),
            pltpu.VMEM(twice, low),
            pltpu.VMEM((hop_count + 1, 2 * tok_rows, tok_rows), full),
        ],
    )
    length = (2 * width + LANES + unit - 1) // unit * unit
    partial, sums, output_first, output_last, gain_parts, moe_blocks = beneath(
        "shift_grads",
        6,
        ("shift", far_grad, [-d for d in hops], True),
        ("swap", moe_partial.reshape(group, own, width)),
        ("turn", output_sum.reshape(depth, width // depth, LANES)),
        after=Stage(
            project_back_body,
            [
                ((tok_rows, width), low),
                ((length, LANES), low),
                ((width // depth // 2, LANES), low),
                ((width // depth // 2, LANES), low),
                ((group, 8, LANES), full),
            ],
            query_grad,
            pair_grad,
            Got(0),
            normed,
            w_query,
            w_pair,
            cosine,
            sine,
            Got(2),
            logit_blocks,
            rows_near,
            gains,
            gain_moe_part,
        ),
        landing=(0, 2),
    )
    pieces = (group, own, LANES)
    block_out, in_grad, gain_sum, summed, output_first = beneath(
        "swap_partial",
        7,
        ("swap", partial.reshape(group, own, width)),
        ("turn", sums.reshape(depth, length // depth, LANES)),
        ("swap", gain_parts),
        ("collect", output_first),
        after=Stage(
            results_body,
            [(pieces, low), (pieces, low), ((8, LANES), full), ((length // depth, LANES), low)],
            Got(0),
            moe_blocks,
            tokens_own,
            middle,
            middle_grad,
            gains,
            Got(2),
            Got(1),
        ),
        landing=(0, 1, 2),
    )
    block_out, in_grad, sums, output_last, gain_all = beneath(
        "swap_results",
        8,
        ("swap", block_out),
        ("swap", in_grad),
        ("collect", summed),
        ("collect", output_last),
        ("collect", gain_sum),
    )
    grad_in, grad_out, block_out, in_grad, gain_attn_sum, gain_moe_sum, query_sum, pair_sum, output_sum, router_sum = outputs(
        in_sums,
        out_sums,
        hidden,
        experts,
        block_out,
        in_grad,
        gain_all,
        sums.reshape(length, LANES),
        output_first,
        output_last,
    )
    return (
        block_out,
        in_grad,
        gain_attn_sum.reshape(LANES),
        query_sum,
        pair_sum.reshape(w_key_value.shape),
        output_sum,
        gain_moe_sum.reshape(LANES),
        router_sum.T,
        grad_in,
        grad_out,
    )


def solution(mesh):
    in_specs = (
        P("dp", ("row", "col")),
        P("dp", ("row", "col")),
        P("dp"),
        P("dp", None),
        P(("row", "col")),
        P(None, ("row", "col")),
        P(None, ("row", "col"), None),
        P(("row", "col"), None),
        P(("row", "col")),
        P(("row", "col"), None),
        P("row", None, None, "col"),
        P("row", "col", None),
    )
    out_specs = (
        P("dp", ("row", "col")),
        P("dp", ("row", "col")),
        P(("row", "col")),
        P(None, ("row", "col")),
        P(None, ("row", "col"), None),
        P(("row", "col"), None),
        P(("row", "col")),
        P(("row", "col"), None),
        P("row", None, None, "col"),
        P("row", "col", None),
    )
    sizes = (mesh.shape["row"], mesh.shape["col"], mesh.shape["dp"])
    return jax.shard_map(
        functools.partial(local, sizes),
        mesh=mesh,
        in_specs=in_specs,
        out_specs=out_specs,
        check_vma=False,
    )
```

```python
import functools
import itertools
import math

import jax
import jax.numpy as jnp
from jax import lax
from jax.experimental import pallas as pl
from jax.experimental.pallas import tpu as pltpu
from jax.sharding import PartitionSpec as P

LONGEST = 4096
EPSILON = 1e-05
RESIDUAL_SCALE = 0.22
SCORE_SCALE = 0.015625
ROPE_BASE = 10000.0
MASKED = -1e30
MESH = pl.DeviceIdType.MESH
GROUP = ("row", "col")
EVERY = ("dp", "row", "col")
LANES = 128
HBM = pl.BlockSpec(memory_space=pl.ANY)
FULL = pl.BlockSpec(memory_space=pltpu.VMEM)
TURN = LANES // 4


class Moves:
    def __init__(self, sizes, kinds, sources, targets, sems):
        self.sizes, self.kinds = sizes, kinds
        self.sources, self.targets = sources, targets
        self.send_sem, self.recv_sem, self.local_sem = sems

    def place(self):
        row, col, layer = lax.axis_index("row"), lax.axis_index("col"), lax.axis_index("dp")
        return row, col, layer, row * self.sizes[1] + col

    def member(self, index):
        rows, cols, depth = self.sizes
        return {"row": index // cols, "col": lax.rem(index, cols)}

    def across(self, row):
        low = lax.rem(row, 2)
        return row + 1 - 2 * low, lax.rem(row + 2, 4), lax.rem(row + 3 - 2 * low, 4)

    def barrier(self):
        rows, cols, depth = self.sizes
        row, col, layer, me = self.place()
        group = rows * cols
        names = [kind[0] for kind in self.kinds]
        barrier = pltpu.get_barrier_semaphore()
        partners = []
        if "swap" in names or "share" in names:
            for k in range(1, group):
                partners.append(self.member(lax.rem(me + k, group)))
        elif "gather" in names:
            for other in self.across(row)[:2]:
                partners.append({"row": other})
            for k in range(1, cols):
                partners.append({"col": lax.rem(col + k, cols)})
        shifts = set()
        for kind in self.kinds:
            if kind[0] == "shift":
                for d in kind[1]:
                    shifts |= {d % depth, -d % depth}
            elif kind[0] in ("turn", "collect"):
                shifts |= set(range(1, depth))
        for k in sorted(shifts - {0}):
            partners.append({"dp": lax.rem(layer + k, depth)})
        ends = [(layer > 0, layer - 1), (layer < depth - 1, layer + 1)]
        ends = ends if "line" in names and not shifts else []
        for partner in partners:
            pl.semaphore_signal(barrier, inc=1, device_id=partner, device_id_type=MESH)
        for there, other in ends:

            @pl.when(there)
            def _(device={"dp": other}):
                pl.semaphore_signal(barrier, inc=1, device_id=device, device_id_type=MESH)

        expected = len(partners)
        for there, _ in ends:
            expected = expected + there.astype(jnp.int32)
        pl.semaphore_wait(barrier, expected)

    def plan(self, only):
        rows, cols, depth = self.sizes
        row, col, layer, me = self.place()
        group = rows * cols
        slots = iter(range(self.send_sem.shape[0]))
        starts, relays, sends, arrivals, local = [], [], [], [], []

        def remote(source, target, device, slot=None):
            slot = next(slots) if slot is None else slot
            return functools.partial(
                pltpu.make_async_remote_copy,
                src_ref=source,
                dst_ref=target,
                send_sem=self.send_sem.at[slot],
                recv_sem=self.recv_sem.at[slot],
                device_id=device,
                device_id_type=MESH,
            )

        for index, (kind, source, target) in enumerate(
            zip(self.kinds, self.sources, self.targets)
        ):
            item = [], [], [], [], []
            begin, follow, sent, got, stay = item

            def keep(source, target):
                sem = self.local_sem.at[index]
                stay.append(functools.partial(pltpu.make_async_copy, source, target, sem))

            def direct(source, target, device):
                copy = None, remote(source, target, device)
                begin.append(copy)
                sent.append(copy)
                got.append(copy)

            if kind[0] == "gather":
                second, parts = kind[1:]
                size = source.shape[0] // parts
                beside, above, away = self.across(row)

                def at(other, part, piece=None):
                    member = other * cols + col
                    first, length, deep = part * size, size, ()
                    if piece is not None and size % 2 == 0:
                        length = size // 2
                        first = first + piece * length
                    elif piece is not None:
                        inner = source.shape[1] // 2
                        deep = (pl.ds(piece * inner, inner),)
                    some = pl.ds(first, length)
                    return target.at[(some, member) + deep if second else (member, some) + deep]

                def to_mates(piece):
                    made = []
                    for j in range(1, cols):
                        copy = None, remote(piece, piece, {"col": lax.rem(col + j, cols)})
                        made.append(copy)
                        sent.append(copy)
                        got.append(copy)
                    return made

                for part in range(parts):
                    some = source.at[pl.ds(part * size, size)]
                    ways = []
                    for near, other, piece in ((beside, above, 0), (above, beside, 1)):
                        first = None, remote(some, at(row, part), {"row": near})
                        passed = at(near, part, piece)
                        onward = None, remote(passed, passed, {"row": other})
                        begin.append(first)
                        sent.extend([first, onward])
                        ways.append((near, piece, first, onward))
                    for near, piece, first, onward in ways:
                        nexts = [onward] + to_mates(at(near, part))
                        follow.append((2 + 3 * part, 0, None, first[1], nexts))
                    for near, piece, first, onward in ways:
                        nexts = to_mates(at(away, part, piece))
                        follow.append((2 + 3 * parts + part, 1, None, onward[1], nexts))
                    for j in range(1, cols):
                        direct(some, at(row, part), {"col": lax.rem(col + j, cols)})
                keep(source, target.at[:, me] if second else target.at[me])
            elif kind[0] in ("swap", "share"):
                for k in range(1, group):
                    other = lax.rem(me + k, group)
                    piece = source.at[other] if kind[0] == "swap" else source
                    direct(piece, target.at[me], self.member(other))
                keep(source.at[me] if kind[0] == "swap" else source, target.at[me])
            elif kind[0] in ("turn", "collect"):
                for k in range(1, depth):
                    other = lax.rem(layer + k, depth)
                    piece = source.at[other] if kind[0] == "turn" else source
                    direct(piece, target.at[layer], {"dp": other})
                keep(source.at[layer] if kind[0] == "turn" else source, target.at[layer])
            elif kind[0] == "line":
                absolute, parts, limit = kind[1:]
                size = source.shape[0] // parts
                steps = limit or depth - 1
                ways = (1,) if limit else (1, -1)
                for part, way in itertools.product(range(parts), ways):
                    behind = layer if way == 1 else depth - 1 - layer
                    onward = layer + way
                    more = (onward >= 0) & (onward < depth)
                    mine = [next(slots) for _ in range(steps)]
                    some = pl.ds(part * size, size)

                    def held(step, where, way=way, some=some):
                        if step == 0:
                            return source.at[some]
                        if absolute:
                            return target.at[where - way * step, some]
                        return target.at[step - 1 if way == 1 else depth - 1 - step, some]

                    def sending(step, onward=onward, mine=mine, held=held):
                        device = {"dp": onward}
                        return remote(
                            held(step - 1, layer), held(step, onward), device, mine[step - 1]
                        )

                    begin.append((more, sending(1)))
                    for step in range(1, steps + 1):
                        sent.append((more & (behind >= step - 1), sending(step)))
                        block = held(step, layer)
                        arrival = remote(block, block, {"dp": onward}, mine[step - 1])
                        nexts = [(more, sending(step + 1))] if step < steps else []
                        when = 4 * step + part
                        follow.append((when, step - 1, behind >= step, arrival, nexts))
                if absolute:
                    keep(source, target.at[layer])
            else:
                for at_slot, d in enumerate(kind[1]):
                    piece = source.at[at_slot] if kind[2] else source
                    direct(piece, target.at[at_slot], {"dp": lax.rem(layer + d % depth, depth)})
            if only is None or index in only:
                starts += begin
                relays += follow
                sends += sent
                arrivals += got
                local += stay
        return starts, sorted(relays, key=lambda entry: entry[0]), sends, arrivals, local

    def given(self, condition, action):
        if condition is None:
            action()
        else:
            pl.when(condition)(action)

    def start(self, only=None):
        starts, _, _, _, local = self.plan(only)
        for condition, copy in starts:
            self.given(condition, lambda copy=copy: copy().start())
        for copy in local:
            copy().start()

    def relay(self, only=None, stages=None):
        for _, stage, condition, copy, nexts in self.plan(only)[1]:
            if stages is not None and stage not in stages:
                continue

            def action(copy=copy, nexts=nexts):
                copy().wait_recv()
                for more, follower in nexts:
                    self.given(more, lambda follower=follower: follower().start())

            self.given(condition, action)

    def finish(self, only=None):
        _, _, sends, arrivals, local = self.plan(only)
        for condition, copy in arrivals:
            self.given(condition, lambda copy=copy: copy().wait_recv())
        for condition, copy in sends:
            self.given(condition, lambda copy=copy: copy().wait_send())
        for copy in local:
            copy().wait()


def planned(sizes, items):
    rows, cols, depth = sizes
    group = rows * cols
    kinds, shapes, copies = [], [], 0
    for item in items:
        name, array = item[0], item[1]
        shape = array.shape
        if name == "gather":
            assert rows == 4
            second, parts = (item[2:] + (False, 1)[len(item) - 2 :])[:2]
            kinds.append((name, second, parts))
            shape = (shape[0], group) + shape[1:] if second else (group,) + shape
            copies += parts * (4 + 5 * (cols - 1))
        elif name == "shift":
            distances, split = item[2], item[3]
            kinds.append((name, tuple(distances), split))
            shape = (len(distances),) + (shape[1:] if split else shape)
            copies += len(distances)
        elif name == "line":
            parts, limit = (item[3:] + (1, 0)[len(item) - 3 :])[:2]
            kinds.append((name, item[2], parts, limit))
            shape = (depth if item[2] else limit or depth - 1,) + shape
            copies += (limit or 2 * (depth - 1)) * parts
        else:
            kinds.append((name,))
            if name in ("share", "collect"):
                shape = (group if name == "share" else depth,) + shape
            copies += (depth if name in ("turn", "collect") else group) - 1
        shapes.append(jax.ShapeDtypeStruct(shape, array.dtype))
    sems = [
        pltpu.SemaphoreType.DMA((copies,)),
        pltpu.SemaphoreType.DMA((copies,)),
        pltpu.SemaphoreType.DMA((len(items),)),
    ]
    return tuple(kinds), shapes, sems


class Got:
    def __init__(self, index):
        self.index = index


class Made:
    def __init__(self, index):
        self.index = index


class Stage:
    def __init__(self, body, shapes, *operands, scratch=()):
        self.body, self.shapes, self.operands = body, shapes, operands
        self.scratch = list(scratch)


def exchange(sizes, name, number, *items, before=None, after=None, cover=None, landing=(), shared=(), delayed=()):
    kinds, moved, sems = planned(sizes, items)
    stages = [stage for stage in (before, after) if stage]
    operands = []
    for stage in stages:
        for operand in stage.operands:
            if not isinstance(operand, (Got, Made)):
                operands.append(operand)
    work = list(cover.work) if cover else []
    outs = [s for stage in stages for s in stage.shapes]
    made_shapes = list(cover.shapes) if cover else []
    flown = [i for i in range(len(items)) if i not in landing]
    late = [o.index for o in (after.operands if after else ()) if isinstance(o, Got)]
    late = [i for i in late if i not in landing]
    scratch = []

    def take(shapes):
        first = len(scratch)
        scratch.extend(shapes)
        return slice(first, len(scratch))

    vmem = lambda s: pltpu.VMEM(tuple(s[0]), s[1])
    of = lambda a: (a.shape, a.dtype)
    operand_at = take([vmem(of(a)) for a in operands])
    result_at = take([vmem(s) for s in outs])
    landed_at = take([vmem(of(moved[i])) for i in landing])
    late_at = take([vmem(of(moved[i])) for i in late])
    stage_at = [take(stage.scratch) for stage in stages]
    shared_at = take(list(shared))
    needed = sorted({o.index for o in (after.operands if after else ()) if isinstance(o, Got)})
    others = [i for i in range(len(items)) if i not in needed]
    prompt = [i for i in range(len(items)) if i not in delayed]
    later = range(1, 2 * sizes[2])
    cover_at = take(cover.scratch) if cover else slice(0, 0)
    copies = len(operands) + len(outs) + len(late)
    copy_at = take([pltpu.SemaphoreType.DMA((max(1, copies),))])
    sems_at = take(sems)

    def body(*refs):
        cuts = [len(operands), len(work), len(items), len(outs), len(made_shapes), len(flown)]
        groups = []
        for cut in cuts:
            groups.append(refs[:cut])
            refs = refs[cut:]
        given, work_refs, sources, results, made_refs, flown_refs = groups
        loaded, held = refs[operand_at], refs[result_at]
        landed, lates, (copy_sem,) = refs[landed_at], refs[late_at], refs[copy_at]
        targets = [None] * len(items)
        for i, ref in zip(flown, flown_refs):
            targets[i] = ref
        for i, ref in zip(landing, landed):
            targets[i] = ref
        moves = Moves(sizes, kinds, sources, targets, refs[sems_at])
        number_of = iter(range(copies))
        copy = lambda a, b: pltpu.make_async_copy(a, b, copy_sem.at[next(number_of)])
        loads = [copy(a, b) for a, b in zip(given, loaded)]
        stores = [copy(a, b) for a, b in zip(held, results)]
        late_loads = [copy(targets[i], b) for i, b in zip(late, lates)]
        split = len([o for o in before.operands if not isinstance(o, Made)]) if before else 0
        first = len(before.shapes) if before else 0
        for load in loads:
            load.start()
        if cover:
            cover.begin(work_refs, refs[cover_at])
        moves.barrier()
        moves.start(prompt)
        if before:
            for load in loads[:split]:
                load.wait()
            before.body(*loaded[:split], *held[:first], *refs[stage_at[0]], *refs[shared_at])
            for store in stores[:first]:
                store.start()
        if cover:
            cover.run(work_refs, made_refs, refs[cover_at])
        moves.relay(prompt, (0,))
        moves.start(delayed)
        if after:
            moves.relay(needed, later)
            moves.finish(needed)
        moves.relay(delayed, (0,))
        if after:
            for load in late_loads:
                load.start()
            for load in loads[split:]:
                load.wait()
            for load in late_loads:
                load.wait()
            plain = iter(loaded[split:])
            values = []
            for operand in after.operands:
                if isinstance(operand, Made):
                    values.append(held[operand.index])
                elif isinstance(operand, Got) and operand.index in landing:
                    values.append(landed[landing.index(operand.index)])
                elif isinstance(operand, Got):
                    values.append(lates[late.index(operand.index)])
                else:
                    values.append(next(plain))
            after.body(*values, *held[first:], *refs[stage_at[-1]], *refs[shared_at])
            for store in stores[first:]:
                store.start()
        moves.relay(others, later)
        moves.finish(others)
        if cover:
            cover.end(made_refs, refs[cover_at])
        for store in stores:
            store.wait()

    shape = lambda s: jax.ShapeDtypeStruct(tuple(s[0]), s[1])
    return pl.pallas_call(
        body,
        out_shape=tuple(shape(s) for s in outs + made_shapes) + tuple(moved[i] for i in flown),
        in_specs=[HBM] * (len(operands) + len(work) + len(items)),
        out_specs=(HBM,) * (len(outs) + len(made_shapes) + len(flown)),
        scratch_shapes=scratch,
        compiler_params=pltpu.CompilerParams(collective_id=number, has_side_effects=True),
        name=name,
    )(*operands, *work, *[item[1] for item in items])


def dot(a, b, left=1, right=0, precision=None):
    return lax.dot_general(
        a,
        b,
        (((left,), (right,)), ((), ())),
        preferred_element_type=jnp.float32,
        precision=precision,
    )


def widened(source, target):
    size = target.shape[0] // 4

    def piece(i, carry):
        at = pl.ds(pl.multiple_of(i * size, size), size)
        target[at, :] = source[at, :].astype(target.dtype)
        return carry

    lax.fori_loop(0, 4, piece, 0)


def cleared(target):
    size = target.shape[0] // 8

    def piece(i, carry):
        at = pl.ds(pl.multiple_of(i * size, size), size)
        target[at, :] = jnp.zeros((size, target.shape[1]), target.dtype)
        return carry

    lax.fori_loop(0, 8, piece, 0)


def lanes_of(shape):
    return lax.broadcasted_iota(jnp.int32, shape, len(shape) - 1)


def flipped(values):
    lanes = lanes_of(values.shape)
    ahead = pltpu.roll(values, LANES - TURN, 1)
    behind = pltpu.roll(values, TURN, 1)
    return jnp.where(lanes % (2 * TURN) < TURN, ahead, behind)


def beside(blocks_ref):
    return jnp.concatenate([blocks_ref[i] for i in range(blocks_ref.shape[0])], axis=1)


def gain_row(gains_ref):
    return beside(gains_ref).astype(jnp.float32)


def added(blocks):
    def more(i, total):
        return total + blocks[i].astype(jnp.float32)

    return lax.fori_loop(1, blocks.shape[0], more, blocks[0].astype(jnp.float32))


def own_rows(count):
    me = lax.axis_index("row") * lax.axis_size("col") + lax.axis_index("col")
    return pl.ds(pl.multiple_of(me * count, count), count)


def column(row):
    return jnp.broadcast_to(row, (8, row.shape[1])).T[:, 0:1]


def tables_body(cosine, sine):
    step = 64
    lanes = lanes_of((step, LANES))
    power = (lanes % TURN).astype(jnp.float32) * (-math.log(ROPE_BASE) / TURN)
    frequencies = jnp.exp(power)
    base = lax.axis_index("dp") * cosine.shape[0]

    def piece(i, carry):
        at = pl.ds(pl.multiple_of(i * step, step), step)
        positions = base + i * step + lax.broadcasted_iota(jnp.int32, lanes.shape, 0)
        angles = positions.astype(jnp.float32) * frequencies
        cosine[at, :] = jnp.cos(angles)
        value = jnp.sin(angles)
        sine[at, :] = jnp.where(lanes % (2 * TURN) < TURN, -value, value)
        return carry

    lax.fori_loop(0, cosine.shape[0] // step, piece, 0)


def turned(source, target):
    def block(i, carry):
        scaled = RESIDUAL_SCALE * source[i].astype(jnp.float32)
        target[i] = scaled.T.astype(jnp.bfloat16)
        return carry

    lax.fori_loop(0, target.shape[0], block, 0)


def project_body(blocks, gains, w_query, w_pair, cosine, sine, normed, query, pair, own):
    gain = gain_row(gains)
    step = 128

    def piece(i, carry):
        at = pl.ds(pl.multiple_of(i * step, step), step)
        parts = [blocks[k, at, :] for k in range(blocks.shape[0])]
        tokens = jnp.concatenate(parts, axis=1).astype(jnp.float32)
        scale = lax.rsqrt(jnp.mean(tokens * tokens, axis=1, keepdims=True) + EPSILON)
        normed[at, :] = (tokens * scale * gain).astype(jnp.bfloat16)
        return carry

    lax.fori_loop(0, normed.shape[0] // step, piece, 0)
    raw = dot(normed[...], w_query[...])
    query[...] = (raw * cosine[...] + flipped(raw) * sine[...]).astype(jnp.bfloat16)
    raw = dot(normed[...], w_pair[...])
    keys = lanes_of(raw.shape) < LANES // 2
    turned = raw * cosine[...] + flipped(raw) * sine[...]
    pair[...] = jnp.where(keys, turned, raw).astype(jnp.bfloat16)
    for i in range(blocks.shape[0]):
        own[:, i * LANES : (i + 1) * LANES] = blocks[i, own_rows(own.shape[0]), :]


def doubled(pair, keys_ref, values_ref, at, distance=0):
    wide = pair.astype(jnp.float32)
    if distance:
        wide = jnp.where(lax.axis_index("dp") >= distance, wide, 0.0)
    other = pltpu.roll(wide, LANES // 2, 1)
    keys = lanes_of(wide.shape) < LANES // 2
    keys_ref[at] = jnp.where(keys, wide, other).astype(jnp.bfloat16)
    values_ref[at] = jnp.where(keys, other, wide).astype(jnp.bfloat16)


def per_head(values):
    first = lanes_of(values.shape) < LANES // 2
    zero = jnp.zeros_like(values)
    return jnp.concatenate(
        [jnp.where(first, values, zero), jnp.where(first, zero, values)], axis=0
    )


def tile_scores(queries, keys_ref, starts, row, block, last, tokens):
    scores = dot(queries, keys_ref[block], 1, 1) * SCORE_SCALE
    at = lanes_of(scores.shape) + block * tokens
    allowed = at >= starts
    if block == last:
        place = row + lax.broadcasted_iota(jnp.int32, scores.shape, 0)
        allowed = allowed & (at <= place + block * tokens)
    return jnp.where(allowed, scores, MASKED)


def doc_row(docs):
    rows = [docs[i : i + 1, :] for i in range(docs.shape[0])]
    return jnp.concatenate(rows, axis=1).astype(jnp.float32)


def attend_tiles(tokens, tile):
    step = 256

    def body(i, carry):
        rows = pl.ds(pl.multiple_of(i * step, step), step)
        tile(rows, lax.rem(i * step, tokens), step)
        return carry

    lax.fori_loop(0, 2 * tokens // step, body, 0)


def attend_first_body(near_grads, far_grads, query, pair, docs, far_docs, own_grad, near_turned, far_turned, start, keys, values, queries, out, tops, totals):
    turned(near_grads, near_turned)
    turned(far_grads, far_turned)
    for i in range(near_grads.shape[0]):
        own_grad[:, i * LANES : (i + 1) * LANES] = near_grads[i, own_rows(own_grad.shape[0]), :]
    tokens = query.shape[0]
    last = keys.shape[0] - 1
    layer = lax.axis_index("dp")
    here = doc_row(docs[...])
    mine = column(here)
    before = jnp.sum((here < mine).astype(jnp.float32), axis=1, keepdims=True)
    for d in range(1, last + 1):
        fewer = (doc_row(far_docs[d - 1]) < mine) | (layer < d)
        before = before + jnp.sum(fewer.astype(jnp.float32), axis=1, keepdims=True)
    start[...] = before.astype(jnp.int32)
    doubled(pair[...], keys, values, last)
    queries[...] = per_head(query[...].astype(jnp.float32)).astype(jnp.bfloat16)

    def tile(rows, row, step):
        starts = start[pl.ds(pl.multiple_of(row, step), step), :]
        scores = tile_scores(queries[rows, :], keys, starts, row, last, last, tokens)
        top = jnp.max(scores, axis=1, keepdims=True)
        terms = jnp.exp(scores - top)
        tops[rows, :] = top
        totals[rows, :] = jnp.sum(terms, axis=1, keepdims=True)
        out[rows, :] = dot(terms.astype(jnp.bfloat16), values[last])

    attend_tiles(tokens, tile)


def attend_rest_body(far, start, mixed, log_total, keys, values, queries, out, tops, totals):
    last, tokens = far.shape[0], far.shape[1]
    for d in range(1, last + 1):
        doubled(far[d - 1], keys, values, last - d, d)

    def tile(rows, row, step):
        starts = start[pl.ds(pl.multiple_of(row, step), step), :]
        parts = [
            tile_scores(queries[rows, :], keys, starts, row, block, last, tokens)
            for block in range(last)
        ]
        top = functools.reduce(
            jnp.maximum, [jnp.max(part, axis=1, keepdims=True) for part in parts], tops[rows, :]
        )
        parts = [jnp.exp(part - top) for part in parts]
        scale = jnp.exp(tops[rows, :] - top)
        total = functools.reduce(
            jnp.add,
            [jnp.sum(p, axis=1, keepdims=True) for p in parts],
            totals[rows, :] * scale,
        )
        sums = [
            dot(part.astype(jnp.bfloat16), values[block]) for block, part in enumerate(parts)
        ]
        out[rows, :] = functools.reduce(jnp.add, sums, out[rows, :] * scale) / total
        log_total[rows, :] = top + jnp.log(total)

    attend_tiles(tokens, tile)
    first = lanes_of((tokens, LANES)) < LANES // 2
    mixed[...] = jnp.where(first, out[:tokens, :], out[tokens:, :]).astype(jnp.bfloat16)


def attend_again_body(query, pair, far, start, log_total, keys, values, queries, chances):
    tokens = query.shape[0]
    last = far.shape[0]
    doubled(pair[...], keys, values, last)
    for d in range(1, last + 1):
        doubled(far[d - 1], keys, values, last - d, d)
    queries[...] = per_head(query[...].astype(jnp.float32)).astype(jnp.bfloat16)

    def tile(rows, row, step):
        starts = start[pl.ds(pl.multiple_of(row, step), step), :]
        for block in range(last + 1):
            scores = tile_scores(queries[rows, :], keys, starts, row, block, last, tokens)
            chances[block, rows, :] = jnp.exp(scores - log_total[rows, :])

    attend_tiles(tokens, tile)


def attend_back_body(grad, w_output, mixed, cosine, sine, query_grad, pair_grad, far_grad, output_grad, grads, turned, key_sums, value_sums, keys, values, queries, chances):
    tokens = mixed.shape[0]
    last = keys.shape[0] - 1
    given_grad = grad[...].reshape(tokens, -1)
    grads[...] = per_head(dot(given_grad, w_output[...], 1, 1)).astype(jnp.bfloat16)
    output_sum = dot(mixed[...], given_grad, 0, 0).astype(jnp.bfloat16)
    for i in range(output_grad.shape[0]):
        output_grad[i] = output_sum[:, i * LANES : (i + 1) * LANES]
    for block in range(last + 1):
        cleared(key_sums.at[block])
        cleared(value_sums.at[block])

    def tile(rows, row, step):
        asked, given = queries[rows, :], grads[rows, :]
        products = [dot(given, values[block], 1, 1) for block in range(last + 1)]
        delta = functools.reduce(
            jnp.add,
            [
                jnp.sum(chances[block, rows, :] * product, axis=1, keepdims=True)
                for block, product in enumerate(products)
            ],
        )
        total = jnp.zeros((step, LANES), jnp.float32)
        for block in range(last + 1):
            chance = chances[block, rows, :]
            back = (chance * (products[block] - delta)).astype(jnp.bfloat16)
            total = total + dot(back, keys[block])
            key_sums[block] += dot(back, asked, 0, 0)
            value_sums[block] += dot(chance.astype(jnp.bfloat16), given, 0, 0)
        turned[rows, :] = total

    attend_tiles(tokens, tile)
    first = lanes_of((tokens, LANES)) < LANES // 2
    raw = jnp.where(first, turned[:tokens, :], turned[tokens:, :]) * SCORE_SCALE
    query_grad[...] = (raw * cosine[...] - flipped(raw) * sine[...]).astype(jnp.bfloat16)

    def joined(block):
        by_key, by_value = key_sums[block], value_sums[block]
        by_key = (by_key + pltpu.roll(by_key, LANES // 2, 1)) * SCORE_SCALE
        by_value = by_value + pltpu.roll(by_value, LANES // 2, 1)
        return jnp.where(first, by_key, by_value)

    pair_grad[...] = joined(last)
    for d in range(1, last + 1):
        far_grad[d - 1] = joined(last - d).astype(jnp.bfloat16)


def router_rows(router):
    rows = beside(router)
    blank = jnp.zeros((LANES - rows.shape[0], rows.shape[1]), rows.dtype)
    return jnp.concatenate([rows, blank], axis=0)


def full_dot(wide, low, left=1, right=0):
    parts, rest = [], wide
    for _ in range(3):
        parts.append(rest.astype(jnp.bfloat16))
        rest = rest - parts[-1].astype(jnp.float32)
    count = wide.shape[0]
    sums = dot(jnp.concatenate(parts, axis=0), low, left, right)
    return sums[:count] + (sums[count : 2 * count] + sums[2 * count :])


def middle_body(mixed, own, w_output, gains, router, ids_turned, rows, middle, weights, ids_ref):
    experts = router.shape[1]
    width = own.shape[1]
    attn = dot(beside(mixed), w_output[...])
    value = own[...].astype(jnp.float32) + RESIDUAL_SCALE * attn
    middle[...] = value
    scale = lax.rsqrt(jnp.mean(value * value, axis=1, keepdims=True) + EPSILON)
    normed = value * scale * gain_row(gains)
    logits = full_dot(normed, router_rows(router), 1, 1)
    count = own.shape[0]
    ids_ref[...] = ids_turned[...].astype(jnp.float32).T
    ids = ids_ref[own_rows(count), :]
    lanes = lanes_of((count, LANES))
    chosen = jnp.zeros((count, LANES), jnp.float32)
    for k in range(ids.shape[1]):
        chosen = chosen + (ids[:, k : k + 1] == lanes.astype(jnp.float32)).astype(
            jnp.float32
        )
    top = jnp.max(jnp.where(lanes < experts, logits, MASKED), axis=1, keepdims=True)
    terms = jnp.exp(jnp.minimum(logits - top, 0.0)) * chosen
    share = terms / jnp.sum(terms, axis=1, keepdims=True)
    weights[...] = share
    high = share.astype(jnp.bfloat16)
    low = share - high.astype(jnp.float32)
    rows[:, :width] = normed.astype(jnp.bfloat16)
    rows[:, width:] = (high.astype(jnp.float32) + pltpu.roll(low, LANES // 2, 1)).astype(
        jnp.bfloat16
    )


def middle_back_body(back, out_grad, middle, weights, gains, router, middle_grad, attn_grad, logit_grad, gain_part):
    width = middle.shape[1]
    normed_grad = back[0, :, :width].astype(jnp.float32)
    weight_grad = back[0, :, width:].astype(jnp.float32)
    for i in range(1, back.shape[0]):
        normed_grad = normed_grad + back[i, :, :width].astype(jnp.float32)
        weight_grad = weight_grad + back[i, :, width:].astype(jnp.float32)
    share, value = weights[...], middle[...]
    mean = jnp.sum(share * weight_grad, axis=1, keepdims=True)
    logit = share * (weight_grad - mean)
    logit_grad[...] = logit.astype(jnp.bfloat16)
    normed_grad = normed_grad + full_dot(logit, router_rows(router))
    scale = lax.rsqrt(jnp.mean(value * value, axis=1, keepdims=True) + EPSILON)
    gain_part[...] = jnp.sum(normed_grad * value * scale, axis=0, keepdims=True)
    scaled = normed_grad * gain_row(gains)
    norm_dot = jnp.sum(scaled * value, axis=1, keepdims=True)
    total = (
        out_grad[...].astype(jnp.float32)
        + scale * scaled
        - value * (scale * scale * scale * norm_dot / width)
    )
    middle_grad[...] = total
    attn_grad[...] = (RESIDUAL_SCALE * total).astype(jnp.bfloat16)


def project_back_body(query_grad, pair_grad, returned, normed, w_query, w_pair, cosine, sine, output_turned, logit, rows, gains, gain_moe, partial, sums, output_first, output_last, gain_parts):
    layer = lax.axis_index("dp")
    depth = lax.axis_size("dp")
    total = pair_grad[...]
    for i in range(returned.shape[0]):
        total = total + jnp.where(
            layer + i + 1 < depth, returned[i].astype(jnp.float32), 0.0
        )
    keys = lanes_of(total.shape) < LANES // 2
    turned = total * cosine[...] - flipped(total) * sine[...]
    pair_low = jnp.where(keys, turned, total).astype(jnp.bfloat16)
    query_low = query_grad[...]
    whole = dot(query_low, w_query[...], 1, 1) + dot(pair_low, w_pair[...], 1, 1)
    partial[...] = whole.astype(jnp.bfloat16)
    gain_attn = jnp.sum(whole * normed[...].astype(jnp.float32), axis=0, keepdims=True)
    gain_attn = gain_attn / gain_row(gains)
    gain_parts[...] = jnp.zeros_like(gain_parts)
    for i in range(gain_parts.shape[0]):
        at = slice(i * LANES, (i + 1) * LANES)
        gain_parts[i, 0:1, :] = gain_attn[:, at]
        gain_parts[i, 1:2, :] = gain_moe[0:1, at]
    width = normed.shape[1]
    sums[:width, :] = dot(normed[...], query_low, 0, 0).astype(jnp.bfloat16)
    sums[width : 2 * width, :] = dot(normed[...], pair_low, 0, 0).astype(jnp.bfloat16)
    output_sum = added(output_turned).astype(jnp.bfloat16)
    output_first[...] = output_sum[: output_first.shape[0], :]
    output_last[...] = output_sum[output_first.shape[0] :, :]
    mine = rows[:, own_rows(LANES)]
    named = logit[...].reshape(normed.shape[0], LANES)
    sums[2 * width : 2 * width + LANES, :] = dot(named, mine, 0, 0).astype(jnp.bfloat16)


def results_body(blocks, moe, own, middle, middle_grad, gains, gain_blocks, turned, block_out, in_grad, gain_sum, summed):
    gain_sum[...] = added(gain_blocks)
    summed[...] = added(turned).astype(jnp.bfloat16)
    width = own.shape[1]
    normed_grad = added(blocks)
    branch = added(moe)
    value = own[...].astype(jnp.float32)
    scale = lax.rsqrt(jnp.mean(value * value, axis=1, keepdims=True) + EPSILON)
    scaled = normed_grad * gain_row(gains)
    norm_dot = jnp.sum(scaled * value, axis=1, keepdims=True)
    grad = (
        middle_grad[...] + scale * scaled - value * (scale * scale * scale * norm_dot / width)
    ).astype(jnp.bfloat16)
    out = (middle[...] + RESIDUAL_SCALE * branch).astype(jnp.bfloat16)
    for i in range(block_out.shape[0]):
        at = slice(i * LANES, (i + 1) * LANES)
        block_out[i] = out[:, at]
        in_grad[i] = grad[:, at]


def expert_terms(gate_up, active_grad, weight):
    hidden = active_grad.shape[0]
    gate, up = gate_up[:hidden], gate_up[hidden:]
    sigmoid = jax.nn.sigmoid(gate)
    silu = gate * sigmoid
    ungated = silu * up
    active = (ungated * weight).astype(jnp.bfloat16)
    scaled = active_grad * weight
    gate_grad = (scaled * up * sigmoid * (1.0 + gate * (1.0 - sigmoid))).astype(jnp.bfloat16)
    up_grad = (scaled * silu).astype(jnp.bfloat16)
    return active, jnp.concatenate([gate_grad, up_grad], axis=0), active_grad * ungated


def weight_rows(extra):
    turned = extra.astype(jnp.float32).T
    return turned[: LANES // 2] + turned[LANES // 2 :]


def local_experts_body(sizes, kinds, rows_hbm, grads_hbm, in_ref, out_ref, sent_grads, sent_rows, flat_ref, in_sum, out_sum, moe_hbm, back_hbm, got_grads, got_rows, rows_ref, grads_ref, moe_ref, back_ref, moe_acc, back_acc, share, weights, spread, copy_sem, *sems):
    step, steps = pl.program_id(0), pl.num_programs(0)
    each, hidden, width = out_ref.shape
    parts = hidden // LANES
    moves = Moves(sizes, kinds, [sent_grads, sent_rows], [got_grads, got_rows], sems)
    ends = [(rows_hbm, rows_ref), (grads_hbm, grads_ref), (moe_ref, moe_hbm), (back_ref, back_hbm)]
    copy = lambda i: pltpu.make_async_copy(*ends[i], copy_sem.at[i])

    @pl.when(step == 0)
    def _():
        copy(0).start()
        copy(1).start()
        moves.barrier()
        moves.start([0])
        cleared(moe_acc)
        cleared(back_acc)
        copy(0).wait()
        copy(1).wait()
        share[...] = jnp.zeros_like(share)
        weights[...] = weight_rows(rows_ref[:, width:])

    @pl.when(step == 2 * steps // 8)
    def _():
        moves.start([1])

    for when, item, stage in ((3, 0, 0), (6, 1, 0), (7, 0, 1)):

        @pl.when(step == when * steps // 8)
        def _(item=item, stage=stage):
            moves.relay([item], (stage,))

    for i in range(each):
        spread[i] = in_ref[i].astype(jnp.float32)
        for part in range(parts):
            for half in range(2):
                at = half * hidden + part * LANES
                flat_ref[i, :, at : at + LANES] = spread[
                    i, pl.ds(part * 2 + half, width, stride=2 * parts), :
                ].astype(jnp.bfloat16)
        expert = (lax.axis_index("row") * steps + step) * each + i
        active, gate_up_grad, shares = expert_terms(
            dot(flat_ref[i], rows_ref[:, :width], 0, 1),
            dot(out_ref[i], grads_ref[...]),
            weights[pl.ds(expert, 1), :],
        )
        share[pl.ds(expert, 1), :] = jnp.sum(shares, axis=0, keepdims=True)
        moe_acc[...] += dot(active, out_ref[i], 0, 0)
        back_acc[...] += dot(gate_up_grad, flat_ref[i], 0, 1)
        in_sum[i] = dot(gate_up_grad, rows_ref[:, :width]).astype(jnp.bfloat16)
        out_sum[i] = dot(active, grads_ref[...], 1, 1).astype(jnp.bfloat16)

    @pl.when(step == steps - 1)
    def _():
        moves.relay([1], (1,))
        widened(moe_acc, moe_ref)
        copy(2).start()
        widened(back_acc, back_ref.at[:, :width])
        back_ref[:, width:] = share[...].T.astype(jnp.bfloat16)
        copy(3).start()
        moves.finish()
        copy(2).wait()
        copy(3).wait()


def local_experts(sizes, number, rows, grads, w_in, w_out, sent_grads, sent_rows):
    tokens, wide = rows.shape
    experts, hidden, width = w_out.shape
    each = 1
    low = jnp.bfloat16
    kinds, shapes, sems = planned(
        sizes,
        [
            ("gather", sent_grads, True, sent_grads.shape[0]),
            ("gather", sent_rows, True, sent_rows.shape[0]),
        ],
    )
    some = lambda s: pl.BlockSpec((each,) + s[1:], lambda e: (e,) + (0,) * (len(s) - 1))
    outs = [
        (experts, width, 2 * hidden),
        (experts, 2 * hidden, width),
        (experts, hidden, width),
        (tokens, width),
        (tokens, wide),
    ]
    return pl.pallas_call(
        functools.partial(local_experts_body, sizes, kinds),
        grid=(experts // each,),
        in_specs=[
            HBM,
            HBM,
            some(w_in.shape),
            some(w_out.shape),
            HBM,
            HBM,
        ],
        out_specs=(*[some(s) for s in outs[:3]], HBM, HBM, HBM, HBM),
        out_shape=tuple(jax.ShapeDtypeStruct(s, low) for s in outs) + tuple(shapes),
        scratch_shapes=[
            pltpu.VMEM(rows.shape, low),
            pltpu.VMEM(grads.shape, low),
            pltpu.VMEM((tokens, width), low),
            pltpu.VMEM((tokens, wide), low),
            pltpu.VMEM((tokens, width), jnp.float32),
            pltpu.VMEM((tokens, width), jnp.float32),
            pltpu.VMEM((LANES, tokens), jnp.float32),
            pltpu.VMEM((LANES // 2, tokens), jnp.float32),
            pltpu.VMEM((each,) + w_in.shape[1:], jnp.float32),
            pltpu.SemaphoreType.DMA((4,)),
        ]
        + sems,
        compiler_params=pltpu.CompilerParams(collective_id=number, has_side_effects=True),
        name="local_experts",
    )(rows, grads, w_in, w_out, sent_grads, sent_rows)


class Sums:
    def __init__(self, rows, grads, weights, turned, load_sem, *sums):
        self.rows, self.grads, self.weights = rows, grads, weights
        self.turned, self.load_sem, self.sums = turned, load_sem, sums

    def load(self, which, source):
        target = (self.rows, self.grads)[which]
        return pltpu.make_async_copy(source, target, self.load_sem.at[which])

    def ready(self):
        layers, width, tokens = self.grads.shape

        def block(i, carry):
            at = pl.ds(pl.multiple_of(i * tokens, tokens), tokens)
            self.weights[i] = weight_rows(self.rows[at, width:])
            return carry

        lax.fori_loop(0, layers, block, 0)

    def make(self, index, w_in, w_out, in_part, out_part, made, arrive):
        layers, width, tokens = self.grads.shape
        hidden = w_out.shape[0]
        arrive(0)
        if self.sums:
            arrive(1)
        later = arrive

        def part_of(at, pieces, arrive=lambda i: None if self.sums else later(i)):
            first = at * tokens if isinstance(at, int) else pl.multiple_of(at * tokens, tokens)
            block = self.rows[pl.ds(first, pieces * tokens), :width]
            gate_up = dot(w_in[...], block, 0, 1)
            arrive(1)
            weight = jnp.concatenate(
                [self.weights[at + i, pl.ds(index, 1), :] for i in range(pieces)], axis=1
            )
            active_grad = jnp.concatenate(
                [dot(w_out[...], self.grads[at + i]) for i in range(pieces)], axis=1
            )
            active, gate_up_grad, _ = expert_terms(gate_up, active_grad, weight)
            out_total = functools.reduce(
                jnp.add,
                [
                    dot(active[:, i * tokens : (i + 1) * tokens], self.grads[at + i], 1, 1)
                    for i in range(pieces)
                ],
            )
            return dot(gate_up_grad, block), out_total

        if not self.sums:
            in_total, out_total = part_of(0, layers)
        else:
            whole, out_acc = self.sums
            whole[...] = jnp.zeros_like(whole)
            out_acc[...] = jnp.zeros_like(out_acc)

            def more(i, carry):
                in_more, out_more = part_of(i, 1)
                whole[...] += in_more
                out_acc[...] += out_more
                return carry

            lax.fori_loop(0, layers, more, 0)
            in_total, out_total = whole[...], out_acc[...]
        arrive(2)
        in_total = in_total + in_part[...].astype(jnp.float32)
        parts = hidden // LANES
        for part in range(parts):
            for half in range(2):
                at = half * hidden + part * LANES
                self.turned[pl.ds(part * 2 + half, width, stride=2 * parts), :] = in_total[
                    at : at + LANES, :
                ].T
        made[...] = self.turned[...].astype(jnp.bfloat16)
        return out_total + out_part[...].astype(jnp.float32)


def sums_scratch(layers, tokens, width, hidden):
    low, full = jnp.bfloat16, jnp.float32
    return [
        pltpu.VMEM((layers * tokens, width + LANES), low),
        pltpu.VMEM((layers, width, tokens), low),
        pltpu.VMEM((layers, LANES // 2, tokens), full),
        pltpu.VMEM((width * 2 * hidden // LANES, LANES), full),
        pltpu.SemaphoreType.DMA((2,)),
    ] + [pltpu.VMEM((k * hidden, width), full) for k in (2, 1) if layers > 4]


class Cover:
    def __init__(self, first, many, work):
        w_in, w_out, in_part, out_part, rows_far, grads_far = work
        layers, width, tokens = grads_far.shape
        self.experts, hidden, _ = w_out.shape
        self.first, self.many, self.work = first, many, work
        low = jnp.bfloat16
        self.shapes = [
            ((many, width * 2 * hidden // LANES, LANES), low),
            ((many, hidden, width), low),
        ]
        self.scratch = [pltpu.VMEM((many,) + a.shape[1:], low) for a in work[:4]]
        self.scratch += [pltpu.VMEM(*s) for s in self.shapes]
        self.scratch += [pltpu.SemaphoreType.DMA((4, many)), pltpu.SemaphoreType.DMA((2, many))]
        self.scratch += sums_scratch(layers, tokens, width, hidden)

    def load(self, which, i, work, refs):
        source, sem = work[which].at[self.first + i], refs[6].at[which, i]
        return pltpu.make_async_copy(source, refs[which].at[i], sem)

    def begin(self, work, refs):
        sums = Sums(*refs[8:])
        sums.load(0, work[4]).start()
        self.load(0, 0, work, refs).start()
        sums.load(1, work[5]).start()
        for which in (1, 2, 3):
            self.load(which, 0, work, refs).start()
        for i in range(1, self.many):
            for which in range(4):
                self.load(which, i, work, refs).start()

    def stores(self, i, made, refs):
        return [
            pltpu.make_async_copy(refs[4 + k].at[i], made[k].at[i], refs[7].at[k, i])
            for k in range(2)
        ]

    def run(self, work, made, refs):
        sums = Sums(*refs[8:])

        def expert(i, carry):
            def arrive(point):
                @pl.when(i == 0)
                def _():
                    if point == 0:
                        sums.load(0, work[4]).wait()
                        sums.ready()
                    if point == 1:
                        sums.load(1, work[5]).wait()

                for which in ((0,), (1,), (2, 3))[point]:
                    self.load(which, i, work, refs).wait()

            index = lax.axis_index("row") * self.experts + self.first + i
            out_total = sums.make(index, *[refs[k].at[i] for k in range(5)], arrive)
            refs[5][i] = out_total.astype(jnp.bfloat16)
            for store in self.stores(i, made, refs):
                store.start()
            return carry

        lax.fori_loop(0, self.many, expert, 0)

    def end(self, made, refs):
        for i in range(self.many):
            for store in self.stores(i, made, refs):
                store.wait()


def outputs_body(count, total, *refs):
    pieces = total // count
    sums, smalls = refs[: 2 * pieces], refs[2 * pieces : 2 * pieces + 6]
    gin, gout, *others = refs[2 * pieces + 6 : 2 * pieces + 16]
    block_out, in_grad, gain_attn, gain_moe, query, pair, output, router = others
    in_low, out_low, in_full, out_full, *refs = refs[2 * pieces + 16 :]
    held, (load_sem, store_sem, small_sem) = refs[:6], refs[6:]
    ring = in_full.shape[0]

    def load(k, i):
        low = (in_low, out_low)[k]
        source = sums[k * pieces + i // count].at[i % count]
        return pltpu.make_async_copy(source, low.at[i], load_sem.at[k, i])

    def store(k, i):
        made, target = ((in_full, gin), (out_full, gout))[k]
        return pltpu.make_async_copy(made.at[i % ring], target.at[i], store_sem.at[k, i % ring])

    for i in range(total):
        for k in range(2):
            load(k, i).start()
        if i == 0:
            fetched = [
                pltpu.make_async_copy(a, b, small_sem.at[j])
                for j, (a, b) in enumerate(zip(smalls, held))
            ]
            for copy in fetched:
                copy.start()
    def small():
        for copy in fetched:
            copy.wait()
        blocks, in_blocks, gains, summed, output_first, output_last = held
        width = gout.shape[2]
        for i in range(blocks.shape[0]):
            at = pl.ds(i * blocks.shape[1], blocks.shape[1])
            block_out[at, :] = blocks[i]
            in_grad[at, :] = in_blocks[i]
        gain_sum = jnp.sum(gains[...], axis=0)
        gain_attn[...] = gain_sum[0:1, :]
        gain_moe[...] = gain_sum[1:2, :]
        query[...] = summed[:width, :].astype(jnp.float32)
        pair[...] = summed[width : 2 * width, :].astype(jnp.float32)
        router[...] = summed[2 * width : 2 * width + router.shape[0], :].astype(jnp.float32)
        half = output_first.shape[1]
        for i in range(width // half):
            from_first = i % 2 == 0
            rows = (output_first if from_first else output_last)[i // 2].astype(jnp.float32)
            for j in range(max(1, half // LANES)):
                place = i * half + j * LANES
                at = place // LANES
                part = rows[j * LANES : (j + 1) * LANES, :]
                first = place % LANES
                output[first : first + part.shape[0], at * LANES : (at + 1) * LANES] = part

    for i in range(total):
        for k in range(2):
            load(k, i).wait()
            if i >= ring:
                store(k, i - ring).wait()
        for low, made in ((in_low, in_full), (out_low, out_full)):
            widened(low.at[i], made.at[i % ring])
        for k in range(2):
            store(k, i).start()
        if i == total - 3:
            small()
    for i in range(total - ring, total):
        for k in range(2):
            store(k, i).wait()


def outputs(in_sums, out_sums, hidden, experts, *smalls):
    count = in_sums[0].shape[0]
    total = count * len(in_sums)
    width = out_sums[0].shape[2]
    parts = hidden // LANES
    lanes = smalls[0].shape[2]
    tokens = smalls[0].shape[0] * smalls[0].shape[1]
    low, full = jnp.bfloat16, jnp.float32
    large = [(width * 2 * parts, LANES), (hidden, width)]
    shapes = [((total,) + s, full) for s in large] + [
        ((tokens, lanes), low),
        ((tokens, lanes), low),
        ((1, LANES), full),
        ((1, LANES), full),
        ((width, LANES), full),
        ((width, LANES), full),
        ((LANES, width), full),
        ((experts, LANES), full),
    ]
    ring = min(4, total)
    gin, *others = pl.pallas_call(
        functools.partial(outputs_body, count, total),
        in_specs=[HBM] * (2 * len(in_sums) + len(smalls)),
        out_specs=(HBM, HBM) + (FULL,) * (len(shapes) - 2),
        out_shape=tuple(jax.ShapeDtypeStruct(*shape) for shape in shapes),
        scratch_shapes=[pltpu.VMEM((total,) + s, low) for s in large]
        + [pltpu.VMEM((ring,) + s, full) for s in large]
        + [pltpu.VMEM(a.shape, a.dtype) for a in smalls]
        + [pltpu.SemaphoreType.DMA(s) for s in ((2, total), (2, ring), (len(smalls),))],
        name="outputs",
    )(*in_sums, *out_sums, *smalls)
    gin = gin.reshape(total, width, parts, 2, LANES).transpose(0, 1, 3, 2, 4)
    return gin.reshape(total, width, 2, hidden), *others


def local(
    sizes,
    tokens,
    out_grad,
    doc_ids,
    expert_ids,
    gain_attn,
    w_query,
    w_key_value,
    w_output,
    gain_moe,
    w_router,
    w_expert_in,
    w_expert_out,
):
    rows, cols, depth = sizes
    group = rows * cols
    tok_rows, feat_local = tokens.shape
    width = w_query.shape[0]
    experts = w_router.shape[1]
    expert_local, hidden = w_expert_out.shape[0], w_expert_out.shape[1]
    longest_doc = min(LONGEST, tok_rows * depth // 2)
    hop_count = longest_doc // tok_rows
    own = tok_rows // group
    low, full = jnp.bfloat16, jnp.float32
    layer = lax.axis_index("dp")
    me = lax.axis_index("row") * cols + lax.axis_index("col")
    everyone = list(range(1, depth))
    hops = list(range(1, hop_count + 1))

    w_pair = w_key_value.reshape(width, -1)
    block = (tok_rows, LANES)
    cosine, sine, normed, query, pair, tokens_own, gains, gains_moe, router, docs_far, grads_shifted, grad_blocks = exchange(
        sizes,
        "gather_tokens",
        0,
        ("gather", tokens, False, 2),
        ("share", gain_attn.reshape(1, LANES)),
        ("share", gain_moe.reshape(1, LANES)),
        ("share", w_router.T),
        ("shift", doc_ids.reshape(-1, LANES), everyone, False),
        ("shift", out_grad, everyone, False),
        ("gather", out_grad, False, 2),
        before=Stage(tables_body, [(block, full), (block, full)]),
        after=Stage(
            project_body,
            [((tok_rows, width), low), (block, low), (block, low), ((own, width), low)],
            Got(0),
            Got(1),
            w_query,
            w_pair,
            Made(0),
            Made(1),
        ),
        landing=(0,),
        delayed=(6,),
    )

    stack = (hop_count + 1,) + block
    twice = (2 * tok_rows, LANES)
    turned_block = (LANES, tok_rows)
    whole = (2 * tok_rows, 1)
    grad_own, grads_near, far_turned, start, mixed, log_total, far, output_blocks = exchange(
        sizes,
        "shift_pairs",
        1,
        ("line", pair, False, 2, hop_count),
        ("gather", w_output, False, 4),
        before=Stage(
            attend_first_body,
            [
                ((own, width), low),
                ((group,) + turned_block, low),
                ((depth - 1,) + turned_block, low),
                ((tok_rows, 1), jnp.int32),
            ],
            grad_blocks,
            grads_shifted,
            query,
            pair,
            doc_ids.reshape(-1, LANES),
            docs_far,
        ),
        after=Stage(
            attend_rest_body,
            [(block, low), (whole, full)],
            Got(0),
            Made(3),
        ),
        shared=[
            pltpu.VMEM(stack, low),
            pltpu.VMEM(stack, low),
            pltpu.VMEM(twice, low),
            pltpu.VMEM(twice, full),
            pltpu.VMEM(whole, full),
            pltpu.VMEM(whole, full),
        ],
    )
    output_full = output_blocks.reshape(-1, width)

    rows_own, middle, weights = exchange(
        sizes,
        "swap_mixed",
        2,
        ("swap", mixed.reshape(group, own, LANES)),
        after=Stage(
            middle_body,
            [((own, width + LANES), low), ((own, width), full), ((own, LANES), full)],
            Got(0),
            tokens_own,
            output_full,
            gains_moe,
            router,
            expert_ids.T,
            scratch=[pltpu.VMEM(expert_ids.shape, full)],
        ),
        landing=(0,),
    )
    rows_blocks, rows_shifted = exchange(
        sizes,
        "gather_rows",
        3,
        ("gather", rows_own, False, 2),
        ("line", rows_own, False, 4),
    )
    rows_near = rows_blocks.reshape(tok_rows, -1)
    parts = hidden // LANES
    in_rows = w_expert_in.reshape(expert_local, width, 2, parts, LANES)
    in_rows = in_rows.transpose(0, 1, 3, 2, 4).reshape(expert_local, -1, LANES)
    in_flat, in_part, out_part, moe_partial, back_partial, grads_far, rows_far = local_experts(
        sizes,
        9,
        rows_near,
        grads_near.reshape(width, tok_rows),
        in_rows,
        w_expert_out,
        far_turned,
        rows_shifted,
    )
    rows_far = rows_far.reshape((depth - 1) * tok_rows, -1)
    grads_far = grads_far.reshape(depth - 1, width, tok_rows)
    work = (in_flat, w_expert_out, in_part, out_part, rows_far, grads_far)
    share = expert_local // 4
    unit = 16 * depth
    in_sums, out_sums = [], []

    def beneath(name, number, *items, after=None, landing=()):
        cover = Cover(len(in_sums) * share, share, work)
        in_sum, out_sum, *moved = exchange(
            sizes, name, number, *items, after=after, cover=cover, landing=landing
        )
        if after:
            count = len(after.shapes)
            results = [in_sum, out_sum, *moved]
            in_sum, out_sum = results[count], results[count + 1]
            moved = results[:count] + results[count + 2 :]
        in_sums.append(in_sum)
        out_sums.append(out_sum)
        return moved

    middle_grad, attn_grad, logit_grad, gain_moe_part = beneath(
        "swap_back",
        4,
        ("swap", back_partial.reshape(group, own, -1)),
        after=Stage(
            middle_back_body,
            [
                ((own, width), full),
                ((own, width), low),
                ((own, LANES), low),
                ((1, width), full),
            ],
            Got(0),
            grad_own,
            middle,
            weights,
            gains_moe,
            router,
        ),
        landing=(0,),
    )
    query_grad, pair_grad, far_grad, output_sum, logit_blocks = exchange(
        sizes,
        "gather_attn_grad",
        5,
        ("gather", attn_grad, False, 2),
        ("gather", logit_grad),
        delayed=(1,),
        before=Stage(attend_again_body, [], query, pair, far, start, log_total),
        after=Stage(
            attend_back_body,
            [
                (block, low),
                (block, full),
                ((hop_count,) + block, low),
                ((group, LANES, LANES), low),
            ],
            Got(0),
            w_output,
            mixed,
            cosine,
            sine,
            scratch=[
                pltpu.VMEM(twice, low),
                pltpu.VMEM(twice, full),
                pltpu.VMEM(stack, full),
                pltpu.VMEM(stack, full),
            ],
        ),
        landing=(0,),
        shared=[
            pltpu.VMEM(stack, low),
            pltpu.VMEM(stack, low),
            pltpu.VMEM(twice, low),
            pltpu.VMEM((hop_count + 1, 2 * tok_rows, tok_rows), full),
        ],
    )
    length = (2 * width + LANES + unit - 1) // unit * unit
    partial, sums, output_first, output_last, gain_parts, moe_blocks = beneath(
        "shift_grads",
        6,
        ("shift", far_grad, [-d for d in hops], True),
        ("swap", moe_partial.reshape(group, own, width)),
        ("turn", output_sum.reshape(depth, width // depth, LANES)),
        after=Stage(
            project_back_body,
            [
                ((tok_rows, width), low),
                ((length, LANES), low),
                ((width // depth // 2, LANES), low),
                ((width // depth // 2, LANES), low),
                ((group, 8, LANES), full),
            ],
            query_grad,
            pair_grad,
            Got(0),
            normed,
            w_query,
            w_pair,
            cosine,
            sine,
            Got(2),
            logit_blocks,
            rows_near,
            gains,
            gain_moe_part,
        ),
        landing=(0, 2),
    )
    pieces = (group, own, LANES)
    block_out, in_grad, gain_sum, summed, output_first = beneath(
        "swap_partial",
        7,
        ("swap", partial.reshape(group, own, width)),
        ("turn", sums.reshape(depth, length // depth, LANES)),
        ("swap", gain_parts),
        ("collect", output_first),
        after=Stage(
            results_body,
            [(pieces, low), (pieces, low), ((8, LANES), full), ((length // depth, LANES), low)],
            Got(0),
            moe_blocks,
            tokens_own,
            middle,
            middle_grad,
            gains,
            Got(2),
            Got(1),
        ),
        landing=(0, 1, 2),
    )
    block_out, in_grad, sums, output_last, gain_all = beneath(
        "swap_results",
        8,
        ("swap", block_out),
        ("swap", in_grad),
        ("collect", summed),
        ("collect", output_last),
        ("collect", gain_sum),
    )
    grad_in, grad_out, block_out, in_grad, gain_attn_sum, gain_moe_sum, query_sum, pair_sum, output_sum, router_sum = outputs(
        in_sums,
        out_sums,
        hidden,
        experts,
        block_out,
        in_grad,
        gain_all,
        sums.reshape(length, LANES),
        output_first,
        output_last,
    )
    return (
        block_out,
        in_grad,
        gain_attn_sum.reshape(LANES),
        query_sum,
        pair_sum.reshape(w_key_value.shape),
        output_sum,
        gain_moe_sum.reshape(LANES),
        router_sum.T,
        grad_in,
        grad_out,
    )


def solution(mesh):
    in_specs = (
        P("dp", ("row", "col")),
        P("dp", ("row", "col")),
        P("dp"),
        P("dp", None),
        P(("row", "col")),
        P(None, ("row", "col")),
        P(None, ("row", "col"), None),
        P(("row", "col"), None),
        P(("row", "col")),
        P(("row", "col"), None),
        P("row", None, None, "col"),
        P("row", "col", None),
    )
    out_specs = (
        P("dp", ("row", "col")),
        P("dp", ("row", "col")),
        P(("row", "col")),
        P(None, ("row", "col")),
        P(None, ("row", "col"), None),
        P(("row", "col"), None),
        P(("row", "col")),
        P(("row", "col"), None),
        P("row", None, None, "col"),
        P("row", "col", None),
    )
    sizes = (mesh.shape["row"], mesh.shape["col"], mesh.shape["dp"])
    return jax.shard_map(
        functools.partial(local, sizes),
        mesh=mesh,
        in_specs=in_specs,
        out_specs=out_specs,
        check_vma=False,
    )
```

```python
import functools
import itertools
import math

import jax
import jax.numpy as jnp
from jax import lax
from jax.experimental import pallas as pl
from jax.experimental.pallas import tpu as pltpu
from jax.sharding import PartitionSpec as P

LONGEST = 4096
EPSILON = 1e-05
RESIDUAL_SCALE = 0.22
SCORE_SCALE = 0.015625
ROPE_BASE = 10000.0
MASKED = -1e30
MESH = pl.DeviceIdType.MESH
GROUP = ("row", "col")
EVERY = ("dp", "row", "col")
LANES = 128
HBM = pl.BlockSpec(memory_space=pl.ANY)
TURN = LANES // 4


class Moves:
    def __init__(self, sizes, kinds, sources, targets, sems):
        self.sizes, self.kinds = sizes, kinds
        self.sources, self.targets = sources, targets
        self.send_sem, self.recv_sem, self.local_sem = sems

    def place(self):
        row, col, layer = lax.axis_index("row"), lax.axis_index("col"), lax.axis_index("dp")
        return row, col, layer, row * self.sizes[1] + col

    def member(self, index):
        rows, cols, depth = self.sizes
        return {"row": index // cols, "col": lax.rem(index, cols)}

    def across(self, row):
        low = lax.rem(row, 2)
        return row + 1 - 2 * low, lax.rem(row + 2, 4), lax.rem(row + 3 - 2 * low, 4)

    def barrier(self):
        rows, cols, depth = self.sizes
        row, col, layer, me = self.place()
        group = rows * cols
        names = [kind[0] for kind in self.kinds]
        barrier = pltpu.get_barrier_semaphore()
        partners = []
        if "swap" in names or "share" in names:
            for k in range(1, group):
                partners.append(self.member(lax.rem(me + k, group)))
        elif "gather" in names:
            for other in self.across(row)[:2]:
                partners.append({"row": other})
            for k in range(1, cols):
                partners.append({"col": lax.rem(col + k, cols)})
        shifts = set()
        for kind in self.kinds:
            if kind[0] == "shift":
                for d in kind[1]:
                    shifts |= {d % depth, -d % depth}
            elif kind[0] in ("turn", "collect"):
                shifts |= set(range(1, depth))
        for k in sorted(shifts - {0}):
            partners.append({"dp": lax.rem(layer + k, depth)})
        ends = [(layer > 0, layer - 1), (layer < depth - 1, layer + 1)]
        ends = ends if "line" in names and not shifts else []
        for partner in partners:
            pl.semaphore_signal(barrier, inc=1, device_id=partner, device_id_type=MESH)
        for there, other in ends:

            @pl.when(there)
            def _(device={"dp": other}):
                pl.semaphore_signal(barrier, inc=1, device_id=device, device_id_type=MESH)

        expected = len(partners)
        for there, _ in ends:
            expected = expected + there.astype(jnp.int32)
        pl.semaphore_wait(barrier, expected)

    def plan(self, only):
        rows, cols, depth = self.sizes
        row, col, layer, me = self.place()
        group = rows * cols
        slots = iter(range(self.send_sem.shape[0]))
        starts, relays, sends, arrivals, local = [], [], [], [], []

        def remote(source, target, device, slot=None):
            slot = next(slots) if slot is None else slot
            return functools.partial(
                pltpu.make_async_remote_copy,
                src_ref=source,
                dst_ref=target,
                send_sem=self.send_sem.at[slot],
                recv_sem=self.recv_sem.at[slot],
                device_id=device,
                device_id_type=MESH,
            )

        for index, (kind, source, target) in enumerate(
            zip(self.kinds, self.sources, self.targets)
        ):
            item = [], [], [], [], []
            begin, follow, sent, got, stay = item

            def keep(source, target):
                sem = self.local_sem.at[index]
                stay.append(functools.partial(pltpu.make_async_copy, source, target, sem))

            def direct(source, target, device):
                copy = None, remote(source, target, device)
                begin.append(copy)
                sent.append(copy)
                got.append(copy)

            if kind[0] == "gather":
                second, parts = kind[1:]
                size = source.shape[0] // parts
                beside, above, away = self.across(row)

                def at(other, part, piece=None):
                    member = other * cols + col
                    first, length, deep = part * size, size, ()
                    if piece is not None and size % 2 == 0:
                        length = size // 2
                        first = first + piece * length
                    elif piece is not None:
                        inner = source.shape[1] // 2
                        deep = (pl.ds(piece * inner, inner),)
                    some = pl.ds(first, length)
                    return target.at[(some, member) + deep if second else (member, some) + deep]

                def to_mates(piece):
                    made = []
                    for j in range(1, cols):
                        copy = None, remote(piece, piece, {"col": lax.rem(col + j, cols)})
                        made.append(copy)
                        sent.append(copy)
                        got.append(copy)
                    return made

                for part in range(parts):
                    some = source.at[pl.ds(part * size, size)]
                    ways = []
                    for near, other, piece in ((beside, above, 0), (above, beside, 1)):
                        first = None, remote(some, at(row, part), {"row": near})
                        passed = at(near, part, piece)
                        onward = None, remote(passed, passed, {"row": other})
                        begin.append(first)
                        sent.extend([first, onward])
                        ways.append((near, piece, first, onward))
                    for near, piece, first, onward in ways:
                        nexts = [onward] + to_mates(at(near, part))
                        follow.append((2 + 3 * part, 0, None, first[1], nexts))
                    for near, piece, first, onward in ways:
                        nexts = to_mates(at(away, part, piece))
                        follow.append((2 + 3 * parts + part, 1, None, onward[1], nexts))
                    for j in range(1, cols):
                        direct(some, at(row, part), {"col": lax.rem(col + j, cols)})
                keep(source, target.at[:, me] if second else target.at[me])
            elif kind[0] in ("swap", "share"):
                for k in range(1, group):
                    other = lax.rem(me + k, group)
                    piece = source.at[other] if kind[0] == "swap" else source
                    direct(piece, target.at[me], self.member(other))
                keep(source.at[me] if kind[0] == "swap" else source, target.at[me])
            elif kind[0] in ("turn", "collect"):
                for k in range(1, depth):
                    other = lax.rem(layer + k, depth)
                    piece = source.at[other] if kind[0] == "turn" else source
                    direct(piece, target.at[layer], {"dp": other})
                keep(source.at[layer] if kind[0] == "turn" else source, target.at[layer])
            elif kind[0] == "line":
                absolute, parts, limit = kind[1:]
                size = source.shape[0] // parts
                steps = limit or depth - 1
                ways = (1,) if limit else (1, -1)
                for part, way in itertools.product(range(parts), ways):
                    behind = layer if way == 1 else depth - 1 - layer
                    onward = layer + way
                    more = (onward >= 0) & (onward < depth)
                    mine = [next(slots) for _ in range(steps)]
                    some = pl.ds(part * size, size)

                    def held(step, where, way=way, some=some):
                        if step == 0:
                            return source.at[some]
                        if absolute:
                            return target.at[where - way * step, some]
                        return target.at[step - 1 if way == 1 else depth - 1 - step, some]

                    def sending(step, onward=onward, mine=mine, held=held):
                        device = {"dp": onward}
                        return remote(
                            held(step - 1, layer), held(step, onward), device, mine[step - 1]
                        )

                    begin.append((more, sending(1)))
                    for step in range(1, steps + 1):
                        sent.append((more & (behind >= step - 1), sending(step)))
                        block = held(step, layer)
                        arrival = remote(block, block, {"dp": onward}, mine[step - 1])
                        nexts = [(more, sending(step + 1))] if step < steps else []
                        when = 4 * step + part
                        follow.append((when, step - 1, behind >= step, arrival, nexts))
                if absolute:
                    keep(source, target.at[layer])
            else:
                for at_slot, d in enumerate(kind[1]):
                    piece = source.at[at_slot] if kind[2] else source
                    direct(piece, target.at[at_slot], {"dp": lax.rem(layer + d % depth, depth)})
            if only is None or index in only:
                starts += begin
                relays += follow
                sends += sent
                arrivals += got
                local += stay
        return starts, sorted(relays, key=lambda entry: entry[0]), sends, arrivals, local

    def given(self, condition, action):
        if condition is None:
            action()
        else:
            pl.when(condition)(action)

    def start(self, only=None):
        starts, _, _, _, local = self.plan(only)
        for condition, copy in starts:
            self.given(condition, lambda copy=copy: copy().start())
        for copy in local:
            copy().start()

    def relay(self, only=None, stages=None):
        for _, stage, condition, copy, nexts in self.plan(only)[1]:
            if stages is not None and stage not in stages:
                continue

            def action(copy=copy, nexts=nexts):
                copy().wait_recv()
                for more, follower in nexts:
                    self.given(more, lambda follower=follower: follower().start())

            self.given(condition, action)

    def finish(self, only=None):
        _, _, sends, arrivals, local = self.plan(only)
        for condition, copy in arrivals:
            self.given(condition, lambda copy=copy: copy().wait_recv())
        for condition, copy in sends:
            self.given(condition, lambda copy=copy: copy().wait_send())
        for copy in local:
            copy().wait()


def planned(sizes, items):
    rows, cols, depth = sizes
    group = rows * cols
    kinds, shapes, copies = [], [], 0
    for item in items:
        name, array = item[0], item[1]
        shape = array.shape
        if name == "gather":
            assert rows == 4
            second, parts = (item[2:] + (False, 1)[len(item) - 2 :])[:2]
            kinds.append((name, second, parts))
            shape = (shape[0], group) + shape[1:] if second else (group,) + shape
            copies += parts * (4 + 5 * (cols - 1))
        elif name == "shift":
            distances, split = item[2], item[3]
            kinds.append((name, tuple(distances), split))
            shape = (len(distances),) + (shape[1:] if split else shape)
            copies += len(distances)
        elif name == "line":
            parts, limit = (item[3:] + (1, 0)[len(item) - 3 :])[:2]
            kinds.append((name, item[2], parts, limit))
            shape = (depth if item[2] else limit or depth - 1,) + shape
            copies += (limit or 2 * (depth - 1)) * parts
        else:
            kinds.append((name,))
            if name in ("share", "collect"):
                shape = (group if name == "share" else depth,) + shape
            copies += (depth if name in ("turn", "collect") else group) - 1
        shapes.append(jax.ShapeDtypeStruct(shape, array.dtype))
    sems = [
        pltpu.SemaphoreType.DMA((copies,)),
        pltpu.SemaphoreType.DMA((copies,)),
        pltpu.SemaphoreType.DMA((len(items),)),
    ]
    return tuple(kinds), shapes, sems


class Got:
    def __init__(self, index):
        self.index = index


class Made:
    def __init__(self, index):
        self.index = index


class Stage:
    def __init__(self, body, shapes, *operands, scratch=()):
        self.body, self.shapes, self.operands = body, shapes, operands
        self.scratch = list(scratch)


def exchange(sizes, name, number, *items, before=None, after=None, cover=None, landing=(), shared=(), delayed=()):
    kinds, moved, sems = planned(sizes, items)
    stages = [stage for stage in (before, after) if stage]
    operands = []
    for stage in stages:
        for operand in stage.operands:
            if not isinstance(operand, (Got, Made)):
                operands.append(operand)
    work = list(cover.work) if cover else []
    outs = [s for stage in stages for s in stage.shapes]
    made_shapes = list(cover.shapes) if cover else []
    flown = [i for i in range(len(items)) if i not in landing]
    late = [o.index for o in (after.operands if after else ()) if isinstance(o, Got)]
    late = [i for i in late if i not in landing]
    scratch = []

    def take(shapes):
        first = len(scratch)
        scratch.extend(shapes)
        return slice(first, len(scratch))

    vmem = lambda s: pltpu.VMEM(tuple(s[0]), s[1])
    of = lambda a: (a.shape, a.dtype)
    operand_at = take([vmem(of(a)) for a in operands])
    result_at = take([vmem(s) for s in outs])
    landed_at = take([vmem(of(moved[i])) for i in landing])
    late_at = take([vmem(of(moved[i])) for i in late])
    stage_at = [take(stage.scratch) for stage in stages]
    shared_at = take(list(shared))
    needed = sorted({o.index for o in (after.operands if after else ()) if isinstance(o, Got)})
    others = [i for i in range(len(items)) if i not in needed]
    prompt = [i for i in range(len(items)) if i not in delayed]
    later = range(1, 2 * sizes[2])
    cover_at = take(cover.scratch) if cover else slice(0, 0)
    copies = len(operands) + len(outs) + len(late)
    copy_at = take([pltpu.SemaphoreType.DMA((max(1, copies),))])
    sems_at = take(sems)

    def body(*refs):
        cuts = [len(operands), len(work), len(items), len(outs), len(made_shapes), len(flown)]
        groups = []
        for cut in cuts:
            groups.append(refs[:cut])
            refs = refs[cut:]
        given, work_refs, sources, results, made_refs, flown_refs = groups
        loaded, held = refs[operand_at], refs[result_at]
        landed, lates, (copy_sem,) = refs[landed_at], refs[late_at], refs[copy_at]
        targets = [None] * len(items)
        for i, ref in zip(flown, flown_refs):
            targets[i] = ref
        for i, ref in zip(landing, landed):
            targets[i] = ref
        moves = Moves(sizes, kinds, sources, targets, refs[sems_at])
        number_of = iter(range(copies))
        copy = lambda a, b: pltpu.make_async_copy(a, b, copy_sem.at[next(number_of)])
        loads = [copy(a, b) for a, b in zip(given, loaded)]
        stores = [copy(a, b) for a, b in zip(held, results)]
        late_loads = [copy(targets[i], b) for i, b in zip(late, lates)]
        split = len([o for o in before.operands if not isinstance(o, Made)]) if before else 0
        first = len(before.shapes) if before else 0
        for load in loads:
            load.start()
        if cover:
            cover.begin(work_refs, refs[cover_at])
        moves.barrier()
        moves.start(prompt)
        if before:
            for load in loads[:split]:
                load.wait()
            before.body(*loaded[:split], *held[:first], *refs[stage_at[0]], *refs[shared_at])
            for store in stores[:first]:
                store.start()
        if cover:
            cover.run(work_refs, made_refs, refs[cover_at])
        moves.relay(prompt, (0,))
        moves.start(delayed)
        if after:
            moves.relay(needed, later)
            moves.finish(needed)
        moves.relay(delayed, (0,))
        if after:
            for load in late_loads:
                load.start()
            for load in loads[split:]:
                load.wait()
            for load in late_loads:
                load.wait()
            plain = iter(loaded[split:])
            values = []
            for operand in after.operands:
                if isinstance(operand, Made):
                    values.append(held[operand.index])
                elif isinstance(operand, Got) and operand.index in landing:
                    values.append(landed[landing.index(operand.index)])
                elif isinstance(operand, Got):
                    values.append(lates[late.index(operand.index)])
                else:
                    values.append(next(plain))
            after.body(*values, *held[first:], *refs[stage_at[-1]], *refs[shared_at])
            for store in stores[first:]:
                store.start()
        moves.relay(others, later)
        moves.finish(others)
        if cover:
            cover.end(made_refs, refs[cover_at])
        for store in stores:
            store.wait()

    shape = lambda s: jax.ShapeDtypeStruct(tuple(s[0]), s[1])
    return pl.pallas_call(
        body,
        out_shape=tuple(shape(s) for s in outs + made_shapes) + tuple(moved[i] for i in flown),
        in_specs=[HBM] * (len(operands) + len(work) + len(items)),
        out_specs=(HBM,) * (len(outs) + len(made_shapes) + len(flown)),
        scratch_shapes=scratch,
        compiler_params=pltpu.CompilerParams(collective_id=number, has_side_effects=True),
        name=name,
    )(*operands, *work, *[item[1] for item in items])


def dot(a, b, left=1, right=0, precision=None):
    return lax.dot_general(
        a,
        b,
        (((left,), (right,)), ((), ())),
        preferred_element_type=jnp.float32,
        precision=precision,
    )


def widened(source, target):
    size = target.shape[0] // 4

    def piece(i, carry):
        at = pl.ds(pl.multiple_of(i * size, size), size)
        target[at, :] = source[at, :].astype(target.dtype)
        return carry

    lax.fori_loop(0, 4, piece, 0)


def cleared(target):
    size = target.shape[0] // 8

    def piece(i, carry):
        at = pl.ds(pl.multiple_of(i * size, size), size)
        target[at, :] = jnp.zeros((size, target.shape[1]), target.dtype)
        return carry

    lax.fori_loop(0, 8, piece, 0)


def lanes_of(shape):
    return lax.broadcasted_iota(jnp.int32, shape, len(shape) - 1)


def flipped(values):
    lanes = lanes_of(values.shape)
    ahead = pltpu.roll(values, LANES - TURN, 1)
    behind = pltpu.roll(values, TURN, 1)
    return jnp.where(lanes % (2 * TURN) < TURN, ahead, behind)


def beside(blocks_ref):
    return jnp.concatenate([blocks_ref[i] for i in range(blocks_ref.shape[0])], axis=1)


def gain_row(gains_ref):
    return beside(gains_ref).astype(jnp.float32)


def added(blocks):
    def more(i, total):
        return total + blocks[i].astype(jnp.float32)

    return lax.fori_loop(1, blocks.shape[0], more, blocks[0].astype(jnp.float32))


def own_rows(count):
    me = lax.axis_index("row") * lax.axis_size("col") + lax.axis_index("col")
    return pl.ds(pl.multiple_of(me * count, count), count)


def column(row):
    return jnp.broadcast_to(row, (8, row.shape[1])).T[:, 0:1]


def tables_body(cosine, sine):
    step = 64
    lanes = lanes_of((step, LANES))
    power = (lanes % TURN).astype(jnp.float32) * (-math.log(ROPE_BASE) / TURN)
    frequencies = jnp.exp(power)
    base = lax.axis_index("dp") * cosine.shape[0]

    def piece(i, carry):
        at = pl.ds(pl.multiple_of(i * step, step), step)
        positions = base + i * step + lax.broadcasted_iota(jnp.int32, lanes.shape, 0)
        angles = positions.astype(jnp.float32) * frequencies
        cosine[at, :] = jnp.cos(angles)
        value = jnp.sin(angles)
        sine[at, :] = jnp.where(lanes % (2 * TURN) < TURN, -value, value)
        return carry

    lax.fori_loop(0, cosine.shape[0] // step, piece, 0)


def turned(source, target):
    def block(i, carry):
        scaled = RESIDUAL_SCALE * source[i].astype(jnp.float32)
        target[i] = scaled.T.astype(jnp.bfloat16)
        return carry

    lax.fori_loop(0, target.shape[0], block, 0)


def project_body(blocks, gains, w_query, w_pair, cosine, sine, normed, query, pair, own):
    gain = gain_row(gains)
    step = 128

    def piece(i, carry):
        at = pl.ds(pl.multiple_of(i * step, step), step)
        parts = [blocks[k, at, :] for k in range(blocks.shape[0])]
        tokens = jnp.concatenate(parts, axis=1).astype(jnp.float32)
        scale = lax.rsqrt(jnp.mean(tokens * tokens, axis=1, keepdims=True) + EPSILON)
        normed[at, :] = (tokens * scale * gain).astype(jnp.bfloat16)
        return carry

    lax.fori_loop(0, normed.shape[0] // step, piece, 0)
    raw = dot(normed[...], w_query[...])
    query[...] = (raw * cosine[...] + flipped(raw) * sine[...]).astype(jnp.bfloat16)
    raw = dot(normed[...], w_pair[...])
    keys = lanes_of(raw.shape) < LANES // 2
    turned = raw * cosine[...] + flipped(raw) * sine[...]
    pair[...] = jnp.where(keys, turned, raw).astype(jnp.bfloat16)
    for i in range(blocks.shape[0]):
        own[:, i * LANES : (i + 1) * LANES] = blocks[i, own_rows(own.shape[0]), :]


def doubled(pair, keys_ref, values_ref, at, distance=0):
    wide = pair.astype(jnp.float32)
    if distance:
        wide = jnp.where(lax.axis_index("dp") >= distance, wide, 0.0)
    other = pltpu.roll(wide, LANES // 2, 1)
    keys = lanes_of(wide.shape) < LANES // 2
    keys_ref[at] = jnp.where(keys, wide, other).astype(jnp.bfloat16)
    values_ref[at] = jnp.where(keys, other, wide).astype(jnp.bfloat16)


def per_head(values):
    first = lanes_of(values.shape) < LANES // 2
    zero = jnp.zeros_like(values)
    return jnp.concatenate(
        [jnp.where(first, values, zero), jnp.where(first, zero, values)], axis=0
    )


def tile_scores(queries, keys_ref, starts, row, block, last, tokens):
    scores = dot(queries, keys_ref[block], 1, 1) * SCORE_SCALE
    at = lanes_of(scores.shape) + block * tokens
    allowed = at >= starts
    if block == last:
        place = row + lax.broadcasted_iota(jnp.int32, scores.shape, 0)
        allowed = allowed & (at <= place + block * tokens)
    return jnp.where(allowed, scores, MASKED)


def doc_row(docs):
    rows = [docs[i : i + 1, :] for i in range(docs.shape[0])]
    return jnp.concatenate(rows, axis=1).astype(jnp.float32)


def attend_tiles(tokens, tile):
    step = 256

    def body(i, carry):
        rows = pl.ds(pl.multiple_of(i * step, step), step)
        tile(rows, lax.rem(i * step, tokens), step)
        return carry

    lax.fori_loop(0, 2 * tokens // step, body, 0)


def attend_first_body(near_grads, far_grads, query, pair, docs, far_docs, own_grad, near_turned, far_turned, start, keys, values, queries, out, tops, totals):
    turned(near_grads, near_turned)
    turned(far_grads, far_turned)
    for i in range(near_grads.shape[0]):
        own_grad[:, i * LANES : (i + 1) * LANES] = near_grads[i, own_rows(own_grad.shape[0]), :]
    tokens = query.shape[0]
    last = keys.shape[0] - 1
    layer = lax.axis_index("dp")
    here = doc_row(docs[...])
    mine = column(here)
    before = jnp.sum((here < mine).astype(jnp.float32), axis=1, keepdims=True)
    for d in range(1, last + 1):
        fewer = (doc_row(far_docs[d - 1]) < mine) | (layer < d)
        before = before + jnp.sum(fewer.astype(jnp.float32), axis=1, keepdims=True)
    start[...] = before.astype(jnp.int32)
    doubled(pair[...], keys, values, last)
    queries[...] = per_head(query[...].astype(jnp.float32)).astype(jnp.bfloat16)

    def tile(rows, row, step):
        starts = start[pl.ds(pl.multiple_of(row, step), step), :]
        scores = tile_scores(queries[rows, :], keys, starts, row, last, last, tokens)
        top = jnp.max(scores, axis=1, keepdims=True)
        terms = jnp.exp(scores - top)
        tops[rows, :] = top
        totals[rows, :] = jnp.sum(terms, axis=1, keepdims=True)
        out[rows, :] = dot(terms.astype(jnp.bfloat16), values[last])

    attend_tiles(tokens, tile)


def attend_rest_body(far, start, mixed, log_total, keys, values, queries, out, tops, totals):
    last, tokens = far.shape[0], far.shape[1]
    for d in range(1, last + 1):
        doubled(far[d - 1], keys, values, last - d, d)

    def tile(rows, row, step):
        starts = start[pl.ds(pl.multiple_of(row, step), step), :]
        parts = [
            tile_scores(queries[rows, :], keys, starts, row, block, last, tokens)
            for block in range(last)
        ]
        top = functools.reduce(
            jnp.maximum, [jnp.max(part, axis=1, keepdims=True) for part in parts], tops[rows, :]
        )
        parts = [jnp.exp(part - top) for part in parts]
        scale = jnp.exp(tops[rows, :] - top)
        total = functools.reduce(
            jnp.add,
            [jnp.sum(p, axis=1, keepdims=True) for p in parts],
            totals[rows, :] * scale,
        )
        sums = [
            dot(part.astype(jnp.bfloat16), values[block]) for block, part in enumerate(parts)
        ]
        out[rows, :] = functools.reduce(jnp.add, sums, out[rows, :] * scale) / total
        log_total[rows, :] = top + jnp.log(total)

    attend_tiles(tokens, tile)
    first = lanes_of((tokens, LANES)) < LANES // 2
    mixed[...] = jnp.where(first, out[:tokens, :], out[tokens:, :]).astype(jnp.bfloat16)


def attend_again_body(query, pair, far, start, log_total, queries, keys, values, queries_turned, chances):
    tokens = query.shape[0]
    last = far.shape[0]
    doubled(pair[...], keys, values, last)
    for d in range(1, last + 1):
        doubled(far[d - 1], keys, values, last - d, d)
    stacked = per_head(query[...].astype(jnp.float32))
    queries[...] = stacked.astype(jnp.bfloat16)
    queries_turned[...] = stacked.T.astype(jnp.bfloat16)

    def tile(rows, row, step):
        starts = start[pl.ds(pl.multiple_of(row, step), step), :]
        for block in range(last + 1):
            scores = tile_scores(queries[rows, :], keys, starts, row, block, last, tokens)
            chances[block, rows, :] = jnp.exp(scores - log_total[rows, :])

    attend_tiles(tokens, tile)


def attend_back_body(grad, w_output, mixed, cosine, sine, query_grad, pair_grad, far_grad, output_grad, grads, grads_turned, turned, key_sums, value_sums, keys, values, queries_turned, chances):
    tokens = mixed.shape[0]
    last = keys.shape[0] - 1
    given_grad = grad[...].reshape(tokens, -1)
    stacked = per_head(dot(given_grad, w_output[...], 1, 1))
    grads[...] = stacked.astype(jnp.bfloat16)
    grads_turned[...] = stacked.T.astype(jnp.bfloat16)
    output_sum = dot(mixed[...], given_grad, 0, 0).astype(jnp.bfloat16)
    for i in range(output_grad.shape[0]):
        output_grad[i] = output_sum[:, i * LANES : (i + 1) * LANES]
    for block in range(last + 1):
        cleared(key_sums.at[block])
        cleared(value_sums.at[block])

    def tile(rows, row, step):
        given = grads[rows, :]
        asked_turned, given_turned = queries_turned[:, rows], grads_turned[:, rows]
        products = [dot(given, values[block], 1, 1) for block in range(last + 1)]
        delta = functools.reduce(
            jnp.add,
            [
                jnp.sum(chances[block, rows, :] * product, axis=1, keepdims=True)
                for block, product in enumerate(products)
            ],
        )
        total = jnp.zeros((step, LANES), jnp.float32)
        for block in range(last + 1):
            chance = chances[block, rows, :]
            back = (chance * (products[block] - delta)).astype(jnp.bfloat16)
            total = total + dot(back, keys[block])
            key_sums[block] += dot(asked_turned, back)
            value_sums[block] += dot(given_turned, chance.astype(jnp.bfloat16))
        turned[rows, :] = total

    attend_tiles(tokens, tile)
    first = lanes_of((tokens, LANES)) < LANES // 2
    raw = jnp.where(first, turned[:tokens, :], turned[tokens:, :]) * SCORE_SCALE
    query_grad[...] = (raw * cosine[...] - flipped(raw) * sine[...]).astype(jnp.bfloat16)

    def joined(block):
        by_key, by_value = key_sums[block].T, value_sums[block].T
        by_key = (by_key + pltpu.roll(by_key, LANES // 2, 1)) * SCORE_SCALE
        by_value = by_value + pltpu.roll(by_value, LANES // 2, 1)
        return jnp.where(first, by_key, by_value)

    pair_grad[...] = joined(last)
    for d in range(1, last + 1):
        far_grad[d - 1] = joined(last - d).astype(jnp.bfloat16)


def router_rows(router):
    rows = beside(router)
    blank = jnp.zeros((LANES - rows.shape[0], rows.shape[1]), rows.dtype)
    return jnp.concatenate([rows, blank], axis=0)


def full_dot(wide, low, left=1, right=0):
    parts, rest = [], wide
    for _ in range(3):
        parts.append(rest.astype(jnp.bfloat16))
        rest = rest - parts[-1].astype(jnp.float32)
    count = wide.shape[0]
    sums = dot(jnp.concatenate(parts, axis=0), low, left, right)
    return sums[:count] + (sums[count : 2 * count] + sums[2 * count :])


def middle_body(mixed, own, w_output, gains, router, ids_turned, rows, middle, weights, ids_ref):
    experts = router.shape[1]
    width = own.shape[1]
    attn = dot(beside(mixed), w_output[...])
    value = own[...].astype(jnp.float32) + RESIDUAL_SCALE * attn
    middle[...] = value
    scale = lax.rsqrt(jnp.mean(value * value, axis=1, keepdims=True) + EPSILON)
    normed = value * scale * gain_row(gains)
    logits = full_dot(normed, router_rows(router), 1, 1)
    count = own.shape[0]
    ids_ref[...] = ids_turned[...].astype(jnp.float32).T
    ids = ids_ref[own_rows(count), :]
    lanes = lanes_of((count, LANES))
    chosen = jnp.zeros((count, LANES), jnp.float32)
    for k in range(ids.shape[1]):
        chosen = chosen + (ids[:, k : k + 1] == lanes.astype(jnp.float32)).astype(
            jnp.float32
        )
    top = jnp.max(jnp.where(lanes < experts, logits, MASKED), axis=1, keepdims=True)
    terms = jnp.exp(jnp.minimum(logits - top, 0.0)) * chosen
    share = terms / jnp.sum(terms, axis=1, keepdims=True)
    weights[...] = share
    high = share.astype(jnp.bfloat16)
    low = share - high.astype(jnp.float32)
    rows[:, :width] = normed.astype(jnp.bfloat16)
    rows[:, width:] = (high.astype(jnp.float32) + pltpu.roll(low, LANES // 2, 1)).astype(
        jnp.bfloat16
    )


def middle_back_body(back, out_grad, middle, weights, gains, router, middle_grad, attn_grad, logit_grad, gain_part):
    width = middle.shape[1]
    normed_grad = back[0, :, :width].astype(jnp.float32)
    weight_grad = back[0, :, width:].astype(jnp.float32)
    for i in range(1, back.shape[0]):
        normed_grad = normed_grad + back[i, :, :width].astype(jnp.float32)
        weight_grad = weight_grad + back[i, :, width:].astype(jnp.float32)
    share, value = weights[...], middle[...]
    mean = jnp.sum(share * weight_grad, axis=1, keepdims=True)
    logit = share * (weight_grad - mean)
    logit_grad[...] = logit.astype(jnp.bfloat16)
    normed_grad = normed_grad + full_dot(logit, router_rows(router))
    scale = lax.rsqrt(jnp.mean(value * value, axis=1, keepdims=True) + EPSILON)
    gain_part[...] = jnp.sum(normed_grad * value * scale, axis=0, keepdims=True)
    scaled = normed_grad * gain_row(gains)
    norm_dot = jnp.sum(scaled * value, axis=1, keepdims=True)
    total = (
        out_grad[...].astype(jnp.float32)
        + scale * scaled
        - value * (scale * scale * scale * norm_dot / width)
    )
    middle_grad[...] = total
    attn_grad[...] = (RESIDUAL_SCALE * total).astype(jnp.bfloat16)


def project_back_body(query_grad, pair_grad, returned, normed, w_query, w_pair, cosine, sine, output_turned, logit, rows, gains, gain_moe, partial, sums, output_first, output_last, gain_parts):
    layer = lax.axis_index("dp")
    depth = lax.axis_size("dp")
    total = pair_grad[...]
    for i in range(returned.shape[0]):
        total = total + jnp.where(
            layer + i + 1 < depth, returned[i].astype(jnp.float32), 0.0
        )
    keys = lanes_of(total.shape) < LANES // 2
    turned = total * cosine[...] - flipped(total) * sine[...]
    pair_low = jnp.where(keys, turned, total).astype(jnp.bfloat16)
    query_low = query_grad[...]
    whole = dot(query_low, w_query[...], 1, 1) + dot(pair_low, w_pair[...], 1, 1)
    partial[...] = whole.astype(jnp.bfloat16)
    gain_attn = jnp.sum(whole * normed[...].astype(jnp.float32), axis=0, keepdims=True)
    gain_attn = gain_attn / gain_row(gains)
    gain_parts[...] = jnp.zeros_like(gain_parts)
    for i in range(gain_parts.shape[0]):
        at = slice(i * LANES, (i + 1) * LANES)
        gain_parts[i, 0:1, :] = gain_attn[:, at]
        gain_parts[i, 1:2, :] = gain_moe[0:1, at]
    width = normed.shape[1]
    sums[:width, :] = dot(normed[...], query_low, 0, 0).astype(jnp.bfloat16)
    sums[width : 2 * width, :] = dot(normed[...], pair_low, 0, 0).astype(jnp.bfloat16)
    output_sum = added(output_turned).astype(jnp.bfloat16)
    output_first[...] = output_sum[: output_first.shape[0], :]
    output_last[...] = output_sum[output_first.shape[0] :, :]
    mine = rows[:, own_rows(LANES)]
    named = logit[...].reshape(normed.shape[0], LANES)
    sums[2 * width : 2 * width + LANES, :] = dot(named, mine, 0, 0).astype(jnp.bfloat16)


def results_body(blocks, moe, own, middle, middle_grad, gains, gain_blocks, turned, block_out, in_grad, gain_sum, summed):
    gain_sum[...] = added(gain_blocks)
    summed[...] = added(turned).astype(jnp.bfloat16)
    width = own.shape[1]
    normed_grad = added(blocks)
    branch = added(moe)
    value = own[...].astype(jnp.float32)
    scale = lax.rsqrt(jnp.mean(value * value, axis=1, keepdims=True) + EPSILON)
    scaled = normed_grad * gain_row(gains)
    norm_dot = jnp.sum(scaled * value, axis=1, keepdims=True)
    grad = (
        middle_grad[...] + scale * scaled - value * (scale * scale * scale * norm_dot / width)
    ).astype(jnp.bfloat16)
    out = (middle[...] + RESIDUAL_SCALE * branch).astype(jnp.bfloat16)
    for i in range(block_out.shape[0]):
        at = slice(i * LANES, (i + 1) * LANES)
        block_out[i] = out[:, at]
        in_grad[i] = grad[:, at]


def expert_terms(gate_up, active_grad, weight):
    hidden = active_grad.shape[0]
    gate, up = gate_up[:hidden], gate_up[hidden:]
    sigmoid = jax.nn.sigmoid(gate)
    silu = gate * sigmoid
    ungated = silu * up
    active = (ungated * weight).astype(jnp.bfloat16)
    scaled = active_grad * weight
    gate_grad = (scaled * up * sigmoid * (1.0 + gate * (1.0 - sigmoid))).astype(jnp.bfloat16)
    up_grad = (scaled * silu).astype(jnp.bfloat16)
    return active, jnp.concatenate([gate_grad, up_grad], axis=0), active_grad * ungated


def weight_rows(extra):
    turned = extra.astype(jnp.float32).T
    return turned[: LANES // 2] + turned[LANES // 2 :]


def local_experts_body(sizes, kinds, rows_hbm, grads_hbm, in_ref, out_ref, sent_grads, sent_rows, flat_ref, in_sum, out_sum, moe_hbm, back_hbm, got_grads, got_rows, rows_ref, grads_ref, moe_ref, back_ref, moe_acc, back_acc, share, weights, spread, copy_sem, *sems):
    step, steps = pl.program_id(0), pl.num_programs(0)
    each, hidden, width = out_ref.shape
    parts = hidden // LANES
    moves = Moves(sizes, kinds, [sent_grads, sent_rows], [got_grads, got_rows], sems)
    ends = [(rows_hbm, rows_ref), (grads_hbm, grads_ref), (moe_ref, moe_hbm), (back_ref, back_hbm)]
    copy = lambda i: pltpu.make_async_copy(*ends[i], copy_sem.at[i])

    @pl.when(step == 0)
    def _():
        copy(0).start()
        copy(1).start()
        moves.barrier()
        moves.start([0])
        cleared(moe_acc)
        cleared(back_acc)
        copy(0).wait()
        copy(1).wait()
        share[...] = jnp.zeros_like(share)
        weights[...] = weight_rows(rows_ref[:, width:])

    @pl.when(step == 2 * steps // 8)
    def _():
        moves.start([1])

    for when, item, stage in ((3, 0, 0), (6, 1, 0), (7, 0, 1)):

        @pl.when(step == when * steps // 8)
        def _(item=item, stage=stage):
            moves.relay([item], (stage,))

    for i in range(each):
        spread[i] = in_ref[i].astype(jnp.float32)
        for part in range(parts):
            for half in range(2):
                at = half * hidden + part * LANES
                flat_ref[i, :, at : at + LANES] = spread[
                    i, pl.ds(part * 2 + half, width, stride=2 * parts), :
                ].astype(jnp.bfloat16)
        expert = (lax.axis_index("row") * steps + step) * each + i
        active, gate_up_grad, shares = expert_terms(
            dot(flat_ref[i], rows_ref[:, :width], 0, 1),
            dot(out_ref[i], grads_ref[...]),
            weights[pl.ds(expert, 1), :],
        )
        share[pl.ds(expert, 1), :] = jnp.sum(shares, axis=0, keepdims=True)
        moe_acc[...] += dot(active, out_ref[i], 0, 0)
        back_acc[...] += dot(gate_up_grad, flat_ref[i], 0, 1)
        in_sum[i] = dot(gate_up_grad, rows_ref[:, :width]).astype(jnp.bfloat16)
        out_sum[i] = dot(active, grads_ref[...], 1, 1).astype(jnp.bfloat16)

    @pl.when(step == steps - 1)
    def _():
        moves.relay([1], (1,))
        widened(moe_acc, moe_ref)
        copy(2).start()
        widened(back_acc, back_ref.at[:, :width])
        back_ref[:, width:] = share[...].T.astype(jnp.bfloat16)
        copy(3).start()
        moves.finish()
        copy(2).wait()
        copy(3).wait()


def local_experts(sizes, number, rows, grads, w_in, w_out, sent_grads, sent_rows):
    tokens, wide = rows.shape
    experts, hidden, width = w_out.shape
    each = 1
    low = jnp.bfloat16
    kinds, shapes, sems = planned(
        sizes,
        [
            ("gather", sent_grads, True, sent_grads.shape[0]),
            ("gather", sent_rows, True, sent_rows.shape[0]),
        ],
    )
    some = lambda s: pl.BlockSpec((each,) + s[1:], lambda e: (e,) + (0,) * (len(s) - 1))
    outs = [
        (experts, width, 2 * hidden),
        (experts, 2 * hidden, width),
        (experts, hidden, width),
        (tokens, width),
        (tokens, wide),
    ]
    return pl.pallas_call(
        functools.partial(local_experts_body, sizes, kinds),
        grid=(experts // each,),
        in_specs=[
            HBM,
            HBM,
            some(w_in.shape),
            some(w_out.shape),
            HBM,
            HBM,
        ],
        out_specs=(*[some(s) for s in outs[:3]], HBM, HBM, HBM, HBM),
        out_shape=tuple(jax.ShapeDtypeStruct(s, low) for s in outs) + tuple(shapes),
        scratch_shapes=[
            pltpu.VMEM(rows.shape, low),
            pltpu.VMEM(grads.shape, low),
            pltpu.VMEM((tokens, width), low),
            pltpu.VMEM((tokens, wide), low),
            pltpu.VMEM((tokens, width), jnp.float32),
            pltpu.VMEM((tokens, width), jnp.float32),
            pltpu.VMEM((LANES, tokens), jnp.float32),
            pltpu.VMEM((LANES // 2, tokens), jnp.float32),
            pltpu.VMEM((each,) + w_in.shape[1:], jnp.float32),
            pltpu.SemaphoreType.DMA((4,)),
        ]
        + sems,
        compiler_params=pltpu.CompilerParams(collective_id=number, has_side_effects=True),
        name="local_experts",
    )(rows, grads, w_in, w_out, sent_grads, sent_rows)


class Sums:
    def __init__(self, rows, grads, weights, turned, load_sem, *sums):
        self.rows, self.grads, self.weights = rows, grads, weights
        self.turned, self.load_sem, self.sums = turned, load_sem, sums

    def load(self, which, source):
        target = (self.rows, self.grads)[which]
        return pltpu.make_async_copy(source, target, self.load_sem.at[which])

    def ready(self):
        layers, width, tokens = self.grads.shape

        def block(i, carry):
            at = pl.ds(pl.multiple_of(i * tokens, tokens), tokens)
            self.weights[i] = weight_rows(self.rows[at, width:])
            return carry

        lax.fori_loop(0, layers, block, 0)

    def make(self, index, w_in, w_out, in_part, out_part, made, arrive):
        layers, width, tokens = self.grads.shape
        hidden = w_out.shape[0]
        arrive(0)
        if self.sums:
            arrive(1)
        later = arrive

        def part_of(at, pieces, arrive=lambda i: None if self.sums else later(i)):
            first = at * tokens if isinstance(at, int) else pl.multiple_of(at * tokens, tokens)
            block = self.rows[pl.ds(first, pieces * tokens), :width]
            gate_up = dot(w_in[...], block, 0, 1)
            arrive(1)
            weight = jnp.concatenate(
                [self.weights[at + i, pl.ds(index, 1), :] for i in range(pieces)], axis=1
            )
            active_grad = jnp.concatenate(
                [dot(w_out[...], self.grads[at + i]) for i in range(pieces)], axis=1
            )
            active, gate_up_grad, _ = expert_terms(gate_up, active_grad, weight)
            out_total = functools.reduce(
                jnp.add,
                [
                    dot(active[:, i * tokens : (i + 1) * tokens], self.grads[at + i], 1, 1)
                    for i in range(pieces)
                ],
            )
            return dot(gate_up_grad, block), out_total

        if not self.sums:
            in_total, out_total = part_of(0, layers)
        else:
            whole, out_acc = self.sums
            whole[...] = jnp.zeros_like(whole)
            out_acc[...] = jnp.zeros_like(out_acc)

            def more(i, carry):
                in_more, out_more = part_of(i, 1)
                whole[...] += in_more
                out_acc[...] += out_more
                return carry

            lax.fori_loop(0, layers, more, 0)
            in_total, out_total = whole[...], out_acc[...]
        arrive(2)
        in_total = in_total + in_part[...].astype(jnp.float32)
        parts = hidden // LANES
        for part in range(parts):
            for half in range(2):
                at = half * hidden + part * LANES
                self.turned[pl.ds(part * 2 + half, width, stride=2 * parts), :] = in_total[
                    at : at + LANES, :
                ].T
        made[...] = self.turned[...].astype(jnp.bfloat16)
        return out_total + out_part[...].astype(jnp.float32)


def sums_scratch(layers, tokens, width, hidden):
    low, full = jnp.bfloat16, jnp.float32
    return [
        pltpu.VMEM((layers * tokens, width + LANES), low),
        pltpu.VMEM((layers, width, tokens), low),
        pltpu.VMEM((layers, LANES // 2, tokens), full),
        pltpu.VMEM((width * 2 * hidden // LANES, LANES), full),
        pltpu.SemaphoreType.DMA((2,)),
    ] + [pltpu.VMEM((k * hidden, width), full) for k in (2, 1) if layers > 4]


class Cover:
    def __init__(self, first, many, work):
        w_in, w_out, in_part, out_part, rows_far, grads_far = work
        layers, width, tokens = grads_far.shape
        self.experts, hidden, _ = w_out.shape
        self.first, self.many, self.work = first, many, work
        low = jnp.bfloat16
        self.shapes = [
            ((many, width * 2 * hidden // LANES, LANES), low),
            ((many, hidden, width), low),
        ]
        self.scratch = [pltpu.VMEM((many,) + a.shape[1:], low) for a in work[:4]]
        self.scratch += [pltpu.VMEM(*s) for s in self.shapes]
        self.scratch += [pltpu.SemaphoreType.DMA((4, many)), pltpu.SemaphoreType.DMA((2, many))]
        self.scratch += sums_scratch(layers, tokens, width, hidden)

    def load(self, which, i, work, refs):
        source, sem = work[which].at[self.first + i], refs[6].at[which, i]
        return pltpu.make_async_copy(source, refs[which].at[i], sem)

    def begin(self, work, refs):
        sums = Sums(*refs[8:])
        sums.load(0, work[4]).start()
        self.load(0, 0, work, refs).start()
        sums.load(1, work[5]).start()
        for which in (1, 2, 3):
            self.load(which, 0, work, refs).start()
        for i in range(1, self.many):
            for which in range(4):
                self.load(which, i, work, refs).start()

    def stores(self, i, made, refs):
        return [
            pltpu.make_async_copy(refs[4 + k].at[i], made[k].at[i], refs[7].at[k, i])
            for k in range(2)
        ]

    def run(self, work, made, refs):
        sums = Sums(*refs[8:])

        def expert(i, carry):
            def arrive(point):
                @pl.when(i == 0)
                def _():
                    if point == 0:
                        sums.load(0, work[4]).wait()
                        sums.ready()
                    if point == 1:
                        sums.load(1, work[5]).wait()

                for which in ((0,), (1,), (2, 3))[point]:
                    self.load(which, i, work, refs).wait()

            index = lax.axis_index("row") * self.experts + self.first + i
            out_total = sums.make(index, *[refs[k].at[i] for k in range(5)], arrive)
            refs[5][i] = out_total.astype(jnp.bfloat16)
            for store in self.stores(i, made, refs):
                store.start()
            return carry

        lax.fori_loop(0, self.many, expert, 0)

    def end(self, made, refs):
        for i in range(self.many):
            for store in self.stores(i, made, refs):
                store.wait()


def outputs_body(count, total, *refs):
    pieces = total // count
    sums, smalls = refs[: 2 * pieces], refs[2 * pieces : 2 * pieces + 6]
    gin, gout, *others = refs[2 * pieces + 6 : 2 * pieces + 16]
    in_low, out_low, in_full, out_full, *refs = refs[2 * pieces + 16 :]
    held, results, (load_sem, store_sem, small_sem) = refs[:6], refs[6:14], refs[14:]
    block_out, in_grad, gain_attn, gain_moe, query, pair, output, router = results
    width = gout.shape[2]
    stored = [
        pltpu.make_async_copy(a, b, small_sem.at[6 + j])
        for j, (a, b) in enumerate(zip(results, others))
    ]
    ring = in_full.shape[0]

    def load(k, i):
        low = (in_low, out_low)[k]
        source = sums[k * pieces + i // count].at[i % count]
        return pltpu.make_async_copy(source, low.at[i], load_sem.at[k, i])

    def store(k, i):
        made, target = ((in_full, gin), (out_full, gout))[k]
        return pltpu.make_async_copy(made.at[i % ring], target.at[i], store_sem.at[k, i % ring])

    for i in range(total):
        for k in range(2):
            load(k, i).start()
        if i == 0:
            fetched = [
                pltpu.make_async_copy(a, b, small_sem.at[j])
                for j, (a, b) in enumerate(zip(smalls, held))
            ]
            for copy in fetched:
                copy.start()
    def small():
        for copy in fetched:
            copy.wait()
        blocks, in_blocks, gains, summed, output_first, output_last = held
        for i in range(blocks.shape[0]):
            at = pl.ds(i * blocks.shape[1], blocks.shape[1])
            block_out[at, :] = blocks[i]
            in_grad[at, :] = in_blocks[i]
        gain_sum = jnp.sum(gains[...], axis=0)
        gain_attn[...] = gain_sum[0:1, :]
        gain_moe[...] = gain_sum[1:2, :]
        query[...] = summed[:width, :].astype(jnp.float32)
        pair[...] = summed[width : 2 * width, :].astype(jnp.float32)
        router[...] = summed[2 * width : 2 * width + router.shape[0], :].astype(jnp.float32)
        half = output_first.shape[1]
        for i in range(width // half):
            from_first = i % 2 == 0
            rows = (output_first if from_first else output_last)[i // 2].astype(jnp.float32)
            for j in range(max(1, half // LANES)):
                place = i * half + j * LANES
                at = place // LANES
                part = rows[j * LANES : (j + 1) * LANES, :]
                first = place % LANES
                output[first : first + part.shape[0], at * LANES : (at + 1) * LANES] = part

    for i in range(total):
        for k in range(2):
            load(k, i).wait()
            if i >= ring:
                store(k, i - ring).wait()
        for low, made in ((in_low, in_full), (out_low, out_full)):
            widened(low.at[i], made.at[i % ring])
        for k in range(2):
            store(k, i).start()
        if i == total - 3:
            small()
            for copy in stored:
                copy.start()
    for i in range(total - ring, total):
        for k in range(2):
            store(k, i).wait()
    for copy in stored:
        copy.wait()


def outputs(in_sums, out_sums, hidden, experts, *smalls):
    count = in_sums[0].shape[0]
    total = count * len(in_sums)
    width = out_sums[0].shape[2]
    parts = hidden // LANES
    lanes = smalls[0].shape[2]
    tokens = smalls[0].shape[0] * smalls[0].shape[1]
    low, full = jnp.bfloat16, jnp.float32
    large = [(width * 2 * parts, LANES), (hidden, width)]
    shapes = [((total,) + s, full) for s in large] + [
        ((tokens, lanes), low),
        ((tokens, lanes), low),
        ((1, LANES), full),
        ((1, LANES), full),
        ((width, LANES), full),
        ((width, LANES), full),
        ((LANES, width), full),
        ((experts, LANES), full),
    ]
    ring = min(4, total)
    gin, *others = pl.pallas_call(
        functools.partial(outputs_body, count, total),
        in_specs=[HBM] * (2 * len(in_sums) + len(smalls)),
        out_specs=(HBM,) * len(shapes),
        out_shape=tuple(jax.ShapeDtypeStruct(*shape) for shape in shapes),
        scratch_shapes=[pltpu.VMEM((total,) + s, low) for s in large]
        + [pltpu.VMEM((ring,) + s, full) for s in large]
        + [pltpu.VMEM(a.shape, a.dtype) for a in smalls]
        + [pltpu.VMEM(*shape) for shape in shapes[2:]]
        + [pltpu.SemaphoreType.DMA(s) for s in ((2, total), (2, ring), (14,))],
        name="outputs",
    )(*in_sums, *out_sums, *smalls)
    gin = gin.reshape(total, width, parts, 2, LANES).transpose(0, 1, 3, 2, 4)
    return gin.reshape(total, width, 2, hidden), *others


def local(
    sizes,
    tokens,
    out_grad,
    doc_ids,
    expert_ids,
    gain_attn,
    w_query,
    w_key_value,
    w_output,
    gain_moe,
    w_router,
    w_expert_in,
    w_expert_out,
):
    rows, cols, depth = sizes
    group = rows * cols
    tok_rows, feat_local = tokens.shape
    width = w_query.shape[0]
    experts = w_router.shape[1]
    expert_local, hidden = w_expert_out.shape[0], w_expert_out.shape[1]
    longest_doc = min(LONGEST, tok_rows * depth // 2)
    hop_count = longest_doc // tok_rows
    own = tok_rows // group
    low, full = jnp.bfloat16, jnp.float32
    layer = lax.axis_index("dp")
    me = lax.axis_index("row") * cols + lax.axis_index("col")
    everyone = list(range(1, depth))
    hops = list(range(1, hop_count + 1))

    w_pair = w_key_value.reshape(width, -1)
    block = (tok_rows, LANES)
    cosine, sine, normed, query, pair, tokens_own, gains, gains_moe, router, docs_far, grads_shifted, grad_blocks = exchange(
        sizes,
        "gather_tokens",
        0,
        ("gather", tokens, False, 2),
        ("share", gain_attn.reshape(1, LANES)),
        ("share", gain_moe.reshape(1, LANES)),
        ("share", w_router.T),
        ("shift", doc_ids.reshape(-1, LANES), everyone, False),
        ("shift", out_grad, everyone, False),
        ("gather", out_grad, False, 2),
        before=Stage(tables_body, [(block, full), (block, full)]),
        after=Stage(
            project_body,
            [((tok_rows, width), low), (block, low), (block, low), ((own, width), low)],
            Got(0),
            Got(1),
            w_query,
            w_pair,
            Made(0),
            Made(1),
        ),
        landing=(0,),
        delayed=(6,),
    )

    stack = (hop_count + 1,) + block
    twice = (2 * tok_rows, LANES)
    turned_block = (LANES, tok_rows)
    whole = (2 * tok_rows, 1)
    grad_own, grads_near, far_turned, start, mixed, log_total, far, output_blocks = exchange(
        sizes,
        "shift_pairs",
        1,
        ("line", pair, False, 2, hop_count),
        ("gather", w_output, False, 4),
        before=Stage(
            attend_first_body,
            [
                ((own, width), low),
                ((group,) + turned_block, low),
                ((depth - 1,) + turned_block, low),
                ((tok_rows, 1), jnp.int32),
            ],
            grad_blocks,
            grads_shifted,
            query,
            pair,
            doc_ids.reshape(-1, LANES),
            docs_far,
        ),
        after=Stage(
            attend_rest_body,
            [(block, low), (whole, full)],
            Got(0),
            Made(3),
        ),
        shared=[
            pltpu.VMEM(stack, low),
            pltpu.VMEM(stack, low),
            pltpu.VMEM(twice, low),
            pltpu.VMEM(twice, full),
            pltpu.VMEM(whole, full),
            pltpu.VMEM(whole, full),
        ],
    )
    output_full = output_blocks.reshape(-1, width)

    rows_own, middle, weights = exchange(
        sizes,
        "swap_mixed",
        2,
        ("swap", mixed.reshape(group, own, LANES)),
        after=Stage(
            middle_body,
            [((own, width + LANES), low), ((own, width), full), ((own, LANES), full)],
            Got(0),
            tokens_own,
            output_full,
            gains_moe,
            router,
            expert_ids.T,
            scratch=[pltpu.VMEM(expert_ids.shape, full)],
        ),
        landing=(0,),
    )
    rows_blocks, rows_shifted = exchange(
        sizes,
        "gather_rows",
        3,
        ("gather", rows_own, False, 2),
        ("line", rows_own, False, 4),
    )
    rows_near = rows_blocks.reshape(tok_rows, -1)
    parts = hidden // LANES
    in_rows = w_expert_in.reshape(expert_local, width, 2, parts, LANES)
    in_rows = in_rows.transpose(0, 1, 3, 2, 4).reshape(expert_local, -1, LANES)
    in_flat, in_part, out_part, moe_partial, back_partial, grads_far, rows_far = local_experts(
        sizes,
        9,
        rows_near,
        grads_near.reshape(width, tok_rows),
        in_rows,
        w_expert_out,
        far_turned,
        rows_shifted,
    )
    rows_far = rows_far.reshape((depth - 1) * tok_rows, -1)
    grads_far = grads_far.reshape(depth - 1, width, tok_rows)
    work = (in_flat, w_expert_out, in_part, out_part, rows_far, grads_far)
    share = expert_local // 4
    unit = 16 * depth
    in_sums, out_sums = [], []

    def beneath(name, number, *items, after=None, landing=()):
        cover = Cover(len(in_sums) * share, share, work)
        in_sum, out_sum, *moved = exchange(
            sizes, name, number, *items, after=after, cover=cover, landing=landing
        )
        if after:
            count = len(after.shapes)
            results = [in_sum, out_sum, *moved]
            in_sum, out_sum = results[count], results[count + 1]
            moved = results[:count] + results[count + 2 :]
        in_sums.append(in_sum)
        out_sums.append(out_sum)
        return moved

    middle_grad, attn_grad, logit_grad, gain_moe_part = beneath(
        "swap_back",
        4,
        ("swap", back_partial.reshape(group, own, -1)),
        after=Stage(
            middle_back_body,
            [
                ((own, width), full),
                ((own, width), low),
                ((own, LANES), low),
                ((1, width), full),
            ],
            Got(0),
            grad_own,
            middle,
            weights,
            gains_moe,
            router,
        ),
        landing=(0,),
    )
    query_grad, pair_grad, far_grad, output_sum, logit_blocks = exchange(
        sizes,
        "gather_attn_grad",
        5,
        ("gather", attn_grad, False, 2),
        ("gather", logit_grad),
        delayed=(1,),
        before=Stage(
            attend_again_body,
            [],
            query,
            pair,
            far,
            start,
            log_total,
            scratch=[pltpu.VMEM(twice, low)],
        ),
        after=Stage(
            attend_back_body,
            [
                (block, low),
                (block, full),
                ((hop_count,) + block, low),
                ((group, LANES, LANES), low),
            ],
            Got(0),
            w_output,
            mixed,
            cosine,
            sine,
            scratch=[
                pltpu.VMEM(twice, low),
                pltpu.VMEM(twice[::-1], low),
                pltpu.VMEM(twice, full),
                pltpu.VMEM((hop_count + 1,) + turned_block, full),
                pltpu.VMEM((hop_count + 1,) + turned_block, full),
            ],
        ),
        landing=(0,),
        shared=[
            pltpu.VMEM(stack, low),
            pltpu.VMEM(stack, low),
            pltpu.VMEM(twice[::-1], low),
            pltpu.VMEM((hop_count + 1, 2 * tok_rows, tok_rows), full),
        ],
    )
    length = (2 * width + LANES + unit - 1) // unit * unit
    partial, sums, output_first, output_last, gain_parts, moe_blocks = beneath(
        "shift_grads",
        6,
        ("shift", far_grad, [-d for d in hops], True),
        ("swap", moe_partial.reshape(group, own, width)),
        ("turn", output_sum.reshape(depth, width // depth, LANES)),
        after=Stage(
            project_back_body,
            [
                ((tok_rows, width), low),
                ((length, LANES), low),
                ((width // depth // 2, LANES), low),
                ((width // depth // 2, LANES), low),
                ((group, 8, LANES), full),
            ],
            query_grad,
            pair_grad,
            Got(0),
            normed,
            w_query,
            w_pair,
            cosine,
            sine,
            Got(2),
            logit_blocks,
            rows_near,
            gains,
            gain_moe_part,
        ),
        landing=(0, 2),
    )
    pieces = (group, own, LANES)
    block_out, in_grad, gain_sum, summed, output_first = beneath(
        "swap_partial",
        7,
        ("swap", partial.reshape(group, own, width)),
        ("turn", sums.reshape(depth, length // depth, LANES)),
        ("swap", gain_parts),
        ("collect", output_first),
        after=Stage(
            results_body,
            [(pieces, low), (pieces, low), ((8, LANES), full), ((length // depth, LANES), low)],
            Got(0),
            moe_blocks,
            tokens_own,
            middle,
            middle_grad,
            gains,
            Got(2),
            Got(1),
        ),
        landing=(0, 1, 2),
    )
    block_out, in_grad, sums, output_last, gain_all = beneath(
        "swap_results",
        8,
        ("swap", block_out),
        ("swap", in_grad),
        ("collect", summed),
        ("collect", output_last),
        ("collect", gain_sum),
    )
    grad_in, grad_out, block_out, in_grad, gain_attn_sum, gain_moe_sum, query_sum, pair_sum, output_sum, router_sum = outputs(
        in_sums,
        out_sums,
        hidden,
        experts,
        block_out,
        in_grad,
        gain_all,
        sums.reshape(length, LANES),
        output_first,
        output_last,
    )
    return (
        block_out,
        in_grad,
        gain_attn_sum.reshape(LANES),
        query_sum,
        pair_sum.reshape(w_key_value.shape),
        output_sum,
        gain_moe_sum.reshape(LANES),
        router_sum.T,
        grad_in,
        grad_out,
    )


def solution(mesh):
    in_specs = (
        P("dp", ("row", "col")),
        P("dp", ("row", "col")),
        P("dp"),
        P("dp", None),
        P(("row", "col")),
        P(None, ("row", "col")),
        P(None, ("row", "col"), None),
        P(("row", "col"), None),
        P(("row", "col")),
        P(("row", "col"), None),
        P("row", None, None, "col"),
        P("row", "col", None),
    )
    out_specs = (
        P("dp", ("row", "col")),
        P("dp", ("row", "col")),
        P(("row", "col")),
        P(None, ("row", "col")),
        P(None, ("row", "col"), None),
        P(("row", "col"), None),
        P(("row", "col")),
        P(("row", "col"), None),
        P("row", None, None, "col"),
        P("row", "col", None),
    )
    sizes = (mesh.shape["row"], mesh.shape["col"], mesh.shape["dp"])
    return jax.shard_map(
        functools.partial(local, sizes),
        mesh=mesh,
        in_specs=in_specs,
        out_specs=out_specs,
        check_vma=False,
    )
```

```python
import functools
import itertools
import math

import jax
import jax.numpy as jnp
from jax import lax
from jax.experimental import pallas as pl
from jax.experimental.pallas import tpu as pltpu
from jax.sharding import PartitionSpec as P

LONGEST = 4096
EPSILON = 1e-05
RESIDUAL_SCALE = 0.22
SCORE_SCALE = 0.015625
ROPE_BASE = 10000.0
MASKED = -1e30
MESH = pl.DeviceIdType.MESH
GROUP = ("row", "col")
EVERY = ("dp", "row", "col")
LANES = 128
HBM = pl.BlockSpec(memory_space=pl.ANY)
TURN = LANES // 4


class Moves:
    def __init__(self, sizes, kinds, sources, targets, sems):
        self.sizes, self.kinds = sizes, kinds
        self.sources, self.targets = sources, targets
        self.send_sem, self.recv_sem, self.local_sem = sems

    def place(self):
        row, col, layer = lax.axis_index("row"), lax.axis_index("col"), lax.axis_index("dp")
        return row, col, layer, row * self.sizes[1] + col

    def member(self, index):
        rows, cols, depth = self.sizes
        return {"row": index // cols, "col": lax.rem(index, cols)}

    def across(self, row):
        low = lax.rem(row, 2)
        return row + 1 - 2 * low, lax.rem(row + 2, 4), lax.rem(row + 3 - 2 * low, 4)

    def barrier(self):
        rows, cols, depth = self.sizes
        row, col, layer, me = self.place()
        group = rows * cols
        names = [kind[0] for kind in self.kinds]
        barrier = pltpu.get_barrier_semaphore()
        partners = []
        if "swap" in names or "share" in names:
            for k in range(1, group):
                partners.append(self.member(lax.rem(me + k, group)))
        elif "gather" in names:
            for other in self.across(row)[:2]:
                partners.append({"row": other})
            for k in range(1, cols):
                partners.append({"col": lax.rem(col + k, cols)})
        shifts = set()
        for kind in self.kinds:
            if kind[0] == "shift":
                for d in kind[1]:
                    shifts |= {d % depth, -d % depth}
            elif kind[0] in ("turn", "collect"):
                shifts |= set(range(1, depth))
        for k in sorted(shifts - {0}):
            partners.append({"dp": lax.rem(layer + k, depth)})
        ends = [(layer > 0, layer - 1), (layer < depth - 1, layer + 1)]
        ends = ends if "line" in names and not shifts else []
        for partner in partners:
            pl.semaphore_signal(barrier, inc=1, device_id=partner, device_id_type=MESH)
        for there, other in ends:

            @pl.when(there)
            def _(device={"dp": other}):
                pl.semaphore_signal(barrier, inc=1, device_id=device, device_id_type=MESH)

        expected = len(partners)
        for there, _ in ends:
            expected = expected + there.astype(jnp.int32)
        pl.semaphore_wait(barrier, expected)

    def plan(self, only):
        rows, cols, depth = self.sizes
        row, col, layer, me = self.place()
        group = rows * cols
        slots = iter(range(self.send_sem.shape[0]))
        starts, relays, sends, arrivals, local = [], [], [], [], []

        def remote(source, target, device, slot=None):
            slot = next(slots) if slot is None else slot
            return functools.partial(
                pltpu.make_async_remote_copy,
                src_ref=source,
                dst_ref=target,
                send_sem=self.send_sem.at[slot],
                recv_sem=self.recv_sem.at[slot],
                device_id=device,
                device_id_type=MESH,
            )

        for index, (kind, source, target) in enumerate(
            zip(self.kinds, self.sources, self.targets)
        ):
            item = [], [], [], [], []
            begin, follow, sent, got, stay = item

            def keep(source, target):
                sem = self.local_sem.at[index]
                stay.append(functools.partial(pltpu.make_async_copy, source, target, sem))

            def direct(source, target, device):
                copy = None, remote(source, target, device)
                begin.append(copy)
                sent.append(copy)
                got.append(copy)

            if kind[0] == "gather":
                second, parts = kind[1:]
                size = source.shape[0] // parts
                beside, above, away = self.across(row)

                def at(other, part, piece=None):
                    member = other * cols + col
                    first, length, deep = part * size, size, ()
                    if piece is not None and size % 2 == 0:
                        length = size // 2
                        first = first + piece * length
                    elif piece is not None:
                        inner = source.shape[1] // 2
                        deep = (pl.ds(piece * inner, inner),)
                    some = pl.ds(first, length)
                    return target.at[(some, member) + deep if second else (member, some) + deep]

                def to_mates(piece):
                    made = []
                    for j in range(1, cols):
                        copy = None, remote(piece, piece, {"col": lax.rem(col + j, cols)})
                        made.append(copy)
                        sent.append(copy)
                        got.append(copy)
                    return made

                for part in range(parts):
                    some = source.at[pl.ds(part * size, size)]
                    ways = []
                    for near, other, piece in ((beside, above, 0), (above, beside, 1)):
                        first = None, remote(some, at(row, part), {"row": near})
                        passed = at(near, part, piece)
                        onward = None, remote(passed, passed, {"row": other})
                        begin.append(first)
                        sent.extend([first, onward])
                        ways.append((near, piece, first, onward))
                    for near, piece, first, onward in ways:
                        nexts = [onward] + to_mates(at(near, part))
                        follow.append((2 + 3 * part, 0, None, first[1], nexts))
                    for near, piece, first, onward in ways:
                        nexts = to_mates(at(away, part, piece))
                        follow.append((2 + 3 * parts + part, 1, None, onward[1], nexts))
                    for j in range(1, cols):
                        direct(some, at(row, part), {"col": lax.rem(col + j, cols)})
                keep(source, target.at[:, me] if second else target.at[me])
            elif kind[0] in ("swap", "share"):
                for k in range(1, group):
                    other = lax.rem(me + k, group)
                    piece = source.at[other] if kind[0] == "swap" else source
                    direct(piece, target.at[me], self.member(other))
                keep(source.at[me] if kind[0] == "swap" else source, target.at[me])
            elif kind[0] in ("turn", "collect"):
                for k in range(1, depth):
                    other = lax.rem(layer + k, depth)
                    piece = source.at[other] if kind[0] == "turn" else source
                    direct(piece, target.at[layer], {"dp": other})
                keep(source.at[layer] if kind[0] == "turn" else source, target.at[layer])
            elif kind[0] == "line":
                absolute, parts, limit = kind[1:]
                size = source.shape[0] // parts
                steps = limit or depth - 1
                ways = (1,) if limit else (1, -1)
                for part, way in itertools.product(range(parts), ways):
                    behind = layer if way == 1 else depth - 1 - layer
                    onward = layer + way
                    more = (onward >= 0) & (onward < depth)
                    mine = [next(slots) for _ in range(steps)]
                    some = pl.ds(part * size, size)

                    def held(step, where, way=way, some=some):
                        if step == 0:
                            return source.at[some]
                        if absolute:
                            return target.at[where - way * step, some]
                        return target.at[step - 1 if way == 1 else depth - 1 - step, some]

                    def sending(step, onward=onward, mine=mine, held=held):
                        device = {"dp": onward}
                        return remote(
                            held(step - 1, layer), held(step, onward), device, mine[step - 1]
                        )

                    begin.append((more, sending(1)))
                    for step in range(1, steps + 1):
                        sent.append((more & (behind >= step - 1), sending(step)))
                        block = held(step, layer)
                        arrival = remote(block, block, {"dp": onward}, mine[step - 1])
                        nexts = [(more, sending(step + 1))] if step < steps else []
                        when = 4 * step + part
                        follow.append((when, step - 1, behind >= step, arrival, nexts))
                if absolute:
                    keep(source, target.at[layer])
            else:
                for at_slot, d in enumerate(kind[1]):
                    piece = source.at[at_slot] if kind[2] else source
                    direct(piece, target.at[at_slot], {"dp": lax.rem(layer + d % depth, depth)})
            if only is None or index in only:
                starts += begin
                relays += follow
                sends += sent
                arrivals += got
                local += stay
        return starts, sorted(relays, key=lambda entry: entry[0]), sends, arrivals, local

    def given(self, condition, action):
        if condition is None:
            action()
        else:
            pl.when(condition)(action)

    def start(self, only=None):
        starts, _, _, _, local = self.plan(only)
        for condition, copy in starts:
            self.given(condition, lambda copy=copy: copy().start())
        for copy in local:
            copy().start()

    def relay(self, only=None, stages=None):
        for _, stage, condition, copy, nexts in self.plan(only)[1]:
            if stages is not None and stage not in stages:
                continue

            def action(copy=copy, nexts=nexts):
                copy().wait_recv()
                for more, follower in nexts:
                    self.given(more, lambda follower=follower: follower().start())

            self.given(condition, action)

    def finish(self, only=None):
        _, _, sends, arrivals, local = self.plan(only)
        for condition, copy in arrivals:
            self.given(condition, lambda copy=copy: copy().wait_recv())
        for condition, copy in sends:
            self.given(condition, lambda copy=copy: copy().wait_send())
        for copy in local:
            copy().wait()


def planned(sizes, items):
    rows, cols, depth = sizes
    group = rows * cols
    kinds, shapes, copies = [], [], 0
    for item in items:
        name, array = item[0], item[1]
        shape = array.shape
        if name == "gather":
            assert rows == 4
            second, parts = (item[2:] + (False, 1)[len(item) - 2 :])[:2]
            kinds.append((name, second, parts))
            shape = (shape[0], group) + shape[1:] if second else (group,) + shape
            copies += parts * (4 + 5 * (cols - 1))
        elif name == "shift":
            distances, split = item[2], item[3]
            kinds.append((name, tuple(distances), split))
            shape = (len(distances),) + (shape[1:] if split else shape)
            copies += len(distances)
        elif name == "line":
            parts, limit = (item[3:] + (1, 0)[len(item) - 3 :])[:2]
            kinds.append((name, item[2], parts, limit))
            shape = (depth if item[2] else limit or depth - 1,) + shape
            copies += (limit or 2 * (depth - 1)) * parts
        else:
            kinds.append((name,))
            if name in ("share", "collect"):
                shape = (group if name == "share" else depth,) + shape
            copies += (depth if name in ("turn", "collect") else group) - 1
        shapes.append(jax.ShapeDtypeStruct(shape, array.dtype))
    sems = [
        pltpu.SemaphoreType.DMA((copies,)),
        pltpu.SemaphoreType.DMA((copies,)),
        pltpu.SemaphoreType.DMA((len(items),)),
    ]
    return tuple(kinds), shapes, sems


class Got:
    def __init__(self, index):
        self.index = index


class Made:
    def __init__(self, index):
        self.index = index


class Stage:
    def __init__(self, body, shapes, *operands, scratch=()):
        self.body, self.shapes, self.operands = body, shapes, operands
        self.scratch = list(scratch)


def exchange(sizes, name, number, *items, before=None, after=None, cover=None, landing=(), shared=(), delayed=()):
    kinds, moved, sems = planned(sizes, items)
    stages = [stage for stage in (before, after) if stage]
    operands = []
    for stage in stages:
        for operand in stage.operands:
            if not isinstance(operand, (Got, Made)):
                operands.append(operand)
    work = list(cover.work) if cover else []
    outs = [s for stage in stages for s in stage.shapes]
    made_shapes = list(cover.shapes) if cover else []
    flown = [i for i in range(len(items)) if i not in landing]
    late = [o.index for o in (after.operands if after else ()) if isinstance(o, Got)]
    late = [i for i in late if i not in landing]
    scratch = []

    def take(shapes):
        first = len(scratch)
        scratch.extend(shapes)
        return slice(first, len(scratch))

    vmem = lambda s: pltpu.VMEM(tuple(s[0]), s[1])
    of = lambda a: (a.shape, a.dtype)
    operand_at = take([vmem(of(a)) for a in operands])
    result_at = take([vmem(s) for s in outs])
    landed_at = take([vmem(of(moved[i])) for i in landing])
    late_at = take([vmem(of(moved[i])) for i in late])
    stage_at = [take(stage.scratch) for stage in stages]
    shared_at = take(list(shared))
    needed = sorted({o.index for o in (after.operands if after else ()) if isinstance(o, Got)})
    others = [i for i in range(len(items)) if i not in needed]
    prompt = [i for i in range(len(items)) if i not in delayed]
    later = range(1, 2 * sizes[2])
    cover_at = take(cover.scratch) if cover else slice(0, 0)
    copies = len(operands) + len(outs) + len(late)
    copy_at = take([pltpu.SemaphoreType.DMA((max(1, copies),))])
    sems_at = take(sems)

    def body(*refs):
        cuts = [len(operands), len(work), len(items), len(outs), len(made_shapes), len(flown)]
        groups = []
        for cut in cuts:
            groups.append(refs[:cut])
            refs = refs[cut:]
        given, work_refs, sources, results, made_refs, flown_refs = groups
        loaded, held = refs[operand_at], refs[result_at]
        landed, lates, (copy_sem,) = refs[landed_at], refs[late_at], refs[copy_at]
        targets = [None] * len(items)
        for i, ref in zip(flown, flown_refs):
            targets[i] = ref
        for i, ref in zip(landing, landed):
            targets[i] = ref
        moves = Moves(sizes, kinds, sources, targets, refs[sems_at])
        number_of = iter(range(copies))
        copy = lambda a, b: pltpu.make_async_copy(a, b, copy_sem.at[next(number_of)])
        loads = [copy(a, b) for a, b in zip(given, loaded)]
        stores = [copy(a, b) for a, b in zip(held, results)]
        late_loads = [copy(targets[i], b) for i, b in zip(late, lates)]
        split = len([o for o in before.operands if not isinstance(o, Made)]) if before else 0
        first = len(before.shapes) if before else 0
        for load in loads:
            load.start()
        if cover:
            cover.begin(work_refs, refs[cover_at])
        moves.barrier()
        moves.start(prompt)
        if before:
            for load in loads[:split]:
                load.wait()
            before.body(*loaded[:split], *held[:first], *refs[stage_at[0]], *refs[shared_at])
            for store in stores[:first]:
                store.start()
        if cover:
            cover.run(work_refs, made_refs, refs[cover_at])
        moves.relay(prompt, (0,))
        moves.start(delayed)
        if after:
            moves.relay(needed, later)
            moves.finish(needed)
        moves.relay(delayed, (0,))
        if after:
            for load in late_loads:
                load.start()
            for load in loads[split:]:
                load.wait()
            for load in late_loads:
                load.wait()
            plain = iter(loaded[split:])
            values = []
            for operand in after.operands:
                if isinstance(operand, Made):
                    values.append(held[operand.index])
                elif isinstance(operand, Got) and operand.index in landing:
                    values.append(landed[landing.index(operand.index)])
                elif isinstance(operand, Got):
                    values.append(lates[late.index(operand.index)])
                else:
                    values.append(next(plain))
            after.body(*values, *held[first:], *refs[stage_at[-1]], *refs[shared_at])
            for store in stores[first:]:
                store.start()
        moves.relay(others, later)
        moves.finish(others)
        if cover:
            cover.end(made_refs, refs[cover_at])
        for store in stores:
            store.wait()

    shape = lambda s: jax.ShapeDtypeStruct(tuple(s[0]), s[1])
    return pl.pallas_call(
        body,
        out_shape=tuple(shape(s) for s in outs + made_shapes) + tuple(moved[i] for i in flown),
        in_specs=[HBM] * (len(operands) + len(work) + len(items)),
        out_specs=(HBM,) * (len(outs) + len(made_shapes) + len(flown)),
        scratch_shapes=scratch,
        compiler_params=pltpu.CompilerParams(collective_id=number, has_side_effects=True),
        name=name,
    )(*operands, *work, *[item[1] for item in items])


def dot(a, b, left=1, right=0, precision=None):
    return lax.dot_general(
        a,
        b,
        (((left,), (right,)), ((), ())),
        preferred_element_type=jnp.float32,
        precision=precision,
    )


def widened(source, target):
    size = target.shape[0] // 4

    def piece(i, carry):
        at = pl.ds(pl.multiple_of(i * size, size), size)
        target[at, :] = source[at, :].astype(target.dtype)
        return carry

    lax.fori_loop(0, 4, piece, 0)


def cleared(target):
    size = target.shape[0] // 8

    def piece(i, carry):
        at = pl.ds(pl.multiple_of(i * size, size), size)
        target[at, :] = jnp.zeros((size, target.shape[1]), target.dtype)
        return carry

    lax.fori_loop(0, 8, piece, 0)


def lanes_of(shape):
    return lax.broadcasted_iota(jnp.int32, shape, len(shape) - 1)


def flipped(values):
    lanes = lanes_of(values.shape)
    ahead = pltpu.roll(values, LANES - TURN, 1)
    behind = pltpu.roll(values, TURN, 1)
    return jnp.where(lanes % (2 * TURN) < TURN, ahead, behind)


def beside(blocks_ref):
    return jnp.concatenate([blocks_ref[i] for i in range(blocks_ref.shape[0])], axis=1)


def gain_row(gains_ref):
    return beside(gains_ref).astype(jnp.float32)


def added(blocks):
    def more(i, total):
        return total + blocks[i].astype(jnp.float32)

    return lax.fori_loop(1, blocks.shape[0], more, blocks[0].astype(jnp.float32))


def own_rows(count):
    me = lax.axis_index("row") * lax.axis_size("col") + lax.axis_index("col")
    return pl.ds(pl.multiple_of(me * count, count), count)


def column(row):
    return jnp.broadcast_to(row, (8, row.shape[1])).T[:, 0:1]


def tables_body(cosine, sine):
    step = 64
    lanes = lanes_of((step, LANES))
    power = (lanes % TURN).astype(jnp.float32) * (-math.log(ROPE_BASE) / TURN)
    frequencies = jnp.exp(power)
    base = lax.axis_index("dp") * cosine.shape[0]

    def piece(i, carry):
        at = pl.ds(pl.multiple_of(i * step, step), step)
        positions = base + i * step + lax.broadcasted_iota(jnp.int32, lanes.shape, 0)
        angles = positions.astype(jnp.float32) * frequencies
        cosine[at, :] = jnp.cos(angles)
        value = jnp.sin(angles)
        sine[at, :] = jnp.where(lanes % (2 * TURN) < TURN, -value, value)
        return carry

    lax.fori_loop(0, cosine.shape[0] // step, piece, 0)


def turned(source, target):
    def block(i, carry):
        scaled = RESIDUAL_SCALE * source[i].astype(jnp.float32)
        target[i] = scaled.T.astype(jnp.bfloat16)
        return carry

    lax.fori_loop(0, target.shape[0], block, 0)


def project_body(blocks, gains, w_query, w_pair, cosine, sine, normed, query, pair, own):
    gain = gain_row(gains)
    step = 128

    def piece(i, carry):
        at = pl.ds(pl.multiple_of(i * step, step), step)
        parts = [blocks[k, at, :] for k in range(blocks.shape[0])]
        tokens = jnp.concatenate(parts, axis=1).astype(jnp.float32)
        scale = lax.rsqrt(jnp.mean(tokens * tokens, axis=1, keepdims=True) + EPSILON)
        normed[at, :] = (tokens * scale * gain).astype(jnp.bfloat16)
        return carry

    lax.fori_loop(0, normed.shape[0] // step, piece, 0)
    raw = dot(normed[...], w_query[...])
    query[...] = (raw * cosine[...] + flipped(raw) * sine[...]).astype(jnp.bfloat16)
    raw = dot(normed[...], w_pair[...])
    keys = lanes_of(raw.shape) < LANES // 2
    turned = raw * cosine[...] + flipped(raw) * sine[...]
    pair[...] = jnp.where(keys, turned, raw).astype(jnp.bfloat16)
    for i in range(blocks.shape[0]):
        own[:, i * LANES : (i + 1) * LANES] = blocks[i, own_rows(own.shape[0]), :]


def doubled(pair, keys_ref, values_ref, at, distance=0):
    wide = pair.astype(jnp.float32)
    if distance:
        wide = jnp.where(lax.axis_index("dp") >= distance, wide, 0.0)
    other = pltpu.roll(wide, LANES // 2, 1)
    keys = lanes_of(wide.shape) < LANES // 2
    keys_ref[at] = jnp.where(keys, wide, other).astype(jnp.bfloat16)
    values_ref[at] = jnp.where(keys, other, wide).astype(jnp.bfloat16)


def per_head(values):
    first = lanes_of(values.shape) < LANES // 2
    zero = jnp.zeros_like(values)
    return jnp.concatenate(
        [jnp.where(first, values, zero), jnp.where(first, zero, values)], axis=0
    )


def tile_scores(queries, keys_ref, starts, row, block, last, tokens):
    scores = dot(queries, keys_ref[block], 1, 1) * SCORE_SCALE
    at = lanes_of(scores.shape) + block * tokens
    allowed = at >= starts
    if block == last:
        place = row + lax.broadcasted_iota(jnp.int32, scores.shape, 0)
        allowed = allowed & (at <= place + block * tokens)
    return jnp.where(allowed, scores, MASKED)


def doc_row(docs):
    rows = [docs[i : i + 1, :] for i in range(docs.shape[0])]
    return jnp.concatenate(rows, axis=1).astype(jnp.float32)


def attend_tiles(tokens, tile):
    step = 256

    def body(i, carry):
        rows = pl.ds(pl.multiple_of(i * step, step), step)
        tile(rows, lax.rem(i * step, tokens), step)
        return carry

    lax.fori_loop(0, 2 * tokens // step, body, 0)


def attend_first_body(near_grads, far_grads, query, pair, docs, far_docs, own_grad, near_turned, far_turned, start, keys, values, queries, out, tops, totals):
    turned(near_grads, near_turned)
    turned(far_grads, far_turned)
    for i in range(near_grads.shape[0]):
        own_grad[:, i * LANES : (i + 1) * LANES] = near_grads[i, own_rows(own_grad.shape[0]), :]
    tokens = query.shape[0]
    last = keys.shape[0] - 1
    layer = lax.axis_index("dp")
    here = doc_row(docs[...])
    mine = column(here)
    before = jnp.sum((here < mine).astype(jnp.float32), axis=1, keepdims=True)
    for d in range(1, last + 1):
        fewer = (doc_row(far_docs[d - 1]) < mine) | (layer < d)
        before = before + jnp.sum(fewer.astype(jnp.float32), axis=1, keepdims=True)
    start[...] = before.astype(jnp.int32)
    doubled(pair[...], keys, values, last)
    queries[...] = per_head(query[...].astype(jnp.float32)).astype(jnp.bfloat16)

    def tile(rows, row, step):
        starts = start[pl.ds(pl.multiple_of(row, step), step), :]
        scores = tile_scores(queries[rows, :], keys, starts, row, last, last, tokens)
        top = jnp.max(scores, axis=1, keepdims=True)
        terms = jnp.exp(scores - top)
        tops[rows, :] = top
        totals[rows, :] = jnp.sum(terms, axis=1, keepdims=True)
        out[rows, :] = dot(terms.astype(jnp.bfloat16), values[last])

    attend_tiles(tokens, tile)


def attend_rest_body(far, start, mixed, log_total, keys, values, queries, out, tops, totals):
    last, tokens = far.shape[0], far.shape[1]
    for d in range(1, last + 1):
        doubled(far[d - 1], keys, values, last - d, d)

    def tile(rows, row, step):
        starts = start[pl.ds(pl.multiple_of(row, step), step), :]
        parts = [
            tile_scores(queries[rows, :], keys, starts, row, block, last, tokens)
            for block in range(last)
        ]
        top = functools.reduce(
            jnp.maximum, [jnp.max(part, axis=1, keepdims=True) for part in parts], tops[rows, :]
        )
        parts = [jnp.exp(part - top) for part in parts]
        scale = jnp.exp(tops[rows, :] - top)
        total = functools.reduce(
            jnp.add,
            [jnp.sum(p, axis=1, keepdims=True) for p in parts],
            totals[rows, :] * scale,
        )
        sums = [
            dot(part.astype(jnp.bfloat16), values[block]) for block, part in enumerate(parts)
        ]
        out[rows, :] = functools.reduce(jnp.add, sums, out[rows, :] * scale) / total
        log_total[rows, :] = top + jnp.log(total)

    attend_tiles(tokens, tile)
    first = lanes_of((tokens, LANES)) < LANES // 2
    mixed[...] = jnp.where(first, out[:tokens, :], out[tokens:, :]).astype(jnp.bfloat16)


def attend_again_body(query, pair, far, start, log_total, queries, keys, values, queries_turned, chances):
    tokens = query.shape[0]
    last = far.shape[0]
    doubled(pair[...], keys, values, last)
    for d in range(1, last + 1):
        doubled(far[d - 1], keys, values, last - d, d)
    stacked = per_head(query[...].astype(jnp.float32))
    queries[...] = stacked.astype(jnp.bfloat16)
    queries_turned[...] = stacked.T.astype(jnp.bfloat16)

    def tile(rows, row, step):
        starts = start[pl.ds(pl.multiple_of(row, step), step), :]
        for block in range(last + 1):
            scores = tile_scores(queries[rows, :], keys, starts, row, block, last, tokens)
            chances[block, rows, :] = jnp.exp(scores - log_total[rows, :])

    attend_tiles(tokens, tile)


def attend_back_body(grad, w_output, mixed, cosine, sine, query_grad, pair_grad, far_grad, output_grad, grads, grads_turned, turned, key_sums, value_sums, keys, values, queries_turned, chances):
    tokens = mixed.shape[0]
    last = keys.shape[0] - 1
    given_grad = grad[...].reshape(tokens, -1)
    stacked = per_head(dot(given_grad, w_output[...], 1, 1))
    grads[...] = stacked.astype(jnp.bfloat16)
    grads_turned[...] = stacked.T.astype(jnp.bfloat16)
    output_sum = dot(mixed[...], given_grad, 0, 0).astype(jnp.bfloat16)
    for i in range(output_grad.shape[0]):
        output_grad[i] = output_sum[:, i * LANES : (i + 1) * LANES]
    for block in range(last + 1):
        cleared(key_sums.at[block])
        cleared(value_sums.at[block])

    def tile(rows, row, step):
        given = grads[rows, :]
        asked_turned, given_turned = queries_turned[:, rows], grads_turned[:, rows]
        products = [dot(given, values[block], 1, 1) for block in range(last + 1)]
        delta = functools.reduce(
            jnp.add,
            [
                jnp.sum(chances[block, rows, :] * product, axis=1, keepdims=True)
                for block, product in enumerate(products)
            ],
        )
        total = jnp.zeros((step, LANES), jnp.float32)
        for block in range(last + 1):
            chance = chances[block, rows, :]
            back = (chance * (products[block] - delta)).astype(jnp.bfloat16)
            total = total + dot(back, keys[block])
            key_sums[block] += dot(asked_turned, back)
            value_sums[block] += dot(given_turned, chance.astype(jnp.bfloat16))
        turned[rows, :] = total

    attend_tiles(tokens, tile)
    first = lanes_of((tokens, LANES)) < LANES // 2
    raw = jnp.where(first, turned[:tokens, :], turned[tokens:, :]) * SCORE_SCALE
    query_grad[...] = (raw * cosine[...] - flipped(raw) * sine[...]).astype(jnp.bfloat16)

    def joined(block):
        by_key, by_value = key_sums[block].T, value_sums[block].T
        by_key = (by_key + pltpu.roll(by_key, LANES // 2, 1)) * SCORE_SCALE
        by_value = by_value + pltpu.roll(by_value, LANES // 2, 1)
        return jnp.where(first, by_key, by_value)

    pair_grad[...] = joined(last)
    for d in range(1, last + 1):
        far_grad[d - 1] = joined(last - d).astype(jnp.bfloat16)


def router_rows(router):
    rows = beside(router)
    blank = jnp.zeros((LANES - rows.shape[0], rows.shape[1]), rows.dtype)
    return jnp.concatenate([rows, blank], axis=0)


def full_dot(wide, low, left=1, right=0):
    parts, rest = [], wide
    for _ in range(3):
        parts.append(rest.astype(jnp.bfloat16))
        rest = rest - parts[-1].astype(jnp.float32)
    count = wide.shape[0]
    sums = dot(jnp.concatenate(parts, axis=0), low, left, right)
    return sums[:count] + (sums[count : 2 * count] + sums[2 * count :])


def middle_body(mixed, own, w_output, gains, router, ids_turned, rows, middle, weights, ids_ref):
    experts = router.shape[1]
    width = own.shape[1]
    attn = dot(beside(mixed), w_output[...])
    value = own[...].astype(jnp.float32) + RESIDUAL_SCALE * attn
    middle[...] = value
    scale = lax.rsqrt(jnp.mean(value * value, axis=1, keepdims=True) + EPSILON)
    normed = value * scale * gain_row(gains)
    logits = full_dot(normed, router_rows(router), 1, 1)
    count = own.shape[0]
    ids_ref[...] = ids_turned[...].astype(jnp.float32).T
    ids = ids_ref[own_rows(count), :]
    lanes = lanes_of((count, LANES))
    chosen = jnp.zeros((count, LANES), jnp.float32)
    for k in range(ids.shape[1]):
        chosen = chosen + (ids[:, k : k + 1] == lanes.astype(jnp.float32)).astype(
            jnp.float32
        )
    top = jnp.max(jnp.where(lanes < experts, logits, MASKED), axis=1, keepdims=True)
    terms = jnp.exp(jnp.minimum(logits - top, 0.0)) * chosen
    share = terms / jnp.sum(terms, axis=1, keepdims=True)
    weights[...] = share
    high = share.astype(jnp.bfloat16)
    low = share - high.astype(jnp.float32)
    rows[:, :width] = normed.astype(jnp.bfloat16)
    rows[:, width:] = (high.astype(jnp.float32) + pltpu.roll(low, LANES // 2, 1)).astype(
        jnp.bfloat16
    )


def middle_back_body(back, out_grad, middle, weights, gains, router, middle_grad, attn_grad, logit_grad, gain_part):
    width = middle.shape[1]
    normed_grad = back[0, :, :width].astype(jnp.float32)
    weight_grad = back[0, :, width:].astype(jnp.float32)
    for i in range(1, back.shape[0]):
        normed_grad = normed_grad + back[i, :, :width].astype(jnp.float32)
        weight_grad = weight_grad + back[i, :, width:].astype(jnp.float32)
    share, value = weights[...], middle[...]
    mean = jnp.sum(share * weight_grad, axis=1, keepdims=True)
    logit = share * (weight_grad - mean)
    logit_grad[...] = logit.astype(jnp.bfloat16)
    normed_grad = normed_grad + full_dot(logit, router_rows(router))
    scale = lax.rsqrt(jnp.mean(value * value, axis=1, keepdims=True) + EPSILON)
    gain_part[...] = jnp.sum(normed_grad * value * scale, axis=0, keepdims=True)
    scaled = normed_grad * gain_row(gains)
    norm_dot = jnp.sum(scaled * value, axis=1, keepdims=True)
    total = (
        out_grad[...].astype(jnp.float32)
        + scale * scaled
        - value * (scale * scale * scale * norm_dot / width)
    )
    middle_grad[...] = total
    attn_grad[...] = (RESIDUAL_SCALE * total).astype(jnp.bfloat16)


def project_back_body(query_grad, pair_grad, returned, normed, w_query, w_pair, cosine, sine, output_turned, logit, rows, gains, gain_moe, partial, sums, output_first, output_last, gain_parts):
    layer = lax.axis_index("dp")
    depth = lax.axis_size("dp")
    total = pair_grad[...]
    for i in range(returned.shape[0]):
        total = total + jnp.where(
            layer + i + 1 < depth, returned[i].astype(jnp.float32), 0.0
        )
    keys = lanes_of(total.shape) < LANES // 2
    turned = total * cosine[...] - flipped(total) * sine[...]
    pair_low = jnp.where(keys, turned, total).astype(jnp.bfloat16)
    query_low = query_grad[...]
    whole = dot(query_low, w_query[...], 1, 1) + dot(pair_low, w_pair[...], 1, 1)
    partial[...] = whole.astype(jnp.bfloat16)
    gain_attn = jnp.sum(whole * normed[...].astype(jnp.float32), axis=0, keepdims=True)
    gain_attn = gain_attn / gain_row(gains)
    gain_parts[...] = jnp.zeros_like(gain_parts)
    for i in range(gain_parts.shape[0]):
        at = slice(i * LANES, (i + 1) * LANES)
        gain_parts[i, 0:1, :] = gain_attn[:, at]
        gain_parts[i, 1:2, :] = gain_moe[0:1, at]
    width = normed.shape[1]
    sums[:width, :] = dot(normed[...], query_low, 0, 0).astype(jnp.bfloat16)
    sums[width : 2 * width, :] = dot(normed[...], pair_low, 0, 0).astype(jnp.bfloat16)
    output_sum = added(output_turned).astype(jnp.bfloat16)
    output_first[...] = output_sum[: output_first.shape[0], :]
    output_last[...] = output_sum[output_first.shape[0] :, :]
    mine = rows[:, own_rows(LANES)]
    named = logit[...].reshape(normed.shape[0], LANES)
    router_sum = dot(named, mine, 0, 0).astype(jnp.bfloat16)
    count = min(LANES, sums.shape[0] - 2 * width)
    sums[2 * width : 2 * width + count, :] = router_sum[:count, :]


def results_body(blocks, moe, own, middle, middle_grad, gains, gain_blocks, turned, block_out, in_grad, gain_sum, summed):
    gain_sum[...] = added(gain_blocks)
    summed[...] = added(turned).astype(jnp.bfloat16)
    width = own.shape[1]
    normed_grad = added(blocks)
    branch = added(moe)
    value = own[...].astype(jnp.float32)
    scale = lax.rsqrt(jnp.mean(value * value, axis=1, keepdims=True) + EPSILON)
    scaled = normed_grad * gain_row(gains)
    norm_dot = jnp.sum(scaled * value, axis=1, keepdims=True)
    grad = (
        middle_grad[...] + scale * scaled - value * (scale * scale * scale * norm_dot / width)
    ).astype(jnp.bfloat16)
    out = (middle[...] + RESIDUAL_SCALE * branch).astype(jnp.bfloat16)
    for i in range(block_out.shape[0]):
        at = slice(i * LANES, (i + 1) * LANES)
        block_out[i] = out[:, at]
        in_grad[i] = grad[:, at]


def expert_terms(gate_up, active_grad, weight):
    hidden = active_grad.shape[0]
    gate, up = gate_up[:hidden], gate_up[hidden:]
    sigmoid = jax.nn.sigmoid(gate)
    silu = gate * sigmoid
    ungated = silu * up
    active = (ungated * weight).astype(jnp.bfloat16)
    scaled = active_grad * weight
    gate_grad = (scaled * up * sigmoid * (1.0 + gate * (1.0 - sigmoid))).astype(jnp.bfloat16)
    up_grad = (scaled * silu).astype(jnp.bfloat16)
    return active, jnp.concatenate([gate_grad, up_grad], axis=0), active_grad * ungated


def weight_rows(extra):
    turned = extra.astype(jnp.float32).T
    return turned[: LANES // 2] + turned[LANES // 2 :]


def local_experts_body(sizes, kinds, rows_hbm, grads_hbm, in_ref, out_ref, sent_grads, sent_rows, flat_ref, in_sum, out_sum, moe_hbm, back_hbm, got_grads, got_rows, rows_ref, grads_ref, moe_ref, back_ref, moe_acc, back_acc, share, weights, spread, copy_sem, *sems):
    step, steps = pl.program_id(0), pl.num_programs(0)
    each, hidden, width = out_ref.shape
    parts = hidden // LANES
    moves = Moves(sizes, kinds, [sent_grads, sent_rows], [got_grads, got_rows], sems)
    ends = [(rows_hbm, rows_ref), (grads_hbm, grads_ref), (moe_ref, moe_hbm), (back_ref, back_hbm)]
    copy = lambda i: pltpu.make_async_copy(*ends[i], copy_sem.at[i])

    @pl.when(step == 0)
    def _():
        copy(0).start()
        copy(1).start()
        moves.barrier()
        moves.start([0])
        cleared(moe_acc)
        cleared(back_acc)
        copy(0).wait()
        copy(1).wait()
        share[...] = jnp.zeros_like(share)
        weights[...] = weight_rows(rows_ref[:, width:])

    @pl.when(step == 2 * steps // 8)
    def _():
        moves.start([1])

    for when, item, stage in ((3, 0, 0), (6, 1, 0), (7, 0, 1)):

        @pl.when(step == when * steps // 8)
        def _(item=item, stage=stage):
            moves.relay([item], (stage,))

    for i in range(each):
        spread[i] = in_ref[i].astype(jnp.float32)
        for part in range(parts):
            for half in range(2):
                at = half * hidden + part * LANES
                flat_ref[i, :, at : at + LANES] = spread[
                    i, pl.ds(part * 2 + half, width, stride=2 * parts), :
                ].astype(jnp.bfloat16)
        expert = (lax.axis_index("row") * steps + step) * each + i
        active, gate_up_grad, shares = expert_terms(
            dot(flat_ref[i], rows_ref[:, :width], 0, 1),
            dot(out_ref[i], grads_ref[...]),
            weights[pl.ds(expert, 1), :],
        )
        share[pl.ds(expert, 1), :] = jnp.sum(shares, axis=0, keepdims=True)
        moe_acc[...] += dot(active, out_ref[i], 0, 0)
        back_acc[...] += dot(gate_up_grad, flat_ref[i], 0, 1)
        in_sum[i] = dot(gate_up_grad, rows_ref[:, :width]).astype(jnp.bfloat16)
        out_sum[i] = dot(active, grads_ref[...], 1, 1).astype(jnp.bfloat16)

    @pl.when(step == steps - 1)
    def _():
        moves.relay([1], (1,))
        widened(moe_acc, moe_ref)
        copy(2).start()
        widened(back_acc, back_ref.at[:, :width])
        back_ref[:, width:] = share[...].T.astype(jnp.bfloat16)
        copy(3).start()
        moves.finish()
        copy(2).wait()
        copy(3).wait()


def local_experts(sizes, number, rows, grads, w_in, w_out, sent_grads, sent_rows):
    tokens, wide = rows.shape
    experts, hidden, width = w_out.shape
    each = 1
    low = jnp.bfloat16
    kinds, shapes, sems = planned(
        sizes,
        [
            ("gather", sent_grads, True, sent_grads.shape[0]),
            ("gather", sent_rows, True, sent_rows.shape[0]),
        ],
    )
    some = lambda s: pl.BlockSpec((each,) + s[1:], lambda e: (e,) + (0,) * (len(s) - 1))
    outs = [
        (experts, width, 2 * hidden),
        (experts, 2 * hidden, width),
        (experts, hidden, width),
        (tokens, width),
        (tokens, wide),
    ]
    return pl.pallas_call(
        functools.partial(local_experts_body, sizes, kinds),
        grid=(experts // each,),
        in_specs=[
            HBM,
            HBM,
            some(w_in.shape),
            some(w_out.shape),
            HBM,
            HBM,
        ],
        out_specs=(*[some(s) for s in outs[:3]], HBM, HBM, HBM, HBM),
        out_shape=tuple(jax.ShapeDtypeStruct(s, low) for s in outs) + tuple(shapes),
        scratch_shapes=[
            pltpu.VMEM(rows.shape, low),
            pltpu.VMEM(grads.shape, low),
            pltpu.VMEM((tokens, width), low),
            pltpu.VMEM((tokens, wide), low),
            pltpu.VMEM((tokens, width), jnp.float32),
            pltpu.VMEM((tokens, width), jnp.float32),
            pltpu.VMEM((LANES, tokens), jnp.float32),
            pltpu.VMEM((LANES // 2, tokens), jnp.float32),
            pltpu.VMEM((each,) + w_in.shape[1:], jnp.float32),
            pltpu.SemaphoreType.DMA((4,)),
        ]
        + sems,
        compiler_params=pltpu.CompilerParams(collective_id=number, has_side_effects=True),
        name="local_experts",
    )(rows, grads, w_in, w_out, sent_grads, sent_rows)


class Sums:
    def __init__(self, rows, grads, weights, turned, load_sem, *sums):
        self.rows, self.grads, self.weights = rows, grads, weights
        self.turned, self.load_sem, self.sums = turned, load_sem, sums

    def load(self, which, source):
        target = (self.rows, self.grads)[which]
        return pltpu.make_async_copy(source, target, self.load_sem.at[which])

    def ready(self):
        layers, width, tokens = self.grads.shape

        def block(i, carry):
            at = pl.ds(pl.multiple_of(i * tokens, tokens), tokens)
            self.weights[i] = weight_rows(self.rows[at, width:])
            return carry

        lax.fori_loop(0, layers, block, 0)

    def make(self, index, w_in, w_out, in_part, out_part, made, arrive):
        layers, width, tokens = self.grads.shape
        hidden = w_out.shape[0]
        arrive(0)
        if self.sums:
            arrive(1)
        later = arrive

        def part_of(at, pieces, arrive=lambda i: None if self.sums else later(i)):
            first = at * tokens if isinstance(at, int) else pl.multiple_of(at * tokens, tokens)
            block = self.rows[pl.ds(first, pieces * tokens), :width]
            gate_up = dot(w_in[...], block, 0, 1)
            arrive(1)
            weight = jnp.concatenate(
                [self.weights[at + i, pl.ds(index, 1), :] for i in range(pieces)], axis=1
            )
            active_grad = jnp.concatenate(
                [dot(w_out[...], self.grads[at + i]) for i in range(pieces)], axis=1
            )
            active, gate_up_grad, _ = expert_terms(gate_up, active_grad, weight)
            out_total = functools.reduce(
                jnp.add,
                [
                    dot(active[:, i * tokens : (i + 1) * tokens], self.grads[at + i], 1, 1)
                    for i in range(pieces)
                ],
            )
            return dot(gate_up_grad, block), out_total

        if not self.sums:
            in_total, out_total = part_of(0, layers)
        else:
            whole, out_acc = self.sums
            whole[...] = jnp.zeros_like(whole)
            out_acc[...] = jnp.zeros_like(out_acc)

            def more(i, carry):
                in_more, out_more = part_of(i, 1)
                whole[...] += in_more
                out_acc[...] += out_more
                return carry

            lax.fori_loop(0, layers, more, 0)
            in_total, out_total = whole[...], out_acc[...]
        arrive(2)
        in_total = in_total + in_part[...].astype(jnp.float32)
        parts = hidden // LANES
        for part in range(parts):
            for half in range(2):
                at = half * hidden + part * LANES
                self.turned[pl.ds(part * 2 + half, width, stride=2 * parts), :] = in_total[
                    at : at + LANES, :
                ].T
        made[...] = self.turned[...].astype(jnp.bfloat16)
        return out_total + out_part[...].astype(jnp.float32)


def sums_scratch(layers, tokens, width, hidden):
    low, full = jnp.bfloat16, jnp.float32
    return [
        pltpu.VMEM((layers * tokens, width + LANES), low),
        pltpu.VMEM((layers, width, tokens), low),
        pltpu.VMEM((layers, LANES // 2, tokens), full),
        pltpu.VMEM((width * 2 * hidden // LANES, LANES), full),
        pltpu.SemaphoreType.DMA((2,)),
    ] + [pltpu.VMEM((k * hidden, width), full) for k in (2, 1) if layers > 4]


class Cover:
    def __init__(self, first, many, work):
        w_in, w_out, in_part, out_part, rows_far, grads_far = work
        layers, width, tokens = grads_far.shape
        self.experts, hidden, _ = w_out.shape
        self.first, self.many, self.work = first, many, work
        low = jnp.bfloat16
        self.shapes = [
            ((many, width * 2 * hidden // LANES, LANES), low),
            ((many, hidden, width), low),
        ]
        self.scratch = [pltpu.VMEM((many,) + a.shape[1:], low) for a in work[:4]]
        self.scratch += [pltpu.VMEM(*s) for s in self.shapes]
        self.scratch += [pltpu.SemaphoreType.DMA((4, many)), pltpu.SemaphoreType.DMA((2, many))]
        self.scratch += sums_scratch(layers, tokens, width, hidden)

    def load(self, which, i, work, refs):
        source, sem = work[which].at[self.first + i], refs[6].at[which, i]
        return pltpu.make_async_copy(source, refs[which].at[i], sem)

    def begin(self, work, refs):
        sums = Sums(*refs[8:])
        sums.load(0, work[4]).start()
        self.load(0, 0, work, refs).start()
        sums.load(1, work[5]).start()
        for which in (1, 2, 3):
            self.load(which, 0, work, refs).start()
        for i in range(1, self.many):
            for which in range(4):
                self.load(which, i, work, refs).start()

    def stores(self, i, made, refs):
        return [
            pltpu.make_async_copy(refs[4 + k].at[i], made[k].at[i], refs[7].at[k, i])
            for k in range(2)
        ]

    def run(self, work, made, refs):
        sums = Sums(*refs[8:])

        def expert(i, carry):
            def arrive(point):
                @pl.when(i == 0)
                def _():
                    if point == 0:
                        sums.load(0, work[4]).wait()
                        sums.ready()
                    if point == 1:
                        sums.load(1, work[5]).wait()

                for which in ((0,), (1,), (2, 3))[point]:
                    self.load(which, i, work, refs).wait()

            index = lax.axis_index("row") * self.experts + self.first + i
            out_total = sums.make(index, *[refs[k].at[i] for k in range(5)], arrive)
            refs[5][i] = out_total.astype(jnp.bfloat16)
            for store in self.stores(i, made, refs):
                store.start()
            return carry

        lax.fori_loop(0, self.many, expert, 0)

    def end(self, made, refs):
        for i in range(self.many):
            for store in self.stores(i, made, refs):
                store.wait()


def outputs_body(count, total, *refs):
    pieces = total // count
    sums, smalls = refs[: 2 * pieces], refs[2 * pieces : 2 * pieces + 6]
    gin, gout, *others = refs[2 * pieces + 6 : 2 * pieces + 16]
    in_low, out_low, in_full, out_full, *refs = refs[2 * pieces + 16 :]
    held, results, (load_sem, store_sem, small_sem) = refs[:6], refs[6:14], refs[14:]
    block_out, in_grad, gain_attn, gain_moe, query, pair, output, router = results
    width = gout.shape[2]
    stored = [
        pltpu.make_async_copy(a, b, small_sem.at[6 + j])
        for j, (a, b) in enumerate(zip(results, others))
    ]
    ring = in_full.shape[0]

    def load(k, i):
        low = (in_low, out_low)[k]
        source = sums[k * pieces + i // count].at[i % count]
        return pltpu.make_async_copy(source, low.at[i], load_sem.at[k, i])

    def store(k, i):
        made, target = ((in_full, gin), (out_full, gout))[k]
        return pltpu.make_async_copy(made.at[i % ring], target.at[i], store_sem.at[k, i % ring])

    for i in range(total):
        for k in range(2):
            load(k, i).start()
        if i == 0:
            fetched = [
                pltpu.make_async_copy(a, b, small_sem.at[j])
                for j, (a, b) in enumerate(zip(smalls, held))
            ]
            for copy in fetched:
                copy.start()
    def small():
        for copy in fetched:
            copy.wait()
        blocks, in_blocks, gains, summed, output_first, output_last = held
        for i in range(blocks.shape[0]):
            at = pl.ds(i * blocks.shape[1], blocks.shape[1])
            block_out[at, :] = blocks[i]
            in_grad[at, :] = in_blocks[i]
        gain_sum = jnp.sum(gains[...], axis=0)
        gain_attn[...] = gain_sum[0:1, :]
        gain_moe[...] = gain_sum[1:2, :]
        query[...] = summed[:width, :].astype(jnp.float32)
        pair[...] = summed[width : 2 * width, :].astype(jnp.float32)
        router[...] = summed[2 * width : 2 * width + router.shape[0], :].astype(jnp.float32)
        half = output_first.shape[1]
        for i in range(width // half):
            from_first = i % 2 == 0
            rows = (output_first if from_first else output_last)[i // 2].astype(jnp.float32)
            for j in range(max(1, half // LANES)):
                place = i * half + j * LANES
                at = place // LANES
                part = rows[j * LANES : (j + 1) * LANES, :]
                first = place % LANES
                output[first : first + part.shape[0], at * LANES : (at + 1) * LANES] = part

    for i in range(total):
        for k in range(2):
            load(k, i).wait()
            if i >= ring:
                store(k, i - ring).wait()
        for low, made in ((in_low, in_full), (out_low, out_full)):
            widened(low.at[i], made.at[i % ring])
        for k in range(2):
            store(k, i).start()
        if i == total - 3:
            small()
            for copy in stored:
                copy.start()
    for i in range(total - ring, total):
        for k in range(2):
            store(k, i).wait()
    for copy in stored:
        copy.wait()


def outputs(in_sums, out_sums, hidden, experts, *smalls):
    count = in_sums[0].shape[0]
    total = count * len(in_sums)
    width = out_sums[0].shape[2]
    parts = hidden // LANES
    lanes = smalls[0].shape[2]
    tokens = smalls[0].shape[0] * smalls[0].shape[1]
    low, full = jnp.bfloat16, jnp.float32
    large = [(width * 2 * parts, LANES), (hidden, width)]
    shapes = [((total,) + s, full) for s in large] + [
        ((tokens, lanes), low),
        ((tokens, lanes), low),
        ((1, LANES), full),
        ((1, LANES), full),
        ((width, LANES), full),
        ((width, LANES), full),
        ((LANES, width), full),
        ((experts, LANES), full),
    ]
    ring = min(4, total)
    gin, *others = pl.pallas_call(
        functools.partial(outputs_body, count, total),
        in_specs=[HBM] * (2 * len(in_sums) + len(smalls)),
        out_specs=(HBM,) * len(shapes),
        out_shape=tuple(jax.ShapeDtypeStruct(*shape) for shape in shapes),
        scratch_shapes=[pltpu.VMEM((total,) + s, low) for s in large]
        + [pltpu.VMEM((ring,) + s, full) for s in large]
        + [pltpu.VMEM(a.shape, a.dtype) for a in smalls]
        + [pltpu.VMEM(*shape) for shape in shapes[2:]]
        + [pltpu.SemaphoreType.DMA(s) for s in ((2, total), (2, ring), (14,))],
        name="outputs",
    )(*in_sums, *out_sums, *smalls)
    gin = gin.reshape(total, width, parts, 2, LANES).transpose(0, 1, 3, 2, 4)
    return gin.reshape(total, width, 2, hidden), *others


def local(
    sizes,
    tokens,
    out_grad,
    doc_ids,
    expert_ids,
    gain_attn,
    w_query,
    w_key_value,
    w_output,
    gain_moe,
    w_router,
    w_expert_in,
    w_expert_out,
):
    rows, cols, depth = sizes
    group = rows * cols
    tok_rows, feat_local = tokens.shape
    width = w_query.shape[0]
    experts = w_router.shape[1]
    expert_local, hidden = w_expert_out.shape[0], w_expert_out.shape[1]
    longest_doc = min(LONGEST, tok_rows * depth // 2)
    hop_count = longest_doc // tok_rows
    own = tok_rows // group
    low, full = jnp.bfloat16, jnp.float32
    layer = lax.axis_index("dp")
    me = lax.axis_index("row") * cols + lax.axis_index("col")
    everyone = list(range(1, depth))
    hops = list(range(1, hop_count + 1))

    w_pair = w_key_value.reshape(width, -1)
    block = (tok_rows, LANES)
    cosine, sine, normed, query, pair, tokens_own, gains, gains_moe, router, docs_far, grads_shifted, grad_blocks = exchange(
        sizes,
        "gather_tokens",
        0,
        ("gather", tokens, False, 2),
        ("share", gain_attn.reshape(1, LANES)),
        ("share", gain_moe.reshape(1, LANES)),
        ("share", w_router.T),
        ("shift", doc_ids.reshape(-1, LANES), everyone, False),
        ("shift", out_grad, everyone, False),
        ("gather", out_grad, False, 2),
        before=Stage(tables_body, [(block, full), (block, full)]),
        after=Stage(
            project_body,
            [((tok_rows, width), low), (block, low), (block, low), ((own, width), low)],
            Got(0),
            Got(1),
            w_query,
            w_pair,
            Made(0),
            Made(1),
        ),
        landing=(0,),
        delayed=(6,),
    )

    stack = (hop_count + 1,) + block
    twice = (2 * tok_rows, LANES)
    turned_block = (LANES, tok_rows)
    whole = (2 * tok_rows, 1)
    grad_own, grads_near, far_turned, start, mixed, log_total, far, output_blocks = exchange(
        sizes,
        "shift_pairs",
        1,
        ("line", pair, False, 2, hop_count),
        ("gather", w_output, False, 4),
        before=Stage(
            attend_first_body,
            [
                ((own, width), low),
                ((group,) + turned_block, low),
                ((depth - 1,) + turned_block, low),
                ((tok_rows, 1), jnp.int32),
            ],
            grad_blocks,
            grads_shifted,
            query,
            pair,
            doc_ids.reshape(-1, LANES),
            docs_far,
        ),
        after=Stage(
            attend_rest_body,
            [(block, low), (whole, full)],
            Got(0),
            Made(3),
        ),
        shared=[
            pltpu.VMEM(stack, low),
            pltpu.VMEM(stack, low),
            pltpu.VMEM(twice, low),
            pltpu.VMEM(twice, full),
            pltpu.VMEM(whole, full),
            pltpu.VMEM(whole, full),
        ],
    )
    output_full = output_blocks.reshape(-1, width)

    rows_own, middle, weights = exchange(
        sizes,
        "swap_mixed",
        2,
        ("swap", mixed.reshape(group, own, LANES)),
        after=Stage(
            middle_body,
            [((own, width + LANES), low), ((own, width), full), ((own, LANES), full)],
            Got(0),
            tokens_own,
            output_full,
            gains_moe,
            router,
            expert_ids.T,
            scratch=[pltpu.VMEM(expert_ids.shape, full)],
        ),
        landing=(0,),
    )
    rows_blocks, rows_shifted = exchange(
        sizes,
        "gather_rows",
        3,
        ("gather", rows_own, False, 2),
        ("line", rows_own, False, 4),
    )
    rows_near = rows_blocks.reshape(tok_rows, -1)
    parts = hidden // LANES
    in_rows = w_expert_in.reshape(expert_local, width, 2, parts, LANES)
    in_rows = in_rows.transpose(0, 1, 3, 2, 4).reshape(expert_local, -1, LANES)
    in_flat, in_part, out_part, moe_partial, back_partial, grads_far, rows_far = local_experts(
        sizes,
        9,
        rows_near,
        grads_near.reshape(width, tok_rows),
        in_rows,
        w_expert_out,
        far_turned,
        rows_shifted,
    )
    rows_far = rows_far.reshape((depth - 1) * tok_rows, -1)
    grads_far = grads_far.reshape(depth - 1, width, tok_rows)
    work = (in_flat, w_expert_out, in_part, out_part, rows_far, grads_far)
    share = expert_local // 4
    unit = 16 * depth
    in_sums, out_sums = [], []

    def beneath(name, number, *items, after=None, landing=()):
        cover = Cover(len(in_sums) * share, share, work)
        in_sum, out_sum, *moved = exchange(
            sizes, name, number, *items, after=after, cover=cover, landing=landing
        )
        if after:
            count = len(after.shapes)
            results = [in_sum, out_sum, *moved]
            in_sum, out_sum = results[count], results[count + 1]
            moved = results[:count] + results[count + 2 :]
        in_sums.append(in_sum)
        out_sums.append(out_sum)
        return moved

    middle_grad, attn_grad, logit_grad, gain_moe_part = beneath(
        "swap_back",
        4,
        ("swap", back_partial.reshape(group, own, -1)),
        after=Stage(
            middle_back_body,
            [
                ((own, width), full),
                ((own, width), low),
                ((own, LANES), low),
                ((1, width), full),
            ],
            Got(0),
            grad_own,
            middle,
            weights,
            gains_moe,
            router,
        ),
        landing=(0,),
    )
    query_grad, pair_grad, far_grad, output_sum, logit_blocks = exchange(
        sizes,
        "gather_attn_grad",
        5,
        ("gather", attn_grad, False, 2),
        ("gather", logit_grad),
        delayed=(1,),
        before=Stage(
            attend_again_body,
            [],
            query,
            pair,
            far,
            start,
            log_total,
            scratch=[pltpu.VMEM(twice, low)],
        ),
        after=Stage(
            attend_back_body,
            [
                (block, low),
                (block, full),
                ((hop_count,) + block, low),
                ((group, LANES, LANES), low),
            ],
            Got(0),
            w_output,
            mixed,
            cosine,
            sine,
            scratch=[
                pltpu.VMEM(twice, low),
                pltpu.VMEM(twice[::-1], low),
                pltpu.VMEM(twice, full),
                pltpu.VMEM((hop_count + 1,) + turned_block, full),
                pltpu.VMEM((hop_count + 1,) + turned_block, full),
            ],
        ),
        landing=(0,),
        shared=[
            pltpu.VMEM(stack, low),
            pltpu.VMEM(stack, low),
            pltpu.VMEM(twice[::-1], low),
            pltpu.VMEM((hop_count + 1, 2 * tok_rows, tok_rows), full),
        ],
    )
    length = (2 * width + experts + unit - 1) // unit * unit
    partial, sums, output_first, output_last, gain_parts, moe_blocks = beneath(
        "shift_grads",
        6,
        ("shift", far_grad, [-d for d in hops], True),
        ("turn", output_sum.reshape(depth, width // depth, LANES)),
        ("swap", moe_partial.reshape(group, own, width)),
        after=Stage(
            project_back_body,
            [
                ((tok_rows, width), low),
                ((length, LANES), low),
                ((width // depth // 2, LANES), low),
                ((width // depth // 2, LANES), low),
                ((group, 8, LANES), full),
            ],
            query_grad,
            pair_grad,
            Got(0),
            normed,
            w_query,
            w_pair,
            cosine,
            sine,
            Got(1),
            logit_blocks,
            rows_near,
            gains,
            gain_moe_part,
        ),
        landing=(0, 1),
    )
    pieces = (group, own, LANES)
    block_out, in_grad, gain_sum, summed, output_first = beneath(
        "swap_partial",
        7,
        ("turn", sums.reshape(depth, length // depth, LANES)),
        ("collect", output_first),
        ("swap", partial.reshape(group, own, width)),
        ("swap", gain_parts),
        after=Stage(
            results_body,
            [(pieces, low), (pieces, low), ((8, LANES), full), ((length // depth, LANES), low)],
            Got(2),
            moe_blocks,
            tokens_own,
            middle,
            middle_grad,
            gains,
            Got(3),
            Got(0),
        ),
        landing=(0, 2, 3),
    )
    sums, output_last, gain_all, block_out, in_grad = beneath(
        "swap_results",
        8,
        ("collect", summed),
        ("collect", output_last),
        ("collect", gain_sum),
        ("swap", block_out),
        ("swap", in_grad),
    )
    grad_in, grad_out, block_out, in_grad, gain_attn_sum, gain_moe_sum, query_sum, pair_sum, output_sum, router_sum = outputs(
        in_sums,
        out_sums,
        hidden,
        experts,
        block_out,
        in_grad,
        gain_all,
        sums.reshape(length, LANES),
        output_first,
        output_last,
    )
    return (
        block_out,
        in_grad,
        gain_attn_sum.reshape(LANES),
        query_sum,
        pair_sum.reshape(w_key_value.shape),
        output_sum,
        gain_moe_sum.reshape(LANES),
        router_sum.T,
        grad_in,
        grad_out,
    )


def solution(mesh):
    in_specs = (
        P("dp", ("row", "col")),
        P("dp", ("row", "col")),
        P("dp"),
        P("dp", None),
        P(("row", "col")),
        P(None, ("row", "col")),
        P(None, ("row", "col"), None),
        P(("row", "col"), None),
        P(("row", "col")),
        P(("row", "col"), None),
        P("row", None, None, "col"),
        P("row", "col", None),
    )
    out_specs = (
        P("dp", ("row", "col")),
        P("dp", ("row", "col")),
        P(("row", "col")),
        P(None, ("row", "col")),
        P(None, ("row", "col"), None),
        P(("row", "col"), None),
        P(("row", "col")),
        P(("row", "col"), None),
        P("row", None, None, "col"),
        P("row", "col", None),
    )
    sizes = (mesh.shape["row"], mesh.shape["col"], mesh.shape["dp"])
    return jax.shard_map(
        functools.partial(local, sizes),
        mesh=mesh,
        in_specs=in_specs,
        out_specs=out_specs,
        check_vma=False,
    )
```

```python
import functools
import itertools
import math

import jax
import jax.numpy as jnp
from jax import lax
from jax.experimental import pallas as pl
from jax.experimental.pallas import tpu as pltpu
from jax.sharding import PartitionSpec as P

LONGEST = 4096
EPSILON = 1e-05
RESIDUAL_SCALE = 0.22
SCORE_SCALE = 0.015625
ROPE_BASE = 10000.0
MASKED = -1e30
MESH = pl.DeviceIdType.MESH
GROUP = ("row", "col")
EVERY = ("dp", "row", "col")
LANES = 128
HBM = pl.BlockSpec(memory_space=pl.ANY)
TURN = LANES // 4


class Moves:
    def __init__(self, sizes, kinds, sources, targets, sems):
        self.sizes, self.kinds = sizes, kinds
        self.sources, self.targets = sources, targets
        self.send_sem, self.recv_sem, self.local_sem = sems

    def place(self):
        row, col, layer = lax.axis_index("row"), lax.axis_index("col"), lax.axis_index("dp")
        return row, col, layer, row * self.sizes[1] + col

    def member(self, index):
        rows, cols, depth = self.sizes
        return {"row": index // cols, "col": lax.rem(index, cols)}

    def across(self, row):
        low = lax.rem(row, 2)
        return row + 1 - 2 * low, lax.rem(row + 2, 4), lax.rem(row + 3 - 2 * low, 4)

    def barrier(self):
        rows, cols, depth = self.sizes
        row, col, layer, me = self.place()
        group = rows * cols
        names = [kind[0] for kind in self.kinds]
        barrier = pltpu.get_barrier_semaphore()
        partners = []
        if "swap" in names or "share" in names:
            for k in range(1, group):
                partners.append(self.member(lax.rem(me + k, group)))
        elif "gather" in names:
            for other in self.across(row)[:2]:
                partners.append({"row": other})
            for k in range(1, cols):
                partners.append({"col": lax.rem(col + k, cols)})
        shifts = set()
        for kind in self.kinds:
            if kind[0] == "shift":
                for d in kind[1]:
                    shifts |= {d % depth, -d % depth}
            elif kind[0] in ("turn", "collect"):
                shifts |= set(range(1, depth))
        for k in sorted(shifts - {0}):
            partners.append({"dp": lax.rem(layer + k, depth)})
        ends = [(layer > 0, layer - 1), (layer < depth - 1, layer + 1)]
        ends = ends if "line" in names and not shifts else []
        for partner in partners:
            pl.semaphore_signal(barrier, inc=1, device_id=partner, device_id_type=MESH)
        for there, other in ends:

            @pl.when(there)
            def _(device={"dp": other}):
                pl.semaphore_signal(barrier, inc=1, device_id=device, device_id_type=MESH)

        expected = len(partners)
        for there, _ in ends:
            expected = expected + there.astype(jnp.int32)
        pl.semaphore_wait(barrier, expected)

    def plan(self, only):
        rows, cols, depth = self.sizes
        row, col, layer, me = self.place()
        group = rows * cols
        slots = iter(range(self.send_sem.shape[0]))
        starts, relays, sends, arrivals, local = [], [], [], [], []

        def remote(source, target, device, slot=None):
            slot = next(slots) if slot is None else slot
            return functools.partial(
                pltpu.make_async_remote_copy,
                src_ref=source,
                dst_ref=target,
                send_sem=self.send_sem.at[slot],
                recv_sem=self.recv_sem.at[slot],
                device_id=device,
                device_id_type=MESH,
            )

        for index, (kind, source, target) in enumerate(
            zip(self.kinds, self.sources, self.targets)
        ):
            item = [], [], [], [], []
            begin, follow, sent, got, stay = item

            def keep(source, target):
                sem = self.local_sem.at[index]
                stay.append(functools.partial(pltpu.make_async_copy, source, target, sem))

            def direct(source, target, device):
                copy = None, remote(source, target, device)
                begin.append(copy)
                sent.append(copy)
                got.append(copy)

            if kind[0] == "gather":
                second, parts = kind[1:]
                size = source.shape[0] // parts
                beside, above, away = self.across(row)

                def at(other, part, piece=None):
                    member = other * cols + col
                    first, length, deep = part * size, size, ()
                    if piece is not None and size % 2 == 0:
                        length = size // 2
                        first = first + piece * length
                    elif piece is not None:
                        inner = source.shape[1] // 2
                        deep = (pl.ds(piece * inner, inner),)
                    some = pl.ds(first, length)
                    return target.at[(some, member) + deep if second else (member, some) + deep]

                def to_mates(piece):
                    made = []
                    for j in range(1, cols):
                        copy = None, remote(piece, piece, {"col": lax.rem(col + j, cols)})
                        made.append(copy)
                        sent.append(copy)
                        got.append(copy)
                    return made

                for part in range(parts):
                    some = source.at[pl.ds(part * size, size)]
                    ways = []
                    for near, other, piece in ((beside, above, 0), (above, beside, 1)):
                        first = None, remote(some, at(row, part), {"row": near})
                        passed = at(near, part, piece)
                        onward = None, remote(passed, passed, {"row": other})
                        begin.append(first)
                        sent.extend([first, onward])
                        ways.append((near, piece, first, onward))
                    for near, piece, first, onward in ways:
                        nexts = [onward] + to_mates(at(near, part))
                        follow.append((2 + 3 * part, 0, None, first[1], nexts))
                    for near, piece, first, onward in ways:
                        nexts = to_mates(at(away, part, piece))
                        follow.append((2 + 3 * parts + part, 1, None, onward[1], nexts))
                    for j in range(1, cols):
                        direct(some, at(row, part), {"col": lax.rem(col + j, cols)})
                keep(source, target.at[:, me] if second else target.at[me])
            elif kind[0] in ("swap", "share"):
                for k in range(1, group):
                    other = lax.rem(me + k, group)
                    piece = source.at[other] if kind[0] == "swap" else source
                    direct(piece, target.at[me], self.member(other))
                keep(source.at[me] if kind[0] == "swap" else source, target.at[me])
            elif kind[0] in ("turn", "collect"):
                for k in range(1, depth):
                    other = lax.rem(layer + k, depth)
                    piece = source.at[other] if kind[0] == "turn" else source
                    direct(piece, target.at[layer], {"dp": other})
                keep(source.at[layer] if kind[0] == "turn" else source, target.at[layer])
            elif kind[0] == "line":
                absolute, parts, limit = kind[1:]
                size = source.shape[0] // parts
                steps = limit or depth - 1
                ways = (1,) if limit else (1, -1)
                for part, way in itertools.product(range(parts), ways):
                    behind = layer if way == 1 else depth - 1 - layer
                    onward = layer + way
                    more = (onward >= 0) & (onward < depth)
                    mine = [next(slots) for _ in range(steps)]
                    some = pl.ds(part * size, size)

                    def held(step, where, way=way, some=some):
                        if step == 0:
                            return source.at[some]
                        if absolute:
                            return target.at[where - way * step, some]
                        return target.at[step - 1 if way == 1 else depth - 1 - step, some]

                    def sending(step, onward=onward, mine=mine, held=held):
                        device = {"dp": onward}
                        return remote(
                            held(step - 1, layer), held(step, onward), device, mine[step - 1]
                        )

                    begin.append((more, sending(1)))
                    for step in range(1, steps + 1):
                        sent.append((more & (behind >= step - 1), sending(step)))
                        block = held(step, layer)
                        arrival = remote(block, block, {"dp": onward}, mine[step - 1])
                        nexts = [(more, sending(step + 1))] if step < steps else []
                        when = 4 * step + part
                        follow.append((when, step - 1, behind >= step, arrival, nexts))
                if absolute:
                    keep(source, target.at[layer])
            else:
                for at_slot, d in enumerate(kind[1]):
                    piece = source.at[at_slot] if kind[2] else source
                    direct(piece, target.at[at_slot], {"dp": lax.rem(layer + d % depth, depth)})
            if only is None or index in only:
                starts += begin
                relays += follow
                sends += sent
                arrivals += got
                local += stay
        return starts, sorted(relays, key=lambda entry: entry[0]), sends, arrivals, local

    def given(self, condition, action):
        if condition is None:
            action()
        else:
            pl.when(condition)(action)

    def start(self, only=None):
        starts, _, _, _, local = self.plan(only)
        for condition, copy in starts:
            self.given(condition, lambda copy=copy: copy().start())
        for copy in local:
            copy().start()

    def relay(self, only=None, stages=None):
        for _, stage, condition, copy, nexts in self.plan(only)[1]:
            if stages is not None and stage not in stages:
                continue

            def action(copy=copy, nexts=nexts):
                copy().wait_recv()
                for more, follower in nexts:
                    self.given(more, lambda follower=follower: follower().start())

            self.given(condition, action)

    def finish(self, only=None):
        _, _, sends, arrivals, local = self.plan(only)
        for condition, copy in arrivals:
            self.given(condition, lambda copy=copy: copy().wait_recv())
        for condition, copy in sends:
            self.given(condition, lambda copy=copy: copy().wait_send())
        for copy in local:
            copy().wait()


def planned(sizes, items):
    rows, cols, depth = sizes
    group = rows * cols
    kinds, shapes, copies = [], [], 0
    for item in items:
        name, array = item[0], item[1]
        shape = array.shape
        if name == "gather":
            assert rows == 4
            second, parts = (item[2:] + (False, 1)[len(item) - 2 :])[:2]
            kinds.append((name, second, parts))
            shape = (shape[0], group) + shape[1:] if second else (group,) + shape
            copies += parts * (4 + 5 * (cols - 1))
        elif name == "shift":
            distances, split = item[2], item[3]
            kinds.append((name, tuple(distances), split))
            shape = (len(distances),) + (shape[1:] if split else shape)
            copies += len(distances)
        elif name == "line":
            parts, limit = (item[3:] + (1, 0)[len(item) - 3 :])[:2]
            kinds.append((name, item[2], parts, limit))
            shape = (depth if item[2] else limit or depth - 1,) + shape
            copies += (limit or 2 * (depth - 1)) * parts
        else:
            kinds.append((name,))
            if name in ("share", "collect"):
                shape = (group if name == "share" else depth,) + shape
            copies += (depth if name in ("turn", "collect") else group) - 1
        shapes.append(jax.ShapeDtypeStruct(shape, array.dtype))
    sems = [
        pltpu.SemaphoreType.DMA((copies,)),
        pltpu.SemaphoreType.DMA((copies,)),
        pltpu.SemaphoreType.DMA((len(items),)),
    ]
    return tuple(kinds), shapes, sems


class Got:
    def __init__(self, index):
        self.index = index


class Made:
    def __init__(self, index):
        self.index = index


class Stage:
    def __init__(self, body, shapes, *operands, scratch=()):
        self.body, self.shapes, self.operands = body, shapes, operands
        self.scratch = list(scratch)


def exchange(sizes, name, number, *items, before=None, after=None, cover=None, landing=(), shared=(), delayed=()):
    kinds, moved, sems = planned(sizes, items)
    stages = [stage for stage in (before, after) if stage]
    operands = []
    for stage in stages:
        for operand in stage.operands:
            if not isinstance(operand, (Got, Made)):
                operands.append(operand)
    work = list(cover.work) if cover else []
    outs = [s for stage in stages for s in stage.shapes]
    made_shapes = list(cover.shapes) if cover else []
    flown = [i for i in range(len(items)) if i not in landing]
    late = [o.index for o in (after.operands if after else ()) if isinstance(o, Got)]
    late = [i for i in late if i not in landing]
    scratch = []

    def take(shapes):
        first = len(scratch)
        scratch.extend(shapes)
        return slice(first, len(scratch))

    vmem = lambda s: pltpu.VMEM(tuple(s[0]), s[1])
    of = lambda a: (a.shape, a.dtype)
    operand_at = take([vmem(of(a)) for a in operands])
    result_at = take([vmem(s) for s in outs])
    landed_at = take([vmem(of(moved[i])) for i in landing])
    late_at = take([vmem(of(moved[i])) for i in late])
    stage_at = [take(stage.scratch) for stage in stages]
    shared_at = take(list(shared))
    needed = sorted({o.index for o in (after.operands if after else ()) if isinstance(o, Got)})
    others = [i for i in range(len(items)) if i not in needed]
    prompt = [i for i in range(len(items)) if i not in delayed]
    later = range(1, 2 * sizes[2])
    cover_at = take(cover.scratch) if cover else slice(0, 0)
    copies = len(operands) + len(outs) + len(late)
    copy_at = take([pltpu.SemaphoreType.DMA((max(1, copies),))])
    sems_at = take(sems)

    def body(*refs):
        cuts = [len(operands), len(work), len(items), len(outs), len(made_shapes), len(flown)]
        groups = []
        for cut in cuts:
            groups.append(refs[:cut])
            refs = refs[cut:]
        given, work_refs, sources, results, made_refs, flown_refs = groups
        loaded, held = refs[operand_at], refs[result_at]
        landed, lates, (copy_sem,) = refs[landed_at], refs[late_at], refs[copy_at]
        targets = [None] * len(items)
        for i, ref in zip(flown, flown_refs):
            targets[i] = ref
        for i, ref in zip(landing, landed):
            targets[i] = ref
        moves = Moves(sizes, kinds, sources, targets, refs[sems_at])
        number_of = iter(range(copies))
        copy = lambda a, b: pltpu.make_async_copy(a, b, copy_sem.at[next(number_of)])
        loads = [copy(a, b) for a, b in zip(given, loaded)]
        stores = [copy(a, b) for a, b in zip(held, results)]
        late_loads = [copy(targets[i], b) for i, b in zip(late, lates)]
        split = len([o for o in before.operands if not isinstance(o, Made)]) if before else 0
        first = len(before.shapes) if before else 0
        for load in loads:
            load.start()
        if cover:
            cover.begin(work_refs, refs[cover_at])
        moves.barrier()
        moves.start(prompt)
        if before:
            for load in loads[:split]:
                load.wait()
            before.body(*loaded[:split], *held[:first], *refs[stage_at[0]], *refs[shared_at])
            for store in stores[:first]:
                store.start()
        if cover:
            cover.run(work_refs, made_refs, refs[cover_at])
        moves.relay(prompt, (0,))
        moves.start(delayed)
        if after:
            moves.relay(needed, later)
            moves.finish(needed)
        moves.relay(delayed, (0,))
        if after:
            for load in late_loads:
                load.start()
            for load in loads[split:]:
                load.wait()
            for load in late_loads:
                load.wait()
            plain = iter(loaded[split:])
            values = []
            for operand in after.operands:
                if isinstance(operand, Made):
                    values.append(held[operand.index])
                elif isinstance(operand, Got) and operand.index in landing:
                    values.append(landed[landing.index(operand.index)])
                elif isinstance(operand, Got):
                    values.append(lates[late.index(operand.index)])
                else:
                    values.append(next(plain))
            after.body(*values, *held[first:], *refs[stage_at[-1]], *refs[shared_at])
            for store in stores[first:]:
                store.start()
        moves.relay(others, later)
        moves.finish(others)
        if cover:
            cover.end(made_refs, refs[cover_at])
        for store in stores:
            store.wait()

    shape = lambda s: jax.ShapeDtypeStruct(tuple(s[0]), s[1])
    return pl.pallas_call(
        body,
        out_shape=tuple(shape(s) for s in outs + made_shapes) + tuple(moved[i] for i in flown),
        in_specs=[HBM] * (len(operands) + len(work) + len(items)),
        out_specs=(HBM,) * (len(outs) + len(made_shapes) + len(flown)),
        scratch_shapes=scratch,
        compiler_params=pltpu.CompilerParams(collective_id=number, has_side_effects=True),
        name=name,
    )(*operands, *work, *[item[1] for item in items])


def dot(a, b, left=1, right=0, precision=None):
    return lax.dot_general(
        a,
        b,
        (((left,), (right,)), ((), ())),
        preferred_element_type=jnp.float32,
        precision=precision,
    )


def widened(source, target):
    size = target.shape[0] // 4

    def piece(i, carry):
        at = pl.ds(pl.multiple_of(i * size, size), size)
        target[at, :] = source[at, :].astype(target.dtype)
        return carry

    lax.fori_loop(0, 4, piece, 0)


def cleared(target):
    size = target.shape[0] // 8

    def piece(i, carry):
        at = pl.ds(pl.multiple_of(i * size, size), size)
        target[at, :] = jnp.zeros((size, target.shape[1]), target.dtype)
        return carry

    lax.fori_loop(0, 8, piece, 0)


def lanes_of(shape):
    return lax.broadcasted_iota(jnp.int32, shape, len(shape) - 1)


def flipped(values):
    lanes = lanes_of(values.shape)
    ahead = pltpu.roll(values, LANES - TURN, 1)
    behind = pltpu.roll(values, TURN, 1)
    return jnp.where(lanes % (2 * TURN) < TURN, ahead, behind)


def beside(blocks_ref):
    return jnp.concatenate([blocks_ref[i] for i in range(blocks_ref.shape[0])], axis=1)


def gain_row(gains_ref):
    return beside(gains_ref).astype(jnp.float32)


def added(blocks):
    def more(i, total):
        return total + blocks[i].astype(jnp.float32)

    return lax.fori_loop(1, blocks.shape[0], more, blocks[0].astype(jnp.float32))


def own_rows(count):
    me = lax.axis_index("row") * lax.axis_size("col") + lax.axis_index("col")
    return pl.ds(pl.multiple_of(me * count, count), count)


def column(row):
    return jnp.broadcast_to(row, (8, row.shape[1])).T[:, 0:1]


def tables_body(cosine, sine):
    step = 64
    lanes = lanes_of((step, LANES))
    power = (lanes % TURN).astype(jnp.float32) * (-math.log(ROPE_BASE) / TURN)
    frequencies = jnp.exp(power)
    base = lax.axis_index("dp") * cosine.shape[0]

    def piece(i, carry):
        at = pl.ds(pl.multiple_of(i * step, step), step)
        positions = base + i * step + lax.broadcasted_iota(jnp.int32, lanes.shape, 0)
        angles = positions.astype(jnp.float32) * frequencies
        cosine[at, :] = jnp.cos(angles)
        value = jnp.sin(angles)
        sine[at, :] = jnp.where(lanes % (2 * TURN) < TURN, -value, value)
        return carry

    lax.fori_loop(0, cosine.shape[0] // step, piece, 0)


def turned(source, target):
    def block(i, carry):
        scaled = RESIDUAL_SCALE * source[i].astype(jnp.float32)
        target[i] = scaled.T.astype(jnp.bfloat16)
        return carry

    lax.fori_loop(0, target.shape[0], block, 0)


def project_body(blocks, gains, w_query, w_pair, cosine, sine, normed, query, pair, own):
    gain = gain_row(gains)
    step = 128

    def piece(i, carry):
        at = pl.ds(pl.multiple_of(i * step, step), step)
        parts = [blocks[k, at, :] for k in range(blocks.shape[0])]
        tokens = jnp.concatenate(parts, axis=1).astype(jnp.float32)
        scale = lax.rsqrt(jnp.mean(tokens * tokens, axis=1, keepdims=True) + EPSILON)
        normed[at, :] = (tokens * scale * gain).astype(jnp.bfloat16)
        return carry

    lax.fori_loop(0, normed.shape[0] // step, piece, 0)
    raw = dot(normed[...], w_query[...])
    query[...] = (raw * cosine[...] + flipped(raw) * sine[...]).astype(jnp.bfloat16)
    raw = dot(normed[...], w_pair[...])
    keys = lanes_of(raw.shape) < LANES // 2
    turned = raw * cosine[...] + flipped(raw) * sine[...]
    pair[...] = jnp.where(keys, turned, raw).astype(jnp.bfloat16)
    for i in range(blocks.shape[0]):
        own[:, i * LANES : (i + 1) * LANES] = blocks[i, own_rows(own.shape[0]), :]


def doubled(pair, keys_ref, values_ref, at, distance=0):
    wide = pair.astype(jnp.float32)
    if distance:
        wide = jnp.where(lax.axis_index("dp") >= distance, wide, 0.0)
    other = pltpu.roll(wide, LANES // 2, 1)
    keys = lanes_of(wide.shape) < LANES // 2
    keys_ref[at] = jnp.where(keys, wide, other).astype(jnp.bfloat16)
    values_ref[at] = jnp.where(keys, other, wide).astype(jnp.bfloat16)


def per_head(values):
    first = lanes_of(values.shape) < LANES // 2
    zero = jnp.zeros_like(values)
    return jnp.concatenate(
        [jnp.where(first, values, zero), jnp.where(first, zero, values)], axis=0
    )


def tile_scores(queries, keys_ref, starts, row, block, last, tokens):
    scores = dot(queries, keys_ref[block], 1, 1) * SCORE_SCALE
    at = lanes_of(scores.shape) + block * tokens
    allowed = at >= starts
    if block == last:
        place = row + lax.broadcasted_iota(jnp.int32, scores.shape, 0)
        allowed = allowed & (at <= place + block * tokens)
    return jnp.where(allowed, scores, MASKED)


def doc_row(docs):
    rows = [docs[i : i + 1, :] for i in range(docs.shape[0])]
    return jnp.concatenate(rows, axis=1).astype(jnp.float32)


def attend_tiles(tokens, tile):
    step = 256

    def body(i, carry):
        rows = pl.ds(pl.multiple_of(i * step, step), step)
        tile(rows, lax.rem(i * step, tokens), step)
        return carry

    lax.fori_loop(0, 2 * tokens // step, body, 0)


def attend_first_body(near_grads, far_grads, query, pair, docs, far_docs, own_grad, near_turned, far_turned, start, keys, values, queries, out, tops, totals):
    turned(near_grads, near_turned)
    turned(far_grads, far_turned)
    for i in range(near_grads.shape[0]):
        own_grad[:, i * LANES : (i + 1) * LANES] = near_grads[i, own_rows(own_grad.shape[0]), :]
    tokens = query.shape[0]
    last = keys.shape[0] - 1
    layer = lax.axis_index("dp")
    here = doc_row(docs[...])
    mine = column(here)
    before = jnp.sum((here < mine).astype(jnp.float32), axis=1, keepdims=True)
    for d in range(1, last + 1):
        fewer = (doc_row(far_docs[d - 1]) < mine) | (layer < d)
        before = before + jnp.sum(fewer.astype(jnp.float32), axis=1, keepdims=True)
    start[...] = before.astype(jnp.int32)
    doubled(pair[...], keys, values, last)
    queries[...] = per_head(query[...].astype(jnp.float32)).astype(jnp.bfloat16)

    def tile(rows, row, step):
        starts = start[pl.ds(pl.multiple_of(row, step), step), :]
        scores = tile_scores(queries[rows, :], keys, starts, row, last, last, tokens)
        top = jnp.max(scores, axis=1, keepdims=True)
        terms = jnp.exp(scores - top)
        tops[rows, :] = top
        totals[rows, :] = jnp.sum(terms, axis=1, keepdims=True)
        out[rows, :] = dot(terms.astype(jnp.bfloat16), values[last])

    attend_tiles(tokens, tile)


def attend_rest_body(far, start, mixed, log_total, keys, values, queries, out, tops, totals):
    last, tokens = far.shape[0], far.shape[1]
    for d in range(1, last + 1):
        doubled(far[d - 1], keys, values, last - d, d)

    def tile(rows, row, step):
        starts = start[pl.ds(pl.multiple_of(row, step), step), :]
        parts = [
            tile_scores(queries[rows, :], keys, starts, row, block, last, tokens)
            for block in range(last)
        ]
        top = functools.reduce(
            jnp.maximum, [jnp.max(part, axis=1, keepdims=True) for part in parts], tops[rows, :]
        )
        parts = [jnp.exp(part - top) for part in parts]
        scale = jnp.exp(tops[rows, :] - top)
        total = functools.reduce(
            jnp.add,
            [jnp.sum(p, axis=1, keepdims=True) for p in parts],
            totals[rows, :] * scale,
        )
        sums = [
            dot(part.astype(jnp.bfloat16), values[block]) for block, part in enumerate(parts)
        ]
        out[rows, :] = functools.reduce(jnp.add, sums, out[rows, :] * scale) / total
        log_total[rows, :] = top + jnp.log(total)

    attend_tiles(tokens, tile)
    first = lanes_of((tokens, LANES)) < LANES // 2
    mixed[...] = jnp.where(first, out[:tokens, :], out[tokens:, :]).astype(jnp.bfloat16)


def attend_again_body(query, pair, far, start, log_total, queries, keys, values, queries_turned, chances):
    tokens = query.shape[0]
    last = far.shape[0]
    doubled(pair[...], keys, values, last)
    for d in range(1, last + 1):
        doubled(far[d - 1], keys, values, last - d, d)
    stacked = per_head(query[...].astype(jnp.float32))
    queries[...] = stacked.astype(jnp.bfloat16)
    queries_turned[...] = stacked.T.astype(jnp.bfloat16)

    def tile(rows, row, step):
        starts = start[pl.ds(pl.multiple_of(row, step), step), :]
        for block in range(last + 1):
            scores = tile_scores(queries[rows, :], keys, starts, row, block, last, tokens)
            chances[block, rows, :] = jnp.exp(scores - log_total[rows, :])

    attend_tiles(tokens, tile)


def attend_back_body(grad, w_output, mixed, cosine, sine, query_grad, pair_grad, far_grad, output_grad, grads, grads_turned, turned, key_sums, value_sums, keys, values, queries_turned, chances):
    tokens = mixed.shape[0]
    last = keys.shape[0] - 1
    given_grad = grad[...].reshape(tokens, -1)
    stacked = per_head(dot(given_grad, w_output[...], 1, 1))
    grads[...] = stacked.astype(jnp.bfloat16)
    grads_turned[...] = stacked.T.astype(jnp.bfloat16)
    output_sum = dot(mixed[...], given_grad, 0, 0).astype(jnp.bfloat16)
    for i in range(output_grad.shape[0]):
        output_grad[i] = output_sum[:, i * LANES : (i + 1) * LANES]
    for block in range(last + 1):
        cleared(key_sums.at[block])
        cleared(value_sums.at[block])

    def tile(rows, row, step):
        given = grads[rows, :]
        asked_turned, given_turned = queries_turned[:, rows], grads_turned[:, rows]
        products = [dot(given, values[block], 1, 1) for block in range(last + 1)]
        delta = functools.reduce(
            jnp.add,
            [
                jnp.sum(chances[block, rows, :] * product, axis=1, keepdims=True)
                for block, product in enumerate(products)
            ],
        )
        total = jnp.zeros((step, LANES), jnp.float32)
        for block in range(last + 1):
            chance = chances[block, rows, :]
            back = (chance * (products[block] - delta)).astype(jnp.bfloat16)
            total = total + dot(back, keys[block])
            key_sums[block] += dot(asked_turned, back)
            value_sums[block] += dot(given_turned, chance.astype(jnp.bfloat16))
        turned[rows, :] = total

    attend_tiles(tokens, tile)
    first = lanes_of((tokens, LANES)) < LANES // 2
    raw = jnp.where(first, turned[:tokens, :], turned[tokens:, :]) * SCORE_SCALE
    query_grad[...] = (raw * cosine[...] - flipped(raw) * sine[...]).astype(jnp.bfloat16)

    def joined(block):
        by_key, by_value = key_sums[block].T, value_sums[block].T
        by_key = (by_key + pltpu.roll(by_key, LANES // 2, 1)) * SCORE_SCALE
        by_value = by_value + pltpu.roll(by_value, LANES // 2, 1)
        return jnp.where(first, by_key, by_value)

    pair_grad[...] = joined(last)
    for d in range(1, last + 1):
        far_grad[d - 1] = joined(last - d).astype(jnp.bfloat16)


def router_rows(router):
    rows = beside(router)
    blank = jnp.zeros((LANES - rows.shape[0], rows.shape[1]), rows.dtype)
    return jnp.concatenate([rows, blank], axis=0)


def full_dot(wide, low, left=1, right=0):
    parts, rest = [], wide
    for _ in range(3):
        parts.append(rest.astype(jnp.bfloat16))
        rest = rest - parts[-1].astype(jnp.float32)
    count = wide.shape[0]
    sums = dot(jnp.concatenate(parts, axis=0), low, left, right)
    return sums[:count] + (sums[count : 2 * count] + sums[2 * count :])


def middle_body(mixed, own, w_output, gains, router, ids_turned, rows, middle, weights, ids_ref):
    experts = router.shape[1]
    width = own.shape[1]
    attn = dot(beside(mixed), w_output[...])
    value = own[...].astype(jnp.float32) + RESIDUAL_SCALE * attn
    middle[...] = value
    scale = lax.rsqrt(jnp.mean(value * value, axis=1, keepdims=True) + EPSILON)
    normed = value * scale * gain_row(gains)
    logits = full_dot(normed, router_rows(router), 1, 1)
    count = own.shape[0]
    ids_ref[...] = ids_turned[...].astype(jnp.float32).T
    ids = ids_ref[own_rows(count), :]
    lanes = lanes_of((count, LANES))
    chosen = jnp.zeros((count, LANES), jnp.float32)
    for k in range(ids.shape[1]):
        chosen = chosen + (ids[:, k : k + 1] == lanes.astype(jnp.float32)).astype(
            jnp.float32
        )
    top = jnp.max(jnp.where(lanes < experts, logits, MASKED), axis=1, keepdims=True)
    terms = jnp.exp(jnp.minimum(logits - top, 0.0)) * chosen
    share = terms / jnp.sum(terms, axis=1, keepdims=True)
    weights[...] = share
    high = share.astype(jnp.bfloat16)
    low = share - high.astype(jnp.float32)
    rows[:, :width] = normed.astype(jnp.bfloat16)
    rows[:, width:] = (high.astype(jnp.float32) + pltpu.roll(low, LANES // 2, 1)).astype(
        jnp.bfloat16
    )


def middle_back_body(back, out_grad, middle, weights, gains, router, middle_grad, attn_grad, logit_grad, gain_part):
    width = middle.shape[1]
    normed_grad = back[0, :, :width].astype(jnp.float32)
    weight_grad = back[0, :, width:].astype(jnp.float32)
    for i in range(1, back.shape[0]):
        normed_grad = normed_grad + back[i, :, :width].astype(jnp.float32)
        weight_grad = weight_grad + back[i, :, width:].astype(jnp.float32)
    share, value = weights[...], middle[...]
    mean = jnp.sum(share * weight_grad, axis=1, keepdims=True)
    logit = share * (weight_grad - mean)
    logit_grad[...] = logit.astype(jnp.bfloat16)
    normed_grad = normed_grad + full_dot(logit, router_rows(router))
    scale = lax.rsqrt(jnp.mean(value * value, axis=1, keepdims=True) + EPSILON)
    gain_part[...] = jnp.sum(normed_grad * value * scale, axis=0, keepdims=True)
    scaled = normed_grad * gain_row(gains)
    norm_dot = jnp.sum(scaled * value, axis=1, keepdims=True)
    total = (
        out_grad[...].astype(jnp.float32)
        + scale * scaled
        - value * (scale * scale * scale * norm_dot / width)
    )
    middle_grad[...] = total
    attn_grad[...] = (RESIDUAL_SCALE * total).astype(jnp.bfloat16)


def project_back_body(query_grad, pair_grad, returned, normed, w_query, w_pair, cosine, sine, output_turned, logit, rows, gains, gain_moe, partial, sums, output_first, output_last, gain_parts):
    layer = lax.axis_index("dp")
    depth = lax.axis_size("dp")
    total = pair_grad[...]
    for i in range(returned.shape[0]):
        total = total + jnp.where(
            layer + i + 1 < depth, returned[i].astype(jnp.float32), 0.0
        )
    keys = lanes_of(total.shape) < LANES // 2
    turned = total * cosine[...] - flipped(total) * sine[...]
    pair_low = jnp.where(keys, turned, total).astype(jnp.bfloat16)
    query_low = query_grad[...]
    whole = dot(query_low, w_query[...], 1, 1) + dot(pair_low, w_pair[...], 1, 1)
    partial[...] = whole.astype(jnp.bfloat16)
    gain_attn = jnp.sum(whole * normed[...].astype(jnp.float32), axis=0, keepdims=True)
    gain_attn = gain_attn / gain_row(gains)
    gain_parts[...] = jnp.zeros_like(gain_parts)
    for i in range(gain_parts.shape[0]):
        at = slice(i * LANES, (i + 1) * LANES)
        gain_parts[i, 0:1, :] = gain_attn[:, at]
        gain_parts[i, 1:2, :] = gain_moe[0:1, at]
    width = normed.shape[1]
    sums[:width, :] = dot(normed[...], query_low, 0, 0).astype(jnp.bfloat16)
    sums[width : 2 * width, :] = dot(normed[...], pair_low, 0, 0).astype(jnp.bfloat16)
    output_sum = added(output_turned).astype(jnp.bfloat16)
    output_first[...] = output_sum[: output_first.shape[0], :]
    output_last[...] = output_sum[output_first.shape[0] :, :]
    mine = rows[:, own_rows(LANES)]
    named = logit[...].reshape(normed.shape[0], LANES)
    router_sum = dot(named, mine, 0, 0).astype(jnp.bfloat16)
    count = min(LANES, sums.shape[0] - 2 * width)
    sums[2 * width : 2 * width + count, :] = router_sum[:count, :]


def results_body(blocks, moe, own, middle, middle_grad, gains, gain_blocks, turned, block_out, in_grad, gain_sum, summed):
    gain_sum[...] = added(gain_blocks)
    summed[...] = added(turned).astype(jnp.bfloat16)
    width = own.shape[1]
    normed_grad = added(blocks)
    branch = added(moe)
    value = own[...].astype(jnp.float32)
    scale = lax.rsqrt(jnp.mean(value * value, axis=1, keepdims=True) + EPSILON)
    scaled = normed_grad * gain_row(gains)
    norm_dot = jnp.sum(scaled * value, axis=1, keepdims=True)
    grad = (
        middle_grad[...] + scale * scaled - value * (scale * scale * scale * norm_dot / width)
    ).astype(jnp.bfloat16)
    out = (middle[...] + RESIDUAL_SCALE * branch).astype(jnp.bfloat16)
    for i in range(block_out.shape[0]):
        at = slice(i * LANES, (i + 1) * LANES)
        block_out[i] = out[:, at]
        in_grad[i] = grad[:, at]


def expert_terms(gate_up, active_grad, weight):
    hidden = active_grad.shape[0]
    gate, up = gate_up[:hidden], gate_up[hidden:]
    sigmoid = jax.nn.sigmoid(gate)
    silu = gate * sigmoid
    ungated = silu * up
    active = (ungated * weight).astype(jnp.bfloat16)
    scaled = active_grad * weight
    gate_grad = (scaled * up * sigmoid * (1.0 + gate * (1.0 - sigmoid))).astype(jnp.bfloat16)
    up_grad = (scaled * silu).astype(jnp.bfloat16)
    return active, jnp.concatenate([gate_grad, up_grad], axis=0), active_grad * ungated


def weight_rows(extra):
    turned = extra.astype(jnp.float32).T
    return turned[: LANES // 2] + turned[LANES // 2 :]


def local_experts_body(sizes, kinds, rows_hbm, grads_hbm, in_ref, out_ref, sent_grads, sent_rows, flat_ref, in_sum, out_sum, moe_hbm, back_hbm, got_grads, got_rows, rows_ref, grads_ref, moe_ref, back_ref, moe_acc, back_acc, share, weights, spread, copy_sem, *sems):
    step, steps = pl.program_id(0), pl.num_programs(0)
    each, hidden, width = out_ref.shape
    parts = hidden // LANES
    moves = Moves(sizes, kinds, [sent_grads, sent_rows], [got_grads, got_rows], sems)
    ends = [(rows_hbm, rows_ref), (grads_hbm, grads_ref), (moe_ref, moe_hbm), (back_ref, back_hbm)]
    copy = lambda i: pltpu.make_async_copy(*ends[i], copy_sem.at[i])

    @pl.when(step == 0)
    def _():
        copy(0).start()
        copy(1).start()
        moves.barrier()
        moves.start([0])
        cleared(moe_acc)
        cleared(back_acc)
        copy(0).wait()
        copy(1).wait()
        share[...] = jnp.zeros_like(share)
        weights[...] = weight_rows(rows_ref[:, width:])

    @pl.when(step == steps // 8)
    def _():
        moves.start([1])

    for when, item, stage in ((3, 0, 0), (5, 1, 0), (7, 0, 1)):

        @pl.when(step == when * steps // 8)
        def _(item=item, stage=stage):
            moves.relay([item], (stage,))

    for i in range(each):
        spread[i] = in_ref[i].astype(jnp.float32)
        for part in range(parts):
            for half in range(2):
                at = half * hidden + part * LANES
                flat_ref[i, :, at : at + LANES] = spread[
                    i, pl.ds(part * 2 + half, width, stride=2 * parts), :
                ].astype(jnp.bfloat16)
        expert = (lax.axis_index("row") * steps + step) * each + i
        active, gate_up_grad, shares = expert_terms(
            dot(flat_ref[i], rows_ref[:, :width], 0, 1),
            dot(out_ref[i], grads_ref[...]),
            weights[pl.ds(expert, 1), :],
        )
        share[pl.ds(expert, 1), :] = jnp.sum(shares, axis=0, keepdims=True)
        moe_acc[...] += dot(active, out_ref[i], 0, 0)
        back_acc[...] += dot(gate_up_grad, flat_ref[i], 0, 1)
        in_sum[i] = dot(gate_up_grad, rows_ref[:, :width]).astype(jnp.bfloat16)
        out_sum[i] = dot(active, grads_ref[...], 1, 1).astype(jnp.bfloat16)

    @pl.when(step == steps - 1)
    def _():
        moves.relay([1], (1,))
        widened(moe_acc, moe_ref)
        copy(2).start()
        widened(back_acc, back_ref.at[:, :width])
        back_ref[:, width:] = share[...].T.astype(jnp.bfloat16)
        copy(3).start()
        moves.finish()
        copy(2).wait()
        copy(3).wait()


def local_experts(sizes, number, rows, grads, w_in, w_out, sent_grads, sent_rows):
    tokens, wide = rows.shape
    experts, hidden, width = w_out.shape
    each = 1
    low = jnp.bfloat16
    kinds, shapes, sems = planned(
        sizes,
        [
            ("gather", sent_grads, True, sent_grads.shape[0]),
            ("gather", sent_rows, True, sent_rows.shape[0]),
        ],
    )
    some = lambda s: pl.BlockSpec((each,) + s[1:], lambda e: (e,) + (0,) * (len(s) - 1))
    outs = [
        (experts, width, 2 * hidden),
        (experts, 2 * hidden, width),
        (experts, hidden, width),
        (tokens, width),
        (tokens, wide),
    ]
    return pl.pallas_call(
        functools.partial(local_experts_body, sizes, kinds),
        grid=(experts // each,),
        in_specs=[
            HBM,
            HBM,
            some(w_in.shape),
            some(w_out.shape),
            HBM,
            HBM,
        ],
        out_specs=(*[some(s) for s in outs[:3]], HBM, HBM, HBM, HBM),
        out_shape=tuple(jax.ShapeDtypeStruct(s, low) for s in outs) + tuple(shapes),
        scratch_shapes=[
            pltpu.VMEM(rows.shape, low),
            pltpu.VMEM(grads.shape, low),
            pltpu.VMEM((tokens, width), low),
            pltpu.VMEM((tokens, wide), low),
            pltpu.VMEM((tokens, width), jnp.float32),
            pltpu.VMEM((tokens, width), jnp.float32),
            pltpu.VMEM((LANES, tokens), jnp.float32),
            pltpu.VMEM((LANES // 2, tokens), jnp.float32),
            pltpu.VMEM((each,) + w_in.shape[1:], jnp.float32),
            pltpu.SemaphoreType.DMA((4,)),
        ]
        + sems,
        compiler_params=pltpu.CompilerParams(collective_id=number, has_side_effects=True),
        name="local_experts",
    )(rows, grads, w_in, w_out, sent_grads, sent_rows)


class Sums:
    def __init__(self, rows, grads, weights, turned, load_sem, *sums):
        self.rows, self.grads, self.weights = rows, grads, weights
        self.turned, self.load_sem, self.sums = turned, load_sem, sums

    def load(self, which, source):
        target = (self.rows, self.grads)[which]
        return pltpu.make_async_copy(source, target, self.load_sem.at[which])

    def ready(self):
        layers, width, tokens = self.grads.shape

        def block(i, carry):
            at = pl.ds(pl.multiple_of(i * tokens, tokens), tokens)
            self.weights[i] = weight_rows(self.rows[at, width:])
            return carry

        lax.fori_loop(0, layers, block, 0)

    def make(self, index, w_in, w_out, in_part, out_part, made, arrive):
        layers, width, tokens = self.grads.shape
        hidden = w_out.shape[0]
        arrive(0)
        if self.sums:
            arrive(1)
        later = arrive

        def part_of(at, pieces, arrive=lambda i: None if self.sums else later(i)):
            first = at * tokens if isinstance(at, int) else pl.multiple_of(at * tokens, tokens)
            block = self.rows[pl.ds(first, pieces * tokens), :width]
            gate_up = dot(w_in[...], block, 0, 1)
            arrive(1)
            weight = jnp.concatenate(
                [self.weights[at + i, pl.ds(index, 1), :] for i in range(pieces)], axis=1
            )
            active_grad = jnp.concatenate(
                [dot(w_out[...], self.grads[at + i]) for i in range(pieces)], axis=1
            )
            active, gate_up_grad, _ = expert_terms(gate_up, active_grad, weight)
            out_total = functools.reduce(
                jnp.add,
                [
                    dot(active[:, i * tokens : (i + 1) * tokens], self.grads[at + i], 1, 1)
                    for i in range(pieces)
                ],
            )
            return dot(gate_up_grad, block), out_total

        if not self.sums:
            in_total, out_total = part_of(0, layers)
        else:
            whole, out_acc = self.sums
            whole[...] = jnp.zeros_like(whole)
            out_acc[...] = jnp.zeros_like(out_acc)

            def more(i, carry):
                in_more, out_more = part_of(i, 1)
                whole[...] += in_more
                out_acc[...] += out_more
                return carry

            lax.fori_loop(0, layers, more, 0)
            in_total, out_total = whole[...], out_acc[...]
        arrive(2)
        in_total = in_total + in_part[...].astype(jnp.float32)
        parts = hidden // LANES
        for part in range(parts):
            for half in range(2):
                at = half * hidden + part * LANES
                self.turned[pl.ds(part * 2 + half, width, stride=2 * parts), :] = in_total[
                    at : at + LANES, :
                ].T
        made[...] = self.turned[...].astype(jnp.bfloat16)
        return out_total + out_part[...].astype(jnp.float32)


def sums_scratch(layers, tokens, width, hidden):
    low, full = jnp.bfloat16, jnp.float32
    return [
        pltpu.VMEM((layers * tokens, width + LANES), low),
        pltpu.VMEM((layers, width, tokens), low),
        pltpu.VMEM((layers, LANES // 2, tokens), full),
        pltpu.VMEM((width * 2 * hidden // LANES, LANES), full),
        pltpu.SemaphoreType.DMA((2,)),
    ] + [pltpu.VMEM((k * hidden, width), full) for k in (2, 1) if layers > 4]


class Cover:
    def __init__(self, first, many, work):
        w_in, w_out, in_part, out_part, rows_far, grads_far = work
        layers, width, tokens = grads_far.shape
        self.experts, hidden, _ = w_out.shape
        self.first, self.many, self.work = first, many, work
        low = jnp.bfloat16
        self.shapes = [
            ((many, width * 2 * hidden // LANES, LANES), low),
            ((many, hidden, width), low),
        ]
        self.scratch = [pltpu.VMEM((many,) + a.shape[1:], low) for a in work[:4]]
        self.scratch += [pltpu.VMEM(*s) for s in self.shapes]
        self.scratch += [pltpu.SemaphoreType.DMA((4, many)), pltpu.SemaphoreType.DMA((2, many))]
        self.scratch += sums_scratch(layers, tokens, width, hidden)

    def load(self, which, i, work, refs):
        source, sem = work[which].at[self.first + i], refs[6].at[which, i]
        return pltpu.make_async_copy(source, refs[which].at[i], sem)

    def begin(self, work, refs):
        sums = Sums(*refs[8:])
        sums.load(0, work[4]).start()
        self.load(0, 0, work, refs).start()
        sums.load(1, work[5]).start()
        for which in (1, 2, 3):
            self.load(which, 0, work, refs).start()
        for i in range(1, self.many):
            for which in range(4):
                self.load(which, i, work, refs).start()

    def stores(self, i, made, refs):
        return [
            pltpu.make_async_copy(refs[4 + k].at[i], made[k].at[i], refs[7].at[k, i])
            for k in range(2)
        ]

    def run(self, work, made, refs):
        sums = Sums(*refs[8:])

        def expert(i, carry):
            def arrive(point):
                @pl.when(i == 0)
                def _():
                    if point == 0:
                        sums.load(0, work[4]).wait()
                        sums.ready()
                    if point == 1:
                        sums.load(1, work[5]).wait()

                for which in ((0,), (1,), (2, 3))[point]:
                    self.load(which, i, work, refs).wait()

            index = lax.axis_index("row") * self.experts + self.first + i
            out_total = sums.make(index, *[refs[k].at[i] for k in range(5)], arrive)
            refs[5][i] = out_total.astype(jnp.bfloat16)
            for store in self.stores(i, made, refs):
                store.start()
            return carry

        lax.fori_loop(0, self.many, expert, 0)

    def end(self, made, refs):
        for i in range(self.many):
            for store in self.stores(i, made, refs):
                store.wait()


def outputs_body(count, total, *refs):
    pieces = total // count
    sums, smalls = refs[: 2 * pieces], refs[2 * pieces : 2 * pieces + 6]
    gin, gout, *others = refs[2 * pieces + 6 : 2 * pieces + 16]
    in_low, out_low, in_full, out_full, *refs = refs[2 * pieces + 16 :]
    held, results, (load_sem, store_sem, small_sem) = refs[:6], refs[6:14], refs[14:]
    block_out, in_grad, gain_attn, gain_moe, query, pair, output, router = results
    width = gout.shape[2]
    stored = [
        pltpu.make_async_copy(a, b, small_sem.at[6 + j])
        for j, (a, b) in enumerate(zip(results, others))
    ]
    ring = in_full.shape[0]

    def load(k, i):
        low = (in_low, out_low)[k]
        source = sums[k * pieces + i // count].at[i % count]
        return pltpu.make_async_copy(source, low.at[i], load_sem.at[k, i])

    def store(k, i):
        made, target = ((in_full, gin), (out_full, gout))[k]
        return pltpu.make_async_copy(made.at[i % ring], target.at[i], store_sem.at[k, i % ring])

    for i in range(total):
        for k in range(2):
            load(k, i).start()
        if i == 0:
            fetched = [
                pltpu.make_async_copy(a, b, small_sem.at[j])
                for j, (a, b) in enumerate(zip(smalls, held))
            ]
            for copy in fetched:
                copy.start()
    def small():
        for copy in fetched:
            copy.wait()
        blocks, in_blocks, gains, summed, output_first, output_last = held
        for i in range(blocks.shape[0]):
            at = pl.ds(i * blocks.shape[1], blocks.shape[1])
            block_out[at, :] = blocks[i]
            in_grad[at, :] = in_blocks[i]
        gain_sum = jnp.sum(gains[...], axis=0)
        gain_attn[...] = gain_sum[0:1, :]
        gain_moe[...] = gain_sum[1:2, :]
        query[...] = summed[:width, :].astype(jnp.float32)
        pair[...] = summed[width : 2 * width, :].astype(jnp.float32)
        router[...] = summed[2 * width : 2 * width + router.shape[0], :].astype(jnp.float32)
        half = output_first.shape[1]
        for i in range(width // half):
            from_first = i % 2 == 0
            rows = (output_first if from_first else output_last)[i // 2].astype(jnp.float32)
            for j in range(max(1, half // LANES)):
                place = i * half + j * LANES
                at = place // LANES
                part = rows[j * LANES : (j + 1) * LANES, :]
                first = place % LANES
                output[first : first + part.shape[0], at * LANES : (at + 1) * LANES] = part

    for i in range(total):
        for k in range(2):
            load(k, i).wait()
            if i >= ring:
                store(k, i - ring).wait()
        for low, made in ((in_low, in_full), (out_low, out_full)):
            widened(low.at[i], made.at[i % ring])
        for k in range(2):
            store(k, i).start()
        if i == total - 3:
            small()
            for copy in stored:
                copy.start()
    for i in range(total - ring, total):
        for k in range(2):
            store(k, i).wait()
    for copy in stored:
        copy.wait()


def outputs(in_sums, out_sums, hidden, experts, *smalls):
    count = in_sums[0].shape[0]
    total = count * len(in_sums)
    width = out_sums[0].shape[2]
    parts = hidden // LANES
    lanes = smalls[0].shape[2]
    tokens = smalls[0].shape[0] * smalls[0].shape[1]
    low, full = jnp.bfloat16, jnp.float32
    large = [(width * 2 * parts, LANES), (hidden, width)]
    shapes = [((total,) + s, full) for s in large] + [
        ((tokens, lanes), low),
        ((tokens, lanes), low),
        ((1, LANES), full),
        ((1, LANES), full),
        ((width, LANES), full),
        ((width, LANES), full),
        ((LANES, width), full),
        ((experts, LANES), full),
    ]
    ring = min(4, total)
    gin, *others = pl.pallas_call(
        functools.partial(outputs_body, count, total),
        in_specs=[HBM] * (2 * len(in_sums) + len(smalls)),
        out_specs=(HBM,) * len(shapes),
        out_shape=tuple(jax.ShapeDtypeStruct(*shape) for shape in shapes),
        scratch_shapes=[pltpu.VMEM((total,) + s, low) for s in large]
        + [pltpu.VMEM((ring,) + s, full) for s in large]
        + [pltpu.VMEM(a.shape, a.dtype) for a in smalls]
        + [pltpu.VMEM(*shape) for shape in shapes[2:]]
        + [pltpu.SemaphoreType.DMA(s) for s in ((2, total), (2, ring), (14,))],
        name="outputs",
    )(*in_sums, *out_sums, *smalls)
    gin = gin.reshape(total, width, parts, 2, LANES).transpose(0, 1, 3, 2, 4)
    return gin.reshape(total, width, 2, hidden), *others


def local(
    sizes,
    tokens,
    out_grad,
    doc_ids,
    expert_ids,
    gain_attn,
    w_query,
    w_key_value,
    w_output,
    gain_moe,
    w_router,
    w_expert_in,
    w_expert_out,
):
    rows, cols, depth = sizes
    group = rows * cols
    tok_rows, feat_local = tokens.shape
    width = w_query.shape[0]
    experts = w_router.shape[1]
    expert_local, hidden = w_expert_out.shape[0], w_expert_out.shape[1]
    longest_doc = min(LONGEST, tok_rows * depth // 2)
    hop_count = longest_doc // tok_rows
    own = tok_rows // group
    low, full = jnp.bfloat16, jnp.float32
    layer = lax.axis_index("dp")
    me = lax.axis_index("row") * cols + lax.axis_index("col")
    everyone = list(range(1, depth))
    hops = list(range(1, hop_count + 1))

    w_pair = w_key_value.reshape(width, -1)
    block = (tok_rows, LANES)
    cosine, sine, normed, query, pair, tokens_own, gains, gains_moe, router, docs_far, grads_shifted, grad_blocks = exchange(
        sizes,
        "gather_tokens",
        0,
        ("gather", tokens, False, 2),
        ("share", gain_attn.reshape(1, LANES)),
        ("share", gain_moe.reshape(1, LANES)),
        ("share", w_router.T),
        ("shift", doc_ids.reshape(-1, LANES), everyone, False),
        ("shift", out_grad, everyone, False),
        ("gather", out_grad, False, 2),
        before=Stage(tables_body, [(block, full), (block, full)]),
        after=Stage(
            project_body,
            [((tok_rows, width), low), (block, low), (block, low), ((own, width), low)],
            Got(0),
            Got(1),
            w_query,
            w_pair,
            Made(0),
            Made(1),
        ),
        landing=(0,),
        delayed=(6,),
    )

    stack = (hop_count + 1,) + block
    twice = (2 * tok_rows, LANES)
    turned_block = (LANES, tok_rows)
    whole = (2 * tok_rows, 1)
    grad_own, grads_near, far_turned, start, mixed, log_total, far, output_blocks = exchange(
        sizes,
        "shift_pairs",
        1,
        ("line", pair, False, 2, hop_count),
        ("gather", w_output, False, 4),
        before=Stage(
            attend_first_body,
            [
                ((own, width), low),
                ((group,) + turned_block, low),
                ((depth - 1,) + turned_block, low),
                ((tok_rows, 1), jnp.int32),
            ],
            grad_blocks,
            grads_shifted,
            query,
            pair,
            doc_ids.reshape(-1, LANES),
            docs_far,
        ),
        after=Stage(
            attend_rest_body,
            [(block, low), (whole, full)],
            Got(0),
            Made(3),
        ),
        shared=[
            pltpu.VMEM(stack, low),
            pltpu.VMEM(stack, low),
            pltpu.VMEM(twice, low),
            pltpu.VMEM(twice, full),
            pltpu.VMEM(whole, full),
            pltpu.VMEM(whole, full),
        ],
    )
    output_full = output_blocks.reshape(-1, width)

    rows_own, middle, weights = exchange(
        sizes,
        "swap_mixed",
        2,
        ("swap", mixed.reshape(group, own, LANES)),
        after=Stage(
            middle_body,
            [((own, width + LANES), low), ((own, width), full), ((own, LANES), full)],
            Got(0),
            tokens_own,
            output_full,
            gains_moe,
            router,
            expert_ids.T,
            scratch=[pltpu.VMEM(expert_ids.shape, full)],
        ),
        landing=(0,),
    )
    rows_blocks, rows_shifted = exchange(
        sizes,
        "gather_rows",
        3,
        ("gather", rows_own, False, 2),
        ("line", rows_own, False, 4),
    )
    rows_near = rows_blocks.reshape(tok_rows, -1)
    parts = hidden // LANES
    in_rows = w_expert_in.reshape(expert_local, width, 2, parts, LANES)
    in_rows = in_rows.transpose(0, 1, 3, 2, 4).reshape(expert_local, -1, LANES)
    in_flat, in_part, out_part, moe_partial, back_partial, grads_far, rows_far = local_experts(
        sizes,
        9,
        rows_near,
        grads_near.reshape(width, tok_rows),
        in_rows,
        w_expert_out,
        far_turned,
        rows_shifted,
    )
    rows_far = rows_far.reshape((depth - 1) * tok_rows, -1)
    grads_far = grads_far.reshape(depth - 1, width, tok_rows)
    work = (in_flat, w_expert_out, in_part, out_part, rows_far, grads_far)
    share = expert_local // 4
    unit = 16 * depth
    in_sums, out_sums = [], []

    def beneath(name, number, *items, after=None, landing=()):
        cover = Cover(len(in_sums) * share, share, work)
        in_sum, out_sum, *moved = exchange(
            sizes, name, number, *items, after=after, cover=cover, landing=landing
        )
        if after:
            count = len(after.shapes)
            results = [in_sum, out_sum, *moved]
            in_sum, out_sum = results[count], results[count + 1]
            moved = results[:count] + results[count + 2 :]
        in_sums.append(in_sum)
        out_sums.append(out_sum)
        return moved

    middle_grad, attn_grad, logit_grad, gain_moe_part = beneath(
        "swap_back",
        4,
        ("swap", back_partial.reshape(group, own, -1)),
        after=Stage(
            middle_back_body,
            [
                ((own, width), full),
                ((own, width), low),
                ((own, LANES), low),
                ((1, width), full),
            ],
            Got(0),
            grad_own,
            middle,
            weights,
            gains_moe,
            router,
        ),
        landing=(0,),
    )
    query_grad, pair_grad, far_grad, output_sum, logit_blocks = exchange(
        sizes,
        "gather_attn_grad",
        5,
        ("gather", attn_grad, False, 2),
        ("gather", logit_grad),
        delayed=(1,),
        before=Stage(
            attend_again_body,
            [],
            query,
            pair,
            far,
            start,
            log_total,
            scratch=[pltpu.VMEM(twice, low)],
        ),
        after=Stage(
            attend_back_body,
            [
                (block, low),
                (block, full),
                ((hop_count,) + block, low),
                ((group, LANES, LANES), low),
            ],
            Got(0),
            w_output,
            mixed,
            cosine,
            sine,
            scratch=[
                pltpu.VMEM(twice, low),
                pltpu.VMEM(twice[::-1], low),
                pltpu.VMEM(twice, full),
                pltpu.VMEM((hop_count + 1,) + turned_block, full),
                pltpu.VMEM((hop_count + 1,) + turned_block, full),
            ],
        ),
        landing=(0,),
        shared=[
            pltpu.VMEM(stack, low),
            pltpu.VMEM(stack, low),
            pltpu.VMEM(twice[::-1], low),
            pltpu.VMEM((hop_count + 1, 2 * tok_rows, tok_rows), full),
        ],
    )
    length = (2 * width + experts + unit - 1) // unit * unit
    partial, sums, output_first, output_last, gain_parts, moe_blocks = beneath(
        "shift_grads",
        6,
        ("shift", far_grad, [-d for d in hops], True),
        ("turn", output_sum.reshape(depth, width // depth, LANES)),
        ("swap", moe_partial.reshape(group, own, width)),
        after=Stage(
            project_back_body,
            [
                ((tok_rows, width), low),
                ((length, LANES), low),
                ((width // depth // 2, LANES), low),
                ((width // depth // 2, LANES), low),
                ((group, 8, LANES), full),
            ],
            query_grad,
            pair_grad,
            Got(0),
            normed,
            w_query,
            w_pair,
            cosine,
            sine,
            Got(1),
            logit_blocks,
            rows_near,
            gains,
            gain_moe_part,
        ),
        landing=(0, 1),
    )
    pieces = (group, own, LANES)
    block_out, in_grad, gain_sum, summed, output_first = beneath(
        "swap_partial",
        7,
        ("turn", sums.reshape(depth, length // depth, LANES)),
        ("collect", output_first),
        ("swap", partial.reshape(group, own, width)),
        ("swap", gain_parts),
        after=Stage(
            results_body,
            [(pieces, low), (pieces, low), ((8, LANES), full), ((length // depth, LANES), low)],
            Got(2),
            moe_blocks,
            tokens_own,
            middle,
            middle_grad,
            gains,
            Got(3),
            Got(0),
        ),
        landing=(0, 2, 3),
    )
    sums, output_last, gain_all, block_out, in_grad = beneath(
        "swap_results",
        8,
        ("collect", summed),
        ("collect", output_last),
        ("collect", gain_sum),
        ("swap", block_out),
        ("swap", in_grad),
    )
    grad_in, grad_out, block_out, in_grad, gain_attn_sum, gain_moe_sum, query_sum, pair_sum, output_sum, router_sum = outputs(
        in_sums,
        out_sums,
        hidden,
        experts,
        block_out,
        in_grad,
        gain_all,
        sums.reshape(length, LANES),
        output_first,
        output_last,
    )
    return (
        block_out,
        in_grad,
        gain_attn_sum.reshape(LANES),
        query_sum,
        pair_sum.reshape(w_key_value.shape),
        output_sum,
        gain_moe_sum.reshape(LANES),
        router_sum.T,
        grad_in,
        grad_out,
    )


def solution(mesh):
    in_specs = (
        P("dp", ("row", "col")),
        P("dp", ("row", "col")),
        P("dp"),
        P("dp", None),
        P(("row", "col")),
        P(None, ("row", "col")),
        P(None, ("row", "col"), None),
        P(("row", "col"), None),
        P(("row", "col")),
        P(("row", "col"), None),
        P("row", None, None, "col"),
        P("row", "col", None),
    )
    out_specs = (
        P("dp", ("row", "col")),
        P("dp", ("row", "col")),
        P(("row", "col")),
        P(None, ("row", "col")),
        P(None, ("row", "col"), None),
        P(("row", "col"), None),
        P(("row", "col")),
        P(("row", "col"), None),
        P("row", None, None, "col"),
        P("row", "col", None),
    )
    sizes = (mesh.shape["row"], mesh.shape["col"], mesh.shape["dp"])
    return jax.shard_map(
        functools.partial(local, sizes),
        mesh=mesh,
        in_specs=in_specs,
        out_specs=out_specs,
        check_vma=False,
    )
```
